32 devices in a mesh: rep: 4 (over x, core), fsdp: 8 (over z, y).
Axes of the slice: x: 2, y: 2, z: 4, core: 2. Of those that a mesh axis runs over, the one named last changes fastest.
Arguments:
- tokens: bfloat16 [32768, 1024], P(('rep', 'fsdp')), may hold values from -6 to 6
- cotangent: bfloat16 [32768, 1024], P(('rep', 'fsdp')), may hold values from -6 to 6
- segment_ids: int32 [32, 1024], P(('rep', 'fsdp')), may hold values from 0 to 15, never falling along the last dimension, each value on 1 to 512 neighbouring positions
- attention_weight: float32 [4, 1024, 1024], P(None, 'fsdp'), may hold values from -0.375 to 0.375
- attention_momentum: float32 [4, 1024, 1024], P(None, 'fsdp'), may hold values from -0.1875 to 0.1875
- attention_first: float32 [4, 4, 1024, 1024], P('rep', None, 'fsdp'), may hold values from -112 to 112
- attention_second: float32 [4, 4, 1024, 1024], P('rep', None, 'fsdp'), may hold values from 54.8864 to 876.544
- expand_weight: float32 [1024, 4096], P('fsdp'), may hold values from -0.1875 to 0.1875
- expand_momentum: float32 [1024, 4096], P('fsdp'), may hold values from -0.1875 to 0.1875
- expand_first: float32 [4, 1024, 4096], P('rep', 'fsdp'), may hold values from -128 to 128
- expand_second: float32 [4, 1024, 4096], P('rep', 'fsdp'), may hold values from 85.1968 to 1368.064
- contract_weight: float32 [4096, 1024], P('fsdp'), may hold values from -0.09375 to 0.09375
- contract_momentum: float32 [4096, 1024], P('fsdp'), may hold values from -0.09375 to 0.09375
- contract_first: float32 [4, 4096, 1024], P('rep', 'fsdp'), may hold values from -256 to 256
- contract_second: float32 [4, 4096, 1024], P('rep', 'fsdp'), may hold values from 341.6064 to 5464.064
- vectors: float32 [12, 1024], P(None, 'fsdp'), may hold values from -0.6 to 1.4
- vectors_momentum: float32 [12, 1024], P(None, 'fsdp'), may hold values from -1.25 to 1.25
- vectors_first: float32 [4, 12, 1024], P('rep', None, 'fsdp'), may hold values from -448 to 448
- vectors_second: float32 [4, 12, 1024], P('rep', None, 'fsdp'), may hold values from 876.544 to 14008.32
Outputs:
- layer_output: bfloat16 [32768, 1024], P(('rep', 'fsdp'))
- input_grad: bfloat16 [32768, 1024], P(('rep', 'fsdp'))
- attention_first_new: float32 [4, 4, 1024, 1024], P('rep', None, 'fsdp')
- attention_second_new: float32 [4, 4, 1024, 1024], P('rep', None, 'fsdp')
- outer_attention: float32 [3, 4, 1024, 1024], P(None, None, 'fsdp')
- copy_attention: bfloat16 [4, 1024, 1024], P(None, 'fsdp')
- expand_first_new: float32 [4, 1024, 4096], P('rep', 'fsdp')
- expand_second_new: float32 [4, 1024, 4096], P('rep', 'fsdp')
- outer_expand: float32 [3, 1024, 4096], P(None, 'fsdp')
- copy_expand: bfloat16 [1024, 4096], P('fsdp')
- contract_first_new: float32 [4, 4096, 1024], P('rep', 'fsdp')
- contract_second_new: float32 [4, 4096, 1024], P('rep', 'fsdp')
- outer_contract: float32 [3, 4096, 1024], P(None, 'fsdp')
- copy_contract: bfloat16 [4096, 1024], P('fsdp')
- vectors_first_new: float32 [4, 12, 1024], P('rep', None, 'fsdp')
- vectors_second_new: float32 [4, 12, 1024], P('rep', None, 'fsdp')
- outer_vectors: float32 [3, 12, 1024], P(None, None, 'fsdp')
- copy_vectors: bfloat16 [12, 1024], P(None, 'fsdp')
The draws below stay inside these ranges and needn't reach their ends.
Inputs may be any that keep to these rules, and one draw needn't show every extreme that they name: `segment_ids`: within a row the numbers never fall; a run of equal numbers is one document, and tokens attend only within their document.
All inputs are finite; a program needn't handle non-finite values.
Results may differ from the reference program's by a relative error of at most 0.012.
The reference program's roundings to bfloat16 on the way count: a program that leaves them out, or rounds other values in their place, can miss the bound.
Values may be sent and summed in bfloat16 or wider, within the bound.
A program may use at most 448 MiB of HBM per device.

```python
import math
import jax
import jax.numpy as jnp
import numpy as np
from jax import lax

D = 1024
H = 16
HD = 64
FF = 4096
LEN = 1024
ADAM_STEP = 4
GROUP_TOKENS = 8192
GROUPS = 4
TOKENS = 32768
SEQS = 32
VECROWS = 12
N_REP = 4


def draw_attention_weight(key, part):
    base_draw = jax.random.truncated_normal(key, -3.0, 3.0, (4, D, D), jnp.float32)
    scales = jnp.array([1.0, 1.0, 1.0, 4.0], jnp.float32) / jnp.sqrt(jnp.float32(D))
    return base_draw * scales[:, None, None]


def draw_vectors(key, part):
    gain_key, bias_key = jax.random.split(key)
    gain_rows = jax.random.uniform(gain_key, (2, D), jnp.float32, 0.6, 1.4)
    biases = 0.2 * jax.random.truncated_normal(bias_key, -3.0, 3.0, (VECROWS - 2, D), jnp.float32)
    return jnp.concatenate([gain_rows, biases], axis=0)


def level_of(stream_key, extent, pieces, least, top_value):
    gain, own = 1.0, jax.random.fold_in(stream_key, 6)
    for axis_at, blocks in pieces:
        draws = jnp.exp(jax.random.uniform(jax.random.fold_in(own, axis_at), (blocks,), jnp.float32, least / len(pieces), top_value / len(pieces)))
        gain = gain * jnp.repeat(draws, extent[axis_at] // blocks).reshape([-1 if axis == axis_at else 1 for axis in range(len(extent))])
    return gain


def length_profile(amount, total, limit, slope):
    portions = [(1 << 20) // math.isqrt(grade ** slope) + 1 for grade in range(2, amount + 1)]
    spare, counts = total - limit - (amount - 1), [1] * (amount - 1)
    while spare > 0:
        free = [i for i in range(amount - 1) if counts[i] < limit]
        whole, remaining = sum([portions[i] for i in free]), spare
        for i in free:
            extra = min(limit - counts[i], max(1, remaining * portions[i] // whole), spare)
            counts[i] = counts[i] + extra
            spare = spare - extra
    return np.array([limit] + counts)


def ragged_sizes(own_key, number_of, total, most, skew):
    if number_of == 2:
        one = jax.random.randint(own_key, (), max(1, total - most), min(most, total - 1) + 1)
        return jnp.stack([one, total - one])
    sizes = jnp.asarray(length_profile(number_of, total, most, skew), jnp.int32)
    couples = (number_of - 1) // 2
    giver, receiver = sizes[1:1 + 2 * couples:2], sizes[2:2 + 2 * couples:2]
    room = jnp.minimum(giver - 1, most - receiver)
    shifted = jax.random.randint(jax.random.fold_in(own_key, 1), (couples,), 0, 1 << 20) % (room + 1)
    sizes = sizes.at[1:1 + 2 * couples:2].set(giver - shifted).at[2:2 + 2 * couples:2].set(receiver + shifted)
    return sizes[jax.random.permutation(jax.random.fold_in(own_key, 2), number_of)]


def scatter_about(stream_key, shape, deviation, bound, cuts=(), dtype=jnp.bfloat16):
    level = level_of(stream_key, shape, cuts, -0.22, 0.18) if cuts else 1.0
    drawn = jax.random.normal(stream_key, shape, jnp.float32) * deviation * level
    return jnp.minimum(jnp.maximum(drawn, -bound), bound).astype(dtype)


def setup_inputs(seed: int = 0) -> dict:
    splits = jax.random.split(jax.random.key(seed), 20)
    tokens = scatter_about(splits[0], (TOKENS, D), 1.0, 6.0, ((0, 32),))
    cotangent = scatter_about(splits[1], (TOKENS, D), 1.0, 6.0, ((0, 32),))
    segment_ids = jax.vmap(lambda own: jnp.searchsorted(jnp.cumsum(ragged_sizes(own, max(4, LEN // 64), LEN, LEN // 2, 2)), jnp.arange(LEN), side="right"))(jax.random.split(splits[2], SEQS)).reshape((SEQS, LEN)).astype(jnp.int32)
    attention_weight = draw_attention_weight(jax.random.fold_in(splits[19], 71), 0)
    attention_momentum = scatter_about(splits[4], (4, D, D), 0.03, 0.1875, ((1, 8),), jnp.float32)
    attention_first = scatter_about(splits[5], (GROUPS, 4, D, D), (0.2 * GROUP_TOKENS ** 0.5), 112.0, ((0, 4), (2, 8)), jnp.float32)
    attention_second = jnp.clip(jnp.exp(math.log(876.544) - 2.77072135 * jax.random.uniform(splits[6], (GROUPS, 4, D, D), jnp.float32) ** level_of(splits[6], (GROUPS, 4, D, D), ((0, 4), (2, 8)), -0.2, 0.2)), 54.8864, 876.544)
    expand_weight = scatter_about(splits[7], (D, FF), D ** -0.5, 0.1875, ((0, 8),), jnp.float32)
    expand_momentum = scatter_about(splits[8], (D, FF), 0.03, 0.1875, ((0, 8),), jnp.float32)
    expand_first = scatter_about(splits[9], (GROUPS, D, FF), (0.25 * GROUP_TOKENS ** 0.5), 128.0, ((0, 4), (1, 8)), jnp.float32)
    expand_second = jnp.clip(jnp.exp(math.log(1368.064) - 2.776188 * jax.random.uniform(splits[10], (GROUPS, D, FF), jnp.float32) ** level_of(splits[10], (GROUPS, D, FF), ((0, 4), (1, 8)), -0.2, 0.2)), 85.1968, 1368.064)
    contract_weight = scatter_about(splits[11], (FF, D), FF ** -0.5, 0.09375, ((0, 8),), jnp.float32)
    contract_momentum = scatter_about(splits[12], (FF, D), 0.015, 0.09375, ((0, 8),), jnp.float32)
    contract_first = scatter_about(splits[13], (GROUPS, FF, D), (0.5 * GROUP_TOKENS ** 0.5), 256.0, ((0, 4), (1, 8)), jnp.float32)
    contract_second = jnp.clip(jnp.exp(math.log(5464.064) - 2.7722889 * jax.random.uniform(splits[14], (GROUPS, FF, D), jnp.float32) ** level_of(splits[14], (GROUPS, FF, D), ((0, 4), (1, 8)), -0.2, 0.2)), 341.6064, 5464.064)
    vectors = draw_vectors(jax.random.fold_in(splits[19], 71), 0)
    vectors_momentum = scatter_about(splits[16], (VECROWS, D), 0.2, 1.25, ((1, 8),), jnp.float32)
    vectors_first = scatter_about(splits[17], (GROUPS, VECROWS, D), (0.8 * GROUP_TOKENS ** 0.5), 448.0, ((0, 4), (2, 8)), jnp.float32)
    vectors_second = jnp.clip(jnp.exp(math.log(14008.32) - 2.7714198 * jax.random.uniform(splits[18], (GROUPS, VECROWS, D), jnp.float32) ** level_of(splits[18], (GROUPS, VECROWS, D), ((0, 4), (2, 8)), -0.2, 0.2)), 876.544, 14008.32)
    return dict(tokens=tokens, cotangent=cotangent, segment_ids=segment_ids, attention_weight=attention_weight, attention_momentum=attention_momentum, attention_first=attention_first, attention_second=attention_second, expand_weight=expand_weight, expand_momentum=expand_momentum, expand_first=expand_first, expand_second=expand_second, contract_weight=contract_weight, contract_momentum=contract_momentum, contract_first=contract_first, contract_second=contract_second, vectors=vectors, vectors_momentum=vectors_momentum, vectors_first=vectors_first, vectors_second=vectors_second)


@jax.custom_vjp
def low(v):
    return lax.optimization_barrier(v.astype(jnp.bfloat16)).astype(jnp.float32)

@jax.custom_vjp
def low_back(v):
    return v

def low_keep(v):
    return (low(v), None)

def low_pass(kept, grad):
    return (grad,)

def back_keep(v):
    return (v, None)

def back_low(kept, grad):
    return (low(grad),)
low.defvjp(low_keep, low_pass)
low_back.defvjp(back_keep, back_low)

def matmul_high(left, right):
    return jnp.dot(left, right, precision=lax.Precision.HIGHEST)

def layer_norm(values_in, gain_row, shift_row):
    center = values_in - lax.optimization_barrier(jnp.mean(values_in, axis=-1, keepdims=True))
    inv_scale = lax.rsqrt(lax.optimization_barrier(jnp.mean(center * center, axis=-1, keepdims=True)) + 1e-05)
    return center * inv_scale * gain_row + shift_row

def forward(seq_tokens, seq_segments, attention, expand, contract, vectors_in):
    attention_low = low(attention)
    expand_low = low(expand)
    contract_low = low(contract)
    vector_low = low(vectors_in)
    length = seq_tokens.shape[0]
    query_all = low_back(low((matmul_high(seq_tokens, attention_low[0]) + vector_low[4]) * 0.125))
    key_all = low_back(low(matmul_high(seq_tokens, attention_low[1])))
    value_all = low_back(low(matmul_high(seq_tokens, attention_low[2]) + vector_low[5]))
    query_heads = query_all.reshape(length, H, HD)
    key_heads = key_all.reshape(length, H, HD)
    value_heads = value_all.reshape(length, H, HD)
    scores = low_back(jnp.einsum('qhd,khd->hqk', query_heads, key_heads, precision=lax.Precision.HIGHEST))
    same_doc = seq_segments[:, None] == seq_segments[None, :]
    scores = jnp.where(same_doc[None], scores, -1e+30)
    row_max = lax.optimization_barrier(jnp.max(scores, axis=-1, keepdims=True))
    exp_score = jnp.exp(scores - row_max)
    probability = exp_score / lax.optimization_barrier(jnp.sum(exp_score, axis=-1, keepdims=True))
    context = jnp.einsum('hqk,khd->qhd', low(probability), value_heads, precision=lax.Precision.HIGHEST)
    context = low_back(low(context.reshape(length, D)))
    attn_out = low_back(matmul_high(context, attention_low[3]) + vector_low[6])
    hidden = layer_norm(seq_tokens + attn_out, vector_low[0], vector_low[2])
    pre_act = low_back(matmul_high(low(hidden), expand_low) + vector_low[8:].reshape(FF))
    activated = low(jax.nn.gelu(pre_act, approximate=False))
    branch = low_back(matmul_high(activated, contract_low) + vector_low[7])
    return layer_norm(hidden + branch, vector_low[1], vector_low[3])

def inner_step(weight, gradient, first_moment, second_moment, learn_rate, weight_decay):
    first_new = 0.5 * first_moment + 0.5 * gradient
    second_new = 0.75 * second_moment + 0.25 * gradient * gradient
    update_dir = first_new / (1.0 - 0.5 ** ADAM_STEP) / (jnp.sqrt(second_new / (1.0 - 0.75 ** ADAM_STEP)) + 1e-08)
    return (weight - learn_rate * (update_dir + weight_decay * weight), first_new, second_new)

def reference(tokens, cotangent, segment_ids, attention_weight, attention_momentum, attention_first, attention_second, expand_weight, expand_momentum, expand_first, expand_second, contract_weight, contract_momentum, contract_first, contract_second, vectors, vectors_momentum, vectors_first, vectors_second):
    params = (attention_weight, expand_weight, contract_weight, vectors)
    momenta = (attention_momentum, expand_momentum, contract_momentum, vectors_momentum)
    firsts = (attention_first, expand_first, contract_first, vectors_first)
    seconds = (attention_second, expand_second, contract_second, vectors_second)
    rates = (0.03, 0.03, 0.015, 0.2)
    decays = (0.1, 0.1, 0.1, 0.0)
    group_rows = tokens.shape[0] // N_REP
    group_seqs = group_rows // LEN
    output_parts = []
    input_parts = []
    first_results = [[], [], [], []]
    second_results = [[], [], [], []]
    differences = [jnp.zeros_like(param_arr) for param_arr in params]
    for member in range(N_REP):
        seq_tokens = tokens[member * group_rows:(member + 1) * group_rows].astype(jnp.float32).reshape(group_seqs, LEN, D)
        seq_cots = cotangent[member * group_rows:(member + 1) * group_rows].astype(jnp.float32).reshape(group_seqs, LEN, D)
        seq_segs = segment_ids[member * group_seqs:(member + 1) * group_seqs]

        def one_sequence(running, sequence_item):
            item_tokens, item_segments, item_cot = sequence_item

            def apply_layer(layer_in, attention, expand, contract, vectors_in):
                return forward(layer_in, item_segments, attention, expand, contract, vectors_in)
            layer_out, pullback = jax.vjp(apply_layer, item_tokens, params[0], params[1], params[2], params[3])
            gradients = pullback(item_cot)
            running = tuple((total + piece for total, piece in zip(running, gradients[1:])))
            return (running, (layer_out.astype(jnp.bfloat16), gradients[0].astype(jnp.bfloat16)))
        zero_sums = tuple((jnp.zeros_like(param_arr) for param_arr in params))
        group_sums, (layer_outs, input_grads) = lax.scan(one_sequence, zero_sums, (seq_tokens, seq_segs, seq_cots))
        output_parts.append(layer_outs.reshape(group_rows, D))
        input_parts.append(input_grads.reshape(group_rows, D))
        for kind_index in range(4):
            new_weight, first_new, second_new = inner_step(params[kind_index], group_sums[kind_index], firsts[kind_index][member], seconds[kind_index][member], rates[kind_index], decays[kind_index])
            first_results[kind_index].append(first_new)
            second_results[kind_index].append(second_new)
            differences[kind_index] = differences[kind_index] + (params[kind_index] - new_weight)
    outer_list = []
    copy_list = []
    for kind_index in range(4):
        mean_diff = differences[kind_index] / N_REP
        momentum_new = 0.5 * momenta[kind_index] + mean_diff
        outer_new = params[kind_index] - 0.7 * (mean_diff + 0.5 * momentum_new)
        outer_list.append(jnp.stack([mean_diff, momentum_new, outer_new]))
        copy_list.append(outer_new.astype(jnp.bfloat16))
    first_arrays = [jnp.stack(first_results[kind_index]) for kind_index in range(4)]
    second_arrays = [jnp.stack(second_results[kind_index]) for kind_index in range(4)]
    return (jnp.concatenate(output_parts, axis=0), jnp.concatenate(input_parts, axis=0), first_arrays[0], second_arrays[0], outer_list[0], copy_list[0], first_arrays[1], second_arrays[1], outer_list[1], copy_list[1], first_arrays[2], second_arrays[2], outer_list[2], copy_list[2], first_arrays[3], second_arrays[3], outer_list[3], copy_list[3])
```

```python
from functools import partial

import jax
import jax.numpy as jnp
from jax import lax
from jax.experimental import pallas as pl
from jax.experimental.pallas import tpu as pltpu
from jax.sharding import PartitionSpec as P

D = 1024
H = 16
HD = 64
FF = 4096
LEN = 1024
SEQ_DEV = 1
ADAM_STEP = 4
TOK_DEV = 1024


def norm_forward(values_in, gain_row, shift_row):
    center = values_in - jnp.mean(values_in, axis=-1, keepdims=True)
    inv_scale = lax.rsqrt(jnp.mean(center * center, axis=-1, keepdims=True) + 1e-05)
    normed = center * inv_scale
    return (normed * gain_row + shift_row, normed, inv_scale)


def norm_backward(grad_out, normed, inv_scale, gain_row):
    grad_gain = jnp.sum(grad_out * normed, axis=0)
    grad_shift = jnp.sum(grad_out, axis=0)
    scaled_grad = grad_out * gain_row
    grad_value = inv_scale * (
        scaled_grad
        - jnp.mean(scaled_grad, axis=-1, keepdims=True)
        - normed * jnp.mean(scaled_grad * normed, axis=-1, keepdims=True)
    )
    return (grad_value, grad_gain, grad_shift)


def product_over(left, right):
    return lax.dot_general(
        left, right, (((0,), (0,)), ((), ())), preferred_element_type=jnp.float32
    )


def product_back(left, right):
    return lax.dot_general(
        left, right, (((1,), (1,)), ((), ())), preferred_element_type=jnp.float32
    )


def block_scores(query_block, key_block, row_segments, all_segments):
    scores = jnp.einsum("qhd,khd->hqk", query_block, key_block, preferred_element_type=jnp.float32)
    same_doc = row_segments[:, None] == all_segments[None, :]
    return jnp.where(same_doc[None], scores, -1e30)


def inner_step(weight, gradient, first_moment, second_moment, learn_rate, weight_decay):
    first_new = 0.5 * first_moment + 0.5 * gradient
    second_new = 0.75 * second_moment + 0.25 * gradient * gradient
    update_dir = (
        first_new
        / (1.0 - 0.5**ADAM_STEP)
        / (jnp.sqrt(second_new / (1.0 - 0.75**ADAM_STEP)) + 1e-08)
    )
    return (weight - learn_rate * (update_dir + weight_decay * weight), first_new, second_new)


def per_device(
    tokens,
    cotangent,
    segment_ids,
    attention_weight,
    attention_momentum,
    attention_first,
    attention_second,
    expand_weight,
    expand_momentum,
    expand_first,
    expand_second,
    contract_weight,
    contract_momentum,
    contract_first,
    contract_second,
    vectors,
    vectors_momentum,
    vectors_first,
    vectors_second,
):
    attn_full, vector_full = (
        lax.all_gather(attention_weight.astype(jnp.bfloat16), "fsdp", axis=1, tiled=True),
        lax.all_gather(vectors.astype(jnp.bfloat16), "fsdp", axis=1, tiled=True),
    )
    vector_rows = vector_full.astype(jnp.float32)
    gain_one, gain_two, shift_one, shift_two = (
        vector_rows[0],
        vector_rows[1],
        vector_rows[2],
        vector_rows[3],
    )
    bias_query, bias_value, bias_mixed, bias_down = (
        vector_rows[4],
        vector_rows[5],
        vector_rows[6],
        vector_rows[7],
    )
    bias_up = vector_rows[8:].reshape(FF)
    projected = jnp.einsum("td,nde->nte", tokens, attn_full[:3], preferred_element_type=jnp.float32)
    query_all = ((projected[0] + bias_query) * 0.125).astype(jnp.bfloat16)
    key_all = projected[1].astype(jnp.bfloat16)
    value_all = (projected[2] + bias_value).astype(jnp.bfloat16)
    query_heads = query_all.reshape(SEQ_DEV, LEN, H, HD)
    key_heads = key_all.reshape(SEQ_DEV, LEN, H, HD)
    value_heads = value_all.reshape(SEQ_DEV, LEN, H, HD)
    block_rows = min(512, LEN)
    head_group = min(8, H)
    context_rows = []
    log_sums = []
    seq_index = 0
    for row_start in range(0, LEN, block_rows):
        block_pieces = []
        for head_start in range(0, H, head_group):
            head_part = slice(head_start, head_start + head_group)
            scores = block_scores(
                query_heads[seq_index, row_start : row_start + block_rows, head_part],
                key_heads[seq_index, :, head_part],
                segment_ids[seq_index, row_start : row_start + block_rows],
                segment_ids[seq_index],
            )
            row_max = jnp.max(scores, axis=-1, keepdims=True)
            exp_score = jnp.exp(scores - row_max)
            row_total = jnp.sum(exp_score, axis=-1, keepdims=True)
            probability = (exp_score / row_total).astype(jnp.bfloat16)
            block_pieces.append(
                jnp.einsum(
                    "hqk,khd->qhd",
                    probability,
                    value_heads[seq_index, :, head_part],
                    preferred_element_type=jnp.float32,
                )
            )
            log_sums.append(row_max + jnp.log(row_total))
        context_rows.append(jnp.concatenate(block_pieces, axis=1))
    mixed = jnp.concatenate(context_rows, axis=0).reshape(TOK_DEV, D).astype(jnp.bfloat16)
    attn_out = jnp.dot(mixed, attn_full[3], preferred_element_type=jnp.float32) + bias_mixed
    hidden, normed_one, scale_one = norm_forward(
        tokens.astype(jnp.float32) + attn_out, gain_one, shift_one
    )
    hidden_low = hidden.astype(jnp.bfloat16)
    ffn_expand, ffn_contract = (
        lax.all_gather(expand_weight.astype(jnp.bfloat16), "fsdp", axis=0, tiled=True),
        lax.all_gather(contract_weight.astype(jnp.bfloat16), "fsdp", axis=0, tiled=True),
    )
    pre_act = jnp.dot(hidden_low, ffn_expand, preferred_element_type=jnp.float32) + bias_up
    activated = jax.nn.gelu(pre_act, approximate=False).astype(jnp.bfloat16)
    branch = jnp.dot(activated, ffn_contract, preferred_element_type=jnp.float32) + bias_down
    layer_output, normed_two, scale_two = norm_forward(hidden + branch, gain_two, shift_two)
    grad_sum, grad_gain_two, grad_shift_two = norm_backward(
        cotangent.astype(jnp.float32), normed_two, scale_two, gain_two
    )
    grad_branch = grad_sum.astype(jnp.bfloat16)
    grad_act = product_back(grad_branch, ffn_contract)
    unused_value, gelu_pull = jax.vjp(partial(jax.nn.gelu, approximate=False), pre_act)
    grad_pre_low = gelu_pull(grad_act)[0].astype(jnp.bfloat16)
    grad_hidden = grad_sum + product_back(grad_pre_low, ffn_expand)
    contract_full = product_over(activated, grad_branch)
    expand_full = product_over(hidden_low, grad_pre_low)
    grad_expand, grad_contract = (
        lax.psum_scatter(expand_full, "fsdp", scatter_dimension=0, tiled=True),
        lax.psum_scatter(contract_full, "fsdp", scatter_dimension=0, tiled=True),
    )
    grad_resid, grad_gain_one, grad_shift_one = norm_backward(
        grad_hidden, normed_one, scale_one, gain_one
    )
    grad_attn_out = grad_resid.astype(jnp.bfloat16)
    grad_bias_mixed = jnp.sum(grad_attn_out.astype(jnp.float32), axis=0)
    grad_output_proj = product_over(mixed, grad_attn_out)
    grad_mixed = product_back(grad_attn_out, attn_full[3]).astype(jnp.bfloat16)
    grad_context = grad_mixed.reshape(SEQ_DEV, LEN, H, HD)
    query_grads = []
    lse_index = 0
    seq_index = 0
    key_totals = [
        jnp.zeros((LEN, head_group, HD), jnp.float32) for head_start in range(0, H, head_group)
    ]
    value_totals = [
        jnp.zeros((LEN, head_group, HD), jnp.float32) for head_start in range(0, H, head_group)
    ]
    for row_start in range(0, LEN, block_rows):
        block_pieces = []
        for group_index, head_start in enumerate(range(0, H, head_group)):
            head_part = slice(head_start, head_start + head_group)
            query_block = query_heads[seq_index, row_start : row_start + block_rows, head_part]
            key_block = key_heads[seq_index, :, head_part]
            value_block = value_heads[seq_index, :, head_part]
            ctx_grad = grad_context[seq_index, row_start : row_start + block_rows, head_part]
            scores = block_scores(
                query_block,
                key_block,
                segment_ids[seq_index, row_start : row_start + block_rows],
                segment_ids[seq_index],
            )
            probability = jnp.exp(scores - log_sums[lse_index])
            lse_index = lse_index + 1
            value_totals[group_index] = value_totals[group_index] + jnp.einsum(
                "hqk,qhd->khd",
                probability.astype(jnp.bfloat16),
                ctx_grad,
                preferred_element_type=jnp.float32,
            )
            prob_grad = jnp.einsum(
                "qhd,khd->hqk", ctx_grad, value_block, preferred_element_type=jnp.float32
            )
            row_dot = jnp.sum(probability * prob_grad, axis=-1, keepdims=True)
            score_grad = (probability * (prob_grad - row_dot)).astype(jnp.bfloat16)
            block_pieces.append(
                jnp.einsum(
                    "hqk,khd->qhd", score_grad, key_block, preferred_element_type=jnp.float32
                ).astype(jnp.bfloat16)
            )
            key_totals[group_index] = key_totals[group_index] + jnp.einsum(
                "hqk,qhd->khd", score_grad, query_block, preferred_element_type=jnp.float32
            )
        query_grads.append(jnp.concatenate(block_pieces, axis=1))
    key_grads = jnp.concatenate(
        [key_total.astype(jnp.bfloat16) for key_total in key_totals], axis=1
    )
    value_grads = jnp.concatenate(
        [value_total.astype(jnp.bfloat16) for value_total in value_totals], axis=1
    )
    grad_query = jnp.concatenate(query_grads, axis=0).reshape(TOK_DEV, D) * 0.125
    grad_keys = key_grads.reshape(TOK_DEV, D)
    grad_values = value_grads.reshape(TOK_DEV, D)
    stacked_grads = jnp.stack([grad_query, grad_keys, grad_values])
    grad_qkv = jnp.einsum("td,nte->nde", tokens, stacked_grads, preferred_element_type=jnp.float32)
    input_grad = (
        grad_resid
        + jnp.einsum(
            "nte,nde->td", stacked_grads, attn_full[:3], preferred_element_type=jnp.float32
        )
    ).astype(jnp.bfloat16)
    grad_attention_full = jnp.concatenate([grad_qkv, grad_output_proj[None]], axis=0)
    vector_head = jnp.stack(
        [
            grad_gain_one,
            grad_gain_two,
            grad_shift_one,
            grad_shift_two,
            jnp.sum(grad_query.astype(jnp.float32), axis=0),
            jnp.sum(grad_values.astype(jnp.float32), axis=0),
            grad_bias_mixed,
            jnp.sum(grad_branch.astype(jnp.float32), axis=0),
        ]
    )
    grad_bias_up = jnp.sum(grad_pre_low.astype(jnp.float32), axis=0).reshape(FF // D, D)
    grad_vectors_full = jnp.concatenate([vector_head, grad_bias_up], axis=0)
    grad_attention, grad_vectors = (
        lax.psum_scatter(grad_attention_full, "fsdp", scatter_dimension=1, tiled=True),
        lax.psum_scatter(grad_vectors_full, "fsdp", scatter_dimension=1, tiled=True),
    )
    attention_new = inner_step(
        attention_weight, grad_attention, attention_first[0], attention_second[0], 0.03, 0.1
    )
    expand_new = inner_step(
        expand_weight, grad_expand, expand_first[0], expand_second[0], 0.03, 0.1
    )
    contract_new = inner_step(
        contract_weight, grad_contract, contract_first[0], contract_second[0], 0.015, 0.1
    )
    vectors_new = inner_step(vectors, grad_vectors, vectors_first[0], vectors_second[0], 0.2, 0.0)
    summed = (
        lax.psum((attention_weight - attention_new[0]).astype(jnp.bfloat16), "rep").astype(
            jnp.float32
        ),
        lax.psum((expand_weight - expand_new[0]).astype(jnp.bfloat16), "rep").astype(jnp.float32),
        lax.psum((contract_weight - contract_new[0]).astype(jnp.bfloat16), "rep").astype(
            jnp.float32
        ),
        lax.psum((vectors - vectors_new[0]).astype(jnp.bfloat16), "rep").astype(jnp.float32),
    )
    groups_count = lax.axis_size("rep")
    results = []
    for weight_now, momentum_now, inner_new, diff_total in zip(
        (attention_weight, expand_weight, contract_weight, vectors),
        (attention_momentum, expand_momentum, contract_momentum, vectors_momentum),
        (attention_new, expand_new, contract_new, vectors_new),
        summed,
    ):
        mean_diff = diff_total / groups_count
        momentum_new = 0.5 * momentum_now + mean_diff
        outer_new = weight_now - 0.7 * (mean_diff + 0.5 * momentum_new)
        results.append(
            (
                inner_new[1][None],
                inner_new[2][None],
                jnp.stack([mean_diff, momentum_new, outer_new]),
                outer_new.astype(jnp.bfloat16),
            )
        )
    return (
        layer_output.astype(jnp.bfloat16),
        input_grad,
        results[0][0],
        results[0][1],
        results[0][2],
        results[0][3],
        results[1][0],
        results[1][1],
        results[1][2],
        results[1][3],
        results[2][0],
        results[2][1],
        results[2][2],
        results[2][3],
        results[3][0],
        results[3][1],
        results[3][2],
        results[3][3],
    )


NEG=-1e30
QB=256
def attn_windows(seg_row):
    length = seg_row.shape[0]
    nb = length // QB
    firsts = seg_row[::QB]
    lasts = seg_row[QB-1::QB]
    begin = jnp.sum((seg_row[None, :] < firsts[:, None]).astype(jnp.int32), axis=1)
    end = jnp.sum((seg_row[None, :] <= lasts[:, None]).astype(jnp.int32), axis=1)
    start = begin // 128
    count = (end - start * 128 + QB - 1) // QB
    start = jnp.minimum(start, (length - count * QB) // 128)
    return start.astype(jnp.int32), count.astype(jnp.int32)
def lane_half(shape, h):
    lane = lax.broadcasted_iota(jnp.int32, shape, len(shape)-1)
    return (lane < 64) if h == 0 else (lane >= 64)
def dot(a, b, ca, cb):
    return lax.dot_general(a, b, (((ca,), (cb,)), ((), ())), preferred_element_type=jnp.float32)
def fold(value, join):
    part = value.shape[0] // 8
    parts = [value[i * part:(i + 1) * part] for i in range(8)]
    while len(parts) > 1:
        parts = [join(a, b) for a, b in zip(parts[::2], parts[1::2])]
    return parts[0]
def fwd_kernel(start_ref, count_ref, qkv_ref, segr_ref, segc_ref, o_ref, lse_ref, vt_ref):
    length = qkv_ref.shape[0]
    vt_ref[...] = qkv_ref[:, 256:384].T
    nb = length // QB
    for i in range(nb):
        rows = slice(i*QB, (i+1)*QB)
        for nn in range(1, nb+1):
            @pl.when(count_ref[i] == nn)
            def _():
                nk = nn*QB
                lo = pl.multiple_of(start_ref[i]*128, 128)
                kw = qkv_ref[pl.ds(lo, nk), 128:256]
                qb = qkv_ref[rows, 0:128]
                same = segc_ref[pl.ds(lo, nk), :] == segr_ref[:, rows]
                outs = []
                for h in range(2):
                    qh = jnp.where(lane_half(qb.shape, h), qb, jnp.zeros_like(qb))
                    st = jnp.where(same, dot(kw, qh, 1, 1), NEG)
                    m = jnp.max(fold(st, jnp.maximum), axis=0, keepdims=True)
                    p = jnp.exp(st - m)
                    l = jnp.sum(fold(p, jnp.add), axis=0, keepdims=True)
                    weighted = dot(vt_ref[h*64:(h+1)*64, pl.ds(lo, nk)], p.astype(jnp.bfloat16), 1, 0)
                    outs.append(weighted * (1.0 / l))
                    lse_ref[0, h:h+1, rows] = m + jnp.log(l)
                o_ref[rows, :] = jnp.concatenate(outs, axis=0).T.astype(jnp.bfloat16)
def bwd_kernel(start_ref, count_ref, qkv_ref, do_ref, lse_ref, segr_ref, segc_ref, d_ref, sums_ref, dk_acc, dv_acc, kt_ref):
    length = qkv_ref.shape[0]
    kt_ref[...] = qkv_ref[:, 128:256].T
    nb = length // QB
    dk_acc[...] = jnp.zeros_like(dk_acc)
    dv_acc[...] = jnp.zeros_like(dv_acc)
    for i in range(nb):
        rows = slice(i*QB, (i+1)*QB)
        for nn in range(1, nb+1):
            @pl.when(count_ref[i] == nn)
            def _():
                nk = nn*QB
                lo = pl.multiple_of(start_ref[i]*128, 128)
                win = pl.ds(lo, nk)
                kw = qkv_ref[win, 128:256]
                vw = qkv_ref[win, 256:384]
                qb = qkv_ref[rows, 0:128]
                db = do_ref[rows, :]
                same = segc_ref[win, :] == segr_ref[:, rows]
                dqs = []; dks = 0.0; dvs = 0.0
                for h in range(2):
                    hm = lane_half(qb.shape, h)
                    qh = jnp.where(hm, qb, jnp.zeros_like(qb))
                    dh = jnp.where(hm, db, jnp.zeros_like(db))
                    st = jnp.where(same, dot(kw, qh, 1, 1), NEG)
                    p = jnp.exp(st - lse_ref[0, h:h+1, rows])
                    dpt = dot(vw, dh, 1, 1)
                    rd = jnp.sum(fold(p * dpt, jnp.add), axis=0, keepdims=True)
                    ds = (p * (dpt - rd)).astype(jnp.bfloat16)
                    dvs = dvs + dot(p.astype(jnp.bfloat16), dh, 1, 0)
                    dks = dks + dot(ds, qh, 1, 0)
                    dqs.append(dot(kt_ref[h*64:(h+1)*64, win], ds, 1, 0))
                d_ref[rows, 0:128] = jnp.concatenate(dqs, axis=0).T.astype(jnp.bfloat16) * 0.125
                dk_acc[win, :] += dks
                dv_acc[win, :] += dvs
    d_ref[:, 128:256] = dk_acc[...].astype(jnp.bfloat16)
    d_ref[:, 256:384] = dv_acc[...].astype(jnp.bfloat16)
    sums_ref[0] = jnp.sum(d_ref[...].astype(jnp.float32), axis=0, keepdims=True)
def attn_fwd(qkv, seg):
    T, width = qkv.shape
    start, count = attn_windows(seg[0])
    segc = seg.reshape(T, 1)
    heads = width // 384
    return pl.pallas_call(
        fwd_kernel,
        out_shape=(jax.ShapeDtypeStruct((T, width // 3), jnp.bfloat16), jax.ShapeDtypeStruct((heads, 2, T), jnp.float32)),
        grid_spec=pltpu.PrefetchScalarGridSpec(
            num_scalar_prefetch=2, grid=(heads,),
            in_specs=[
                pl.BlockSpec((T, 384), lambda h, *_: (0, h)),
                pl.BlockSpec((1, T), lambda h, *_: (0, 0)),
                pl.BlockSpec((T, 1), lambda h, *_: (0, 0)),
            ],
            out_specs=(pl.BlockSpec((T, 128), lambda h, *_: (0, h)), pl.BlockSpec((1, 2, T), lambda h, *_: (h, 0, 0))),
            scratch_shapes=[pltpu.VMEM((128, T), jnp.bfloat16)],
        ),
        cost_estimate=cost(20 * T * T * width, 3 * T * width, T * T * width // 128),
        name="attn_fwd",
    )(start, count, qkv, seg, segc)


def attn_bwd(qkv, do, lse, seg, part):
    T, width = qkv.shape
    start, count = attn_windows(seg[0])
    segc = seg.reshape(T, 1)
    heads = width // 768
    first = part * heads
    return pl.pallas_call(
        bwd_kernel,
        out_shape=(jax.ShapeDtypeStruct((T, width // 2), jnp.bfloat16), jax.ShapeDtypeStruct((heads, 1, 384), jnp.float32)),
        grid_spec=pltpu.PrefetchScalarGridSpec(
            num_scalar_prefetch=2, grid=(heads,),
            in_specs=[
                pl.BlockSpec((T, 384), lambda h, *_: (0, first + h)),
                pl.BlockSpec((T, 128), lambda h, *_: (0, first + h)),
                pl.BlockSpec((1, 2, T), lambda h, *_: (first + h, 0, 0)),
                pl.BlockSpec((1, T), lambda h, *_: (0, 0)),
                pl.BlockSpec((T, 1), lambda h, *_: (0, 0)),
            ],
            out_specs=(pl.BlockSpec((T, 384), lambda h, *_: (0, h)), pl.BlockSpec((1, 1, 384), lambda h, *_: (h, 0, 0))),
            scratch_shapes=[pltpu.VMEM((T, 128), jnp.float32)] * 2 + [pltpu.VMEM((128, T), jnp.bfloat16)],
        ),
        cost_estimate=cost(20 * T * T * width, 6 * T * width, T * T * width // 64),
        name="attn_bwd",
    )(start, count, qkv, do, lse, seg, segc)


MESH_ID = pl.DeviceIdType.MESH


def bits_of():
    rep = lax.axis_index("rep")
    fsdp = lax.axis_index("fsdp")
    return dict(
        rep=rep, fsdp=fsdp, x=rep // 2, c=rep % 2, z1=fsdp // 4, z0=(fsdp // 2) % 2, y=fsdp % 2
    )


def partner_of(at, which):
    rep, fsdp = at["rep"], at["fsdp"]
    if which == "c":
        rep = rep + 1 - 2 * at["c"]
    elif which == "x":
        rep = rep + 2 - 4 * at["x"]
    elif which == "y":
        fsdp = fsdp + 1 - 2 * at["y"]
    elif which == "z0":
        fsdp = fsdp + 2 - 4 * at["z0"]
    elif which == "z1":
        fsdp = fsdp + 4 - 8 * at["z1"]
    else:
        rep = rep + 1 - 2 * at["c"]
        fsdp = fsdp + 4 - 8 * at["z1"]
    return (rep, fsdp)


REL = [(a, b, d) for d in (0, 1) for b in (0, 1) for a in (0, 1)]


def gather_kernel(
    qkv_in, wo_in, we_in, wc_in, vec_in, tok_in, seg_in,
    qkv_out, wo_out, we_out, wc_out, vec_out, tok_out, seg_out,
    tok_buf, seg_buf, send_sem, recv_sem, local_sem,
):
    at = bits_of()
    other = {k: partner_of(at, k) for k in ("c", "x", "y", "z0", "z1", "swap")}
    barrier = pltpu.get_barrier_semaphore()
    for k in ("c", "x", "y", "z0", "z1"):
        pl.semaphore_signal(barrier, inc=1, device_id=other[k], device_id_type=MESH_ID)
    moves = at["c"] != at["z1"]

    @pl.when(moves)
    def _():
        pl.semaphore_signal(barrier, inc=1, device_id=other["swap"], device_id_type=MESH_ID)
        pl.semaphore_wait(barrier, 6)

    @pl.when(jnp.logical_not(moves))
    def _():
        pl.semaphore_wait(barrier, 5)

    def flip(bit, rel):
        return bit + rel - 2 * bit * rel

    def shard(rel):
        return 4 * flip(at["z1"], rel[1]) + 2 * flip(at["z0"], rel[0]) + flip(at["y"], rel[2])

    counter = [0]
    started = []

    def send(src, dst, which):
        k = counter[0]
        counter[0] += 1
        copy = pltpu.make_async_remote_copy(
            src_ref=src, dst_ref=dst, send_sem=send_sem.at[k], recv_sem=recv_sem.at[k],
            device_id=other[which], device_id_type=MESH_ID,
        )
        copy.start()
        started.append(copy)
        return copy

    class Piece:
        def __init__(self, own, slot, split_x):
            self.own, self.slot, self.split_x = own, slot, split_x
            self.part = (2 * at["x"] + at["c"]) if split_x else at["c"]
            self.part_x = (2 * (1 - at["x"]) + at["c"]) if split_x else None
            self.copies = {}

        def first(self):
            zero = (0, 0, 0)
            for which in ("z1", "z0", "y"):
                self.copies[which, zero] = send(
                    self.own(self.part), self.slot(shard(zero), self.part), which
                )
            self.copies["c", zero] = send(self.own(None), self.slot(shard(zero), None), "c")

        def onward(self, rel):
            here = self.slot(shard(rel), self.part)
            if rel == (0, 1, 0):
                self.copies["z0", rel] = send(here, here, "z0")
            if rel[2] == 0:
                self.copies["y", rel] = send(here, here, "y")
            if self.split_x:
                self.copies["x", rel] = send(here, here, "x")
            self.copies["c", rel] = send(here, here, "c")

        def arrive(self, which, came):
            self.copies[which, came].wait_recv()
            step = {"z0": (1, 0, 0), "z1": (0, 1, 0), "y": (0, 0, 1)}[which]
            self.onward(tuple(p + q for p, q in zip(came, step)))

        def near(self):
            self.arrive("z1", (0, 0, 0))
            self.arrive("z0", (0, 0, 0))

        def rest(self):
            self.arrive("y", (0, 0, 0))
            self.arrive("z0", (0, 1, 0))
            self.arrive("y", (0, 1, 0))
            self.arrive("y", (1, 0, 0))
            self.arrive("y", (1, 1, 0))

        def last(self):
            if self.split_x:
                for rel in REL[1:]:
                    self.copies["x", rel].wait_recv()
                    there = self.slot(shard(rel), self.part_x)
                    self.copies["cx", rel] = send(there, there, "c")

        def finish(self):
            for (which, rel), copy in self.copies.items():
                if which in ("c", "cx"):
                    copy.wait_recv()

    def rows(ref, count):
        full = ref.shape[-2] // 8
        def slot(f, part):
            if part is None:
                at_row, n = f * full, full
            else:
                at_row, n = f * full + part * (full // count), full // count
            at_row = pl.multiple_of(at_row, 8)
            return ref.at[pl.ds(at_row, n), :]
        return slot

    def own_rows(ref, count):
        full = ref.shape[-2]
        def own(part):
            if part is None:
                return ref
            row = pl.multiple_of(part * (full // count), 8)
            n = full // count
            return ref.at[pl.ds(row, n), :]
        return own

    qkv, wo, we, wc = pieces = [
        Piece(own_rows(qkv_in, 4), rows(qkv_out, 4), True),
        Piece(own_rows(wo_in, 4), rows(wo_out, 4), True),
        Piece(own_rows(we_in, 2), rows(we_out, 2), False),
        Piece(own_rows(wc_in, 4), rows(wc_out, 4), True),
    ]
    zero = (0, 0, 0)
    vec_copies = [
        send(vec_in, vec_out.at[shard(zero)], which) for which in ("c", "z1", "z0", "y")
    ]
    pieces[0].first()
    tok_k, seg_k = counter[0], counter[0] + 1
    counter[0] += 2

    def swap_copy(src, dst, k):
        return pltpu.make_async_remote_copy(
            src_ref=src, dst_ref=dst, send_sem=send_sem.at[k], recv_sem=recv_sem.at[k],
            device_id=other["swap"], device_id_type=MESH_ID,
        )

    @pl.when(moves)
    def _():
        swap_copy(tok_in, tok_out, tok_k).start()
        swap_copy(seg_in, seg_out, seg_k).start()

    @pl.when(jnp.logical_not(moves))
    def _():
        one = pltpu.make_async_copy(tok_in, tok_buf, local_sem.at[0])
        two = pltpu.make_async_copy(seg_in, seg_buf, local_sem.at[1])
        one.start()
        two.start()
        one.wait()
        two.wait()
        three = pltpu.make_async_copy(tok_buf, tok_out, local_sem.at[0])
        four = pltpu.make_async_copy(seg_buf, seg_out, local_sem.at[1])
        three.start()
        four.start()
        three.wait()
        four.wait()

    wo.first()
    qkv.near()
    we.first()
    vec_copies[1].wait_recv()
    here = vec_out.at[shard((0, 1, 0))]
    vec_far = send(here, here, "z0")
    vec_more = [send(here, here, "y")]
    vec_copies[2].wait_recv()
    here = vec_out.at[shard((1, 0, 0))]
    vec_more.append(send(here, here, "y"))
    qkv.rest()
    wo.near()
    wo.rest()
    vec_far.wait_recv()
    here = vec_out.at[shard((1, 1, 0))]
    vec_more.append(send(here, here, "y"))
    we.near()
    wc.first()
    qkv.last()
    we.rest()
    wo.last()
    wc.near()
    wc.rest()
    wc.last()
    for piece in pieces:
        piece.finish()
    for copy in [vec_copies[0], vec_copies[3]] + vec_more:
        copy.wait_recv()
    for copy in started:
        copy.wait_send()

    @pl.when(moves)
    def _():
        swap_copy(tok_in, tok_out, tok_k).wait()
        swap_copy(seg_in, seg_out, seg_k).wait()


GATHER_COPIES = 29 * 3 + 15 + 8 + 2


def gather_all(qkv, wo, we, wc, vec, tok, seg):
    bf = jnp.bfloat16
    shape = jax.ShapeDtypeStruct
    whole = pl.BlockSpec(memory_space=pl.ANY)
    return pl.pallas_call(
        gather_kernel,
        out_shape=(
            shape((8 * qkv.shape[0], qkv.shape[1]), bf),
            shape((8 * wo.shape[0], wo.shape[1]), bf),
            shape((8 * we.shape[0], we.shape[1]), bf),
            shape((8 * wc.shape[0], wc.shape[1]), bf),
            shape((8,) + vec.shape, bf),
            shape(tok.shape, bf),
            shape(seg.shape, seg.dtype),
        ),
        in_specs=[whole] * 7,
        out_specs=(whole,) * 7,
        scratch_shapes=[
            pltpu.VMEM(tok.shape, bf),
            pltpu.VMEM(seg.shape, seg.dtype),
            pltpu.SemaphoreType.DMA((GATHER_COPIES,)),
            pltpu.SemaphoreType.DMA((GATHER_COPIES,)),
            pltpu.SemaphoreType.DMA((2,)),
        ],
        compiler_params=pltpu.CompilerParams(collective_id=0, has_side_effects=True),
        name="gather_weights",
    )(qkv, wo, we, wc, vec, tok, seg)


SHRINK = 1000
BF, F32 = jnp.bfloat16, jnp.float32
SHAPE = jax.ShapeDtypeStruct


def full_spec(shape):
    return pl.BlockSpec(shape, lambda *_: (0,) * len(shape), pipeline_mode=pl.Buffered(1))


def cost(flops, moved, exps=0):
    return pl.CostEstimate(flops=int(flops) // SHRINK, bytes_accessed=int(moved) // SHRINK, transcendentals=int(exps) // SHRINK)


def qkv_kernel(x_ref, w_ref, bias_ref, scale_ref, o_ref):
    for i in range(4):
        rows = slice(i * 256, (i + 1) * 256)
        z = dot(x_ref[rows, :], w_ref[...], 1, 0)
        o_ref[rows, :] = ((z + bias_ref[...]) * scale_ref[...]).astype(BF)


def qkv_call(x, w, bias, scale):
    tokens, width = x.shape[0], w.shape[1]
    tile = 768
    return pl.pallas_call(
        qkv_kernel,
        out_shape=SHAPE((tokens, width), BF),
        grid=(width // tile,),
        in_specs=[
            full_spec(x.shape),
            pl.BlockSpec((x.shape[1], tile), lambda j: (0, j)),
            pl.BlockSpec((1, tile), lambda j: (0, j)),
            pl.BlockSpec((1, tile), lambda j: (0, j)),
        ],
        out_specs=pl.BlockSpec((tokens, tile), lambda j: (0, j)),
        cost_estimate=cost(2 * tokens * D * width, 2 * (tokens * D + D * width + tokens * width)),
        name="qkv",
    )(x, w, bias, scale)


def mean_row(value):
    return jnp.mean(value, axis=-1, keepdims=True)


def mix_kernel(c_ref, w_ref, x_ref, rows_ref, n_ref, q_ref, low_ref):
    value = x_ref[...].astype(F32) + dot(c_ref[...], w_ref[...], 1, 0) + rows_ref[6:7, :]
    center = value - mean_row(value)
    inv = lax.rsqrt(mean_row(center * center) + 1e-05)
    normed = center * inv
    n_ref[...] = normed
    q_ref[...] = inv
    low_ref[...] = (normed * rows_ref[0:1, :] + rows_ref[2:3, :]).astype(BF)


def mix_call(mixed, w_out, tok, rows):
    t = tok.shape[0]
    tile = pl.BlockSpec((256, D), lambda i: (i, 0))
    return pl.pallas_call(
        mix_kernel,
        out_shape=(SHAPE((t, D), F32), SHAPE((t, 1), F32), SHAPE((t, D), BF)),
        grid=(t // 256,),
        in_specs=[tile, full_spec((D, D)), tile, full_spec(rows.shape)],
        out_specs=(tile, pl.BlockSpec((256, 1), lambda i: (i, 0)), tile),
        cost_estimate=cost(2 * t * D * D, 12 * t * D + 2 * D * D),
        name="mix_norm",
    )(mixed, w_out, tok, rows)


def up_kernel(h_ref, w_ref, bias_ref, g_ref, s_ref):
    for i in range(8):
        rows = slice(i * 128, (i + 1) * 128)
        z = dot(h_ref[rows, :], w_ref[...], 1, 0) + bias_ref[...]
        phi, bell = erf_parts(z)
        g_ref[rows, :] = (z * phi).astype(BF)
        s_ref[rows, :] = (phi + z * bell * 0.3989422804014327).astype(BF)


def up_call(low, w_in, bias):
    t = low.shape[0]
    tile = 512
    out = pl.BlockSpec((t, tile), lambda j: (0, j))
    return pl.pallas_call(
        up_kernel,
        out_shape=(SHAPE((t, FF), BF), SHAPE((t, FF), BF)),
        grid=(FF // tile,),
        in_specs=[
            full_spec(low.shape),
            pl.BlockSpec((D, tile), lambda j: (0, j)),
            pl.BlockSpec((1, tile), lambda j: (0, j)),
        ],
        out_specs=(out, out),
        cost_estimate=cost(2 * t * D * FF, 2 * (t * D + D * FF + 2 * t * FF), 2 * t * FF),
        name="up_gelu",
    )(low, w_in, bias)


def row_sum(value):
    return jnp.sum(value, axis=0, keepdims=True)


def norm_back(grad, normed, inv, gain):
    scaled = grad * gain
    return inv * (scaled - mean_row(scaled) - normed * mean_row(scaled * normed))


def down_kernel(g_ref, w_ref, n_ref, cot_ref, rows_ref, out_ref, dr_ref, dm_ref, sums_ref):
    hidden = n_ref[...] * rows_ref[0:1, :] + rows_ref[2:3, :]
    value = hidden + dot(g_ref[...], w_ref[...], 1, 0) + rows_ref[7:8, :]
    center = value - mean_row(value)
    inv = lax.rsqrt(mean_row(center * center) + 1e-05)
    normed = center * inv
    gain = rows_ref[1:2, :]
    out_ref[...] = (normed * gain + rows_ref[3:4, :]).astype(BF)
    grad = cot_ref[...].astype(F32)
    back = norm_back(grad, normed, inv, gain)
    low = back.astype(BF)
    dr_ref[...] = back
    dm_ref[...] = low

    @pl.when(pl.program_id(0) == 0)
    def _():
        sums_ref[...] = jnp.zeros_like(sums_ref)

    sums_ref[0:1, :] += row_sum(grad * normed)
    sums_ref[1:2, :] += row_sum(grad)
    sums_ref[2:3, :] += row_sum(low.astype(F32))


def down_call(act, w_down, normed, cot, rows):
    t = act.shape[0]
    tile = pl.BlockSpec((256, D), lambda i: (i, 0))
    return pl.pallas_call(
        down_kernel,
        out_shape=(SHAPE((t, D), BF), SHAPE((t, D), F32), SHAPE((t, D), BF), SHAPE((8, D), F32)),
        grid=(t // 256,),
        in_specs=[
            pl.BlockSpec((256, FF), lambda i: (i, 0)), full_spec((FF, D)), tile, tile,
            full_spec(rows.shape),
        ],
        out_specs=(tile, tile, tile, pl.BlockSpec((8, D), lambda i: (0, 0))),
        cost_estimate=cost(2 * t * D * FF, 2 * (t * FF + D * FF) + 14 * t * D),
        name="down_norm",
    )(act, w_down, normed, cot, rows)


def slope_kernel(dm_ref, w_ref, s_ref, o_ref, sums_ref):
    total = 0.0
    for i in range(4):
        rows = slice(i * 256, (i + 1) * 256)
        z = (dot(dm_ref[rows, :], w_ref[...], 1, 1) * s_ref[rows, :].astype(F32)).astype(BF)
        o_ref[rows, :] = z
        total = total + row_sum(z.astype(F32))
    sums_ref[...] = total


def slope_call(dm, w_down, slope):
    t = dm.shape[0]
    tile = 512
    wide = pl.BlockSpec((t, tile), lambda j: (0, j))
    return pl.pallas_call(
        slope_kernel,
        out_shape=(SHAPE((t, FF), BF), SHAPE((1, FF), F32)),
        grid=(FF // tile,),
        in_specs=[full_spec(dm.shape), pl.BlockSpec((tile, D), lambda j: (j, 0)), wide],
        out_specs=(wide, pl.BlockSpec((1, tile), lambda j: (0, j))),
        cost_estimate=cost(2 * t * D * FF, 2 * (t * D + D * FF + 2 * t * FF)),
        name="down_back",
    )(dm, w_down, slope)


def hidden_kernel(dz_ref, w_ref, dr_ref, n_ref, q_ref, wo_ref, rows_ref, r_ref, a_ref, c_ref, sums_ref):
    grad = dr_ref[...] + dot(dz_ref[...], w_ref[...], 1, 1)
    normed = n_ref[...]
    back = norm_back(grad, normed, q_ref[...], rows_ref[0:1, :])
    low = back.astype(BF)
    r_ref[...] = back
    a_ref[...] = low
    c_ref[...] = dot(low, wo_ref[...], 1, 1).astype(BF)

    @pl.when(pl.program_id(0) == 0)
    def _():
        sums_ref[...] = jnp.zeros_like(sums_ref)

    sums_ref[0:1, :] += row_sum(grad * normed)
    sums_ref[1:2, :] += row_sum(grad)
    sums_ref[2:3, :] += row_sum(low.astype(F32))


def hidden_call(dz, w_in, dr, normed, inv, w_out, rows):
    t = dz.shape[0]
    tile = pl.BlockSpec((256, D), lambda i: (i, 0))
    return pl.pallas_call(
        hidden_kernel,
        out_shape=(SHAPE((t, D), F32), SHAPE((t, D), BF), SHAPE((t, D), BF), SHAPE((8, D), F32)),
        grid=(t // 256,),
        in_specs=[
            pl.BlockSpec((256, FF), lambda i: (i, 0)), full_spec((D, FF)), tile, tile,
            pl.BlockSpec((256, 1), lambda i: (i, 0)), full_spec((D, D)), full_spec(rows.shape),
        ],
        out_specs=(tile, tile, tile, pl.BlockSpec((8, D), lambda i: (0, 0))),
        cost_estimate=cost(2 * t * D * (FF + D), 2 * (t * FF + D * FF) + 16 * t * D),
        name="up_back_norm",
    )(dz, w_in, dr, normed, inv, w_out, rows)


def input_kernel(a_ref, b_ref, w_ref, r_ref, o_ref):
    half = a_ref.shape[1]
    value = dot(a_ref[...], w_ref[:, :half], 1, 1) + dot(b_ref[...], w_ref[:, half:], 1, 1)
    o_ref[...] = (r_ref[...] + value).astype(BF)


def input_call(part_a, part_b, w_qkv, resid):
    t, width = part_a.shape
    tile = pl.BlockSpec((256, D), lambda i: (i, 0))
    wide = pl.BlockSpec((256, width), lambda i: (i, 0))
    return pl.pallas_call(
        input_kernel,
        out_shape=SHAPE((t, D), BF),
        grid=(t // 256,),
        in_specs=[wide, wide, full_spec(w_qkv.shape), tile],
        out_specs=tile,
        cost_estimate=cost(4 * t * D * width, 4 * (t * width + D * width) + 6 * t * D),
        name="input_back",
    )(part_a, part_b, w_qkv, resid)


def weight_kernel(half_ref, left_ref, right_ref, *refs):
    o_ref, turned = refs[-2], refs[-1]

    @pl.when(pl.program_id(1) == 0)
    def _():
        turned[...] = left_ref[...].T

    value = dot(turned[...], right_ref[...], 1, 0)
    if len(refs) == 3:
        value = value + refs[0][...].astype(F32)
    o_ref[...] = value.astype(BF)


def weight_call(left, right, half, came=None):
    t, rows = left.shape
    width = right.shape[1]
    bm = 512
    bn = 1024 if width == 1024 else 512
    steps = rows // 2 // bm
    specs = [
        pl.BlockSpec((t, bm), lambda i, j, h: (0, h[0] * steps + i)),
        pl.BlockSpec((t, bn), lambda i, j, h: (0, j)),
    ]
    values = [left, right]
    out = pl.BlockSpec((bm, bn), lambda i, j, h: (i, j))
    if came is not None:
        specs.append(out)
        values.append(came)
    return pl.pallas_call(
        weight_kernel,
        out_shape=SHAPE((rows // 2, width), BF),
        grid_spec=pltpu.PrefetchScalarGridSpec(
            num_scalar_prefetch=1, grid=(steps, width // bn), in_specs=specs, out_specs=out,
            scratch_shapes=[pltpu.VMEM((bm, t), BF)],
        ),
        cost_estimate=cost(t * rows * width, t * rows + 2 * t * width + 2 * rows * width),
        name="weight_grad",
    )(half.reshape(1), *values)


def inner_kernel(rate, decay, w_ref, g_ref, m_ref, v_ref, m_out, v_out, d_out):
    weight = w_ref[...]
    new, m_out[...], v_out[...] = inner_step(
        weight, g_ref[...].astype(F32), m_ref[...], v_ref[...], rate, decay
    )
    d_out[...] = (weight - new).astype(BF)


def inner_call(weight, grad, first, second, rate, decay):
    rows, width = weight.shape
    block = 32 * 4096 // width
    tile = pl.BlockSpec((block, width), lambda i: (i, 0))
    like = SHAPE((rows, width), F32)
    return pl.pallas_call(
        partial(inner_kernel, rate, decay),
        out_shape=(like, like, SHAPE((rows, width), BF)),
        grid=(rows // block,),
        in_specs=[tile] * 4,
        out_specs=(tile,) * 3,
        cost_estimate=cost(20 * rows * width, 24 * rows * width),
        name="inner_step",
    )(weight, grad, first, second)


def outer_kernel(core_ref, w_ref, u_ref, own_ref, came_ref, o_ref, c_ref):
    mine = (core_ref[0] == pl.program_id(0)).astype(F32)
    total = own_ref[...].astype(F32) * mine + came_ref[...].astype(F32) * (1.0 - mine)
    mean = total * 0.25
    weight = w_ref[...]
    momentum = 0.5 * u_ref[...] + mean
    new = weight - 0.7 * (mean + 0.5 * momentum)
    o_ref[0] = mean
    o_ref[1] = momentum
    o_ref[2] = new
    c_ref[...] = new.astype(BF)


def outer_call(weight, momentum, own, came, core):
    rows, width = weight.shape
    block = 32 * 4096 // width
    steps = rows // 2 // block
    tile = pl.BlockSpec((block, width), lambda h, i, c: (h * steps + i, 0))
    part = pl.BlockSpec((block, width), lambda h, i, c: (i, 0))
    return pl.pallas_call(
        outer_kernel,
        out_shape=(SHAPE((3, rows, width), F32), SHAPE((rows, width), BF)),
        grid_spec=pltpu.PrefetchScalarGridSpec(
            num_scalar_prefetch=1, grid=(2, steps), in_specs=[tile, tile, part, part],
            out_specs=(pl.BlockSpec((3, block, width), lambda h, i, c: (0, h * steps + i, 0)), tile),
        ),
        cost_estimate=cost(10 * rows * width, 26 * rows * width),
        name="outer_step",
    )(core.reshape(1), weight, momentum, own, came)


def erf_parts(value):
    size = jnp.abs(value) * 0.7071067811865476
    share = 1.0 / (1.0 + 0.5 * size)
    inner = 0.17087277
    for coefficient in (
        -0.82215223, 1.48851587, -1.13520398, 0.27886807, -0.18628806, 0.09678418, 0.37409196, 1.00002368
    ):
        inner = coefficient + share * inner
    square = size * size
    half = 0.5 * share * jnp.exp(share * inner - 1.26551223 - square)
    return jnp.where(value >= 0, 1.0 - half, half), jnp.exp(-square)


def xor_pairs(bits):
    place = {"y": 0, "z0": 1, "z1": 2, "c": 3, "x": 4}
    flip = sum(1 << place[bit] for bit in bits)
    pairs = []
    for device in range(32):
        if bits == ("c", "z1") and ((device >> 3) & 1) == ((device >> 2) & 1):
            continue
        pairs.append((device, device ^ flip))
    return pairs


def exchange(value, *bits):
    return lax.ppermute(value, ("rep", "fsdp"), xor_pairs(bits))


def swap(at, value):
    return jnp.where(at["c"] != at["z1"], exchange(value, "c", "z1"), value)


def add_low(left, right):
    return (left.astype(jnp.float32) + right.astype(jnp.float32)).astype(jnp.bfloat16)


def pick(value, index, axis):
    return lax.dynamic_index_in_dim(value, index, axis, keepdims=False)


def stage(at, total, which):
    axis = 1 if which == "y" and total.ndim == 4 else 0
    came = exchange(pick(total, 1 - at[which], axis), which)
    return add_low(pick(total, at[which], axis), came)


def slabs(total):
    return total.reshape(2, 2, -1, total.shape[-1])


def after(value, *earlier):
    return lax.optimization_barrier((value,) + earlier)[0]


def rep_total(at, diff):
    halves = diff.reshape(2, diff.shape[0] // 2, diff.shape[1])
    came = exchange(pick(halves, 1 - at["c"], 0), "c")
    total = add_low(pick(halves, at["c"], 0), came)
    total = add_low(total, exchange(total, "x"))
    return total, exchange(total, "c")


def weave(value):
    rows = value.shape[1]
    return jnp.transpose(value.reshape(3, rows, D // 128, 128), (1, 2, 0, 3)).reshape(rows, 3 * D)


def unweave(value):
    rows = value.shape[0]
    return jnp.transpose(value.reshape(rows, D // 128, 3, 128), (2, 0, 1, 3)).reshape(3, rows, D)


def per_device_fast(
    tokens,
    cotangent,
    segment_ids,
    attention_weight,
    attention_momentum,
    attention_first,
    attention_second,
    expand_weight,
    expand_momentum,
    expand_first,
    expand_second,
    contract_weight,
    contract_momentum,
    contract_first,
    contract_second,
    vectors,
    vectors_momentum,
    vectors_first,
    vectors_second,
):
    bf, f32 = jnp.bfloat16, jnp.float32
    at = bits_of()
    core = at["c"].astype(jnp.int32)
    attn_low = attention_weight.astype(bf)
    w_qkv, w_out, w_in, w_down, vector_full, tok, seg = gather_all(
        weave(attn_low[:3]), attn_low[3], expand_weight.astype(bf), contract_weight.astype(bf),
        vectors.astype(bf), tokens, segment_ids,
    )
    cot = swap(at, after(cotangent, w_qkv))
    rows = jnp.swapaxes(vector_full, 0, 1).reshape(-1, D).astype(f32)
    bias_up = rows[8:].reshape(1, FF)
    bias_qkv = weave(jnp.stack([rows[4], jnp.zeros_like(rows[4]), rows[5]])[:, None])
    scale_qkv = weave(jnp.stack([jnp.full((1, D), 0.125, f32)] + [jnp.ones((1, D), f32)] * 2))
    qkv = qkv_call(tok, w_qkv, bias_qkv, scale_qkv)
    mixed, log_sum = attn_fwd(qkv, seg)
    normed, inv, hidden_low = mix_call(mixed, w_out, tok, rows)
    activated, slope = up_call(hidden_low, w_in, bias_up)
    layer_output, grad_sum, grad_branch, sums_two = down_call(activated, w_down, normed, cot, rows)
    down_send = weight_call(activated, grad_branch, 1 - core)
    grad_pre, sums_up = slope_call(after(grad_branch, down_send), w_down, slope)
    down_came = exchange(down_send, "c")
    up_send = weight_call(hidden_low, grad_pre, 1 - core)
    down_total = weight_call(activated, after(grad_branch, up_send), core, down_came)
    up_came = exchange(up_send, "c")
    up_total = weight_call(hidden_low, after(grad_pre, down_total), core, up_came)
    grad_resid, grad_attn, grad_mixed, sums_one = hidden_call(
        after(grad_pre, up_total), w_in, grad_sum, normed, inv, w_out, rows
    )
    down_one = stage(at, slabs(down_total), "y")
    up_one = stage(at, slabs(up_total), "z0")
    proj_send = weight_call(mixed, grad_attn, 1 - core)
    proj_came = exchange(proj_send, "c")
    grad_a, sums_a = attn_bwd(qkv, after(grad_mixed, proj_send), log_sum, seg, 0)
    qkv_send_a = weight_call(tok, grad_a, 1 - core)
    down_one, up_one, qkv_send_a = lax.optimization_barrier((down_one, up_one, qkv_send_a))
    came_a = exchange(qkv_send_a, "c")
    down_two = stage(at, down_one, "z0")
    up_two = stage(at, up_one, "y")
    proj_total = weight_call(mixed, after(grad_attn, qkv_send_a, down_one, up_one), core, proj_came)
    total_a = weight_call(tok, after(grad_a, proj_total), core, came_a)
    proj_one = stage(at, slabs(proj_total), "y")
    a_one = stage(at, slabs(total_a), "z0")
    grad_b, sums_b = attn_bwd(qkv, after(grad_mixed, total_a), log_sum, seg, 1)
    qkv_send_b = weight_call(tok, grad_b, 1 - core)
    down_two, up_two, proj_one, a_one, qkv_send_b = lax.optimization_barrier(
        (down_two, up_two, proj_one, a_one, qkv_send_b)
    )
    came_b = exchange(qkv_send_b, "c")
    grad_contract = swap(at, down_two)
    grad_expand = swap(at, up_two)
    proj_two = stage(at, proj_one, "z0")
    a_two = stage(at, a_one, "y")
    input_grad = input_call(after(grad_a, down_two, qkv_send_b), grad_b, w_qkv, grad_resid)
    total_b = weight_call(tok, after(grad_b, input_grad), core, came_b)
    b_one = stage(at, slabs(total_b), "y")
    b_two = stage(at, b_one, "z0")
    sums_qkv = jnp.concatenate([sums_a, sums_b], axis=0).reshape(D // 128, 3, 128)
    vector_grad = jnp.concatenate(
        [
            sums_one[0:1],
            sums_two[0:1],
            sums_one[1:2],
            sums_two[1:2],
            sums_qkv[:, 0].reshape(1, D),
            sums_qkv[:, 2].reshape(1, D),
            sums_one[2:3],
            sums_two[2:3],
            sums_up.reshape(FF // D, D),
        ],
        axis=0,
    )
    parts = after(vector_grad)
    for which in ("c", "z0", "y"):
        half = parts.shape[1] // 2
        away = lax.dynamic_slice_in_dim(parts, (1 - at[which]) * half, half, axis=1)
        parts = lax.dynamic_slice_in_dim(parts, at[which] * half, half, axis=1) + exchange(away, which)
    grad_vectors = swap(at, parts)
    grad_qkv_own = jnp.concatenate([a_two, b_two], axis=1)
    grad_proj = proj_two
    output = swap(at, layer_output)
    input_grad = swap(at, input_grad)
    grad_attention = jnp.concatenate([unweave(swap(at, grad_qkv_own)), swap(at, grad_proj)[None]], axis=0)
    results = []
    for weight, momentum, first, second, grad, rate, decay in (
        (attention_weight, attention_momentum, attention_first, attention_second, grad_attention, 0.03, 0.1),
        (expand_weight, expand_momentum, expand_first, expand_second, grad_expand, 0.03, 0.1),
        (contract_weight, contract_momentum, contract_first, contract_second, grad_contract, 0.015, 0.1),
    ):
        flat = (-1, weight.shape[-1])
        flat_weight = weight.reshape(flat)
        first_new, second_new, diff = inner_call(
            flat_weight, grad.reshape(flat), first.reshape(flat), second.reshape(flat), rate, decay
        )
        own, came = rep_total(at, diff)
        outer, copy = outer_call(flat_weight, momentum.reshape(flat), own, came, core)
        results += [
            first_new.reshape(first.shape),
            second_new.reshape(first.shape),
            outer.reshape((3,) + weight.shape),
            copy.reshape(weight.shape),
        ]
    inner_new, first_new, second_new = inner_step(
        vectors, grad_vectors, vectors_first[0], vectors_second[0], 0.2, 0.0
    )
    mean_diff = lax.psum((vectors - inner_new).astype(bf), "rep").astype(f32) / 4
    momentum_new = 0.5 * vectors_momentum + mean_diff
    outer_new = vectors - 0.7 * (mean_diff + 0.5 * momentum_new)
    results += [
        first_new[None],
        second_new[None],
        jnp.stack([mean_diff, momentum_new, outer_new]),
        outer_new.astype(bf),
    ]
    return (output, input_grad) + tuple(results)


def solution(mesh):
    placed = (
        P(("rep", "fsdp"), None),
        P(("rep", "fsdp"), None),
        P(("rep", "fsdp"), None),
        P(None, "fsdp", None),
        P(None, "fsdp", None),
        P("rep", None, "fsdp", None),
        P("rep", None, "fsdp", None),
        P("fsdp", None),
        P("fsdp", None),
        P("rep", "fsdp", None),
        P("rep", "fsdp", None),
        P("fsdp", None),
        P("fsdp", None),
        P("rep", "fsdp", None),
        P("rep", "fsdp", None),
        P(None, "fsdp"),
        P(None, "fsdp"),
        P("rep", None, "fsdp"),
        P("rep", None, "fsdp"),
    )
    small = mesh.shape["rep"] == 4 and mesh.shape["fsdp"] == 8
    body = per_device_fast if small else per_device
    return jax.shard_map(
        body,
        mesh=mesh,
        in_specs=placed,
        out_specs=(
            P(("rep", "fsdp"), None),
            P(("rep", "fsdp"), None),
            P("rep", None, "fsdp", None),
            P("rep", None, "fsdp", None),
            P(None, None, "fsdp", None),
            P(None, "fsdp", None),
            P("rep", "fsdp", None),
            P("rep", "fsdp", None),
            P(None, "fsdp", None),
            P("fsdp", None),
            P("rep", "fsdp", None),
            P("rep", "fsdp", None),
            P(None, "fsdp", None),
            P("fsdp", None),
            P("rep", None, "fsdp"),
            P("rep", None, "fsdp"),
            P(None, None, "fsdp"),
            P(None, "fsdp"),
        ),
        check_vma=False,
    )
```

```python
from functools import partial

import jax
import jax.numpy as jnp
from jax import lax
from jax.experimental import pallas as pl
from jax.experimental.pallas import tpu as pltpu
from jax.sharding import PartitionSpec as P

D = 1024
H = 16
HD = 64
FF = 4096
LEN = 1024
SEQ_DEV = 1
ADAM_STEP = 4
TOK_DEV = 1024


def norm_forward(values_in, gain_row, shift_row):
    center = values_in - jnp.mean(values_in, axis=-1, keepdims=True)
    inv_scale = lax.rsqrt(jnp.mean(center * center, axis=-1, keepdims=True) + 1e-05)
    normed = center * inv_scale
    return (normed * gain_row + shift_row, normed, inv_scale)


def norm_backward(grad_out, normed, inv_scale, gain_row):
    grad_gain = jnp.sum(grad_out * normed, axis=0)
    grad_shift = jnp.sum(grad_out, axis=0)
    scaled_grad = grad_out * gain_row
    grad_value = inv_scale * (
        scaled_grad
        - jnp.mean(scaled_grad, axis=-1, keepdims=True)
        - normed * jnp.mean(scaled_grad * normed, axis=-1, keepdims=True)
    )
    return (grad_value, grad_gain, grad_shift)


def product_over(left, right):
    return lax.dot_general(
        left, right, (((0,), (0,)), ((), ())), preferred_element_type=jnp.float32
    )


def product_back(left, right):
    return lax.dot_general(
        left, right, (((1,), (1,)), ((), ())), preferred_element_type=jnp.float32
    )


def block_scores(query_block, key_block, row_segments, all_segments):
    scores = jnp.einsum("qhd,khd->hqk", query_block, key_block, preferred_element_type=jnp.float32)
    same_doc = row_segments[:, None] == all_segments[None, :]
    return jnp.where(same_doc[None], scores, -1e30)


def inner_step(weight, gradient, first_moment, second_moment, learn_rate, weight_decay):
    first_new = 0.5 * first_moment + 0.5 * gradient
    second_new = 0.75 * second_moment + 0.25 * gradient * gradient
    update_dir = (
        first_new
        / (1.0 - 0.5**ADAM_STEP)
        / (jnp.sqrt(second_new / (1.0 - 0.75**ADAM_STEP)) + 1e-08)
    )
    return (weight - learn_rate * (update_dir + weight_decay * weight), first_new, second_new)


def per_device(
    tokens,
    cotangent,
    segment_ids,
    attention_weight,
    attention_momentum,
    attention_first,
    attention_second,
    expand_weight,
    expand_momentum,
    expand_first,
    expand_second,
    contract_weight,
    contract_momentum,
    contract_first,
    contract_second,
    vectors,
    vectors_momentum,
    vectors_first,
    vectors_second,
):
    attn_full, vector_full = (
        lax.all_gather(attention_weight.astype(jnp.bfloat16), "fsdp", axis=1, tiled=True),
        lax.all_gather(vectors.astype(jnp.bfloat16), "fsdp", axis=1, tiled=True),
    )
    vector_rows = vector_full.astype(jnp.float32)
    gain_one, gain_two, shift_one, shift_two = (
        vector_rows[0],
        vector_rows[1],
        vector_rows[2],
        vector_rows[3],
    )
    bias_query, bias_value, bias_mixed, bias_down = (
        vector_rows[4],
        vector_rows[5],
        vector_rows[6],
        vector_rows[7],
    )
    bias_up = vector_rows[8:].reshape(FF)
    projected = jnp.einsum("td,nde->nte", tokens, attn_full[:3], preferred_element_type=jnp.float32)
    query_all = ((projected[0] + bias_query) * 0.125).astype(jnp.bfloat16)
    key_all = projected[1].astype(jnp.bfloat16)
    value_all = (projected[2] + bias_value).astype(jnp.bfloat16)
    query_heads = query_all.reshape(SEQ_DEV, LEN, H, HD)
    key_heads = key_all.reshape(SEQ_DEV, LEN, H, HD)
    value_heads = value_all.reshape(SEQ_DEV, LEN, H, HD)
    block_rows = min(512, LEN)
    head_group = min(8, H)
    context_rows = []
    log_sums = []
    seq_index = 0
    for row_start in range(0, LEN, block_rows):
        block_pieces = []
        for head_start in range(0, H, head_group):
            head_part = slice(head_start, head_start + head_group)
            scores = block_scores(
                query_heads[seq_index, row_start : row_start + block_rows, head_part],
                key_heads[seq_index, :, head_part],
                segment_ids[seq_index, row_start : row_start + block_rows],
                segment_ids[seq_index],
            )
            row_max = jnp.max(scores, axis=-1, keepdims=True)
            exp_score = jnp.exp(scores - row_max)
            row_total = jnp.sum(exp_score, axis=-1, keepdims=True)
            probability = (exp_score / row_total).astype(jnp.bfloat16)
            block_pieces.append(
                jnp.einsum(
                    "hqk,khd->qhd",
                    probability,
                    value_heads[seq_index, :, head_part],
                    preferred_element_type=jnp.float32,
                )
            )
            log_sums.append(row_max + jnp.log(row_total))
        context_rows.append(jnp.concatenate(block_pieces, axis=1))
    mixed = jnp.concatenate(context_rows, axis=0).reshape(TOK_DEV, D).astype(jnp.bfloat16)
    attn_out = jnp.dot(mixed, attn_full[3], preferred_element_type=jnp.float32) + bias_mixed
    hidden, normed_one, scale_one = norm_forward(
        tokens.astype(jnp.float32) + attn_out, gain_one, shift_one
    )
    hidden_low = hidden.astype(jnp.bfloat16)
    ffn_expand, ffn_contract = (
        lax.all_gather(expand_weight.astype(jnp.bfloat16), "fsdp", axis=0, tiled=True),
        lax.all_gather(contract_weight.astype(jnp.bfloat16), "fsdp", axis=0, tiled=True),
    )
    pre_act = jnp.dot(hidden_low, ffn_expand, preferred_element_type=jnp.float32) + bias_up
    activated = jax.nn.gelu(pre_act, approximate=False).astype(jnp.bfloat16)
    branch = jnp.dot(activated, ffn_contract, preferred_element_type=jnp.float32) + bias_down
    layer_output, normed_two, scale_two = norm_forward(hidden + branch, gain_two, shift_two)
    grad_sum, grad_gain_two, grad_shift_two = norm_backward(
        cotangent.astype(jnp.float32), normed_two, scale_two, gain_two
    )
    grad_branch = grad_sum.astype(jnp.bfloat16)
    grad_act = product_back(grad_branch, ffn_contract)
    unused_value, gelu_pull = jax.vjp(partial(jax.nn.gelu, approximate=False), pre_act)
    grad_pre_low = gelu_pull(grad_act)[0].astype(jnp.bfloat16)
    grad_hidden = grad_sum + product_back(grad_pre_low, ffn_expand)
    contract_full = product_over(activated, grad_branch)
    expand_full = product_over(hidden_low, grad_pre_low)
    grad_expand, grad_contract = (
        lax.psum_scatter(expand_full, "fsdp", scatter_dimension=0, tiled=True),
        lax.psum_scatter(contract_full, "fsdp", scatter_dimension=0, tiled=True),
    )
    grad_resid, grad_gain_one, grad_shift_one = norm_backward(
        grad_hidden, normed_one, scale_one, gain_one
    )
    grad_attn_out = grad_resid.astype(jnp.bfloat16)
    grad_bias_mixed = jnp.sum(grad_attn_out.astype(jnp.float32), axis=0)
    grad_output_proj = product_over(mixed, grad_attn_out)
    grad_mixed = product_back(grad_attn_out, attn_full[3]).astype(jnp.bfloat16)
    grad_context = grad_mixed.reshape(SEQ_DEV, LEN, H, HD)
    query_grads = []
    lse_index = 0
    seq_index = 0
    key_totals = [
        jnp.zeros((LEN, head_group, HD), jnp.float32) for head_start in range(0, H, head_group)
    ]
    value_totals = [
        jnp.zeros((LEN, head_group, HD), jnp.float32) for head_start in range(0, H, head_group)
    ]
    for row_start in range(0, LEN, block_rows):
        block_pieces = []
        for group_index, head_start in enumerate(range(0, H, head_group)):
            head_part = slice(head_start, head_start + head_group)
            query_block = query_heads[seq_index, row_start : row_start + block_rows, head_part]
            key_block = key_heads[seq_index, :, head_part]
            value_block = value_heads[seq_index, :, head_part]
            ctx_grad = grad_context[seq_index, row_start : row_start + block_rows, head_part]
            scores = block_scores(
                query_block,
                key_block,
                segment_ids[seq_index, row_start : row_start + block_rows],
                segment_ids[seq_index],
            )
            probability = jnp.exp(scores - log_sums[lse_index])
            lse_index = lse_index + 1
            value_totals[group_index] = value_totals[group_index] + jnp.einsum(
                "hqk,qhd->khd",
                probability.astype(jnp.bfloat16),
                ctx_grad,
                preferred_element_type=jnp.float32,
            )
            prob_grad = jnp.einsum(
                "qhd,khd->hqk", ctx_grad, value_block, preferred_element_type=jnp.float32
            )
            row_dot = jnp.sum(probability * prob_grad, axis=-1, keepdims=True)
            score_grad = (probability * (prob_grad - row_dot)).astype(jnp.bfloat16)
            block_pieces.append(
                jnp.einsum(
                    "hqk,khd->qhd", score_grad, key_block, preferred_element_type=jnp.float32
                ).astype(jnp.bfloat16)
            )
            key_totals[group_index] = key_totals[group_index] + jnp.einsum(
                "hqk,qhd->khd", score_grad, query_block, preferred_element_type=jnp.float32
            )
        query_grads.append(jnp.concatenate(block_pieces, axis=1))
    key_grads = jnp.concatenate(
        [key_total.astype(jnp.bfloat16) for key_total in key_totals], axis=1
    )
    value_grads = jnp.concatenate(
        [value_total.astype(jnp.bfloat16) for value_total in value_totals], axis=1
    )
    grad_query = jnp.concatenate(query_grads, axis=0).reshape(TOK_DEV, D) * 0.125
    grad_keys = key_grads.reshape(TOK_DEV, D)
    grad_values = value_grads.reshape(TOK_DEV, D)
    stacked_grads = jnp.stack([grad_query, grad_keys, grad_values])
    grad_qkv = jnp.einsum("td,nte->nde", tokens, stacked_grads, preferred_element_type=jnp.float32)
    input_grad = (
        grad_resid
        + jnp.einsum(
            "nte,nde->td", stacked_grads, attn_full[:3], preferred_element_type=jnp.float32
        )
    ).astype(jnp.bfloat16)
    grad_attention_full = jnp.concatenate([grad_qkv, grad_output_proj[None]], axis=0)
    vector_head = jnp.stack(
        [
            grad_gain_one,
            grad_gain_two,
            grad_shift_one,
            grad_shift_two,
            jnp.sum(grad_query.astype(jnp.float32), axis=0),
            jnp.sum(grad_values.astype(jnp.float32), axis=0),
            grad_bias_mixed,
            jnp.sum(grad_branch.astype(jnp.float32), axis=0),
        ]
    )
    grad_bias_up = jnp.sum(grad_pre_low.astype(jnp.float32), axis=0).reshape(FF // D, D)
    grad_vectors_full = jnp.concatenate([vector_head, grad_bias_up], axis=0)
    grad_attention, grad_vectors = (
        lax.psum_scatter(grad_attention_full, "fsdp", scatter_dimension=1, tiled=True),
        lax.psum_scatter(grad_vectors_full, "fsdp", scatter_dimension=1, tiled=True),
    )
    attention_new = inner_step(
        attention_weight, grad_attention, attention_first[0], attention_second[0], 0.03, 0.1
    )
    expand_new = inner_step(
        expand_weight, grad_expand, expand_first[0], expand_second[0], 0.03, 0.1
    )
    contract_new = inner_step(
        contract_weight, grad_contract, contract_first[0], contract_second[0], 0.015, 0.1
    )
    vectors_new = inner_step(vectors, grad_vectors, vectors_first[0], vectors_second[0], 0.2, 0.0)
    summed = (
        lax.psum((attention_weight - attention_new[0]).astype(jnp.bfloat16), "rep").astype(
            jnp.float32
        ),
        lax.psum((expand_weight - expand_new[0]).astype(jnp.bfloat16), "rep").astype(jnp.float32),
        lax.psum((contract_weight - contract_new[0]).astype(jnp.bfloat16), "rep").astype(
            jnp.float32
        ),
        lax.psum((vectors - vectors_new[0]).astype(jnp.bfloat16), "rep").astype(jnp.float32),
    )
    groups_count = lax.axis_size("rep")
    results = []
    for weight_now, momentum_now, inner_new, diff_total in zip(
        (attention_weight, expand_weight, contract_weight, vectors),
        (attention_momentum, expand_momentum, contract_momentum, vectors_momentum),
        (attention_new, expand_new, contract_new, vectors_new),
        summed,
    ):
        mean_diff = diff_total / groups_count
        momentum_new = 0.5 * momentum_now + mean_diff
        outer_new = weight_now - 0.7 * (mean_diff + 0.5 * momentum_new)
        results.append(
            (
                inner_new[1][None],
                inner_new[2][None],
                jnp.stack([mean_diff, momentum_new, outer_new]),
                outer_new.astype(jnp.bfloat16),
            )
        )
    return (
        layer_output.astype(jnp.bfloat16),
        input_grad,
        results[0][0],
        results[0][1],
        results[0][2],
        results[0][3],
        results[1][0],
        results[1][1],
        results[1][2],
        results[1][3],
        results[2][0],
        results[2][1],
        results[2][2],
        results[2][3],
        results[3][0],
        results[3][1],
        results[3][2],
        results[3][3],
    )


NEG=-1e30
QB=256
def attn_windows(seg_row):
    length = seg_row.shape[0]
    nb = length // QB
    firsts = seg_row[::QB]
    lasts = seg_row[QB-1::QB]
    begin = jnp.sum((seg_row[None, :] < firsts[:, None]).astype(jnp.int32), axis=1)
    end = jnp.sum((seg_row[None, :] <= lasts[:, None]).astype(jnp.int32), axis=1)
    start = begin // 128
    count = (end - start * 128 + QB - 1) // QB
    start = jnp.minimum(start, (length - count * QB) // 128)
    return start.astype(jnp.int32), count.astype(jnp.int32)
def lane_half(shape, h):
    lane = lax.broadcasted_iota(jnp.int32, shape, len(shape)-1)
    return (lane < 64) if h == 0 else (lane >= 64)
def dot(a, b, ca, cb):
    return lax.dot_general(a, b, (((ca,), (cb,)), ((), ())), preferred_element_type=jnp.float32)
def fold(value, join):
    part = value.shape[0] // 8
    parts = [value[i * part:(i + 1) * part] for i in range(8)]
    while len(parts) > 1:
        parts = [join(a, b) for a, b in zip(parts[::2], parts[1::2])]
    return parts[0]
def fwd_kernel(start_ref, count_ref, qkv_ref, segr_ref, segc_ref, o_ref, lse_ref, vt_ref):
    length = qkv_ref.shape[0]
    vt_ref[...] = qkv_ref[:, 256:384].T
    nb = length // QB
    for i in range(nb):
        rows = slice(i*QB, (i+1)*QB)
        for nn in range(1, nb+1):
            @pl.when(count_ref[i] == nn)
            def _():
                nk = nn*QB
                lo = pl.multiple_of(start_ref[i]*128, 128)
                kw = qkv_ref[pl.ds(lo, nk), 128:256]
                qb = qkv_ref[rows, 0:128]
                same = segc_ref[pl.ds(lo, nk), :] == segr_ref[:, rows]
                outs = []
                for h in range(2):
                    qh = jnp.where(lane_half(qb.shape, h), qb, jnp.zeros_like(qb))
                    st = jnp.where(same, dot(kw, qh, 1, 1), NEG)
                    m = jnp.max(fold(st, jnp.maximum), axis=0, keepdims=True)
                    p = jnp.exp(st - m)
                    l = jnp.sum(fold(p, jnp.add), axis=0, keepdims=True)
                    weighted = dot(vt_ref[h*64:(h+1)*64, pl.ds(lo, nk)], p.astype(jnp.bfloat16), 1, 0)
                    outs.append(weighted * (1.0 / l))
                    lse_ref[0, h:h+1, rows] = m + jnp.log(l)
                o_ref[rows, :] = jnp.concatenate(outs, axis=0).T.astype(jnp.bfloat16)
def bwd_kernel(start_ref, count_ref, qkv_ref, do_ref, lse_ref, segr_ref, segc_ref, d_ref, sums_ref, dk_acc, dv_acc, kt_ref):
    length = qkv_ref.shape[0]
    kt_ref[...] = qkv_ref[:, 128:256].T
    nb = length // QB
    dk_acc[...] = jnp.zeros_like(dk_acc)
    dv_acc[...] = jnp.zeros_like(dv_acc)
    for i in range(nb):
        rows = slice(i*QB, (i+1)*QB)
        for nn in range(1, nb+1):
            @pl.when(count_ref[i] == nn)
            def _():
                nk = nn*QB
                lo = pl.multiple_of(start_ref[i]*128, 128)
                win = pl.ds(lo, nk)
                kw = qkv_ref[win, 128:256]
                vw = qkv_ref[win, 256:384]
                qb = qkv_ref[rows, 0:128]
                db = do_ref[rows, :]
                same = segc_ref[win, :] == segr_ref[:, rows]
                dqs = []; dks = 0.0; dvs = 0.0
                for h in range(2):
                    hm = lane_half(qb.shape, h)
                    qh = jnp.where(hm, qb, jnp.zeros_like(qb))
                    dh = jnp.where(hm, db, jnp.zeros_like(db))
                    st = jnp.where(same, dot(kw, qh, 1, 1), NEG)
                    p = jnp.exp(st - lse_ref[0, h:h+1, rows])
                    dpt = dot(vw, dh, 1, 1)
                    rd = jnp.sum(fold(p * dpt, jnp.add), axis=0, keepdims=True)
                    ds = (p * (dpt - rd)).astype(jnp.bfloat16)
                    dvs = dvs + dot(p.astype(jnp.bfloat16), dh, 1, 0)
                    dks = dks + dot(ds, qh, 1, 0)
                    dqs.append(dot(kt_ref[h*64:(h+1)*64, win], ds, 1, 0))
                d_ref[rows, 0:128] = jnp.concatenate(dqs, axis=0).T.astype(jnp.bfloat16) * 0.125
                dk_acc[win, :] += dks
                dv_acc[win, :] += dvs
    d_ref[:, 128:256] = dk_acc[...].astype(jnp.bfloat16)
    d_ref[:, 256:384] = dv_acc[...].astype(jnp.bfloat16)
    sums_ref[0] = jnp.sum(d_ref[...].astype(jnp.float32), axis=0, keepdims=True)
def attn_fwd(qkv, seg):
    T, width = qkv.shape
    start, count = attn_windows(seg[0])
    segc = seg.reshape(T, 1)
    heads = width // 384
    return pl.pallas_call(
        fwd_kernel,
        out_shape=(jax.ShapeDtypeStruct((T, width // 3), jnp.bfloat16), jax.ShapeDtypeStruct((heads, 2, T), jnp.float32)),
        grid_spec=pltpu.PrefetchScalarGridSpec(
            num_scalar_prefetch=2, grid=(heads,),
            in_specs=[
                pl.BlockSpec((T, 384), lambda h, *_: (0, h)),
                pl.BlockSpec((1, T), lambda h, *_: (0, 0)),
                pl.BlockSpec((T, 1), lambda h, *_: (0, 0)),
            ],
            out_specs=(pl.BlockSpec((T, 128), lambda h, *_: (0, h)), pl.BlockSpec((1, 2, T), lambda h, *_: (h, 0, 0))),
            scratch_shapes=[pltpu.VMEM((128, T), jnp.bfloat16)],
        ),
        cost_estimate=cost(20 * T * T * width, 3 * T * width, T * T * width // 128),
        name="attn_fwd",
    )(start, count, qkv, seg, segc)


def attn_bwd(qkv, do, lse, seg, part):
    T, width = qkv.shape
    start, count = attn_windows(seg[0])
    segc = seg.reshape(T, 1)
    heads = width // 768
    first = part * heads
    return pl.pallas_call(
        bwd_kernel,
        out_shape=(jax.ShapeDtypeStruct((T, width // 2), jnp.bfloat16), jax.ShapeDtypeStruct((heads, 1, 384), jnp.float32)),
        grid_spec=pltpu.PrefetchScalarGridSpec(
            num_scalar_prefetch=2, grid=(heads,),
            in_specs=[
                pl.BlockSpec((T, 384), lambda h, *_: (0, first + h)),
                pl.BlockSpec((T, 128), lambda h, *_: (0, first + h)),
                pl.BlockSpec((1, 2, T), lambda h, *_: (first + h, 0, 0)),
                pl.BlockSpec((1, T), lambda h, *_: (0, 0)),
                pl.BlockSpec((T, 1), lambda h, *_: (0, 0)),
            ],
            out_specs=(pl.BlockSpec((T, 384), lambda h, *_: (0, h)), pl.BlockSpec((1, 1, 384), lambda h, *_: (h, 0, 0))),
            scratch_shapes=[pltpu.VMEM((T, 128), jnp.float32)] * 2 + [pltpu.VMEM((128, T), jnp.bfloat16)],
        ),
        cost_estimate=cost(20 * T * T * width, 6 * T * width, T * T * width // 64),
        name="attn_bwd",
    )(start, count, qkv, do, lse, seg, segc)


MESH_ID = pl.DeviceIdType.MESH


def bits_of():
    rep = lax.axis_index("rep")
    fsdp = lax.axis_index("fsdp")
    return dict(
        rep=rep, fsdp=fsdp, x=rep // 2, c=rep % 2, z1=fsdp // 4, z0=(fsdp // 2) % 2, y=fsdp % 2
    )


def partner_of(at, which):
    rep, fsdp = at["rep"], at["fsdp"]
    if which == "c":
        rep = rep + 1 - 2 * at["c"]
    elif which == "x":
        rep = rep + 2 - 4 * at["x"]
    elif which == "y":
        fsdp = fsdp + 1 - 2 * at["y"]
    elif which == "z0":
        fsdp = fsdp + 2 - 4 * at["z0"]
    elif which == "z1":
        fsdp = fsdp + 4 - 8 * at["z1"]
    else:
        rep = rep + 1 - 2 * at["c"]
        fsdp = fsdp + 4 - 8 * at["z1"]
    return (rep, fsdp)


REL = [(a, b, d) for d in (0, 1) for b in (0, 1) for a in (0, 1)]


def gather_kernel(
    qkv_in, wo_in, vec_in, tok_in, seg_in,
    qkv_out, wo_out, vec_out, tok_out, seg_out,
    tok_buf, seg_buf, send_sem, recv_sem, local_sem,
):
    at = bits_of()
    other = {k: partner_of(at, k) for k in ("c", "x", "y", "z0", "z1", "swap")}
    barrier = pltpu.get_barrier_semaphore()
    for k in ("c", "x", "y", "z0", "z1"):
        pl.semaphore_signal(barrier, inc=1, device_id=other[k], device_id_type=MESH_ID)
    moves = at["c"] != at["z1"]

    @pl.when(moves)
    def _():
        pl.semaphore_signal(barrier, inc=1, device_id=other["swap"], device_id_type=MESH_ID)
        pl.semaphore_wait(barrier, 6)

    @pl.when(jnp.logical_not(moves))
    def _():
        pl.semaphore_wait(barrier, 5)

    def flip(bit, rel):
        return bit + rel - 2 * bit * rel

    def shard(rel):
        return 4 * flip(at["z1"], rel[1]) + 2 * flip(at["z0"], rel[0]) + flip(at["y"], rel[2])

    counter = [0]
    started = []

    def send(src, dst, which):
        k = counter[0]
        counter[0] += 1
        copy = pltpu.make_async_remote_copy(
            src_ref=src, dst_ref=dst, send_sem=send_sem.at[k], recv_sem=recv_sem.at[k],
            device_id=other[which], device_id_type=MESH_ID,
        )
        copy.start()
        started.append(copy)
        return copy

    class Piece:
        def __init__(self, own, slot, split_x):
            self.own, self.slot, self.split_x = own, slot, split_x
            self.part = (2 * at["x"] + at["c"]) if split_x else at["c"]
            self.part_x = (2 * (1 - at["x"]) + at["c"]) if split_x else None
            self.copies = {}

        def first(self):
            zero = (0, 0, 0)
            for which in ("z1", "z0", "y"):
                self.copies[which, zero] = send(
                    self.own(self.part), self.slot(shard(zero), self.part), which
                )
            self.copies["c", zero] = send(self.own(None), self.slot(shard(zero), None), "c")

        def onward(self, rel):
            here = self.slot(shard(rel), self.part)
            if rel == (0, 1, 0):
                self.copies["z0", rel] = send(here, here, "z0")
            if rel[2] == 0:
                self.copies["y", rel] = send(here, here, "y")
            if self.split_x:
                self.copies["x", rel] = send(here, here, "x")
            self.copies["c", rel] = send(here, here, "c")

        def arrive(self, which, came):
            self.copies[which, came].wait_recv()
            step = {"z0": (1, 0, 0), "z1": (0, 1, 0), "y": (0, 0, 1)}[which]
            self.onward(tuple(p + q for p, q in zip(came, step)))

        def near(self):
            self.arrive("z1", (0, 0, 0))
            self.arrive("z0", (0, 0, 0))

        def rest(self):
            self.arrive("y", (0, 0, 0))
            self.arrive("z0", (0, 1, 0))
            self.arrive("y", (0, 1, 0))
            self.arrive("y", (1, 0, 0))
            self.arrive("y", (1, 1, 0))

        def last(self):
            if self.split_x:
                for rel in REL[1:]:
                    self.copies["x", rel].wait_recv()
                    there = self.slot(shard(rel), self.part_x)
                    self.copies["cx", rel] = send(there, there, "c")

        def finish(self):
            for (which, rel), copy in self.copies.items():
                if which in ("c", "cx"):
                    copy.wait_recv()

    def rows(ref, count):
        full = ref.shape[-2] // 8
        def slot(f, part):
            if part is None:
                at_row, n = f * full, full
            else:
                at_row, n = f * full + part * (full // count), full // count
            at_row = pl.multiple_of(at_row, 8)
            return ref.at[pl.ds(at_row, n), :]
        return slot

    def own_rows(ref, count):
        full = ref.shape[-2]
        def own(part):
            if part is None:
                return ref
            row = pl.multiple_of(part * (full // count), 8)
            n = full // count
            return ref.at[pl.ds(row, n), :]
        return own

    qkv, wo = pieces = [
        Piece(own_rows(qkv_in, 4), rows(qkv_out, 4), True),
        Piece(own_rows(wo_in, 4), rows(wo_out, 4), True),
    ]
    zero = (0, 0, 0)
    vec_copies = [
        send(vec_in, vec_out.at[shard(zero)], which) for which in ("c", "z1", "z0", "y")
    ]
    pieces[0].first()
    tok_k, seg_k = counter[0], counter[0] + 1
    counter[0] += 2

    def swap_copy(src, dst, k):
        return pltpu.make_async_remote_copy(
            src_ref=src, dst_ref=dst, send_sem=send_sem.at[k], recv_sem=recv_sem.at[k],
            device_id=other["swap"], device_id_type=MESH_ID,
        )

    @pl.when(moves)
    def _():
        swap_copy(tok_in, tok_out, tok_k).start()
        swap_copy(seg_in, seg_out, seg_k).start()

    @pl.when(jnp.logical_not(moves))
    def _():
        one = pltpu.make_async_copy(tok_in, tok_buf, local_sem.at[0])
        two = pltpu.make_async_copy(seg_in, seg_buf, local_sem.at[1])
        one.start()
        two.start()
        one.wait()
        two.wait()
        three = pltpu.make_async_copy(tok_buf, tok_out, local_sem.at[0])
        four = pltpu.make_async_copy(seg_buf, seg_out, local_sem.at[1])
        three.start()
        four.start()
        three.wait()
        four.wait()

    wo.first()
    qkv.near()
    vec_copies[1].wait_recv()
    here = vec_out.at[shard((0, 1, 0))]
    vec_far = send(here, here, "z0")
    vec_more = [send(here, here, "y")]
    vec_copies[2].wait_recv()
    here = vec_out.at[shard((1, 0, 0))]
    vec_more.append(send(here, here, "y"))
    qkv.rest()
    wo.near()
    wo.rest()
    vec_far.wait_recv()
    here = vec_out.at[shard((1, 1, 0))]
    vec_more.append(send(here, here, "y"))
    qkv.last()
    wo.last()
    for piece in pieces:
        piece.finish()
    for copy in [vec_copies[0], vec_copies[3]] + vec_more:
        copy.wait_recv()
    for copy in started:
        copy.wait_send()

    @pl.when(moves)
    def _():
        swap_copy(tok_in, tok_out, tok_k).wait()
        swap_copy(seg_in, seg_out, seg_k).wait()


GATHER_COPIES = 29 * 2 + 8 + 2


def gather_all(qkv, wo, vec, tok, seg):
    bf = jnp.bfloat16
    shape = jax.ShapeDtypeStruct
    whole = pl.BlockSpec(memory_space=pl.ANY)
    return pl.pallas_call(
        gather_kernel,
        out_shape=(
            shape((8 * qkv.shape[0], qkv.shape[1]), bf),
            shape((8 * wo.shape[0], wo.shape[1]), bf),
            shape((8,) + vec.shape, bf),
            shape(tok.shape, bf),
            shape(seg.shape, seg.dtype),
        ),
        in_specs=[whole] * 5,
        out_specs=(whole,) * 5,
        scratch_shapes=[
            pltpu.VMEM(tok.shape, bf),
            pltpu.VMEM(seg.shape, seg.dtype),
            pltpu.SemaphoreType.DMA((GATHER_COPIES,)),
            pltpu.SemaphoreType.DMA((GATHER_COPIES,)),
            pltpu.SemaphoreType.DMA((2,)),
        ],
        compiler_params=pltpu.CompilerParams(collective_id=0, has_side_effects=True),
        name="gather_weights",
    )(qkv, wo, vec, tok, seg)


SHRINK = 1000
BF, F32 = jnp.bfloat16, jnp.float32
SHAPE = jax.ShapeDtypeStruct


def full_spec(shape):
    return pl.BlockSpec(shape, lambda *_: (0,) * len(shape), pipeline_mode=pl.Buffered(1))


def cost(flops, moved, exps=0):
    return pl.CostEstimate(flops=int(flops) // SHRINK, bytes_accessed=int(moved) // SHRINK, transcendentals=int(exps) // SHRINK)


def qkv_kernel(x_ref, w_ref, bias_ref, scale_ref, o_ref):
    for i in range(4):
        rows = slice(i * 256, (i + 1) * 256)
        z = dot(x_ref[rows, :], w_ref[...], 1, 0)
        o_ref[rows, :] = ((z + bias_ref[...]) * scale_ref[...]).astype(BF)


def qkv_call(x, w, bias, scale):
    tokens, width = x.shape[0], w.shape[1]
    tile = 768
    return pl.pallas_call(
        qkv_kernel,
        out_shape=SHAPE((tokens, width), BF),
        grid=(width // tile,),
        in_specs=[
            full_spec(x.shape),
            pl.BlockSpec((x.shape[1], tile), lambda j: (0, j)),
            pl.BlockSpec((1, tile), lambda j: (0, j)),
            pl.BlockSpec((1, tile), lambda j: (0, j)),
        ],
        out_specs=pl.BlockSpec((tokens, tile), lambda j: (0, j)),
        cost_estimate=cost(2 * tokens * D * width, 2 * (tokens * D + D * width + tokens * width)),
        name="qkv",
    )(x, w, bias, scale)


def mean_row(value):
    return jnp.mean(value, axis=-1, keepdims=True)


def mix_kernel(c_ref, w_ref, x_ref, rows_ref, n_ref, q_ref, low_ref):
    value = x_ref[...].astype(F32) + dot(c_ref[...], w_ref[...], 1, 0) + rows_ref[6:7, :]
    center = value - mean_row(value)
    inv = lax.rsqrt(mean_row(center * center) + 1e-05)
    normed = center * inv
    n_ref[...] = normed
    q_ref[...] = inv
    low_ref[...] = (normed * rows_ref[0:1, :] + rows_ref[2:3, :]).astype(BF)


def mix_call(mixed, w_out, tok, rows):
    t = tok.shape[0]
    tile = pl.BlockSpec((256, D), lambda i: (i, 0))
    return pl.pallas_call(
        mix_kernel,
        out_shape=(SHAPE((t, D), F32), SHAPE((t, 1), F32), SHAPE((t, D), BF)),
        grid=(t // 256,),
        in_specs=[tile, full_spec((D, D)), tile, full_spec(rows.shape)],
        out_specs=(tile, pl.BlockSpec((256, 1), lambda i: (i, 0)), tile),
        cost_estimate=cost(2 * t * D * D, 12 * t * D + 2 * D * D),
        name="mix_norm",
    )(mixed, w_out, tok, rows)


def up_kernel(core_ref, h_ref, own_ref, came_ref, bias_ref, g_ref, s_ref):
    def tile(w_ref):
        for i in range(8):
            rows = slice(i * 128, (i + 1) * 128)
            z = dot(h_ref[rows, :], w_ref[...], 1, 0) + bias_ref[...]
            phi, bell = erf_parts(z)
            g_ref[rows, :] = (z * phi).astype(BF)
            s_ref[rows, :] = (phi + z * bell * 0.3989422804014327).astype(BF)

    first = pl.program_id(0) < pl.num_programs(0) // 2

    @pl.when(first)
    def _():
        tile(own_ref)

    @pl.when(jnp.logical_not(first))
    def _():
        tile(came_ref)


def up_call(low, own, came, bias, core):
    t = low.shape[0]
    tile = 512
    half = FF // tile // 2
    place = lambda j, c: (0, lax.rem(j + half * c[0], 2 * half))
    out = pl.BlockSpec((t, tile), place)
    return pl.pallas_call(
        up_kernel,
        out_shape=(SHAPE((t, FF), BF), SHAPE((t, FF), BF)),
        grid_spec=pltpu.PrefetchScalarGridSpec(
            num_scalar_prefetch=1, grid=(FF // tile,),
            in_specs=[
                full_spec(low.shape),
                pl.BlockSpec((D, tile), lambda j, c: (0, jnp.minimum(j, half - 1))),
                pl.BlockSpec((D, tile), lambda j, c: (0, jnp.maximum(j - half, 0))),
                pl.BlockSpec((1, tile), place),
            ],
            out_specs=(out, out),
        ),
        cost_estimate=cost(2 * t * D * FF, 2 * (t * D + D * FF + 2 * t * FF), 2 * t * FF),
        name="up_gelu",
    )(core.reshape(1), low, own, came, bias)


def row_sum(value):
    return jnp.sum(value, axis=0, keepdims=True)


def norm_back(grad, normed, inv, gain):
    scaled = grad * gain
    return inv * (scaled - mean_row(scaled) - normed * mean_row(scaled * normed))


def down_kernel(
    core_ref, g_ref, own_ref, came_ref, n_ref, cot_ref, rows_ref, out_ref, dr_ref, dm_ref, sums_ref, m_ref
):
    half = D // 2
    m_ref[:, pl.ds(pl.multiple_of(core_ref[0] * half, half), half)] = dot(g_ref[...], own_ref[...], 1, 0)
    m_ref[:, pl.ds(pl.multiple_of((1 - core_ref[0]) * half, half), half)] = dot(g_ref[...], came_ref[...], 1, 0)
    hidden = n_ref[...] * rows_ref[0:1, :] + rows_ref[2:3, :]
    value = hidden + m_ref[...] + rows_ref[7:8, :]
    center = value - mean_row(value)
    inv = lax.rsqrt(mean_row(center * center) + 1e-05)
    normed = center * inv
    gain = rows_ref[1:2, :]
    out_ref[...] = (normed * gain + rows_ref[3:4, :]).astype(BF)
    grad = cot_ref[...].astype(F32)
    back = norm_back(grad, normed, inv, gain)
    low = back.astype(BF)
    dr_ref[...] = back
    dm_ref[...] = low

    @pl.when(pl.program_id(0) == 0)
    def _():
        sums_ref[...] = jnp.zeros_like(sums_ref)

    sums_ref[0:1, :] += row_sum(grad * normed)
    sums_ref[1:2, :] += row_sum(grad)
    sums_ref[2:3, :] += row_sum(low.astype(F32))


def down_call(act, own, came, normed, cot, rows, core):
    t = act.shape[0]
    tile = pl.BlockSpec((256, D), lambda i, c: (i, 0))
    return pl.pallas_call(
        down_kernel,
        out_shape=(SHAPE((t, D), BF), SHAPE((t, D), F32), SHAPE((t, D), BF), SHAPE((8, D), F32)),
        grid_spec=pltpu.PrefetchScalarGridSpec(
            num_scalar_prefetch=1, grid=(t // 256,),
            in_specs=[
                pl.BlockSpec((256, FF), lambda i, c: (i, 0)), full_spec((FF, D // 2)), full_spec((FF, D // 2)),
                tile, tile, full_spec(rows.shape),
            ],
            out_specs=(tile, tile, tile, pl.BlockSpec((8, D), lambda i, c: (0, 0))),
            scratch_shapes=[pltpu.VMEM((256, D), F32)],
        ),
        cost_estimate=cost(2 * t * D * FF, 2 * (t * FF + D * FF) + 14 * t * D),
        name="down_norm",
    )(core.reshape(1), act, own, came, normed, cot, rows)


def slope_kernel(core_ref, left_ref, right_ref, own_ref, came_ref, s_ref, o_ref, sums_ref):
    total = 0.0
    for i in range(4):
        rows = slice(i * 256, (i + 1) * 256)
        back = dot(left_ref[rows, :], own_ref[...], 1, 1) + dot(right_ref[rows, :], came_ref[...], 1, 1)
        z = (back * s_ref[rows, :].astype(F32)).astype(BF)
        o_ref[rows, :] = z
        total = total + row_sum(z.astype(F32))
    sums_ref[...] = total


def slope_call(dm, own, came, slope, core):
    t = dm.shape[0]
    tile = 512
    wide = pl.BlockSpec((t, tile), lambda j, c: (0, j))
    part = pl.BlockSpec((tile, D // 2), lambda j, c: (j, 0))
    return pl.pallas_call(
        slope_kernel,
        out_shape=(SHAPE((t, FF), BF), SHAPE((1, FF), F32)),
        grid_spec=pltpu.PrefetchScalarGridSpec(
            num_scalar_prefetch=1, grid=(FF // tile,),
            in_specs=[
                pl.BlockSpec((t, D // 2), lambda j, c: (0, c[0])),
                pl.BlockSpec((t, D // 2), lambda j, c: (0, 1 - c[0])),
                part, part, wide,
            ],
            out_specs=(wide, pl.BlockSpec((1, tile), lambda j, c: (0, j))),
        ),
        cost_estimate=cost(2 * t * D * FF, 2 * (t * D + D * FF + 2 * t * FF)),
        name="down_back",
    )(core.reshape(1), dm, dm, own, came, slope)


def hidden_kernel(core_ref, left_ref, right_ref, own_ref, came_ref, dr_ref, n_ref, q_ref, wo_ref, rows_ref, r_ref, a_ref, c_ref, sums_ref):
    grad = dr_ref[...] + dot(left_ref[...], own_ref[...], 1, 1) + dot(right_ref[...], came_ref[...], 1, 1)
    normed = n_ref[...]
    back = norm_back(grad, normed, q_ref[...], rows_ref[0:1, :])
    low = back.astype(BF)
    r_ref[...] = back
    a_ref[...] = low
    c_ref[...] = dot(low, wo_ref[...], 1, 1).astype(BF)

    @pl.when(pl.program_id(0) == 0)
    def _():
        sums_ref[...] = jnp.zeros_like(sums_ref)

    sums_ref[0:1, :] += row_sum(grad * normed)
    sums_ref[1:2, :] += row_sum(grad)
    sums_ref[2:3, :] += row_sum(low.astype(F32))


def hidden_call(dz, own, came, dr, normed, inv, w_out, rows, core):
    t = dz.shape[0]
    tile = pl.BlockSpec((256, D), lambda i, c: (i, 0))
    return pl.pallas_call(
        hidden_kernel,
        out_shape=(SHAPE((t, D), F32), SHAPE((t, D), BF), SHAPE((t, D), BF), SHAPE((8, D), F32)),
        grid_spec=pltpu.PrefetchScalarGridSpec(
            num_scalar_prefetch=1, grid=(t // 256,),
            in_specs=[
                pl.BlockSpec((256, FF // 2), lambda i, c: (i, c[0])),
                pl.BlockSpec((256, FF // 2), lambda i, c: (i, 1 - c[0])),
                full_spec((D, FF // 2)), full_spec((D, FF // 2)), tile, tile,
                pl.BlockSpec((256, 1), lambda i, c: (i, 0)), full_spec((D, D)), full_spec(rows.shape),
            ],
            out_specs=(tile, tile, tile, pl.BlockSpec((8, D), lambda i, c: (0, 0))),
        ),
        cost_estimate=cost(2 * t * D * (FF + D), 2 * (t * FF + D * FF) + 16 * t * D),
        name="up_back_norm",
    )(core.reshape(1), dz, dz, own, came, dr, normed, inv, w_out, rows)


def input_kernel(a_ref, b_ref, w_ref, r_ref, o_ref):
    half = a_ref.shape[1]
    value = dot(a_ref[...], w_ref[:, :half], 1, 1) + dot(b_ref[...], w_ref[:, half:], 1, 1)
    o_ref[...] = (r_ref[...] + value).astype(BF)


def input_call(part_a, part_b, w_qkv, resid):
    t, width = part_a.shape
    tile = pl.BlockSpec((256, D), lambda i: (i, 0))
    wide = pl.BlockSpec((256, width), lambda i: (i, 0))
    return pl.pallas_call(
        input_kernel,
        out_shape=SHAPE((t, D), BF),
        grid=(t // 256,),
        in_specs=[wide, wide, full_spec(w_qkv.shape), tile],
        out_specs=tile,
        cost_estimate=cost(4 * t * D * width, 4 * (t * width + D * width) + 6 * t * D),
        name="input_back",
    )(part_a, part_b, w_qkv, resid)


def weight_kernel(half_ref, left_ref, right_ref, *refs):
    o_ref, turned = refs[-2], refs[-1]

    @pl.when(pl.program_id(1) == 0)
    def _():
        turned[...] = left_ref[...].T

    value = dot(turned[...], right_ref[...], 1, 0)
    if len(refs) == 3:
        value = value + refs[0][...].astype(F32)
    o_ref[...] = value.astype(BF)


def weight_call(left, right, half, came=None):
    t, rows = left.shape
    width = right.shape[1]
    bm = 512
    bn = 1024 if width == 1024 else 512
    steps = rows // 2 // bm
    specs = [
        pl.BlockSpec((t, bm), lambda i, j, h: (0, h[0] * steps + i)),
        pl.BlockSpec((t, bn), lambda i, j, h: (0, j)),
    ]
    values = [left, right]
    out = pl.BlockSpec((bm, bn), lambda i, j, h: (i, j))
    if came is not None:
        specs.append(out)
        values.append(came)
    return pl.pallas_call(
        weight_kernel,
        out_shape=SHAPE((rows // 2, width), BF),
        grid_spec=pltpu.PrefetchScalarGridSpec(
            num_scalar_prefetch=1, grid=(steps, width // bn), in_specs=specs, out_specs=out,
            scratch_shapes=[pltpu.VMEM((bm, t), BF)],
        ),
        cost_estimate=cost(t * rows * width, t * rows + 2 * t * width + 2 * rows * width),
        name="weight_grad",
    )(half.reshape(1), *values)


def inner_kernel(rate, decay, w_ref, g_ref, m_ref, v_ref, m_out, v_out, d_out):
    weight = w_ref[...]
    new, m_out[...], v_out[...] = inner_step(
        weight, g_ref[...].astype(F32), m_ref[...], v_ref[...], rate, decay
    )
    d_out[...] = (weight - new).astype(BF)


def inner_call(weight, grad, first, second, rate, decay):
    rows, width = weight.shape
    block = 32 * 4096 // width
    tile = pl.BlockSpec((block, width), lambda i: (i, 0))
    like = SHAPE((rows, width), F32)
    return pl.pallas_call(
        partial(inner_kernel, rate, decay),
        out_shape=(like, like, SHAPE((rows, width), BF)),
        grid=(rows // block,),
        in_specs=[tile] * 4,
        out_specs=(tile,) * 3,
        cost_estimate=cost(20 * rows * width, 24 * rows * width),
        name="inner_step",
    )(weight, grad, first, second)


def outer_kernel(core_ref, w_ref, u_ref, own_ref, came_ref, o_ref, c_ref):
    mine = (core_ref[0] == pl.program_id(0)).astype(F32)
    total = own_ref[...].astype(F32) * mine + came_ref[...].astype(F32) * (1.0 - mine)
    mean = total * 0.25
    weight = w_ref[...]
    momentum = 0.5 * u_ref[...] + mean
    new = weight - 0.7 * (mean + 0.5 * momentum)
    o_ref[0] = mean
    o_ref[1] = momentum
    o_ref[2] = new
    c_ref[...] = new.astype(BF)


def outer_call(weight, momentum, own, came, core):
    rows, width = weight.shape
    block = 32 * 4096 // width
    steps = rows // 2 // block
    tile = pl.BlockSpec((block, width), lambda h, i, c: (h * steps + i, 0))
    part = pl.BlockSpec((block, width), lambda h, i, c: (i, 0))
    return pl.pallas_call(
        outer_kernel,
        out_shape=(SHAPE((3, rows, width), F32), SHAPE((rows, width), BF)),
        grid_spec=pltpu.PrefetchScalarGridSpec(
            num_scalar_prefetch=1, grid=(2, steps), in_specs=[tile, tile, part, part],
            out_specs=(pl.BlockSpec((3, block, width), lambda h, i, c: (0, h * steps + i, 0)), tile),
        ),
        cost_estimate=cost(10 * rows * width, 26 * rows * width),
        name="outer_step",
    )(core.reshape(1), weight, momentum, own, came)


def erf_parts(value):
    size = jnp.abs(value) * 0.7071067811865476
    share = 1.0 / (1.0 + 0.5 * size)
    inner = 0.17087277
    for coefficient in (
        -0.82215223, 1.48851587, -1.13520398, 0.27886807, -0.18628806, 0.09678418, 0.37409196, 1.00002368
    ):
        inner = coefficient + share * inner
    square = size * size
    half = 0.5 * share * jnp.exp(share * inner - 1.26551223 - square)
    return jnp.where(value >= 0, 1.0 - half, half), jnp.exp(-square)


def xor_pairs(bits):
    place = {"y": 0, "z0": 1, "z1": 2, "c": 3, "x": 4}
    flip = sum(1 << place[bit] for bit in bits)
    pairs = []
    for device in range(32):
        if bits == ("c", "z1") and ((device >> 3) & 1) == ((device >> 2) & 1):
            continue
        pairs.append((device, device ^ flip))
    return pairs


def exchange(value, *bits):
    return lax.ppermute(value, ("rep", "fsdp"), xor_pairs(bits))


def swap(at, value):
    return jnp.where(at["c"] != at["z1"], exchange(value, "c", "z1"), value)


def add_low(left, right):
    return (left.astype(jnp.float32) + right.astype(jnp.float32)).astype(jnp.bfloat16)


def pick(value, index, axis):
    return lax.dynamic_index_in_dim(value, index, axis, keepdims=False)


def half_axis(total, which):
    return 1 if which == "y" and total.ndim == 4 else 0


def halve(at, total, which):
    away = pick(total, 1 - at[which], half_axis(total, which))
    return away, exchange(away, which)


def join(at, total, came, which, *gates):
    return add_low(pick(total, at[which], half_axis(total, which)), after(came, *gates))


def slabs(total):
    return total.reshape(2, 2, -1, total.shape[-1])


def after(value, *earlier):
    return lax.optimization_barrier((value,) + earlier)[0]


def weave(value):
    rows = value.shape[1]
    return jnp.transpose(value.reshape(3, rows, D // 128, 128), (1, 2, 0, 3)).reshape(rows, 3 * D)


def unweave(value):
    rows = value.shape[0]
    return jnp.transpose(value.reshape(rows, D // 128, 3, 128), (2, 0, 1, 3)).reshape(3, rows, D)


def per_device_fast(
    tokens,
    cotangent,
    segment_ids,
    attention_weight,
    attention_momentum,
    attention_first,
    attention_second,
    expand_weight,
    expand_momentum,
    expand_first,
    expand_second,
    contract_weight,
    contract_momentum,
    contract_first,
    contract_second,
    vectors,
    vectors_momentum,
    vectors_first,
    vectors_second,
):
    bf, f32 = jnp.bfloat16, jnp.float32
    at = bits_of()
    core = at["c"].astype(jnp.int32)
    def swapped(value, came):
        return jnp.where(at["c"] != at["z1"], came, value)

    def cross(value):
        return exchange(value, "c", "z1")

    def half_of(weight):
        part = weight.shape[1] // 2
        return lax.dynamic_slice_in_dim(weight, core * part, part, axis=1).astype(bf)

    in_own = lax.all_gather(half_of(expand_weight), "fsdp", axis=0, tiled=True)
    down_own = lax.all_gather(half_of(contract_weight), "fsdp", axis=0, tiled=True)
    attn_low = attention_weight.astype(bf)
    w_qkv, w_out, vector_full, tok, seg = gather_all(
        weave(attn_low[:3]), attn_low[3], vectors.astype(bf), tokens, segment_ids,
    )
    cot_came = cross(after(cotangent, w_qkv))
    rows = jnp.swapaxes(vector_full, 0, 1).reshape(-1, D).astype(f32)
    bias_up = rows[8:].reshape(1, FF)
    bias_qkv = weave(jnp.stack([rows[4], jnp.zeros_like(rows[4]), rows[5]])[:, None])
    scale_qkv = weave(jnp.stack([jnp.full((1, D), 0.125, f32)] + [jnp.ones((1, D), f32)] * 2))
    qkv = qkv_call(tok, w_qkv, bias_qkv, scale_qkv)
    mixed, log_sum = attn_fwd(qkv, seg)
    in_other = exchange(after(in_own, mixed), "c")
    normed, inv, hidden_low = mix_call(mixed, w_out, tok, rows)
    down_other = exchange(after(down_own, hidden_low), "c")
    activated, slope = up_call(hidden_low, in_own, in_other, bias_up, core)
    cot = swapped(cotangent, after(cot_came, activated))
    layer_output, grad_sum, grad_branch, sums_two = down_call(
        activated, down_own, down_other, normed, cot, rows, core
    )
    output_came = cross(layer_output)
    down_send = weight_call(activated, grad_branch, 1 - core)
    grad_pre, sums_up = slope_call(after(grad_branch, down_send), down_own, down_other, slope, core)
    down_came = exchange(down_send, "c")
    up_send = weight_call(hidden_low, grad_pre, 1 - core)
    down_total = slabs(weight_call(activated, after(grad_branch, up_send), core, down_came))
    up_came = exchange(up_send, "c")
    away_d, came_d = halve(at, down_total, "y")
    up_total = slabs(weight_call(hidden_low, after(grad_pre, away_d), core, up_came))
    away_u, came_u = halve(at, up_total, "z0")
    grad_resid, grad_attn, grad_mixed, sums_one = hidden_call(
        after(grad_pre, away_u), in_own, in_other, grad_sum, normed, inv, w_out, rows, core
    )
    proj_send = weight_call(mixed, grad_attn, 1 - core)
    proj_came = exchange(proj_send, "c")
    output = swapped(layer_output, after(output_came, proj_send))
    grad_a, sums_a = attn_bwd(qkv, after(grad_mixed, proj_send, output), log_sum, seg, 0)
    send_a = weight_call(tok, grad_a, 1 - core)
    came_a = exchange(send_a, "c")
    down_one = join(at, down_total, came_d, "y", send_a)
    away_d, came_d = halve(at, down_one, "z0")
    up_one = join(at, up_total, came_u, "z0", away_d)
    away_u, came_u = halve(at, up_one, "y")
    proj_total = slabs(weight_call(mixed, after(grad_attn, away_u), core, proj_came))
    away_p, came_p = halve(at, proj_total, "y")
    total_a = slabs(weight_call(tok, after(grad_a, away_p), core, came_a))
    away_a, came_one = halve(at, total_a, "z0")
    grad_b, sums_b = attn_bwd(qkv, after(grad_mixed, away_a), log_sum, seg, 1)
    send_b = weight_call(tok, grad_b, 1 - core)
    came_b = exchange(send_b, "c")
    down_two = join(at, down_one, came_d, "z0", send_b)
    cross_d = cross(down_two)
    up_two = join(at, up_one, came_u, "y", down_two)
    cross_u = cross(up_two)
    proj_one = join(at, proj_total, came_p, "y", up_two)
    away_p, came_p = halve(at, proj_one, "z0")
    a_one = join(at, total_a, came_one, "z0", away_p)
    away_a, came_a = halve(at, a_one, "y")
    total_b = slabs(weight_call(tok, after(grad_b, away_a), core, came_b))
    away_b, came_b = halve(at, total_b, "y")
    sums_qkv = jnp.concatenate([sums_a, sums_b], axis=0).reshape(D // 128, 3, 128)
    vector_grad = jnp.concatenate(
        [
            sums_one[0:1],
            sums_two[0:1],
            sums_one[1:2],
            sums_two[1:2],
            sums_qkv[:, 0].reshape(1, D),
            sums_qkv[:, 2].reshape(1, D),
            sums_one[2:3],
            sums_two[2:3],
            sums_up.reshape(FF // D, D),
        ],
        axis=0,
    )

    def vector_send(parts, which):
        half = parts.shape[1] // 2
        away = lax.dynamic_slice_in_dim(parts, (1 - at[which]) * half, half, axis=1)
        return exchange(away, which)

    def vector_join(parts, came, which, *gates):
        half = parts.shape[1] // 2
        return lax.dynamic_slice_in_dim(parts, at[which] * half, half, axis=1) + after(came, *gates)

    vec_came = vector_send(vector_grad, "c")
    input_grad = input_call(after(grad_a, away_b), grad_b, w_qkv, grad_resid)
    vec_one = vector_join(vector_grad, vec_came, "c", input_grad)
    vec_came = vector_send(vec_one, "z0")
    proj_two = join(at, proj_one, came_p, "z0", input_grad)
    a_two = join(at, a_one, came_a, "y", input_grad)
    cross_pa = cross(jnp.concatenate([proj_two, a_two], axis=1))
    b_one = join(at, total_b, came_b, "y", proj_two, a_two)
    away_b, came_b = halve(at, b_one, "z0")

    def inner(weight, grad, first, second, rate, decay):
        flat = (-1, weight.shape[-1])
        return inner_call(
            weight.reshape(flat), grad.reshape(flat), first.reshape(flat), second.reshape(flat), rate, decay
        )

    def rep_send(diff):
        halves = diff.reshape(2, diff.shape[0] // 2, diff.shape[1])
        away = pick(halves, 1 - at["c"], 0)
        return away, exchange(away, "c")

    def rep_join(diff, came, *gates):
        halves = diff.reshape(2, diff.shape[0] // 2, diff.shape[1])
        return add_low(pick(halves, at["c"], 0), after(came, *gates))

    vec_two = vector_join(vec_one, vec_came, "z0", away_b)
    vec_came = vector_send(vec_two, "y")
    grad_contract = swapped(down_two, after(cross_d, away_b))
    contract_new = inner(contract_weight, grad_contract, contract_first, contract_second, 0.015, 0.1)
    sent_c, came_c = rep_send(contract_new[2])
    b_two = join(at, b_one, came_b, "z0", sent_c)
    cross_b = cross(b_two)
    input_came = cross(after(input_grad, b_two))
    grad_expand = swapped(up_two, after(cross_u, b_two))
    expand_new = inner(expand_weight, grad_expand, expand_first, expand_second, 0.03, 0.1)
    sent_e, came_e = rep_send(expand_new[2])
    half_c = rep_join(contract_new[2], came_c, sent_e)
    rest_c = exchange(half_c, "x")
    vec_three = vector_join(vec_two, vec_came, "y", half_c)
    vec_cross = cross(vec_three)
    half_e = rep_join(expand_new[2], came_e, half_c)
    rest_e = exchange(half_e, "x")
    pa = swapped(jnp.concatenate([proj_two, a_two], axis=1), after(cross_pa, half_e))
    b_own = swapped(b_two, after(cross_b, half_e))
    grad_qkv = jnp.concatenate([pa[:, D:], b_own], axis=1)
    grad_attention = jnp.concatenate([unweave(grad_qkv), pa[None, :, :D]], axis=0)
    attention_new = inner(attention_weight, grad_attention, attention_first, attention_second, 0.03, 0.1)
    sent_a, came_a = rep_send(attention_new[2])
    grad_vectors = swapped(vec_three, after(vec_cross, sent_a))
    inner_new, first_new, second_new = inner_step(
        vectors, grad_vectors, vectors_first[0], vectors_second[0], 0.2, 0.0
    )
    vec_diff = (vectors - inner_new).astype(bf)
    vec_near = exchange(vec_diff, "c")
    full_c = add_low(half_c, after(rest_c, sent_a))
    back_c = exchange(full_c, "c")
    half_a = rep_join(attention_new[2], came_a, full_c)
    rest_a = exchange(half_a, "x")
    full_e = add_low(half_e, after(rest_e, half_a))
    back_e = exchange(full_e, "c")
    vec_half = add_low(vec_diff, after(vec_near, full_e))
    vec_far = exchange(vec_half, "x")

    def outer(weight, momentum, own, came):
        flat = (-1, weight.shape[-1])
        return outer_call(weight.reshape(flat), momentum.reshape(flat), own, came, core)

    outer_c = outer(contract_weight, contract_momentum, after(full_c, vec_half), back_c)
    full_a = add_low(half_a, after(rest_a, outer_c[1]))
    back_a = exchange(full_a, "c")
    outer_e = outer(expand_weight, expand_momentum, after(full_e, full_a), back_e)
    mean_diff = add_low(vec_half, after(vec_far, outer_e[1])).astype(f32) / 4
    momentum_new = 0.5 * vectors_momentum + mean_diff
    outer_new = vectors - 0.7 * (mean_diff + 0.5 * momentum_new)
    outer_a = outer(attention_weight, attention_momentum, after(full_a, outer_e[1]), back_a)
    input_grad = swapped(input_grad, after(input_came, outer_e[1]))
    results = []
    for weight, first, new, (total, copy) in (
        (attention_weight, attention_first, attention_new, outer_a),
        (expand_weight, expand_first, expand_new, outer_e),
        (contract_weight, contract_first, contract_new, outer_c),
    ):
        results += [
            new[0].reshape(first.shape),
            new[1].reshape(first.shape),
            total.reshape((3,) + weight.shape),
            copy.reshape(weight.shape),
        ]
    results += [
        first_new[None],
        second_new[None],
        jnp.stack([mean_diff, momentum_new, outer_new]),
        outer_new.astype(bf),
    ]
    return (output, input_grad) + tuple(results)


def solution(mesh):
    placed = (
        P(("rep", "fsdp"), None),
        P(("rep", "fsdp"), None),
        P(("rep", "fsdp"), None),
        P(None, "fsdp", None),
        P(None, "fsdp", None),
        P("rep", None, "fsdp", None),
        P("rep", None, "fsdp", None),
        P("fsdp", None),
        P("fsdp", None),
        P("rep", "fsdp", None),
        P("rep", "fsdp", None),
        P("fsdp", None),
        P("fsdp", None),
        P("rep", "fsdp", None),
        P("rep", "fsdp", None),
        P(None, "fsdp"),
        P(None, "fsdp"),
        P("rep", None, "fsdp"),
        P("rep", None, "fsdp"),
    )
    small = mesh.shape["rep"] == 4 and mesh.shape["fsdp"] == 8
    body = per_device_fast if small else per_device
    return jax.shard_map(
        body,
        mesh=mesh,
        in_specs=placed,
        out_specs=(
            P(("rep", "fsdp"), None),
            P(("rep", "fsdp"), None),
            P("rep", None, "fsdp", None),
            P("rep", None, "fsdp", None),
            P(None, None, "fsdp", None),
            P(None, "fsdp", None),
            P("rep", "fsdp", None),
            P("rep", "fsdp", None),
            P(None, "fsdp", None),
            P("fsdp", None),
            P("rep", "fsdp", None),
            P("rep", "fsdp", None),
            P(None, "fsdp", None),
            P("fsdp", None),
            P("rep", None, "fsdp"),
            P("rep", None, "fsdp"),
            P(None, None, "fsdp"),
            P(None, "fsdp"),
        ),
        check_vma=False,
    )
```

```python
from functools import partial

import jax
import jax.numpy as jnp
from jax import lax
from jax.experimental import pallas as pl
from jax.experimental.pallas import tpu as pltpu
from jax.sharding import PartitionSpec as P

D = 1024
H = 16
HD = 64
FF = 4096
LEN = 1024
SEQ_DEV = 1
ADAM_STEP = 4
TOK_DEV = 1024


def norm_forward(values_in, gain_row, shift_row):
    center = values_in - jnp.mean(values_in, axis=-1, keepdims=True)
    inv_scale = lax.rsqrt(jnp.mean(center * center, axis=-1, keepdims=True) + 1e-05)
    normed = center * inv_scale
    return (normed * gain_row + shift_row, normed, inv_scale)


def norm_backward(grad_out, normed, inv_scale, gain_row):
    grad_gain = jnp.sum(grad_out * normed, axis=0)
    grad_shift = jnp.sum(grad_out, axis=0)
    scaled_grad = grad_out * gain_row
    grad_value = inv_scale * (
        scaled_grad
        - jnp.mean(scaled_grad, axis=-1, keepdims=True)
        - normed * jnp.mean(scaled_grad * normed, axis=-1, keepdims=True)
    )
    return (grad_value, grad_gain, grad_shift)


def product_over(left, right):
    return lax.dot_general(
        left, right, (((0,), (0,)), ((), ())), preferred_element_type=jnp.float32
    )


def product_back(left, right):
    return lax.dot_general(
        left, right, (((1,), (1,)), ((), ())), preferred_element_type=jnp.float32
    )


def block_scores(query_block, key_block, row_segments, all_segments):
    scores = jnp.einsum("qhd,khd->hqk", query_block, key_block, preferred_element_type=jnp.float32)
    same_doc = row_segments[:, None] == all_segments[None, :]
    return jnp.where(same_doc[None], scores, -1e30)


def inner_step(weight, gradient, first_moment, second_moment, learn_rate, weight_decay):
    first_new = 0.5 * first_moment + 0.5 * gradient
    second_new = 0.75 * second_moment + 0.25 * gradient * gradient
    update_dir = (
        first_new
        / (1.0 - 0.5**ADAM_STEP)
        / (jnp.sqrt(second_new / (1.0 - 0.75**ADAM_STEP)) + 1e-08)
    )
    return (weight - learn_rate * (update_dir + weight_decay * weight), first_new, second_new)


def per_device(
    tokens,
    cotangent,
    segment_ids,
    attention_weight,
    attention_momentum,
    attention_first,
    attention_second,
    expand_weight,
    expand_momentum,
    expand_first,
    expand_second,
    contract_weight,
    contract_momentum,
    contract_first,
    contract_second,
    vectors,
    vectors_momentum,
    vectors_first,
    vectors_second,
):
    attn_full, vector_full = (
        lax.all_gather(attention_weight.astype(jnp.bfloat16), "fsdp", axis=1, tiled=True),
        lax.all_gather(vectors.astype(jnp.bfloat16), "fsdp", axis=1, tiled=True),
    )
    vector_rows = vector_full.astype(jnp.float32)
    gain_one, gain_two, shift_one, shift_two = (
        vector_rows[0],
        vector_rows[1],
        vector_rows[2],
        vector_rows[3],
    )
    bias_query, bias_value, bias_mixed, bias_down = (
        vector_rows[4],
        vector_rows[5],
        vector_rows[6],
        vector_rows[7],
    )
    bias_up = vector_rows[8:].reshape(FF)
    projected = jnp.einsum("td,nde->nte", tokens, attn_full[:3], preferred_element_type=jnp.float32)
    query_all = ((projected[0] + bias_query) * 0.125).astype(jnp.bfloat16)
    key_all = projected[1].astype(jnp.bfloat16)
    value_all = (projected[2] + bias_value).astype(jnp.bfloat16)
    query_heads = query_all.reshape(SEQ_DEV, LEN, H, HD)
    key_heads = key_all.reshape(SEQ_DEV, LEN, H, HD)
    value_heads = value_all.reshape(SEQ_DEV, LEN, H, HD)
    block_rows = min(512, LEN)
    head_group = min(8, H)
    context_rows = []
    log_sums = []
    seq_index = 0
    for row_start in range(0, LEN, block_rows):
        block_pieces = []
        for head_start in range(0, H, head_group):
            head_part = slice(head_start, head_start + head_group)
            scores = block_scores(
                query_heads[seq_index, row_start : row_start + block_rows, head_part],
                key_heads[seq_index, :, head_part],
                segment_ids[seq_index, row_start : row_start + block_rows],
                segment_ids[seq_index],
            )
            row_max = jnp.max(scores, axis=-1, keepdims=True)
            exp_score = jnp.exp(scores - row_max)
            row_total = jnp.sum(exp_score, axis=-1, keepdims=True)
            probability = (exp_score / row_total).astype(jnp.bfloat16)
            block_pieces.append(
                jnp.einsum(
                    "hqk,khd->qhd",
                    probability,
                    value_heads[seq_index, :, head_part],
                    preferred_element_type=jnp.float32,
                )
            )
            log_sums.append(row_max + jnp.log(row_total))
        context_rows.append(jnp.concatenate(block_pieces, axis=1))
    mixed = jnp.concatenate(context_rows, axis=0).reshape(TOK_DEV, D).astype(jnp.bfloat16)
    attn_out = jnp.dot(mixed, attn_full[3], preferred_element_type=jnp.float32) + bias_mixed
    hidden, normed_one, scale_one = norm_forward(
        tokens.astype(jnp.float32) + attn_out, gain_one, shift_one
    )
    hidden_low = hidden.astype(jnp.bfloat16)
    ffn_expand, ffn_contract = (
        lax.all_gather(expand_weight.astype(jnp.bfloat16), "fsdp", axis=0, tiled=True),
        lax.all_gather(contract_weight.astype(jnp.bfloat16), "fsdp", axis=0, tiled=True),
    )
    pre_act = jnp.dot(hidden_low, ffn_expand, preferred_element_type=jnp.float32) + bias_up
    activated = jax.nn.gelu(pre_act, approximate=False).astype(jnp.bfloat16)
    branch = jnp.dot(activated, ffn_contract, preferred_element_type=jnp.float32) + bias_down
    layer_output, normed_two, scale_two = norm_forward(hidden + branch, gain_two, shift_two)
    grad_sum, grad_gain_two, grad_shift_two = norm_backward(
        cotangent.astype(jnp.float32), normed_two, scale_two, gain_two
    )
    grad_branch = grad_sum.astype(jnp.bfloat16)
    grad_act = product_back(grad_branch, ffn_contract)
    unused_value, gelu_pull = jax.vjp(partial(jax.nn.gelu, approximate=False), pre_act)
    grad_pre_low = gelu_pull(grad_act)[0].astype(jnp.bfloat16)
    grad_hidden = grad_sum + product_back(grad_pre_low, ffn_expand)
    contract_full = product_over(activated, grad_branch)
    expand_full = product_over(hidden_low, grad_pre_low)
    grad_expand, grad_contract = (
        lax.psum_scatter(expand_full, "fsdp", scatter_dimension=0, tiled=True),
        lax.psum_scatter(contract_full, "fsdp", scatter_dimension=0, tiled=True),
    )
    grad_resid, grad_gain_one, grad_shift_one = norm_backward(
        grad_hidden, normed_one, scale_one, gain_one
    )
    grad_attn_out = grad_resid.astype(jnp.bfloat16)
    grad_bias_mixed = jnp.sum(grad_attn_out.astype(jnp.float32), axis=0)
    grad_output_proj = product_over(mixed, grad_attn_out)
    grad_mixed = product_back(grad_attn_out, attn_full[3]).astype(jnp.bfloat16)
    grad_context = grad_mixed.reshape(SEQ_DEV, LEN, H, HD)
    query_grads = []
    lse_index = 0
    seq_index = 0
    key_totals = [
        jnp.zeros((LEN, head_group, HD), jnp.float32) for head_start in range(0, H, head_group)
    ]
    value_totals = [
        jnp.zeros((LEN, head_group, HD), jnp.float32) for head_start in range(0, H, head_group)
    ]
    for row_start in range(0, LEN, block_rows):
        block_pieces = []
        for group_index, head_start in enumerate(range(0, H, head_group)):
            head_part = slice(head_start, head_start + head_group)
            query_block = query_heads[seq_index, row_start : row_start + block_rows, head_part]
            key_block = key_heads[seq_index, :, head_part]
            value_block = value_heads[seq_index, :, head_part]
            ctx_grad = grad_context[seq_index, row_start : row_start + block_rows, head_part]
            scores = block_scores(
                query_block,
                key_block,
                segment_ids[seq_index, row_start : row_start + block_rows],
                segment_ids[seq_index],
            )
            probability = jnp.exp(scores - log_sums[lse_index])
            lse_index = lse_index + 1
            value_totals[group_index] = value_totals[group_index] + jnp.einsum(
                "hqk,qhd->khd",
                probability.astype(jnp.bfloat16),
                ctx_grad,
                preferred_element_type=jnp.float32,
            )
            prob_grad = jnp.einsum(
                "qhd,khd->hqk", ctx_grad, value_block, preferred_element_type=jnp.float32
            )
            row_dot = jnp.sum(probability * prob_grad, axis=-1, keepdims=True)
            score_grad = (probability * (prob_grad - row_dot)).astype(jnp.bfloat16)
            block_pieces.append(
                jnp.einsum(
                    "hqk,khd->qhd", score_grad, key_block, preferred_element_type=jnp.float32
                ).astype(jnp.bfloat16)
            )
            key_totals[group_index] = key_totals[group_index] + jnp.einsum(
                "hqk,qhd->khd", score_grad, query_block, preferred_element_type=jnp.float32
            )
        query_grads.append(jnp.concatenate(block_pieces, axis=1))
    key_grads = jnp.concatenate(
        [key_total.astype(jnp.bfloat16) for key_total in key_totals], axis=1
    )
    value_grads = jnp.concatenate(
        [value_total.astype(jnp.bfloat16) for value_total in value_totals], axis=1
    )
    grad_query = jnp.concatenate(query_grads, axis=0).reshape(TOK_DEV, D) * 0.125
    grad_keys = key_grads.reshape(TOK_DEV, D)
    grad_values = value_grads.reshape(TOK_DEV, D)
    stacked_grads = jnp.stack([grad_query, grad_keys, grad_values])
    grad_qkv = jnp.einsum("td,nte->nde", tokens, stacked_grads, preferred_element_type=jnp.float32)
    input_grad = (
        grad_resid
        + jnp.einsum(
            "nte,nde->td", stacked_grads, attn_full[:3], preferred_element_type=jnp.float32
        )
    ).astype(jnp.bfloat16)
    grad_attention_full = jnp.concatenate([grad_qkv, grad_output_proj[None]], axis=0)
    vector_head = jnp.stack(
        [
            grad_gain_one,
            grad_gain_two,
            grad_shift_one,
            grad_shift_two,
            jnp.sum(grad_query.astype(jnp.float32), axis=0),
            jnp.sum(grad_values.astype(jnp.float32), axis=0),
            grad_bias_mixed,
            jnp.sum(grad_branch.astype(jnp.float32), axis=0),
        ]
    )
    grad_bias_up = jnp.sum(grad_pre_low.astype(jnp.float32), axis=0).reshape(FF // D, D)
    grad_vectors_full = jnp.concatenate([vector_head, grad_bias_up], axis=0)
    grad_attention, grad_vectors = (
        lax.psum_scatter(grad_attention_full, "fsdp", scatter_dimension=1, tiled=True),
        lax.psum_scatter(grad_vectors_full, "fsdp", scatter_dimension=1, tiled=True),
    )
    attention_new = inner_step(
        attention_weight, grad_attention, attention_first[0], attention_second[0], 0.03, 0.1
    )
    expand_new = inner_step(
        expand_weight, grad_expand, expand_first[0], expand_second[0], 0.03, 0.1
    )
    contract_new = inner_step(
        contract_weight, grad_contract, contract_first[0], contract_second[0], 0.015, 0.1
    )
    vectors_new = inner_step(vectors, grad_vectors, vectors_first[0], vectors_second[0], 0.2, 0.0)
    summed = (
        lax.psum((attention_weight - attention_new[0]).astype(jnp.bfloat16), "rep").astype(
            jnp.float32
        ),
        lax.psum((expand_weight - expand_new[0]).astype(jnp.bfloat16), "rep").astype(jnp.float32),
        lax.psum((contract_weight - contract_new[0]).astype(jnp.bfloat16), "rep").astype(
            jnp.float32
        ),
        lax.psum((vectors - vectors_new[0]).astype(jnp.bfloat16), "rep").astype(jnp.float32),
    )
    groups_count = lax.axis_size("rep")
    results = []
    for weight_now, momentum_now, inner_new, diff_total in zip(
        (attention_weight, expand_weight, contract_weight, vectors),
        (attention_momentum, expand_momentum, contract_momentum, vectors_momentum),
        (attention_new, expand_new, contract_new, vectors_new),
        summed,
    ):
        mean_diff = diff_total / groups_count
        momentum_new = 0.5 * momentum_now + mean_diff
        outer_new = weight_now - 0.7 * (mean_diff + 0.5 * momentum_new)
        results.append(
            (
                inner_new[1][None],
                inner_new[2][None],
                jnp.stack([mean_diff, momentum_new, outer_new]),
                outer_new.astype(jnp.bfloat16),
            )
        )
    return (
        layer_output.astype(jnp.bfloat16),
        input_grad,
        results[0][0],
        results[0][1],
        results[0][2],
        results[0][3],
        results[1][0],
        results[1][1],
        results[1][2],
        results[1][3],
        results[2][0],
        results[2][1],
        results[2][2],
        results[2][3],
        results[3][0],
        results[3][1],
        results[3][2],
        results[3][3],
    )


NEG=-1e30
QB=256
def attn_windows(seg_row):
    length = seg_row.shape[0]
    nb = length // QB
    firsts = seg_row[::QB]
    lasts = seg_row[QB-1::QB]
    begin = jnp.sum((seg_row[None, :] < firsts[:, None]).astype(jnp.int32), axis=1)
    end = jnp.sum((seg_row[None, :] <= lasts[:, None]).astype(jnp.int32), axis=1)
    start = begin // 128
    count = (end - start * 128 + QB - 1) // QB
    start = jnp.minimum(start, (length - count * QB) // 128)
    return start.astype(jnp.int32), count.astype(jnp.int32)
def lane_half(shape, h):
    lane = lax.broadcasted_iota(jnp.int32, shape, len(shape)-1)
    return (lane < 64) if h == 0 else (lane >= 64)
def dot(a, b, ca, cb):
    return lax.dot_general(a, b, (((ca,), (cb,)), ((), ())), preferred_element_type=jnp.float32)
def fold(value, join):
    part = value.shape[0] // 8
    parts = [value[i * part:(i + 1) * part] for i in range(8)]
    while len(parts) > 1:
        parts = [join(a, b) for a, b in zip(parts[::2], parts[1::2])]
    return parts[0]
def fwd_kernel(start_ref, count_ref, qkv_ref, segr_ref, segc_ref, o_ref, lse_ref, vt_ref):
    length = qkv_ref.shape[0]
    vt_ref[...] = qkv_ref[:, 256:384].T
    nb = length // QB
    for i in range(nb):
        rows = slice(i*QB, (i+1)*QB)
        for nn in range(1, nb+1):
            @pl.when(count_ref[i] == nn)
            def _():
                nk = nn*QB
                lo = pl.multiple_of(start_ref[i]*128, 128)
                kw = qkv_ref[pl.ds(lo, nk), 128:256]
                qb = qkv_ref[rows, 0:128]
                same = segc_ref[pl.ds(lo, nk), :] == segr_ref[:, rows]
                outs = []
                for h in range(2):
                    qh = jnp.where(lane_half(qb.shape, h), qb, jnp.zeros_like(qb))
                    st = jnp.where(same, dot(kw, qh, 1, 1), NEG)
                    m = jnp.max(fold(st, jnp.maximum), axis=0, keepdims=True)
                    p = jnp.exp(st - m)
                    l = jnp.sum(fold(p, jnp.add), axis=0, keepdims=True)
                    weighted = dot(vt_ref[h*64:(h+1)*64, pl.ds(lo, nk)], p.astype(jnp.bfloat16), 1, 0)
                    outs.append(weighted * (1.0 / l))
                    lse_ref[0, h:h+1, rows] = m + jnp.log(l)
                o_ref[rows, :] = jnp.concatenate(outs, axis=0).T.astype(jnp.bfloat16)
def bwd_kernel(start_ref, count_ref, qkv_ref, do_ref, lse_ref, segr_ref, segc_ref, d_ref, sums_ref, dk_acc, dv_acc, kt_ref):
    length = qkv_ref.shape[0]
    kt_ref[...] = qkv_ref[:, 128:256].T
    nb = length // QB
    dk_acc[...] = jnp.zeros_like(dk_acc)
    dv_acc[...] = jnp.zeros_like(dv_acc)
    for i in range(nb):
        rows = slice(i*QB, (i+1)*QB)
        for nn in range(1, nb+1):
            @pl.when(count_ref[i] == nn)
            def _():
                nk = nn*QB
                lo = pl.multiple_of(start_ref[i]*128, 128)
                win = pl.ds(lo, nk)
                kw = qkv_ref[win, 128:256]
                vw = qkv_ref[win, 256:384]
                qb = qkv_ref[rows, 0:128]
                db = do_ref[rows, :]
                same = segc_ref[win, :] == segr_ref[:, rows]
                dqs = []; dks = 0.0; dvs = 0.0
                for h in range(2):
                    hm = lane_half(qb.shape, h)
                    qh = jnp.where(hm, qb, jnp.zeros_like(qb))
                    dh = jnp.where(hm, db, jnp.zeros_like(db))
                    st = jnp.where(same, dot(kw, qh, 1, 1), NEG)
                    p = jnp.exp(st - lse_ref[0, h:h+1, rows])
                    dpt = dot(vw, dh, 1, 1)
                    rd = jnp.sum(fold(p * dpt, jnp.add), axis=0, keepdims=True)
                    ds = (p * (dpt - rd)).astype(jnp.bfloat16)
                    dvs = dvs + dot(p.astype(jnp.bfloat16), dh, 1, 0)
                    dks = dks + dot(ds, qh, 1, 0)
                    dqs.append(dot(kt_ref[h*64:(h+1)*64, win], ds, 1, 0))
                d_ref[rows, 0:128] = jnp.concatenate(dqs, axis=0).T.astype(jnp.bfloat16) * 0.125
                dk_acc[win, :] += dks
                dv_acc[win, :] += dvs
    d_ref[:, 128:256] = dk_acc[...].astype(jnp.bfloat16)
    d_ref[:, 256:384] = dv_acc[...].astype(jnp.bfloat16)
    sums_ref[0] = jnp.sum(d_ref[...].astype(jnp.float32), axis=0, keepdims=True)
def attn_fwd(qkv, seg):
    T, width = qkv.shape
    start, count = attn_windows(seg[0])
    segc = seg.reshape(T, 1)
    heads = width // 384
    return pl.pallas_call(
        fwd_kernel,
        out_shape=(jax.ShapeDtypeStruct((T, width // 3), jnp.bfloat16), jax.ShapeDtypeStruct((heads, 2, T), jnp.float32)),
        grid_spec=pltpu.PrefetchScalarGridSpec(
            num_scalar_prefetch=2, grid=(heads,),
            in_specs=[
                pl.BlockSpec((T, 384), lambda h, *_: (0, h)),
                pl.BlockSpec((1, T), lambda h, *_: (0, 0)),
                pl.BlockSpec((T, 1), lambda h, *_: (0, 0)),
            ],
            out_specs=(pl.BlockSpec((T, 128), lambda h, *_: (0, h)), pl.BlockSpec((1, 2, T), lambda h, *_: (h, 0, 0))),
            scratch_shapes=[pltpu.VMEM((128, T), jnp.bfloat16)],
        ),
        cost_estimate=cost(20 * T * T * width, 3 * T * width, T * T * width // 128),
        name="attn_fwd",
    )(start, count, qkv, seg, segc)


def attn_bwd(qkv, do, lse, seg, part):
    T, width = qkv.shape
    start, count = attn_windows(seg[0])
    segc = seg.reshape(T, 1)
    heads = width // 768
    first = part * heads
    return pl.pallas_call(
        bwd_kernel,
        out_shape=(jax.ShapeDtypeStruct((T, width // 2), jnp.bfloat16), jax.ShapeDtypeStruct((heads, 1, 384), jnp.float32)),
        grid_spec=pltpu.PrefetchScalarGridSpec(
            num_scalar_prefetch=2, grid=(heads,),
            in_specs=[
                pl.BlockSpec((T, 384), lambda h, *_: (0, first + h)),
                pl.BlockSpec((T, 128), lambda h, *_: (0, first + h)),
                pl.BlockSpec((1, 2, T), lambda h, *_: (first + h, 0, 0)),
                pl.BlockSpec((1, T), lambda h, *_: (0, 0)),
                pl.BlockSpec((T, 1), lambda h, *_: (0, 0)),
            ],
            out_specs=(pl.BlockSpec((T, 384), lambda h, *_: (0, h)), pl.BlockSpec((1, 1, 384), lambda h, *_: (h, 0, 0))),
            scratch_shapes=[pltpu.VMEM((T, 128), jnp.float32)] * 2 + [pltpu.VMEM((128, T), jnp.bfloat16)],
        ),
        cost_estimate=cost(20 * T * T * width, 6 * T * width, T * T * width // 64),
        name="attn_bwd",
    )(start, count, qkv, do, lse, seg, segc)


MESH_ID = pl.DeviceIdType.MESH


def bits_of():
    rep = lax.axis_index("rep")
    fsdp = lax.axis_index("fsdp")
    return dict(
        rep=rep, fsdp=fsdp, x=rep // 2, c=rep % 2, z1=fsdp // 4, z0=(fsdp // 2) % 2, y=fsdp % 2
    )


def partner_of(at, which):
    rep, fsdp = at["rep"], at["fsdp"]
    if which == "c":
        rep = rep + 1 - 2 * at["c"]
    elif which == "x":
        rep = rep + 2 - 4 * at["x"]
    elif which == "y":
        fsdp = fsdp + 1 - 2 * at["y"]
    elif which == "z0":
        fsdp = fsdp + 2 - 4 * at["z0"]
    elif which == "z1":
        fsdp = fsdp + 4 - 8 * at["z1"]
    else:
        rep = rep + 1 - 2 * at["c"]
        fsdp = fsdp + 4 - 8 * at["z1"]
    return (rep, fsdp)


REL = [(a, b, d) for d in (0, 1) for b in (0, 1) for a in (0, 1)]


def gather_kernel(
    qkv_in, wo_in, vec_in, tok_in, seg_in,
    qkv_out, wo_out, vec_out, tok_out, seg_out,
    tok_buf, seg_buf, send_sem, recv_sem, local_sem,
):
    at = bits_of()
    other = {k: partner_of(at, k) for k in ("c", "x", "y", "z0", "z1", "swap")}
    barrier = pltpu.get_barrier_semaphore()
    for k in ("c", "x", "y", "z0", "z1"):
        pl.semaphore_signal(barrier, inc=1, device_id=other[k], device_id_type=MESH_ID)
    moves = at["c"] != at["z1"]

    @pl.when(moves)
    def _():
        pl.semaphore_signal(barrier, inc=1, device_id=other["swap"], device_id_type=MESH_ID)
        pl.semaphore_wait(barrier, 6)

    @pl.when(jnp.logical_not(moves))
    def _():
        pl.semaphore_wait(barrier, 5)

    def flip(bit, rel):
        return bit + rel - 2 * bit * rel

    def shard(rel):
        return 4 * flip(at["z1"], rel[1]) + 2 * flip(at["z0"], rel[0]) + flip(at["y"], rel[2])

    counter = [0]
    started = []

    def send(src, dst, which):
        k = counter[0]
        counter[0] += 1
        copy = pltpu.make_async_remote_copy(
            src_ref=src, dst_ref=dst, send_sem=send_sem.at[k], recv_sem=recv_sem.at[k],
            device_id=other[which], device_id_type=MESH_ID,
        )
        copy.start()
        started.append(copy)
        return copy

    class Piece:
        def __init__(self, own, slot, split_x):
            self.own, self.slot, self.split_x = own, slot, split_x
            self.part = (2 * at["x"] + at["c"]) if split_x else at["c"]
            self.part_x = (2 * (1 - at["x"]) + at["c"]) if split_x else None
            self.copies = {}

        def first(self):
            zero = (0, 0, 0)
            for which in ("z1", "z0", "y"):
                self.copies[which, zero] = send(
                    self.own(self.part), self.slot(shard(zero), self.part), which
                )
            self.copies["c", zero] = send(self.own(None), self.slot(shard(zero), None), "c")

        def onward(self, rel):
            here = self.slot(shard(rel), self.part)
            if rel == (0, 1, 0):
                self.copies["z0", rel] = send(here, here, "z0")
            if rel[2] == 0:
                self.copies["y", rel] = send(here, here, "y")
            if self.split_x:
                self.copies["x", rel] = send(here, here, "x")
            self.copies["c", rel] = send(here, here, "c")

        def arrive(self, which, came):
            self.copies[which, came].wait_recv()
            step = {"z0": (1, 0, 0), "z1": (0, 1, 0), "y": (0, 0, 1)}[which]
            self.onward(tuple(p + q for p, q in zip(came, step)))

        def near(self):
            self.arrive("z1", (0, 0, 0))
            self.arrive("z0", (0, 0, 0))

        def rest(self):
            self.arrive("y", (0, 0, 0))
            self.arrive("z0", (0, 1, 0))
            self.arrive("y", (0, 1, 0))
            self.arrive("y", (1, 0, 0))
            self.arrive("y", (1, 1, 0))

        def last(self):
            if self.split_x:
                for rel in REL[1:]:
                    self.copies["x", rel].wait_recv()
                    there = self.slot(shard(rel), self.part_x)
                    self.copies["cx", rel] = send(there, there, "c")

        def finish(self):
            for (which, rel), copy in self.copies.items():
                if which in ("c", "cx"):
                    copy.wait_recv()

    def rows(ref, count):
        full = ref.shape[-2] // 8
        def slot(f, part):
            if part is None:
                at_row, n = f * full, full
            else:
                at_row, n = f * full + part * (full // count), full // count
            at_row = pl.multiple_of(at_row, 8)
            return ref.at[pl.ds(at_row, n), :]
        return slot

    def own_rows(ref, count):
        full = ref.shape[-2]
        def own(part):
            if part is None:
                return ref
            row = pl.multiple_of(part * (full // count), 8)
            n = full // count
            return ref.at[pl.ds(row, n), :]
        return own

    qkv, wo = pieces = [
        Piece(own_rows(qkv_in, 4), rows(qkv_out, 4), True),
        Piece(own_rows(wo_in, 4), rows(wo_out, 4), True),
    ]
    zero = (0, 0, 0)
    vec_copies = [
        send(vec_in, vec_out.at[shard(zero)], which) for which in ("c", "z1", "z0", "y")
    ]
    pieces[0].first()
    tok_k, seg_k = counter[0], counter[0] + 1
    counter[0] += 2

    def swap_copy(src, dst, k):
        return pltpu.make_async_remote_copy(
            src_ref=src, dst_ref=dst, send_sem=send_sem.at[k], recv_sem=recv_sem.at[k],
            device_id=other["swap"], device_id_type=MESH_ID,
        )

    @pl.when(moves)
    def _():
        swap_copy(tok_in, tok_out, tok_k).start()
        swap_copy(seg_in, seg_out, seg_k).start()

    @pl.when(jnp.logical_not(moves))
    def _():
        one = pltpu.make_async_copy(tok_in, tok_buf, local_sem.at[0])
        two = pltpu.make_async_copy(seg_in, seg_buf, local_sem.at[1])
        one.start()
        two.start()
        one.wait()
        two.wait()
        three = pltpu.make_async_copy(tok_buf, tok_out, local_sem.at[0])
        four = pltpu.make_async_copy(seg_buf, seg_out, local_sem.at[1])
        three.start()
        four.start()
        three.wait()
        four.wait()

    wo.first()
    qkv.near()
    vec_copies[1].wait_recv()
    here = vec_out.at[shard((0, 1, 0))]
    vec_far = send(here, here, "z0")
    vec_more = [send(here, here, "y")]
    vec_copies[2].wait_recv()
    here = vec_out.at[shard((1, 0, 0))]
    vec_more.append(send(here, here, "y"))
    qkv.rest()
    wo.near()
    wo.rest()
    vec_far.wait_recv()
    here = vec_out.at[shard((1, 1, 0))]
    vec_more.append(send(here, here, "y"))
    qkv.last()
    wo.last()
    for piece in pieces:
        piece.finish()
    for copy in [vec_copies[0], vec_copies[3]] + vec_more:
        copy.wait_recv()
    for copy in started:
        copy.wait_send()

    @pl.when(moves)
    def _():
        swap_copy(tok_in, tok_out, tok_k).wait()
        swap_copy(seg_in, seg_out, seg_k).wait()


GATHER_COPIES = 29 * 2 + 8 + 2


def gather_all(qkv, wo, vec, tok, seg):
    bf = jnp.bfloat16
    shape = jax.ShapeDtypeStruct
    whole = pl.BlockSpec(memory_space=pl.ANY)
    return pl.pallas_call(
        gather_kernel,
        out_shape=(
            shape((8 * qkv.shape[0], qkv.shape[1]), bf),
            shape((8 * wo.shape[0], wo.shape[1]), bf),
            shape((8,) + vec.shape, bf),
            shape(tok.shape, bf),
            shape(seg.shape, seg.dtype),
        ),
        in_specs=[whole] * 5,
        out_specs=(whole,) * 5,
        scratch_shapes=[
            pltpu.VMEM(tok.shape, bf),
            pltpu.VMEM(seg.shape, seg.dtype),
            pltpu.SemaphoreType.DMA((GATHER_COPIES,)),
            pltpu.SemaphoreType.DMA((GATHER_COPIES,)),
            pltpu.SemaphoreType.DMA((2,)),
        ],
        compiler_params=pltpu.CompilerParams(collective_id=0, has_side_effects=True),
        name="gather_weights",
    )(qkv, wo, vec, tok, seg)


SHRINK = 1000
BF, F32 = jnp.bfloat16, jnp.float32
SHAPE = jax.ShapeDtypeStruct


def full_spec(shape):
    return pl.BlockSpec(shape, lambda *_: (0,) * len(shape), pipeline_mode=pl.Buffered(1))


def cost(flops, moved, exps=0):
    return pl.CostEstimate(flops=int(flops) // SHRINK, bytes_accessed=int(moved) // SHRINK, transcendentals=int(exps) // SHRINK)


def qkv_kernel(x_ref, w_ref, bias_ref, scale_ref, o_ref):
    for i in range(4):
        rows = slice(i * 256, (i + 1) * 256)
        z = dot(x_ref[rows, :], w_ref[...], 1, 0)
        o_ref[rows, :] = ((z + bias_ref[...]) * scale_ref[...]).astype(BF)


def qkv_call(x, w, bias, scale):
    tokens, width = x.shape[0], w.shape[1]
    tile = 768
    return pl.pallas_call(
        qkv_kernel,
        out_shape=SHAPE((tokens, width), BF),
        grid=(width // tile,),
        in_specs=[
            full_spec(x.shape),
            pl.BlockSpec((x.shape[1], tile), lambda j: (0, j)),
            pl.BlockSpec((1, tile), lambda j: (0, j)),
            pl.BlockSpec((1, tile), lambda j: (0, j)),
        ],
        out_specs=pl.BlockSpec((tokens, tile), lambda j: (0, j)),
        cost_estimate=cost(2 * tokens * D * width, 2 * (tokens * D + D * width + tokens * width)),
        name="qkv",
    )(x, w, bias, scale)


def mean_row(value):
    return jnp.mean(value, axis=-1, keepdims=True)


def mix_kernel(c_ref, w_ref, x_ref, rows_ref, n_ref, q_ref, low_ref):
    value = x_ref[...].astype(F32) + dot(c_ref[...], w_ref[...], 1, 0) + rows_ref[6:7, :]
    center = value - mean_row(value)
    inv = lax.rsqrt(mean_row(center * center) + 1e-05)
    normed = center * inv
    n_ref[...] = normed
    q_ref[...] = inv
    low_ref[...] = (normed * rows_ref[0:1, :] + rows_ref[2:3, :]).astype(BF)


def mix_call(mixed, w_out, tok, rows):
    t = tok.shape[0]
    tile = pl.BlockSpec((256, D), lambda i: (i, 0))
    return pl.pallas_call(
        mix_kernel,
        out_shape=(SHAPE((t, D), F32), SHAPE((t, 1), F32), SHAPE((t, D), BF)),
        grid=(t // 256,),
        in_specs=[tile, full_spec((D, D)), tile, full_spec(rows.shape)],
        out_specs=(tile, pl.BlockSpec((256, 1), lambda i: (i, 0)), tile),
        cost_estimate=cost(2 * t * D * D, 12 * t * D + 2 * D * D),
        name="mix_norm",
    )(mixed, w_out, tok, rows)


def up_kernel(place_ref, h_ref, *refs):
    parts, (bias_ref, g_ref, s_ref) = refs[:4], refs[4:]
    each = pl.num_programs(0) // 4

    def tile(w_ref):
        for i in range(8):
            rows = slice(i * 128, (i + 1) * 128)
            z = dot(h_ref[rows, :], w_ref[...], 1, 0) + bias_ref[...]
            phi, bell = erf_parts(z)
            g_ref[rows, :] = (z * phi).astype(BF)
            s_ref[rows, :] = (phi + z * bell * 0.3989422804014327).astype(BF)

    for k in range(4):
        pl.when(pl.program_id(0) // each == k)(partial(tile, parts[k]))


def up_call(low, parts, place, bias):
    t = low.shape[0]
    tile = 512
    each = FF // tile // 4
    where = lambda j, p: (0, p[j // each] * each + lax.rem(j, each))
    out = pl.BlockSpec((t, tile), where)

    def part(k):
        return pl.BlockSpec((D, tile), lambda j, p: (0, jnp.clip(j - k * each, 0, each - 1)))

    return pl.pallas_call(
        up_kernel,
        out_shape=(SHAPE((t, FF), BF), SHAPE((t, FF), BF)),
        grid_spec=pltpu.PrefetchScalarGridSpec(
            num_scalar_prefetch=1, grid=(FF // tile,),
            in_specs=[full_spec(low.shape)] + [part(k) for k in range(4)] + [pl.BlockSpec((1, tile), where)],
            out_specs=(out, out),
        ),
        cost_estimate=cost(2 * t * D * FF, 2 * (t * D + D * FF + 2 * t * FF), 2 * t * FF),
        name="up_gelu",
    )(place, low, *parts, bias)


def row_sum(value):
    return jnp.sum(value, axis=0, keepdims=True)


def norm_back(grad, normed, inv, gain):
    scaled = grad * gain
    return inv * (scaled - mean_row(scaled) - normed * mean_row(scaled * normed))


def down_kernel(
    core_ref, g_ref, own_ref, came_ref, n_ref, cot_ref, rows_ref, out_ref, dr_ref, dm_ref, sums_ref, m_ref
):
    half = D // 2
    m_ref[:, pl.ds(pl.multiple_of(core_ref[0] * half, half), half)] = dot(g_ref[...], own_ref[...], 1, 0)
    m_ref[:, pl.ds(pl.multiple_of((1 - core_ref[0]) * half, half), half)] = dot(g_ref[...], came_ref[...], 1, 0)
    hidden = n_ref[...] * rows_ref[0:1, :] + rows_ref[2:3, :]
    value = hidden + m_ref[...] + rows_ref[7:8, :]
    center = value - mean_row(value)
    inv = lax.rsqrt(mean_row(center * center) + 1e-05)
    normed = center * inv
    gain = rows_ref[1:2, :]
    out_ref[...] = (normed * gain + rows_ref[3:4, :]).astype(BF)
    grad = cot_ref[...].astype(F32)
    back = norm_back(grad, normed, inv, gain)
    low = back.astype(BF)
    dr_ref[...] = back
    dm_ref[...] = low

    @pl.when(pl.program_id(0) == 0)
    def _():
        sums_ref[...] = jnp.zeros_like(sums_ref)

    sums_ref[0:1, :] += row_sum(grad * normed)
    sums_ref[1:2, :] += row_sum(grad)
    sums_ref[2:3, :] += row_sum(low.astype(F32))


def down_call(act, own, came, normed, cot, rows, core):
    t = act.shape[0]
    tile = pl.BlockSpec((256, D), lambda i, c: (i, 0))
    return pl.pallas_call(
        down_kernel,
        out_shape=(SHAPE((t, D), BF), SHAPE((t, D), F32), SHAPE((t, D), BF), SHAPE((8, D), F32)),
        grid_spec=pltpu.PrefetchScalarGridSpec(
            num_scalar_prefetch=1, grid=(t // 256,),
            in_specs=[
                pl.BlockSpec((256, FF), lambda i, c: (i, 0)), full_spec((FF, D // 2)), full_spec((FF, D // 2)),
                tile, tile, full_spec(rows.shape),
            ],
            out_specs=(tile, tile, tile, pl.BlockSpec((8, D), lambda i, c: (0, 0))),
            scratch_shapes=[pltpu.VMEM((256, D), F32)],
        ),
        cost_estimate=cost(2 * t * D * FF, 2 * (t * FF + D * FF) + 14 * t * D),
        name="down_norm",
    )(core.reshape(1), act, own, came, normed, cot, rows)


def slope_kernel(core_ref, left_ref, right_ref, own_ref, came_ref, s_ref, o_ref, sums_ref):
    total = 0.0
    for i in range(4):
        rows = slice(i * 256, (i + 1) * 256)
        back = dot(left_ref[rows, :], own_ref[...], 1, 1) + dot(right_ref[rows, :], came_ref[...], 1, 1)
        z = (back * s_ref[rows, :].astype(F32)).astype(BF)
        o_ref[rows, :] = z
        total = total + row_sum(z.astype(F32))
    sums_ref[...] = total


def slope_call(dm, own, came, slope, core):
    t = dm.shape[0]
    tile = 512
    wide = pl.BlockSpec((t, tile), lambda j, c: (0, j))
    part = pl.BlockSpec((tile, D // 2), lambda j, c: (j, 0))
    return pl.pallas_call(
        slope_kernel,
        out_shape=(SHAPE((t, FF), BF), SHAPE((1, FF), F32)),
        grid_spec=pltpu.PrefetchScalarGridSpec(
            num_scalar_prefetch=1, grid=(FF // tile,),
            in_specs=[
                pl.BlockSpec((t, D // 2), lambda j, c: (0, c[0])),
                pl.BlockSpec((t, D // 2), lambda j, c: (0, 1 - c[0])),
                part, part, wide,
            ],
            out_specs=(wide, pl.BlockSpec((1, tile), lambda j, c: (0, j))),
        ),
        cost_estimate=cost(2 * t * D * FF, 2 * (t * D + D * FF + 2 * t * FF)),
        name="down_back",
    )(core.reshape(1), dm, dm, own, came, slope)


def hidden_kernel(place_ref, *refs):
    grads, parts = refs[:4], refs[4:8]
    dr_ref, n_ref, q_ref, wo_ref, rows_ref, r_ref, a_ref, c_ref, sums_ref = refs[8:]
    grad = dr_ref[...]
    for grad_ref, w_ref in zip(grads, parts):
        grad = grad + dot(grad_ref[...], w_ref[...], 1, 1)
    normed = n_ref[...]
    back = norm_back(grad, normed, q_ref[...], rows_ref[0:1, :])
    low = back.astype(BF)
    r_ref[...] = back
    a_ref[...] = low
    c_ref[...] = dot(low, wo_ref[...], 1, 1).astype(BF)

    @pl.when(pl.program_id(0) == 0)
    def _():
        sums_ref[...] = jnp.zeros_like(sums_ref)

    sums_ref[0:1, :] += row_sum(grad * normed)
    sums_ref[1:2, :] += row_sum(grad)
    sums_ref[2:3, :] += row_sum(low.astype(F32))


def hidden_call(dz, parts, place, dr, normed, inv, w_out, rows):
    t = dz.shape[0]
    tile = pl.BlockSpec((256, D), lambda i, p: (i, 0))

    def quarter(k):
        return pl.BlockSpec((256, FF // 4), lambda i, p: (i, p[k]))

    return pl.pallas_call(
        hidden_kernel,
        out_shape=(SHAPE((t, D), F32), SHAPE((t, D), BF), SHAPE((t, D), BF), SHAPE((8, D), F32)),
        grid_spec=pltpu.PrefetchScalarGridSpec(
            num_scalar_prefetch=1, grid=(t // 256,),
            in_specs=[quarter(k) for k in range(4)] + [full_spec((D, FF // 4))] * 4 + [
                tile, tile,
                pl.BlockSpec((256, 1), lambda i, p: (i, 0)), full_spec((D, D)), full_spec(rows.shape),
            ],
            out_specs=(tile, tile, tile, pl.BlockSpec((8, D), lambda i, p: (0, 0))),
        ),
        cost_estimate=cost(2 * t * D * (FF + D), 2 * (t * FF + D * FF) + 16 * t * D),
        name="up_back_norm",
    )(place, *([dz] * 4), *parts, dr, normed, inv, w_out, rows)


def input_kernel(a_ref, b_ref, w_ref, r_ref, o_ref):
    half = a_ref.shape[1]
    value = dot(a_ref[...], w_ref[:, :half], 1, 1) + dot(b_ref[...], w_ref[:, half:], 1, 1)
    o_ref[...] = (r_ref[...] + value).astype(BF)


def input_call(part_a, part_b, w_qkv, resid):
    t, width = part_a.shape
    tile = pl.BlockSpec((256, D), lambda i: (i, 0))
    wide = pl.BlockSpec((256, width), lambda i: (i, 0))
    return pl.pallas_call(
        input_kernel,
        out_shape=SHAPE((t, D), BF),
        grid=(t // 256,),
        in_specs=[wide, wide, full_spec(w_qkv.shape), tile],
        out_specs=tile,
        cost_estimate=cost(4 * t * D * width, 4 * (t * width + D * width) + 6 * t * D),
        name="input_back",
    )(part_a, part_b, w_qkv, resid)


def weight_kernel(half_ref, left_ref, right_ref, *refs):
    o_ref, turned = refs[-2], refs[-1]

    @pl.when(pl.program_id(1) == 0)
    def _():
        turned[...] = left_ref[...].T

    value = dot(turned[...], right_ref[...], 1, 0)
    if len(refs) == 3:
        value = value + refs[0][...].astype(F32)
    o_ref[...] = value.astype(BF)


def weight_call(left, right, half, came=None):
    t, rows = left.shape
    width = right.shape[1]
    bm = 512
    bn = 1024 if width == 1024 else 512
    steps = rows // 2 // bm
    specs = [
        pl.BlockSpec((t, bm), lambda i, j, h: (0, h[0] * steps + i)),
        pl.BlockSpec((t, bn), lambda i, j, h: (0, j)),
    ]
    values = [left, right]
    out = pl.BlockSpec((bm, bn), lambda i, j, h: (i, j))
    if came is not None:
        specs.append(out)
        values.append(came)
    return pl.pallas_call(
        weight_kernel,
        out_shape=SHAPE((rows // 2, width), BF),
        grid_spec=pltpu.PrefetchScalarGridSpec(
            num_scalar_prefetch=1, grid=(steps, width // bn), in_specs=specs, out_specs=out,
            scratch_shapes=[pltpu.VMEM((bm, t), BF)],
        ),
        cost_estimate=cost(t * rows * width, t * rows + 2 * t * width + 2 * rows * width),
        name="weight_grad",
    )(half.reshape(1), *values)


def inner_kernel(rate, decay, w_ref, g_ref, m_ref, v_ref, m_out, v_out, d_out):
    weight = w_ref[...]
    new, m_out[...], v_out[...] = inner_step(
        weight, g_ref[...].astype(F32), m_ref[...], v_ref[...], rate, decay
    )
    d_out[...] = (weight - new).astype(BF)


def inner_call(weight, grad, first, second, rate, decay):
    rows, width = weight.shape
    block = 32 * 4096 // width
    tile = pl.BlockSpec((block, width), lambda i: (i, 0))
    like = SHAPE((rows, width), F32)
    return pl.pallas_call(
        partial(inner_kernel, rate, decay),
        out_shape=(like, like, SHAPE((rows, width), BF)),
        grid=(rows // block,),
        in_specs=[tile] * 4,
        out_specs=(tile,) * 3,
        cost_estimate=cost(20 * rows * width, 24 * rows * width),
        name="inner_step",
    )(weight, grad, first, second)


def outer_kernel(core_ref, w_ref, u_ref, own_ref, came_ref, o_ref, c_ref):
    mine = (core_ref[0] == pl.program_id(0)).astype(F32)
    total = own_ref[...].astype(F32) * mine + came_ref[...].astype(F32) * (1.0 - mine)
    mean = total * 0.25
    weight = w_ref[...]
    momentum = 0.5 * u_ref[...] + mean
    new = weight - 0.7 * (mean + 0.5 * momentum)
    o_ref[0] = mean
    o_ref[1] = momentum
    o_ref[2] = new
    c_ref[...] = new.astype(BF)


def outer_call(weight, momentum, own, came, core):
    rows, width = weight.shape
    block = 32 * 4096 // width
    steps = rows // 2 // block
    tile = pl.BlockSpec((block, width), lambda h, i, c: (h * steps + i, 0))
    part = pl.BlockSpec((block, width), lambda h, i, c: (i, 0))
    return pl.pallas_call(
        outer_kernel,
        out_shape=(SHAPE((3, rows, width), F32), SHAPE((rows, width), BF)),
        grid_spec=pltpu.PrefetchScalarGridSpec(
            num_scalar_prefetch=1, grid=(2, steps), in_specs=[tile, tile, part, part],
            out_specs=(pl.BlockSpec((3, block, width), lambda h, i, c: (0, h * steps + i, 0)), tile),
        ),
        cost_estimate=cost(10 * rows * width, 26 * rows * width),
        name="outer_step",
    )(core.reshape(1), weight, momentum, own, came)


def erf_parts(value):
    size = jnp.abs(value) * 0.7071067811865476
    share = 1.0 / (1.0 + 0.5 * size)
    inner = 0.17087277
    for coefficient in (
        -0.82215223, 1.48851587, -1.13520398, 0.27886807, -0.18628806, 0.09678418, 0.37409196, 1.00002368
    ):
        inner = coefficient + share * inner
    square = size * size
    half = 0.5 * share * jnp.exp(share * inner - 1.26551223 - square)
    return jnp.where(value >= 0, 1.0 - half, half), jnp.exp(-square)


def xor_pairs(bits):
    place = {"y": 0, "z0": 1, "z1": 2, "c": 3, "x": 4}
    flip = sum(1 << place[bit] for bit in bits)
    pairs = []
    for device in range(32):
        if bits == ("c", "z1") and ((device >> 3) & 1) == ((device >> 2) & 1):
            continue
        pairs.append((device, device ^ flip))
    return pairs


def exchange(value, *bits):
    return lax.ppermute(value, ("rep", "fsdp"), xor_pairs(bits))


def swap(at, value):
    return jnp.where(at["c"] != at["z1"], exchange(value, "c", "z1"), value)


def add_low(left, right):
    return (left.astype(jnp.float32) + right.astype(jnp.float32)).astype(jnp.bfloat16)


def pick(value, index, axis):
    return lax.dynamic_index_in_dim(value, index, axis, keepdims=False)


def half_axis(total, which):
    return 1 if which == "y" and total.ndim == 4 else 0


def halve(at, total, which):
    away = pick(total, 1 - at[which], half_axis(total, which))
    return away, exchange(away, which)


def join(at, total, came, which, *gates):
    return add_low(pick(total, at[which], half_axis(total, which)), after(came, *gates))


def slabs(total):
    return total.reshape(2, 2, -1, total.shape[-1])


def after(value, *earlier):
    return lax.optimization_barrier((value,) + earlier)[0]


def weave(value):
    rows = value.shape[1]
    return jnp.transpose(value.reshape(3, rows, D // 128, 128), (1, 2, 0, 3)).reshape(rows, 3 * D)


def unweave(value):
    rows = value.shape[0]
    return jnp.transpose(value.reshape(rows, D // 128, 3, 128), (2, 0, 1, 3)).reshape(3, rows, D)


def per_device_fast(
    tokens,
    cotangent,
    segment_ids,
    attention_weight,
    attention_momentum,
    attention_first,
    attention_second,
    expand_weight,
    expand_momentum,
    expand_first,
    expand_second,
    contract_weight,
    contract_momentum,
    contract_first,
    contract_second,
    vectors,
    vectors_momentum,
    vectors_first,
    vectors_second,
):
    bf, f32 = jnp.bfloat16, jnp.float32
    at = bits_of()
    core = at["c"].astype(jnp.int32)
    def swapped(value, came):
        return jnp.where(at["c"] != at["z1"], came, value)

    def cross(value):
        return exchange(value, "c", "z1")

    quarter = 2 * core + at["x"].astype(jnp.int32)
    place = jnp.stack([quarter, 2 * (1 - core) + quarter - 2 * core, quarter + 1 - 2 * at["x"], 3 - quarter])
    part = expand_weight.shape[1] // 4
    in_own = lax.all_gather(
        lax.dynamic_slice_in_dim(expand_weight, quarter * part, part, axis=1).astype(bf), "fsdp", axis=0, tiled=True
    )
    attn_low = attention_weight.astype(bf)
    w_qkv, w_out, vector_full, tok, seg = gather_all(
        weave(attn_low[:3]), attn_low[3], vectors.astype(bf), tokens, segment_ids,
    )
    cot_came = cross(after(cotangent, w_qkv))
    rows = jnp.swapaxes(vector_full, 0, 1).reshape(-1, D).astype(f32)
    bias_up = rows[8:].reshape(1, FF)
    bias_qkv = weave(jnp.stack([rows[4], jnp.zeros_like(rows[4]), rows[5]])[:, None])
    scale_qkv = weave(jnp.stack([jnp.full((1, D), 0.125, f32)] + [jnp.ones((1, D), f32)] * 2))
    part = contract_weight.shape[1] // 2
    down_half = lax.dynamic_slice_in_dim(contract_weight, core * part, part, axis=1).astype(bf)
    down_own = lax.all_gather(after(down_half, w_qkv), "fsdp", axis=0, tiled=True)
    in_near = after(in_own, w_qkv)
    in_far = exchange(in_near, "x")
    in_side = exchange(in_near, "c")
    qkv = qkv_call(tok, w_qkv, bias_qkv, scale_qkv)
    mixed, log_sum = attn_fwd(qkv, seg)
    in_parts = [in_own, after(in_side, mixed), in_far, exchange(after(in_far, mixed), "c")]
    normed, inv, hidden_low = mix_call(mixed, w_out, tok, rows)
    cot = swapped(cotangent, after(cot_came, hidden_low))
    activated, slope = up_call(after(hidden_low, cot), in_parts, place, bias_up)
    down_other = exchange(after(down_own, activated), "c")
    layer_output, grad_sum, grad_branch, sums_two = down_call(
        activated, down_own, down_other, normed, cot, rows, core
    )
    output_came = cross(layer_output)
    down_send = weight_call(activated, grad_branch, 1 - core)
    grad_pre, sums_up = slope_call(after(grad_branch, down_send), down_own, down_other, slope, core)
    down_came = exchange(down_send, "c")
    up_send = weight_call(hidden_low, grad_pre, 1 - core)
    down_total = slabs(weight_call(activated, after(grad_branch, up_send), core, down_came))
    up_came = exchange(up_send, "c")
    away_d, came_d = halve(at, down_total, "y")
    up_total = slabs(weight_call(hidden_low, after(grad_pre, away_d), core, up_came))
    away_u, came_u = halve(at, up_total, "z0")
    grad_resid, grad_attn, grad_mixed, sums_one = hidden_call(
        after(grad_pre, away_u), in_parts, place, grad_sum, normed, inv, w_out, rows
    )
    proj_send = weight_call(mixed, grad_attn, 1 - core)
    proj_came = exchange(proj_send, "c")
    output = swapped(layer_output, after(output_came, proj_send))
    grad_a, sums_a = attn_bwd(qkv, after(grad_mixed, proj_send, output), log_sum, seg, 0)
    send_a = weight_call(tok, grad_a, 1 - core)
    came_a = exchange(send_a, "c")
    down_one = join(at, down_total, came_d, "y", send_a)
    away_d, came_d = halve(at, down_one, "z0")
    up_one = join(at, up_total, came_u, "z0", away_d)
    away_u, came_u = halve(at, up_one, "y")
    proj_total = slabs(weight_call(mixed, after(grad_attn, away_u), core, proj_came))
    away_p, came_p = halve(at, proj_total, "y")
    total_a = slabs(weight_call(tok, after(grad_a, away_p), core, came_a))
    away_a, came_one = halve(at, total_a, "z0")
    grad_b, sums_b = attn_bwd(qkv, after(grad_mixed, away_a), log_sum, seg, 1)
    send_b = weight_call(tok, grad_b, 1 - core)
    came_b = exchange(send_b, "c")
    down_two = join(at, down_one, came_d, "z0", send_b)
    cross_d = cross(down_two)
    up_two = join(at, up_one, came_u, "y", down_two)
    cross_u = cross(up_two)
    proj_one = join(at, proj_total, came_p, "y", up_two)
    away_p, came_p = halve(at, proj_one, "z0")
    a_one = join(at, total_a, came_one, "z0", away_p)
    away_a, came_a = halve(at, a_one, "y")
    total_b = slabs(weight_call(tok, after(grad_b, away_a), core, came_b))
    away_b, came_b = halve(at, total_b, "y")
    sums_qkv = jnp.concatenate([sums_a, sums_b], axis=0).reshape(D // 128, 3, 128)
    vector_grad = jnp.concatenate(
        [
            sums_one[0:1],
            sums_two[0:1],
            sums_one[1:2],
            sums_two[1:2],
            sums_qkv[:, 0].reshape(1, D),
            sums_qkv[:, 2].reshape(1, D),
            sums_one[2:3],
            sums_two[2:3],
            sums_up.reshape(FF // D, D),
        ],
        axis=0,
    )

    def vector_send(parts, which):
        half = parts.shape[1] // 2
        away = lax.dynamic_slice_in_dim(parts, (1 - at[which]) * half, half, axis=1)
        return exchange(away, which)

    def vector_join(parts, came, which, *gates):
        half = parts.shape[1] // 2
        return lax.dynamic_slice_in_dim(parts, at[which] * half, half, axis=1) + after(came, *gates)

    vec_came = vector_send(vector_grad, "c")
    input_grad = input_call(after(grad_a, away_b), grad_b, w_qkv, grad_resid)
    vec_one = vector_join(vector_grad, vec_came, "c", input_grad)
    vec_came = vector_send(vec_one, "z0")
    def inner(weight, grad, first, second, rate, decay):
        flat = (-1, weight.shape[-1])
        return inner_call(
            weight.reshape(flat), grad.reshape(flat), first.reshape(flat), second.reshape(flat), rate, decay
        )

    def rep_send(diff):
        halves = diff.reshape(2, diff.shape[0] // 2, diff.shape[1])
        away = pick(halves, 1 - at["c"], 0)
        return away, exchange(away, "c")

    def rep_join(diff, came, *gates):
        halves = diff.reshape(2, diff.shape[0] // 2, diff.shape[1])
        return add_low(pick(halves, at["c"], 0), after(came, *gates))

    def outer(weight, momentum, own, came):
        flat = (-1, weight.shape[-1])
        return outer_call(weight.reshape(flat), momentum.reshape(flat), own, came, core)

    proj_two = join(at, proj_one, came_p, "z0", input_grad)
    a_two = join(at, a_one, came_a, "y", input_grad)
    cross_pa = cross(jnp.concatenate([proj_two, a_two], axis=1))
    grad_contract = swapped(down_two, after(cross_d, proj_two, a_two))
    contract_new = inner(contract_weight, grad_contract, contract_first, contract_second, 0.015, 0.1)
    sent_c, came_c = rep_send(contract_new[2])
    b_one = join(at, total_b, came_b, "y", sent_c)
    away_b, came_b = halve(at, b_one, "z0")
    vec_two = vector_join(vec_one, vec_came, "z0", away_b)
    vec_came = vector_send(vec_two, "y")
    grad_expand = swapped(up_two, after(cross_u, away_b))
    expand_new = inner(expand_weight, grad_expand, expand_first, expand_second, 0.03, 0.1)
    sent_e, came_e = rep_send(expand_new[2])
    half_c = rep_join(contract_new[2], came_c, sent_e)
    rest_c = exchange(half_c, "x")
    b_two = join(at, b_one, came_b, "z0", half_c)
    cross_b = cross(b_two)
    half_e = rep_join(expand_new[2], came_e, b_two)
    rest_e = exchange(half_e, "x")
    vec_three = vector_join(vec_two, vec_came, "y", half_e)
    vec_cross = cross(vec_three)
    full_c = add_low(half_c, after(rest_c, half_e))
    back_c = exchange(full_c, "c")
    pa = swapped(jnp.concatenate([proj_two, a_two], axis=1), after(cross_pa, full_c))
    outer_c = outer(contract_weight, contract_momentum, full_c, after(back_c, pa))
    grad_vectors = swapped(vec_three, after(vec_cross, outer_c[1]))
    inner_new, first_new, second_new = inner_step(
        vectors, grad_vectors, vectors_first[0], vectors_second[0], 0.2, 0.0
    )
    vec_diff = (vectors - inner_new).astype(bf)
    vec_near = exchange(vec_diff, "c")
    input_came = cross(after(input_grad, b_two, vec_diff))
    b_own = swapped(b_two, after(cross_b, vec_diff))
    grad_qkv = jnp.concatenate([pa[:, D:], b_own], axis=1)
    grad_attention = jnp.concatenate([unweave(grad_qkv), pa[None, :, :D]], axis=0)
    attention_new = inner(attention_weight, grad_attention, attention_first, attention_second, 0.03, 0.1)
    sent_a, came_a = rep_send(attention_new[2])
    vec_half = add_low(vec_diff, after(vec_near, sent_a))
    vec_far = exchange(vec_half, "x")
    full_e = add_low(half_e, after(rest_e, sent_a))
    back_e = exchange(full_e, "c")
    half_a = rep_join(attention_new[2], came_a, full_e)
    rest_a = exchange(half_a, "x")
    outer_e = outer(expand_weight, expand_momentum, full_e, after(back_e, half_a))
    full_a = add_low(half_a, after(rest_a, outer_e[1]))
    back_a = exchange(full_a, "c")
    mean_diff = add_low(vec_half, after(vec_far, full_a)).astype(f32) / 4
    momentum_new = 0.5 * vectors_momentum + mean_diff
    outer_new = vectors - 0.7 * (mean_diff + 0.5 * momentum_new)
    input_grad = swapped(input_grad, after(input_came, full_a))
    outer_a = outer(attention_weight, attention_momentum, full_a, back_a)
    results = []
    for weight, first, new, (total, copy) in (
        (attention_weight, attention_first, attention_new, outer_a),
        (expand_weight, expand_first, expand_new, outer_e),
        (contract_weight, contract_first, contract_new, outer_c),
    ):
        results += [
            new[0].reshape(first.shape),
            new[1].reshape(first.shape),
            total.reshape((3,) + weight.shape),
            copy.reshape(weight.shape),
        ]
    results += [
        first_new[None],
        second_new[None],
        jnp.stack([mean_diff, momentum_new, outer_new]),
        outer_new.astype(bf),
    ]
    return (output, input_grad) + tuple(results)


def solution(mesh):
    placed = (
        P(("rep", "fsdp"), None),
        P(("rep", "fsdp"), None),
        P(("rep", "fsdp"), None),
        P(None, "fsdp", None),
        P(None, "fsdp", None),
        P("rep", None, "fsdp", None),
        P("rep", None, "fsdp", None),
        P("fsdp", None),
        P("fsdp", None),
        P("rep", "fsdp", None),
        P("rep", "fsdp", None),
        P("fsdp", None),
        P("fsdp", None),
        P("rep", "fsdp", None),
        P("rep", "fsdp", None),
        P(None, "fsdp"),
        P(None, "fsdp"),
        P("rep", None, "fsdp"),
        P("rep", None, "fsdp"),
    )
    small = mesh.shape["rep"] == 4 and mesh.shape["fsdp"] == 8
    body = per_device_fast if small else per_device
    return jax.shard_map(
        body,
        mesh=mesh,
        in_specs=placed,
        out_specs=(
            P(("rep", "fsdp"), None),
            P(("rep", "fsdp"), None),
            P("rep", None, "fsdp", None),
            P("rep", None, "fsdp", None),
            P(None, None, "fsdp", None),
            P(None, "fsdp", None),
            P("rep", "fsdp", None),
            P("rep", "fsdp", None),
            P(None, "fsdp", None),
            P("fsdp", None),
            P("rep", "fsdp", None),
            P("rep", "fsdp", None),
            P(None, "fsdp", None),
            P("fsdp", None),
            P("rep", None, "fsdp"),
            P("rep", None, "fsdp"),
            P(None, None, "fsdp"),
            P(None, "fsdp"),
        ),
        check_vma=False,
    )
```

```python
from functools import partial

import jax
import jax.numpy as jnp
from jax import lax
from jax.experimental import pallas as pl
from jax.experimental.pallas import tpu as pltpu
from jax.sharding import PartitionSpec as P

D = 1024
H = 16
HD = 64
FF = 4096
LEN = 1024
SEQ_DEV = 1
ADAM_STEP = 4
TOK_DEV = 1024


def norm_forward(values_in, gain_row, shift_row):
    center = values_in - jnp.mean(values_in, axis=-1, keepdims=True)
    inv_scale = lax.rsqrt(jnp.mean(center * center, axis=-1, keepdims=True) + 1e-05)
    normed = center * inv_scale
    return (normed * gain_row + shift_row, normed, inv_scale)


def norm_backward(grad_out, normed, inv_scale, gain_row):
    grad_gain = jnp.sum(grad_out * normed, axis=0)
    grad_shift = jnp.sum(grad_out, axis=0)
    scaled_grad = grad_out * gain_row
    grad_value = inv_scale * (
        scaled_grad
        - jnp.mean(scaled_grad, axis=-1, keepdims=True)
        - normed * jnp.mean(scaled_grad * normed, axis=-1, keepdims=True)
    )
    return (grad_value, grad_gain, grad_shift)


def product_over(left, right):
    return lax.dot_general(
        left, right, (((0,), (0,)), ((), ())), preferred_element_type=jnp.float32
    )


def product_back(left, right):
    return lax.dot_general(
        left, right, (((1,), (1,)), ((), ())), preferred_element_type=jnp.float32
    )


def block_scores(query_block, key_block, row_segments, all_segments):
    scores = jnp.einsum("qhd,khd->hqk", query_block, key_block, preferred_element_type=jnp.float32)
    same_doc = row_segments[:, None] == all_segments[None, :]
    return jnp.where(same_doc[None], scores, -1e30)


def inner_step(weight, gradient, first_moment, second_moment, learn_rate, weight_decay):
    first_new = 0.5 * first_moment + 0.5 * gradient
    second_new = 0.75 * second_moment + 0.25 * gradient * gradient
    update_dir = (
        first_new
        / (1.0 - 0.5**ADAM_STEP)
        / (jnp.sqrt(second_new / (1.0 - 0.75**ADAM_STEP)) + 1e-08)
    )
    return (weight - learn_rate * (update_dir + weight_decay * weight), first_new, second_new)


def per_device(
    tokens,
    cotangent,
    segment_ids,
    attention_weight,
    attention_momentum,
    attention_first,
    attention_second,
    expand_weight,
    expand_momentum,
    expand_first,
    expand_second,
    contract_weight,
    contract_momentum,
    contract_first,
    contract_second,
    vectors,
    vectors_momentum,
    vectors_first,
    vectors_second,
):
    attn_full, vector_full = (
        lax.all_gather(attention_weight.astype(jnp.bfloat16), "fsdp", axis=1, tiled=True),
        lax.all_gather(vectors.astype(jnp.bfloat16), "fsdp", axis=1, tiled=True),
    )
    vector_rows = vector_full.astype(jnp.float32)
    gain_one, gain_two, shift_one, shift_two = (
        vector_rows[0],
        vector_rows[1],
        vector_rows[2],
        vector_rows[3],
    )
    bias_query, bias_value, bias_mixed, bias_down = (
        vector_rows[4],
        vector_rows[5],
        vector_rows[6],
        vector_rows[7],
    )
    bias_up = vector_rows[8:].reshape(FF)
    projected = jnp.einsum("td,nde->nte", tokens, attn_full[:3], preferred_element_type=jnp.float32)
    query_all = ((projected[0] + bias_query) * 0.125).astype(jnp.bfloat16)
    key_all = projected[1].astype(jnp.bfloat16)
    value_all = (projected[2] + bias_value).astype(jnp.bfloat16)
    query_heads = query_all.reshape(SEQ_DEV, LEN, H, HD)
    key_heads = key_all.reshape(SEQ_DEV, LEN, H, HD)
    value_heads = value_all.reshape(SEQ_DEV, LEN, H, HD)
    block_rows = min(512, LEN)
    head_group = min(8, H)
    context_rows = []
    log_sums = []
    seq_index = 0
    for row_start in range(0, LEN, block_rows):
        block_pieces = []
        for head_start in range(0, H, head_group):
            head_part = slice(head_start, head_start + head_group)
            scores = block_scores(
                query_heads[seq_index, row_start : row_start + block_rows, head_part],
                key_heads[seq_index, :, head_part],
                segment_ids[seq_index, row_start : row_start + block_rows],
                segment_ids[seq_index],
            )
            row_max = jnp.max(scores, axis=-1, keepdims=True)
            exp_score = jnp.exp(scores - row_max)
            row_total = jnp.sum(exp_score, axis=-1, keepdims=True)
            probability = (exp_score / row_total).astype(jnp.bfloat16)
            block_pieces.append(
                jnp.einsum(
                    "hqk,khd->qhd",
                    probability,
                    value_heads[seq_index, :, head_part],
                    preferred_element_type=jnp.float32,
                )
            )
            log_sums.append(row_max + jnp.log(row_total))
        context_rows.append(jnp.concatenate(block_pieces, axis=1))
    mixed = jnp.concatenate(context_rows, axis=0).reshape(TOK_DEV, D).astype(jnp.bfloat16)
    attn_out = jnp.dot(mixed, attn_full[3], preferred_element_type=jnp.float32) + bias_mixed
    hidden, normed_one, scale_one = norm_forward(
        tokens.astype(jnp.float32) + attn_out, gain_one, shift_one
    )
    hidden_low = hidden.astype(jnp.bfloat16)
    ffn_expand, ffn_contract = (
        lax.all_gather(expand_weight.astype(jnp.bfloat16), "fsdp", axis=0, tiled=True),
        lax.all_gather(contract_weight.astype(jnp.bfloat16), "fsdp", axis=0, tiled=True),
    )
    pre_act = jnp.dot(hidden_low, ffn_expand, preferred_element_type=jnp.float32) + bias_up
    activated = jax.nn.gelu(pre_act, approximate=False).astype(jnp.bfloat16)
    branch = jnp.dot(activated, ffn_contract, preferred_element_type=jnp.float32) + bias_down
    layer_output, normed_two, scale_two = norm_forward(hidden + branch, gain_two, shift_two)
    grad_sum, grad_gain_two, grad_shift_two = norm_backward(
        cotangent.astype(jnp.float32), normed_two, scale_two, gain_two
    )
    grad_branch = grad_sum.astype(jnp.bfloat16)
    grad_act = product_back(grad_branch, ffn_contract)
    unused_value, gelu_pull = jax.vjp(partial(jax.nn.gelu, approximate=False), pre_act)
    grad_pre_low = gelu_pull(grad_act)[0].astype(jnp.bfloat16)
    grad_hidden = grad_sum + product_back(grad_pre_low, ffn_expand)
    contract_full = product_over(activated, grad_branch)
    expand_full = product_over(hidden_low, grad_pre_low)
    grad_expand, grad_contract = (
        lax.psum_scatter(expand_full, "fsdp", scatter_dimension=0, tiled=True),
        lax.psum_scatter(contract_full, "fsdp", scatter_dimension=0, tiled=True),
    )
    grad_resid, grad_gain_one, grad_shift_one = norm_backward(
        grad_hidden, normed_one, scale_one, gain_one
    )
    grad_attn_out = grad_resid.astype(jnp.bfloat16)
    grad_bias_mixed = jnp.sum(grad_attn_out.astype(jnp.float32), axis=0)
    grad_output_proj = product_over(mixed, grad_attn_out)
    grad_mixed = product_back(grad_attn_out, attn_full[3]).astype(jnp.bfloat16)
    grad_context = grad_mixed.reshape(SEQ_DEV, LEN, H, HD)
    query_grads = []
    lse_index = 0
    seq_index = 0
    key_totals = [
        jnp.zeros((LEN, head_group, HD), jnp.float32) for head_start in range(0, H, head_group)
    ]
    value_totals = [
        jnp.zeros((LEN, head_group, HD), jnp.float32) for head_start in range(0, H, head_group)
    ]
    for row_start in range(0, LEN, block_rows):
        block_pieces = []
        for group_index, head_start in enumerate(range(0, H, head_group)):
            head_part = slice(head_start, head_start + head_group)
            query_block = query_heads[seq_index, row_start : row_start + block_rows, head_part]
            key_block = key_heads[seq_index, :, head_part]
            value_block = value_heads[seq_index, :, head_part]
            ctx_grad = grad_context[seq_index, row_start : row_start + block_rows, head_part]
            scores = block_scores(
                query_block,
                key_block,
                segment_ids[seq_index, row_start : row_start + block_rows],
                segment_ids[seq_index],
            )
            probability = jnp.exp(scores - log_sums[lse_index])
            lse_index = lse_index + 1
            value_totals[group_index] = value_totals[group_index] + jnp.einsum(
                "hqk,qhd->khd",
                probability.astype(jnp.bfloat16),
                ctx_grad,
                preferred_element_type=jnp.float32,
            )
            prob_grad = jnp.einsum(
                "qhd,khd->hqk", ctx_grad, value_block, preferred_element_type=jnp.float32
            )
            row_dot = jnp.sum(probability * prob_grad, axis=-1, keepdims=True)
            score_grad = (probability * (prob_grad - row_dot)).astype(jnp.bfloat16)
            block_pieces.append(
                jnp.einsum(
                    "hqk,khd->qhd", score_grad, key_block, preferred_element_type=jnp.float32
                ).astype(jnp.bfloat16)
            )
            key_totals[group_index] = key_totals[group_index] + jnp.einsum(
                "hqk,qhd->khd", score_grad, query_block, preferred_element_type=jnp.float32
            )
        query_grads.append(jnp.concatenate(block_pieces, axis=1))
    key_grads = jnp.concatenate(
        [key_total.astype(jnp.bfloat16) for key_total in key_totals], axis=1
    )
    value_grads = jnp.concatenate(
        [value_total.astype(jnp.bfloat16) for value_total in value_totals], axis=1
    )
    grad_query = jnp.concatenate(query_grads, axis=0).reshape(TOK_DEV, D) * 0.125
    grad_keys = key_grads.reshape(TOK_DEV, D)
    grad_values = value_grads.reshape(TOK_DEV, D)
    stacked_grads = jnp.stack([grad_query, grad_keys, grad_values])
    grad_qkv = jnp.einsum("td,nte->nde", tokens, stacked_grads, preferred_element_type=jnp.float32)
    input_grad = (
        grad_resid
        + jnp.einsum(
            "nte,nde->td", stacked_grads, attn_full[:3], preferred_element_type=jnp.float32
        )
    ).astype(jnp.bfloat16)
    grad_attention_full = jnp.concatenate([grad_qkv, grad_output_proj[None]], axis=0)
    vector_head = jnp.stack(
        [
            grad_gain_one,
            grad_gain_two,
            grad_shift_one,
            grad_shift_two,
            jnp.sum(grad_query.astype(jnp.float32), axis=0),
            jnp.sum(grad_values.astype(jnp.float32), axis=0),
            grad_bias_mixed,
            jnp.sum(grad_branch.astype(jnp.float32), axis=0),
        ]
    )
    grad_bias_up = jnp.sum(grad_pre_low.astype(jnp.float32), axis=0).reshape(FF // D, D)
    grad_vectors_full = jnp.concatenate([vector_head, grad_bias_up], axis=0)
    grad_attention, grad_vectors = (
        lax.psum_scatter(grad_attention_full, "fsdp", scatter_dimension=1, tiled=True),
        lax.psum_scatter(grad_vectors_full, "fsdp", scatter_dimension=1, tiled=True),
    )
    attention_new = inner_step(
        attention_weight, grad_attention, attention_first[0], attention_second[0], 0.03, 0.1
    )
    expand_new = inner_step(
        expand_weight, grad_expand, expand_first[0], expand_second[0], 0.03, 0.1
    )
    contract_new = inner_step(
        contract_weight, grad_contract, contract_first[0], contract_second[0], 0.015, 0.1
    )
    vectors_new = inner_step(vectors, grad_vectors, vectors_first[0], vectors_second[0], 0.2, 0.0)
    summed = (
        lax.psum((attention_weight - attention_new[0]).astype(jnp.bfloat16), "rep").astype(
            jnp.float32
        ),
        lax.psum((expand_weight - expand_new[0]).astype(jnp.bfloat16), "rep").astype(jnp.float32),
        lax.psum((contract_weight - contract_new[0]).astype(jnp.bfloat16), "rep").astype(
            jnp.float32
        ),
        lax.psum((vectors - vectors_new[0]).astype(jnp.bfloat16), "rep").astype(jnp.float32),
    )
    groups_count = lax.axis_size("rep")
    results = []
    for weight_now, momentum_now, inner_new, diff_total in zip(
        (attention_weight, expand_weight, contract_weight, vectors),
        (attention_momentum, expand_momentum, contract_momentum, vectors_momentum),
        (attention_new, expand_new, contract_new, vectors_new),
        summed,
    ):
        mean_diff = diff_total / groups_count
        momentum_new = 0.5 * momentum_now + mean_diff
        outer_new = weight_now - 0.7 * (mean_diff + 0.5 * momentum_new)
        results.append(
            (
                inner_new[1][None],
                inner_new[2][None],
                jnp.stack([mean_diff, momentum_new, outer_new]),
                outer_new.astype(jnp.bfloat16),
            )
        )
    return (
        layer_output.astype(jnp.bfloat16),
        input_grad,
        results[0][0],
        results[0][1],
        results[0][2],
        results[0][3],
        results[1][0],
        results[1][1],
        results[1][2],
        results[1][3],
        results[2][0],
        results[2][1],
        results[2][2],
        results[2][3],
        results[3][0],
        results[3][1],
        results[3][2],
        results[3][3],
    )


NEG=-1e30
QB=256
def attn_windows(seg_row):
    length = seg_row.shape[0]
    nb = length // QB
    firsts = seg_row[::QB]
    lasts = seg_row[QB-1::QB]
    begin = jnp.sum((seg_row[None, :] < firsts[:, None]).astype(jnp.int32), axis=1)
    end = jnp.sum((seg_row[None, :] <= lasts[:, None]).astype(jnp.int32), axis=1)
    start = begin // 128
    count = (end - start * 128 + QB - 1) // QB
    start = jnp.minimum(start, (length - count * QB) // 128)
    return start.astype(jnp.int32), count.astype(jnp.int32)
def lane_half(shape, h):
    lane = lax.broadcasted_iota(jnp.int32, shape, len(shape)-1)
    return (lane < 64) if h == 0 else (lane >= 64)
def dot(a, b, ca, cb):
    return lax.dot_general(a, b, (((ca,), (cb,)), ((), ())), preferred_element_type=jnp.float32)
def fold(value, join):
    part = value.shape[0] // 8
    parts = [value[i * part:(i + 1) * part] for i in range(8)]
    while len(parts) > 1:
        parts = [join(a, b) for a, b in zip(parts[::2], parts[1::2])]
    return parts[0]
def fwd_kernel(start_ref, count_ref, qkv_ref, segr_ref, segc_ref, o_ref, lse_ref, vt_ref):
    length = qkv_ref.shape[0]
    vt_ref[...] = qkv_ref[:, 256:384].T
    nb = length // QB
    for i in range(nb):
        rows = slice(i*QB, (i+1)*QB)
        for nn in range(1, nb+1):
            @pl.when(count_ref[i] == nn)
            def _():
                nk = nn*QB
                lo = pl.multiple_of(start_ref[i]*128, 128)
                kw = qkv_ref[pl.ds(lo, nk), 128:256]
                qb = qkv_ref[rows, 0:128]
                same = segc_ref[pl.ds(lo, nk), :] == segr_ref[:, rows]
                outs = []
                for h in range(2):
                    qh = jnp.where(lane_half(qb.shape, h), qb, jnp.zeros_like(qb))
                    st = jnp.where(same, dot(kw, qh, 1, 1), NEG)
                    m = jnp.max(fold(st, jnp.maximum), axis=0, keepdims=True)
                    p = jnp.exp(st - m)
                    l = jnp.sum(fold(p, jnp.add), axis=0, keepdims=True)
                    weighted = dot(vt_ref[h*64:(h+1)*64, pl.ds(lo, nk)], p.astype(jnp.bfloat16), 1, 0)
                    outs.append(weighted * (1.0 / l))
                    lse_ref[0, h:h+1, rows] = m + jnp.log(l)
                o_ref[rows, :] = jnp.concatenate(outs, axis=0).T.astype(jnp.bfloat16)
def bwd_kernel(start_ref, count_ref, qkv_ref, do_ref, lse_ref, segr_ref, segc_ref, d_ref, sums_ref, dk_acc, dv_acc, kt_ref):
    length = qkv_ref.shape[0]
    kt_ref[...] = qkv_ref[:, 128:256].T
    nb = length // QB
    dk_acc[...] = jnp.zeros_like(dk_acc)
    dv_acc[...] = jnp.zeros_like(dv_acc)
    for i in range(nb):
        rows = slice(i*QB, (i+1)*QB)
        for nn in range(1, nb+1):
            @pl.when(count_ref[i] == nn)
            def _():
                nk = nn*QB
                lo = pl.multiple_of(start_ref[i]*128, 128)
                win = pl.ds(lo, nk)
                kw = qkv_ref[win, 128:256]
                vw = qkv_ref[win, 256:384]
                qb = qkv_ref[rows, 0:128]
                db = do_ref[rows, :]
                same = segc_ref[win, :] == segr_ref[:, rows]
                dqs = []; dks = 0.0; dvs = 0.0
                for h in range(2):
                    hm = lane_half(qb.shape, h)
                    qh = jnp.where(hm, qb, jnp.zeros_like(qb))
                    dh = jnp.where(hm, db, jnp.zeros_like(db))
                    st = jnp.where(same, dot(kw, qh, 1, 1), NEG)
                    p = jnp.exp(st - lse_ref[0, h:h+1, rows])
                    dpt = dot(vw, dh, 1, 1)
                    rd = jnp.sum(fold(p * dpt, jnp.add), axis=0, keepdims=True)
                    ds = (p * (dpt - rd)).astype(jnp.bfloat16)
                    dvs = dvs + dot(p.astype(jnp.bfloat16), dh, 1, 0)
                    dks = dks + dot(ds, qh, 1, 0)
                    dqs.append(dot(kt_ref[h*64:(h+1)*64, win], ds, 1, 0))
                d_ref[rows, 0:128] = jnp.concatenate(dqs, axis=0).T.astype(jnp.bfloat16) * 0.125
                dk_acc[win, :] += dks
                dv_acc[win, :] += dvs
    d_ref[:, 128:256] = dk_acc[...].astype(jnp.bfloat16)
    d_ref[:, 256:384] = dv_acc[...].astype(jnp.bfloat16)
    sums_ref[0] = jnp.sum(d_ref[...].astype(jnp.float32), axis=0, keepdims=True)
def attn_fwd(qkv, seg):
    T, width = qkv.shape
    start, count = attn_windows(seg[0])
    segc = seg.reshape(T, 1)
    heads = width // 384
    return pl.pallas_call(
        fwd_kernel,
        out_shape=(jax.ShapeDtypeStruct((T, width // 3), jnp.bfloat16), jax.ShapeDtypeStruct((heads, 2, T), jnp.float32)),
        grid_spec=pltpu.PrefetchScalarGridSpec(
            num_scalar_prefetch=2, grid=(heads,),
            in_specs=[
                pl.BlockSpec((T, 384), lambda h, *_: (0, h)),
                pl.BlockSpec((1, T), lambda h, *_: (0, 0)),
                pl.BlockSpec((T, 1), lambda h, *_: (0, 0)),
            ],
            out_specs=(pl.BlockSpec((T, 128), lambda h, *_: (0, h)), pl.BlockSpec((1, 2, T), lambda h, *_: (h, 0, 0))),
            scratch_shapes=[pltpu.VMEM((128, T), jnp.bfloat16)],
        ),
        cost_estimate=cost(20 * T * T * width, 3 * T * width, T * T * width // 128),
        name="attn_fwd",
    )(start, count, qkv, seg, segc)


def attn_bwd(qkv, do, lse, seg, part):
    T, width = qkv.shape
    start, count = attn_windows(seg[0])
    segc = seg.reshape(T, 1)
    heads = width // 768
    first = part * heads
    return pl.pallas_call(
        bwd_kernel,
        out_shape=(jax.ShapeDtypeStruct((T, width // 2), jnp.bfloat16), jax.ShapeDtypeStruct((heads, 1, 384), jnp.float32)),
        grid_spec=pltpu.PrefetchScalarGridSpec(
            num_scalar_prefetch=2, grid=(heads,),
            in_specs=[
                pl.BlockSpec((T, 384), lambda h, *_: (0, first + h)),
                pl.BlockSpec((T, 128), lambda h, *_: (0, first + h)),
                pl.BlockSpec((1, 2, T), lambda h, *_: (first + h, 0, 0)),
                pl.BlockSpec((1, T), lambda h, *_: (0, 0)),
                pl.BlockSpec((T, 1), lambda h, *_: (0, 0)),
            ],
            out_specs=(pl.BlockSpec((T, 384), lambda h, *_: (0, h)), pl.BlockSpec((1, 1, 384), lambda h, *_: (h, 0, 0))),
            scratch_shapes=[pltpu.VMEM((T, 128), jnp.float32)] * 2 + [pltpu.VMEM((128, T), jnp.bfloat16)],
        ),
        cost_estimate=cost(20 * T * T * width, 6 * T * width, T * T * width // 64),
        name="attn_bwd",
    )(start, count, qkv, do, lse, seg, segc)


MESH_ID = pl.DeviceIdType.MESH


def bits_of():
    rep = lax.axis_index("rep")
    fsdp = lax.axis_index("fsdp")
    return dict(
        rep=rep, fsdp=fsdp, x=rep // 2, c=rep % 2, z1=fsdp // 4, z0=(fsdp // 2) % 2, y=fsdp % 2
    )


def partner_of(at, which):
    rep, fsdp = at["rep"], at["fsdp"]
    if which == "c":
        rep = rep + 1 - 2 * at["c"]
    elif which == "x":
        rep = rep + 2 - 4 * at["x"]
    elif which == "y":
        fsdp = fsdp + 1 - 2 * at["y"]
    elif which == "z0":
        fsdp = fsdp + 2 - 4 * at["z0"]
    elif which == "z1":
        fsdp = fsdp + 4 - 8 * at["z1"]
    else:
        rep = rep + 1 - 2 * at["c"]
        fsdp = fsdp + 2 - 4 * at["z0"]
    return (rep, fsdp)


REL = [(a, b, d) for d in (0, 1) for b in (0, 1) for a in (0, 1)]


def gather_kernel(
    qkv_in, wo_in, vec_in, tok_in, seg_in,
    qkv_out, wo_out, vec_out, tok_out, seg_out,
    tok_buf, seg_buf, send_sem, recv_sem, local_sem,
):
    at = bits_of()
    other = {k: partner_of(at, k) for k in ("c", "x", "y", "z0", "z1", "swap")}
    barrier = pltpu.get_barrier_semaphore()
    for k in ("c", "x", "y", "z0", "z1"):
        pl.semaphore_signal(barrier, inc=1, device_id=other[k], device_id_type=MESH_ID)
    moves = at["c"] != at["z0"]

    @pl.when(moves)
    def _():
        pl.semaphore_signal(barrier, inc=1, device_id=other["swap"], device_id_type=MESH_ID)
        pl.semaphore_wait(barrier, 6)

    @pl.when(jnp.logical_not(moves))
    def _():
        pl.semaphore_wait(barrier, 5)

    def flip(bit, rel):
        return bit + rel - 2 * bit * rel

    def shard(rel):
        return 4 * flip(at["z1"], rel[1]) + 2 * flip(at["z0"], rel[0]) + flip(at["y"], rel[2])

    counter = [0]
    started = []

    def send(src, dst, which):
        k = counter[0]
        counter[0] += 1
        copy = pltpu.make_async_remote_copy(
            src_ref=src, dst_ref=dst, send_sem=send_sem.at[k], recv_sem=recv_sem.at[k],
            device_id=other[which], device_id_type=MESH_ID,
        )
        copy.start()
        started.append(copy)
        return copy

    class Piece:
        def __init__(self, own, slot, split_x):
            self.own, self.slot, self.split_x = own, slot, split_x
            self.part = (2 * at["x"] + at["c"]) if split_x else at["c"]
            self.part_x = (2 * (1 - at["x"]) + at["c"]) if split_x else None
            self.copies = {}

        def first(self):
            zero = (0, 0, 0)
            for which in ("z1", "z0", "y"):
                self.copies[which, zero] = send(
                    self.own(self.part), self.slot(shard(zero), self.part), which
                )
            self.copies["c", zero] = send(self.own(None), self.slot(shard(zero), None), "c")

        def onward(self, rel):
            here = self.slot(shard(rel), self.part)
            if rel == (0, 1, 0):
                self.copies["z0", rel] = send(here, here, "z0")
            if rel[2] == 0:
                self.copies["y", rel] = send(here, here, "y")
            if self.split_x:
                self.copies["x", rel] = send(here, here, "x")
            self.copies["c", rel] = send(here, here, "c")

        def arrive(self, which, came):
            self.copies[which, came].wait_recv()
            step = {"z0": (1, 0, 0), "z1": (0, 1, 0), "y": (0, 0, 1)}[which]
            self.onward(tuple(p + q for p, q in zip(came, step)))

        def near(self):
            self.arrive("z1", (0, 0, 0))
            self.arrive("z0", (0, 0, 0))

        def rest(self):
            self.arrive("y", (0, 0, 0))
            self.arrive("z0", (0, 1, 0))
            self.arrive("y", (0, 1, 0))
            self.arrive("y", (1, 0, 0))
            self.arrive("y", (1, 1, 0))

        def last(self):
            if self.split_x:
                for rel in REL[1:]:
                    self.copies["x", rel].wait_recv()
                    there = self.slot(shard(rel), self.part_x)
                    self.copies["cx", rel] = send(there, there, "c")

        def finish(self):
            for (which, rel), copy in self.copies.items():
                if which in ("c", "cx"):
                    copy.wait_recv()

    def rows(ref, count):
        full = ref.shape[-2] // 8
        def slot(f, part):
            if part is None:
                at_row, n = f * full, full
            else:
                at_row, n = f * full + part * (full // count), full // count
            at_row = pl.multiple_of(at_row, 8)
            return ref.at[pl.ds(at_row, n), :]
        return slot

    def own_rows(ref, count):
        full = ref.shape[-2]
        def own(part):
            if part is None:
                return ref
            row = pl.multiple_of(part * (full // count), 8)
            n = full // count
            return ref.at[pl.ds(row, n), :]
        return own

    qkv, wo = pieces = [
        Piece(own_rows(qkv_in, 4), rows(qkv_out, 4), True),
        Piece(own_rows(wo_in, 4), rows(wo_out, 4), True),
    ]
    zero = (0, 0, 0)
    vec_copies = [
        send(vec_in, vec_out.at[shard(zero)], which) for which in ("c", "z1", "z0", "y")
    ]
    pieces[0].first()
    tok_k, seg_k = counter[0], counter[0] + 1
    counter[0] += 2

    def swap_copy(src, dst, k):
        return pltpu.make_async_remote_copy(
            src_ref=src, dst_ref=dst, send_sem=send_sem.at[k], recv_sem=recv_sem.at[k],
            device_id=other["swap"], device_id_type=MESH_ID,
        )

    @pl.when(moves)
    def _():
        swap_copy(tok_in, tok_out, tok_k).start()
        swap_copy(seg_in, seg_out, seg_k).start()

    @pl.when(jnp.logical_not(moves))
    def _():
        one = pltpu.make_async_copy(tok_in, tok_buf, local_sem.at[0])
        two = pltpu.make_async_copy(seg_in, seg_buf, local_sem.at[1])
        one.start()
        two.start()
        one.wait()
        two.wait()
        three = pltpu.make_async_copy(tok_buf, tok_out, local_sem.at[0])
        four = pltpu.make_async_copy(seg_buf, seg_out, local_sem.at[1])
        three.start()
        four.start()
        three.wait()
        four.wait()

    wo.first()
    qkv.near()
    vec_copies[1].wait_recv()
    here = vec_out.at[shard((0, 1, 0))]
    vec_far = send(here, here, "z0")
    vec_more = [send(here, here, "y")]
    vec_copies[2].wait_recv()
    here = vec_out.at[shard((1, 0, 0))]
    vec_more.append(send(here, here, "y"))
    qkv.rest()
    wo.near()
    wo.rest()
    vec_far.wait_recv()
    here = vec_out.at[shard((1, 1, 0))]
    vec_more.append(send(here, here, "y"))
    qkv.last()
    wo.last()
    for piece in pieces:
        piece.finish()
    for copy in [vec_copies[0], vec_copies[3]] + vec_more:
        copy.wait_recv()
    for copy in started:
        copy.wait_send()

    @pl.when(moves)
    def _():
        swap_copy(tok_in, tok_out, tok_k).wait()
        swap_copy(seg_in, seg_out, seg_k).wait()


GATHER_COPIES = 29 * 2 + 8 + 2


def gather_all(qkv, wo, vec, tok, seg):
    bf = jnp.bfloat16
    shape = jax.ShapeDtypeStruct
    whole = pl.BlockSpec(memory_space=pl.ANY)
    return pl.pallas_call(
        gather_kernel,
        out_shape=(
            shape((8 * qkv.shape[0], qkv.shape[1]), bf),
            shape((8 * wo.shape[0], wo.shape[1]), bf),
            shape((8,) + vec.shape, bf),
            shape(tok.shape, bf),
            shape(seg.shape, seg.dtype),
        ),
        in_specs=[whole] * 5,
        out_specs=(whole,) * 5,
        scratch_shapes=[
            pltpu.VMEM(tok.shape, bf),
            pltpu.VMEM(seg.shape, seg.dtype),
            pltpu.SemaphoreType.DMA((GATHER_COPIES,)),
            pltpu.SemaphoreType.DMA((GATHER_COPIES,)),
            pltpu.SemaphoreType.DMA((2,)),
        ],
        compiler_params=pltpu.CompilerParams(collective_id=0, has_side_effects=True),
        name="gather_weights",
    )(qkv, wo, vec, tok, seg)


SHRINK = 1000
BF, F32 = jnp.bfloat16, jnp.float32
SHAPE = jax.ShapeDtypeStruct


def full_spec(shape):
    return pl.BlockSpec(shape, lambda *_: (0,) * len(shape), pipeline_mode=pl.Buffered(1))


def cost(flops, moved, exps=0):
    return pl.CostEstimate(flops=int(flops) // SHRINK, bytes_accessed=int(moved) // SHRINK, transcendentals=int(exps) // SHRINK)


def qkv_kernel(x_ref, w_ref, bias_ref, scale_ref, o_ref):
    for i in range(4):
        rows = slice(i * 256, (i + 1) * 256)
        z = dot(x_ref[rows, :], w_ref[...], 1, 0)
        o_ref[rows, :] = ((z + bias_ref[...]) * scale_ref[...]).astype(BF)


def qkv_call(x, w, bias, scale):
    tokens, width = x.shape[0], w.shape[1]
    tile = 768
    return pl.pallas_call(
        qkv_kernel,
        out_shape=SHAPE((tokens, width), BF),
        grid=(width // tile,),
        in_specs=[
            full_spec(x.shape),
            pl.BlockSpec((x.shape[1], tile), lambda j: (0, j)),
            pl.BlockSpec((1, tile), lambda j: (0, j)),
            pl.BlockSpec((1, tile), lambda j: (0, j)),
        ],
        out_specs=pl.BlockSpec((tokens, tile), lambda j: (0, j)),
        cost_estimate=cost(2 * tokens * D * width, 2 * (tokens * D + D * width + tokens * width)),
        name="qkv",
    )(x, w, bias, scale)


def mean_row(value):
    return jnp.mean(value, axis=-1, keepdims=True)


def mix_kernel(c_ref, w_ref, x_ref, rows_ref, n_ref, q_ref, low_ref):
    value = x_ref[...].astype(F32) + dot(c_ref[...], w_ref[...], 1, 0) + rows_ref[6:7, :]
    center = value - mean_row(value)
    inv = lax.rsqrt(mean_row(center * center) + 1e-05)
    normed = center * inv
    n_ref[...] = normed
    q_ref[...] = inv
    low_ref[...] = (normed * rows_ref[0:1, :] + rows_ref[2:3, :]).astype(BF)


def mix_call(mixed, w_out, tok, rows):
    t = tok.shape[0]
    tile = pl.BlockSpec((256, D), lambda i: (i, 0))
    return pl.pallas_call(
        mix_kernel,
        out_shape=(SHAPE((t, D), F32), SHAPE((t, 1), F32), SHAPE((t, D), BF)),
        grid=(t // 256,),
        in_specs=[tile, full_spec((D, D)), tile, full_spec(rows.shape)],
        out_specs=(tile, pl.BlockSpec((256, 1), lambda i: (i, 0)), tile),
        cost_estimate=cost(2 * t * D * D, 12 * t * D + 2 * D * D),
        name="mix_norm",
    )(mixed, w_out, tok, rows)


def up_kernel(place_ref, h_ref, *refs):
    parts, (bias_ref, g_ref, s_ref) = refs[:4], refs[4:]
    each = pl.num_programs(0) // 4

    def tile(w_ref):
        for i in range(8):
            rows = slice(i * 128, (i + 1) * 128)
            z = dot(h_ref[rows, :], w_ref[...], 1, 0) + bias_ref[...]
            phi, bell = erf_parts(z)
            g_ref[rows, :] = (z * phi).astype(BF)
            s_ref[rows, :] = (phi + z * bell * 0.3989422804014327).astype(BF)

    for k in range(4):
        pl.when(pl.program_id(0) // each == k)(partial(tile, parts[k]))


def up_call(low, parts, place, bias):
    t = low.shape[0]
    tile = 512
    each = FF // tile // 4
    where = lambda j, p: (0, p[j // each] * each + lax.rem(j, each))
    out = pl.BlockSpec((t, tile), where)

    def part(k):
        return pl.BlockSpec((D, tile), lambda j, p: (0, jnp.clip(j - k * each, 0, each - 1)))

    return pl.pallas_call(
        up_kernel,
        out_shape=(SHAPE((t, FF), BF), SHAPE((t, FF), BF)),
        grid_spec=pltpu.PrefetchScalarGridSpec(
            num_scalar_prefetch=1, grid=(FF // tile,),
            in_specs=[full_spec(low.shape)] + [part(k) for k in range(4)] + [pl.BlockSpec((1, tile), where)],
            out_specs=(out, out),
        ),
        cost_estimate=cost(2 * t * D * FF, 2 * (t * D + D * FF + 2 * t * FF), 2 * t * FF),
        name="up_gelu",
    )(place, low, *parts, bias)


def row_sum(value):
    return jnp.sum(value, axis=0, keepdims=True)


def norm_back(grad, normed, inv, gain):
    scaled = grad * gain
    return inv * (scaled - mean_row(scaled) - normed * mean_row(scaled * normed))


def down_kernel(
    core_ref, g_ref, own_ref, came_ref, n_ref, cot_ref, rows_ref, out_ref, dr_ref, dm_ref, sums_ref, m_ref
):
    half = D // 2
    m_ref[:, pl.ds(pl.multiple_of(core_ref[0] * half, half), half)] = dot(g_ref[...], own_ref[...], 1, 0)
    m_ref[:, pl.ds(pl.multiple_of((1 - core_ref[0]) * half, half), half)] = dot(g_ref[...], came_ref[...], 1, 0)
    hidden = n_ref[...] * rows_ref[0:1, :] + rows_ref[2:3, :]
    value = hidden + m_ref[...] + rows_ref[7:8, :]
    center = value - mean_row(value)
    inv = lax.rsqrt(mean_row(center * center) + 1e-05)
    normed = center * inv
    gain = rows_ref[1:2, :]
    out_ref[...] = (normed * gain + rows_ref[3:4, :]).astype(BF)
    grad = cot_ref[...].astype(F32)
    back = norm_back(grad, normed, inv, gain)
    low = back.astype(BF)
    dr_ref[...] = back
    dm_ref[...] = low

    @pl.when(pl.program_id(0) == 0)
    def _():
        sums_ref[...] = jnp.zeros_like(sums_ref)

    sums_ref[0:1, :] += row_sum(grad * normed)
    sums_ref[1:2, :] += row_sum(grad)
    sums_ref[2:3, :] += row_sum(low.astype(F32))


def down_call(act, own, came, normed, cot, rows, core):
    t = act.shape[0]
    tile = pl.BlockSpec((256, D), lambda i, c: (i, 0))
    return pl.pallas_call(
        down_kernel,
        out_shape=(SHAPE((t, D), BF), SHAPE((t, D), F32), SHAPE((t, D), BF), SHAPE((8, D), F32)),
        grid_spec=pltpu.PrefetchScalarGridSpec(
            num_scalar_prefetch=1, grid=(t // 256,),
            in_specs=[
                pl.BlockSpec((256, FF), lambda i, c: (i, 0)), full_spec((FF, D // 2)), full_spec((FF, D // 2)),
                tile, tile, full_spec(rows.shape),
            ],
            out_specs=(tile, tile, tile, pl.BlockSpec((8, D), lambda i, c: (0, 0))),
            scratch_shapes=[pltpu.VMEM((256, D), F32)],
        ),
        cost_estimate=cost(2 * t * D * FF, 2 * (t * FF + D * FF) + 14 * t * D),
        name="down_norm",
    )(core.reshape(1), act, own, came, normed, cot, rows)


def slope_kernel(core_ref, left_ref, right_ref, own_ref, came_ref, s_ref, o_ref, sums_ref):
    total = 0.0
    for i in range(4):
        rows = slice(i * 256, (i + 1) * 256)
        back = dot(left_ref[rows, :], own_ref[...], 1, 1) + dot(right_ref[rows, :], came_ref[...], 1, 1)
        z = (back * s_ref[rows, :].astype(F32)).astype(BF)
        o_ref[rows, :] = z
        total = total + row_sum(z.astype(F32))
    sums_ref[...] = total


def slope_call(dm, own, came, slope, core):
    t = dm.shape[0]
    tile = 512
    wide = pl.BlockSpec((t, tile), lambda j, c: (0, j))
    part = pl.BlockSpec((tile, D // 2), lambda j, c: (j, 0))
    return pl.pallas_call(
        slope_kernel,
        out_shape=(SHAPE((t, FF), BF), SHAPE((1, FF), F32)),
        grid_spec=pltpu.PrefetchScalarGridSpec(
            num_scalar_prefetch=1, grid=(FF // tile,),
            in_specs=[
                pl.BlockSpec((t, D // 2), lambda j, c: (0, c[0])),
                pl.BlockSpec((t, D // 2), lambda j, c: (0, 1 - c[0])),
                part, part, wide,
            ],
            out_specs=(wide, pl.BlockSpec((1, tile), lambda j, c: (0, j))),
        ),
        cost_estimate=cost(2 * t * D * FF, 2 * (t * D + D * FF + 2 * t * FF)),
        name="down_back",
    )(core.reshape(1), dm, dm, own, came, slope)


def hidden_kernel(place_ref, *refs):
    grads, parts = refs[:4], refs[4:8]
    dr_ref, n_ref, q_ref, wo_ref, rows_ref, r_ref, a_ref, c_ref, sums_ref = refs[8:]
    grad = dr_ref[...]
    for grad_ref, w_ref in zip(grads, parts):
        grad = grad + dot(grad_ref[...], w_ref[...], 1, 1)
    normed = n_ref[...]
    back = norm_back(grad, normed, q_ref[...], rows_ref[0:1, :])
    low = back.astype(BF)
    r_ref[...] = back
    a_ref[...] = low
    c_ref[...] = dot(low, wo_ref[...], 1, 1).astype(BF)

    @pl.when(pl.program_id(0) == 0)
    def _():
        sums_ref[...] = jnp.zeros_like(sums_ref)

    sums_ref[0:1, :] += row_sum(grad * normed)
    sums_ref[1:2, :] += row_sum(grad)
    sums_ref[2:3, :] += row_sum(low.astype(F32))


def hidden_call(dz, parts, place, dr, normed, inv, w_out, rows):
    t = dz.shape[0]
    tile = pl.BlockSpec((256, D), lambda i, p: (i, 0))

    def quarter(k):
        return pl.BlockSpec((256, FF // 4), lambda i, p: (i, p[k]))

    return pl.pallas_call(
        hidden_kernel,
        out_shape=(SHAPE((t, D), F32), SHAPE((t, D), BF), SHAPE((t, D), BF), SHAPE((8, D), F32)),
        grid_spec=pltpu.PrefetchScalarGridSpec(
            num_scalar_prefetch=1, grid=(t // 256,),
            in_specs=[quarter(k) for k in range(4)] + [full_spec((D, FF // 4))] * 4 + [
                tile, tile,
                pl.BlockSpec((256, 1), lambda i, p: (i, 0)), full_spec((D, D)), full_spec(rows.shape),
            ],
            out_specs=(tile, tile, tile, pl.BlockSpec((8, D), lambda i, p: (0, 0))),
        ),
        cost_estimate=cost(2 * t * D * (FF + D), 2 * (t * FF + D * FF) + 16 * t * D),
        name="up_back_norm",
    )(place, *([dz] * 4), *parts, dr, normed, inv, w_out, rows)


def input_kernel(a_ref, b_ref, w_ref, r_ref, o_ref):
    half = a_ref.shape[1]
    value = dot(a_ref[...], w_ref[:, :half], 1, 1) + dot(b_ref[...], w_ref[:, half:], 1, 1)
    o_ref[...] = (r_ref[...] + value).astype(BF)


def input_call(part_a, part_b, w_qkv, resid):
    t, width = part_a.shape
    tile = pl.BlockSpec((256, D), lambda i: (i, 0))
    wide = pl.BlockSpec((256, width), lambda i: (i, 0))
    return pl.pallas_call(
        input_kernel,
        out_shape=SHAPE((t, D), BF),
        grid=(t // 256,),
        in_specs=[wide, wide, full_spec(w_qkv.shape), tile],
        out_specs=tile,
        cost_estimate=cost(4 * t * D * width, 4 * (t * width + D * width) + 6 * t * D),
        name="input_back",
    )(part_a, part_b, w_qkv, resid)


def weight_kernel(half_ref, first_ref, second_ref, right_ref, *refs):
    o_ref, turned = refs[-2], refs[-1]

    @pl.when(pl.program_id(1) == 0)
    def _():
        part = first_ref.shape[1]
        turned[:part, :] = first_ref[...].T
        turned[part:, :] = second_ref[...].T

    value = dot(turned[...], right_ref[...], 1, 0)
    if len(refs) == 3:
        value = value + refs[0][...].astype(F32)
    o_ref[...] = value.astype(BF)


def weight_call(left, right, half, came=None):
    t, rows = left.shape
    width = right.shape[1]
    bm = 512
    bn = 1024 if width == 1024 else 512
    steps = rows // 2 // bm
    if steps == 1:
        first = lambda i, j, h: (0, h[0])
        second = lambda i, j, h: (0, 2 + h[0])
    else:
        block = lambda i, h: lax.div(i, steps // 2) * steps + h[0] * (steps // 2) + lax.rem(i, steps // 2)
        first = lambda i, j, h: (0, 2 * block(i, h))
        second = lambda i, j, h: (0, 2 * block(i, h) + 1)
    specs = [
        pl.BlockSpec((t, bm // 2), first),
        pl.BlockSpec((t, bm // 2), second),
        pl.BlockSpec((t, bn), lambda i, j, h: (0, j)),
    ]
    values = [left, left, right]
    out = pl.BlockSpec((bm, bn), lambda i, j, h: (i, j))
    if came is not None:
        specs.append(out)
        values.append(came)
    return pl.pallas_call(
        weight_kernel,
        out_shape=SHAPE((rows // 2, width), BF),
        grid_spec=pltpu.PrefetchScalarGridSpec(
            num_scalar_prefetch=1, grid=(steps, width // bn), in_specs=specs, out_specs=out,
            scratch_shapes=[pltpu.VMEM((bm, t), BF)],
        ),
        cost_estimate=cost(t * rows * width, t * rows + 2 * t * width + 2 * rows * width),
        name="weight_grad",
    )(half.reshape(1), *values)


def inner_kernel(rate, decay, w_ref, g_ref, m_ref, v_ref, m_out, v_out, d_out):
    weight = w_ref[...]
    new, m_out[...], v_out[...] = inner_step(
        weight, g_ref[...].astype(F32), m_ref[...], v_ref[...], rate, decay
    )
    d_out[...] = (weight - new).astype(BF)


def inner_call(weight, grad, first, second, rate, decay):
    rows, width = weight.shape
    block = 32 * 4096 // width
    tile = pl.BlockSpec((block, width), lambda i: (i, 0))
    like = SHAPE((rows, width), F32)
    return pl.pallas_call(
        partial(inner_kernel, rate, decay),
        out_shape=(like, like, SHAPE((rows, width), BF)),
        grid=(rows // block,),
        in_specs=[tile] * 4,
        out_specs=(tile,) * 3,
        cost_estimate=cost(20 * rows * width, 24 * rows * width),
        name="inner_step",
    )(weight, grad, first, second)


def outer_kernel(core_ref, w_ref, u_ref, own_ref, came_ref, o_ref, c_ref):
    mine = (core_ref[0] == pl.program_id(0)).astype(F32)
    total = own_ref[...].astype(F32) * mine + came_ref[...].astype(F32) * (1.0 - mine)
    mean = total * 0.25
    weight = w_ref[...]
    momentum = 0.5 * u_ref[...] + mean
    new = weight - 0.7 * (mean + 0.5 * momentum)
    o_ref[0] = mean
    o_ref[1] = momentum
    o_ref[2] = new
    c_ref[...] = new.astype(BF)


def outer_call(weight, momentum, own, came, core):
    rows, width = weight.shape
    block = 32 * 4096 // width
    steps = rows // 2 // block
    tile = pl.BlockSpec((block, width), lambda h, i, c: (h * steps + i, 0))
    part = pl.BlockSpec((block, width), lambda h, i, c: (i, 0))
    return pl.pallas_call(
        outer_kernel,
        out_shape=(SHAPE((3, rows, width), F32), SHAPE((rows, width), BF)),
        grid_spec=pltpu.PrefetchScalarGridSpec(
            num_scalar_prefetch=1, grid=(2, steps), in_specs=[tile, tile, part, part],
            out_specs=(pl.BlockSpec((3, block, width), lambda h, i, c: (0, h * steps + i, 0)), tile),
        ),
        cost_estimate=cost(10 * rows * width, 26 * rows * width),
        name="outer_step",
    )(core.reshape(1), weight, momentum, own, came)


def erf_parts(value):
    size = jnp.abs(value) * 0.7071067811865476
    share = 1.0 / (1.0 + 0.5 * size)
    inner = 0.17087277
    for coefficient in (
        -0.82215223, 1.48851587, -1.13520398, 0.27886807, -0.18628806, 0.09678418, 0.37409196, 1.00002368
    ):
        inner = coefficient + share * inner
    square = size * size
    half = 0.5 * share * jnp.exp(share * inner - 1.26551223 - square)
    return jnp.where(value >= 0, 1.0 - half, half), jnp.exp(-square)


def xor_pairs(bits):
    place = {"y": 0, "z0": 1, "z1": 2, "c": 3, "x": 4}
    flip = sum(1 << place[bit] for bit in bits)
    pairs = []
    for device in range(32):
        if bits == ("c", "z0") and ((device >> 3) & 1) == ((device >> 1) & 1):
            continue
        pairs.append((device, device ^ flip))
    return pairs


def exchange(value, *bits):
    return lax.ppermute(value, ("rep", "fsdp"), xor_pairs(bits))


def add_low(left, right):
    return (left.astype(jnp.float32) + right.astype(jnp.float32)).astype(jnp.bfloat16)


def pick(value, index, axis):
    return lax.dynamic_index_in_dim(value, index, axis, keepdims=False)


def half_axis(total, which):
    return 1 if which == "y" and total.ndim == 4 else 0


def halve(at, total, which):
    away = pick(total, 1 - at[which], half_axis(total, which))
    return away, exchange(away, which)


def join(at, total, came, which, *gates):
    return add_low(pick(total, at[which], half_axis(total, which)), after(came, *gates))


def slabs(total):
    return total.reshape(2, 2, -1, total.shape[-1])


def after(value, *earlier):
    return lax.optimization_barrier((value,) + earlier)[0]


def weave(value):
    rows = value.shape[1]
    return jnp.transpose(value.reshape(3, rows, D // 128, 128), (1, 2, 0, 3)).reshape(rows, 3 * D)


def unweave(value):
    rows = value.shape[0]
    return jnp.transpose(value.reshape(rows, D // 128, 3, 128), (2, 0, 1, 3)).reshape(3, rows, D)


def per_device_fast(
    tokens,
    cotangent,
    segment_ids,
    attention_weight,
    attention_momentum,
    attention_first,
    attention_second,
    expand_weight,
    expand_momentum,
    expand_first,
    expand_second,
    contract_weight,
    contract_momentum,
    contract_first,
    contract_second,
    vectors,
    vectors_momentum,
    vectors_first,
    vectors_second,
):
    bf, f32 = jnp.bfloat16, jnp.float32
    at = bits_of()
    core = at["c"].astype(jnp.int32)
    def swapped(value, came):
        return jnp.where(at["c"] != at["z0"], came, value)

    def cross(value):
        return exchange(value, "c", "z0")

    quarter = 2 * core + at["x"].astype(jnp.int32)
    place = jnp.stack([quarter, 2 * (1 - core) + quarter - 2 * core, quarter + 1 - 2 * at["x"], 3 - quarter])
    part = expand_weight.shape[1] // 4
    in_own = lax.all_gather(
        lax.dynamic_slice_in_dim(expand_weight, quarter * part, part, axis=1).astype(bf), "fsdp", axis=0, tiled=True
    )
    attn_low = attention_weight.astype(bf)
    w_qkv, w_out, vector_full, tok, seg = gather_all(
        weave(attn_low[:3]), attn_low[3], vectors.astype(bf), tokens, segment_ids,
    )
    cot_came = cross(after(cotangent, w_qkv))
    rows = jnp.swapaxes(vector_full, 0, 1).reshape(-1, D).astype(f32)
    bias_up = rows[8:].reshape(1, FF)
    bias_qkv = weave(jnp.stack([rows[4], jnp.zeros_like(rows[4]), rows[5]])[:, None])
    scale_qkv = weave(jnp.stack([jnp.full((1, D), 0.125, f32)] + [jnp.ones((1, D), f32)] * 2))
    part = contract_weight.shape[1] // 2
    down_half = lax.dynamic_slice_in_dim(contract_weight, core * part, part, axis=1).astype(bf)
    down_own = lax.all_gather(after(down_half, w_qkv), "fsdp", axis=0, tiled=True)
    in_near = after(in_own, w_qkv)
    in_far = exchange(in_near, "x")
    in_side = exchange(in_near, "c")
    qkv = qkv_call(tok, w_qkv, bias_qkv, scale_qkv)
    mixed, log_sum = attn_fwd(qkv, seg)
    in_parts = [in_own, after(in_side, mixed), in_far, exchange(after(in_far, mixed), "c")]
    normed, inv, hidden_low = mix_call(mixed, w_out, tok, rows)
    cot = swapped(cotangent, after(cot_came, hidden_low))
    activated, slope = up_call(after(hidden_low, cot), in_parts, place, bias_up)
    down_other = exchange(after(down_own, activated), "c")
    layer_output, grad_sum, grad_branch, sums_two = down_call(
        activated, down_own, down_other, normed, cot, rows, core
    )
    output_came = cross(layer_output)
    down_send = weight_call(activated, grad_branch, 1 - core)
    grad_pre, sums_up = slope_call(after(grad_branch, down_send), down_own, down_other, slope, core)
    down_came = exchange(down_send, "c")
    up_send = weight_call(hidden_low, grad_pre, 1 - core)
    down_total = slabs(weight_call(activated, after(grad_branch, up_send), core, down_came))
    up_came = exchange(up_send, "c")
    away_d, came_d = halve(at, down_total, "y")
    up_total = slabs(weight_call(hidden_low, after(grad_pre, away_d), core, up_came))
    away_u, came_u = halve(at, up_total, "z1")
    grad_resid, grad_attn, grad_mixed, sums_one = hidden_call(
        after(grad_pre, away_u), in_parts, place, grad_sum, normed, inv, w_out, rows
    )
    proj_send = weight_call(mixed, grad_attn, 1 - core)
    proj_came = exchange(proj_send, "c")
    output = swapped(layer_output, after(output_came, proj_send))
    grad_a, sums_a = attn_bwd(qkv, after(grad_mixed, proj_send, output), log_sum, seg, 0)
    send_a = weight_call(tok, grad_a, 1 - core)
    came_a = exchange(send_a, "c")
    down_one = join(at, down_total, came_d, "y", send_a)
    away_d, came_d = halve(at, down_one, "z1")
    proj_total = slabs(weight_call(mixed, after(grad_attn, away_d), core, proj_came))
    away_p, came_p = halve(at, proj_total, "y")
    total_a = slabs(weight_call(tok, after(grad_a, away_p), core, came_a))
    away_a, came_one = halve(at, total_a, "y")
    up_one = join(at, up_total, came_u, "z1", away_a)
    away_u, came_u = halve(at, up_one, "y")
    grad_b, sums_b = attn_bwd(qkv, after(grad_mixed, away_u), log_sum, seg, 1)
    send_b = weight_call(tok, grad_b, 1 - core)
    came_b = exchange(send_b, "c")
    down_two = join(at, down_one, came_d, "z1", send_b)
    cross_d = cross(down_two)
    up_two = join(at, up_one, came_u, "y", down_two)
    cross_u = cross(up_two)
    proj_one = join(at, proj_total, came_p, "y", up_two)
    away_p, came_p = halve(at, proj_one, "z1")
    a_one = join(at, total_a, came_one, "y", away_p)
    away_a, came_a = halve(at, a_one, "z1")
    total_b = slabs(weight_call(tok, after(grad_b, away_a), core, came_b))
    away_b, came_b = halve(at, total_b, "y")
    sums_qkv = jnp.concatenate([sums_a, sums_b], axis=0).reshape(D // 128, 3, 128)
    vector_grad = jnp.concatenate(
        [
            sums_one[0:1],
            sums_two[0:1],
            sums_one[1:2],
            sums_two[1:2],
            sums_qkv[:, 0].reshape(1, D),
            sums_qkv[:, 2].reshape(1, D),
            sums_one[2:3],
            sums_two[2:3],
            sums_up.reshape(FF // D, D),
        ],
        axis=0,
    )

    def vector_send(parts, which):
        half = parts.shape[1] // 2
        away = lax.dynamic_slice_in_dim(parts, (1 - at[which]) * half, half, axis=1)
        return exchange(away, which)

    def vector_join(parts, came, which, *gates):
        half = parts.shape[1] // 2
        return lax.dynamic_slice_in_dim(parts, at[which] * half, half, axis=1) + after(came, *gates)

    vec_came = vector_send(vector_grad, "z1")
    input_grad = input_call(after(grad_a, away_b), grad_b, w_qkv, grad_resid)
    vec_one = vector_join(vector_grad, vec_came, "z1", input_grad)
    vec_came = vector_send(vec_one, "c")
    def inner(weight, grad, first, second, rate, decay):
        flat = (-1, weight.shape[-1])
        return inner_call(
            weight.reshape(flat), grad.reshape(flat), first.reshape(flat), second.reshape(flat), rate, decay
        )

    def rep_send(diff):
        halves = diff.reshape(2, diff.shape[0] // 2, diff.shape[1])
        away = pick(halves, 1 - at["c"], 0)
        return away, exchange(away, "c")

    def rep_join(diff, came, *gates):
        halves = diff.reshape(2, diff.shape[0] // 2, diff.shape[1])
        return add_low(pick(halves, at["c"], 0), after(came, *gates))

    def outer(weight, momentum, own, came):
        flat = (-1, weight.shape[-1])
        return outer_call(weight.reshape(flat), momentum.reshape(flat), own, came, core)

    proj_two = join(at, proj_one, came_p, "z1", input_grad)
    a_two = join(at, a_one, came_a, "z1", input_grad)
    cross_pa = cross(jnp.concatenate([proj_two, a_two], axis=1))
    grad_contract = swapped(down_two, after(cross_d, proj_two, a_two))
    contract_new = inner(contract_weight, grad_contract, contract_first, contract_second, 0.015, 0.1)
    sent_c, came_c = rep_send(contract_new[2])
    b_one = join(at, total_b, came_b, "y", sent_c)
    away_b, came_b = halve(at, b_one, "z1")
    vec_two = vector_join(vec_one, vec_came, "c", away_b)
    vec_came = vector_send(vec_two, "y")
    grad_expand = swapped(up_two, after(cross_u, away_b))
    expand_new = inner(expand_weight, grad_expand, expand_first, expand_second, 0.03, 0.1)
    sent_e, came_e = rep_send(expand_new[2])
    half_c = rep_join(contract_new[2], came_c, sent_e)
    rest_c = exchange(half_c, "x")
    b_two = join(at, b_one, came_b, "z1", half_c)
    cross_b = cross(b_two)
    half_e = rep_join(expand_new[2], came_e, b_two)
    rest_e = exchange(half_e, "x")
    vec_three = vector_join(vec_two, vec_came, "y", half_e)
    vec_cross = cross(vec_three)
    full_c = add_low(half_c, after(rest_c, half_e))
    back_c = exchange(full_c, "c")
    pa = swapped(jnp.concatenate([proj_two, a_two], axis=1), after(cross_pa, full_c))
    outer_c = outer(contract_weight, contract_momentum, full_c, after(back_c, pa))
    grad_vectors = swapped(vec_three, after(vec_cross, outer_c[1]))
    inner_new, first_new, second_new = inner_step(
        vectors, grad_vectors, vectors_first[0], vectors_second[0], 0.2, 0.0
    )
    vec_diff = (vectors - inner_new).astype(bf)
    vec_near = exchange(vec_diff, "c")
    input_came = cross(after(input_grad, b_two, vec_diff))
    b_own = swapped(b_two, after(cross_b, vec_diff))
    grad_qkv = jnp.concatenate([pa[:, D:], b_own], axis=1)
    grad_attention = jnp.concatenate([unweave(grad_qkv), pa[None, :, :D]], axis=0)
    attention_new = inner(attention_weight, grad_attention, attention_first, attention_second, 0.03, 0.1)
    sent_a, came_a = rep_send(attention_new[2])
    vec_half = add_low(vec_diff, after(vec_near, sent_a))
    vec_far = exchange(vec_half, "x")
    full_e = add_low(half_e, after(rest_e, sent_a))
    back_e = exchange(full_e, "c")
    half_a = rep_join(attention_new[2], came_a, full_e)
    rest_a = exchange(half_a, "x")
    outer_e = outer(expand_weight, expand_momentum, full_e, after(back_e, half_a))
    full_a = add_low(half_a, after(rest_a, outer_e[1]))
    back_a = exchange(full_a, "c")
    mean_diff = add_low(vec_half, after(vec_far, full_a)).astype(f32) / 4
    momentum_new = 0.5 * vectors_momentum + mean_diff
    outer_new = vectors - 0.7 * (mean_diff + 0.5 * momentum_new)
    input_grad = swapped(input_grad, after(input_came, full_a))
    outer_a = outer(attention_weight, attention_momentum, full_a, back_a)
    results = []
    for weight, first, new, (total, copy) in (
        (attention_weight, attention_first, attention_new, outer_a),
        (expand_weight, expand_first, expand_new, outer_e),
        (contract_weight, contract_first, contract_new, outer_c),
    ):
        results += [
            new[0].reshape(first.shape),
            new[1].reshape(first.shape),
            total.reshape((3,) + weight.shape),
            copy.reshape(weight.shape),
        ]
    results += [
        first_new[None],
        second_new[None],
        jnp.stack([mean_diff, momentum_new, outer_new]),
        outer_new.astype(bf),
    ]
    return (output, input_grad) + tuple(results)


def solution(mesh):
    placed = (
        P(("rep", "fsdp"), None),
        P(("rep", "fsdp"), None),
        P(("rep", "fsdp"), None),
        P(None, "fsdp", None),
        P(None, "fsdp", None),
        P("rep", None, "fsdp", None),
        P("rep", None, "fsdp", None),
        P("fsdp", None),
        P("fsdp", None),
        P("rep", "fsdp", None),
        P("rep", "fsdp", None),
        P("fsdp", None),
        P("fsdp", None),
        P("rep", "fsdp", None),
        P("rep", "fsdp", None),
        P(None, "fsdp"),
        P(None, "fsdp"),
        P("rep", None, "fsdp"),
        P("rep", None, "fsdp"),
    )
    small = mesh.shape["rep"] == 4 and mesh.shape["fsdp"] == 8
    body = per_device_fast if small else per_device
    return jax.shard_map(
        body,
        mesh=mesh,
        in_specs=placed,
        out_specs=(
            P(("rep", "fsdp"), None),
            P(("rep", "fsdp"), None),
            P("rep", None, "fsdp", None),
            P("rep", None, "fsdp", None),
            P(None, None, "fsdp", None),
            P(None, "fsdp", None),
            P("rep", "fsdp", None),
            P("rep", "fsdp", None),
            P(None, "fsdp", None),
            P("fsdp", None),
            P("rep", "fsdp", None),
            P("rep", "fsdp", None),
            P(None, "fsdp", None),
            P("fsdp", None),
            P("rep", None, "fsdp"),
            P("rep", None, "fsdp"),
            P(None, None, "fsdp"),
            P(None, "fsdp"),
        ),
        check_vma=False,
    )
```

```python
from functools import partial

import jax
import jax.numpy as jnp
from jax import lax
from jax.experimental import pallas as pl
from jax.experimental.pallas import tpu as pltpu
from jax.sharding import PartitionSpec as P

D = 1024
H = 16
HD = 64
FF = 4096
LEN = 1024
SEQ_DEV = 1
ADAM_STEP = 4
TOK_DEV = 1024


def norm_forward(values_in, gain_row, shift_row):
    center = values_in - jnp.mean(values_in, axis=-1, keepdims=True)
    inv_scale = lax.rsqrt(jnp.mean(center * center, axis=-1, keepdims=True) + 1e-05)
    normed = center * inv_scale
    return (normed * gain_row + shift_row, normed, inv_scale)


def norm_backward(grad_out, normed, inv_scale, gain_row):
    grad_gain = jnp.sum(grad_out * normed, axis=0)
    grad_shift = jnp.sum(grad_out, axis=0)
    scaled_grad = grad_out * gain_row
    grad_value = inv_scale * (
        scaled_grad
        - jnp.mean(scaled_grad, axis=-1, keepdims=True)
        - normed * jnp.mean(scaled_grad * normed, axis=-1, keepdims=True)
    )
    return (grad_value, grad_gain, grad_shift)


def product_over(left, right):
    return lax.dot_general(
        left, right, (((0,), (0,)), ((), ())), preferred_element_type=jnp.float32
    )


def product_back(left, right):
    return lax.dot_general(
        left, right, (((1,), (1,)), ((), ())), preferred_element_type=jnp.float32
    )


def block_scores(query_block, key_block, row_segments, all_segments):
    scores = jnp.einsum("qhd,khd->hqk", query_block, key_block, preferred_element_type=jnp.float32)
    same_doc = row_segments[:, None] == all_segments[None, :]
    return jnp.where(same_doc[None], scores, -1e30)


def inner_step(weight, gradient, first_moment, second_moment, learn_rate, weight_decay):
    first_new = 0.5 * first_moment + 0.5 * gradient
    second_new = 0.75 * second_moment + 0.25 * gradient * gradient
    update_dir = (
        first_new
        / (1.0 - 0.5**ADAM_STEP)
        / (jnp.sqrt(second_new / (1.0 - 0.75**ADAM_STEP)) + 1e-08)
    )
    return (weight - learn_rate * (update_dir + weight_decay * weight), first_new, second_new)


def per_device(
    tokens,
    cotangent,
    segment_ids,
    attention_weight,
    attention_momentum,
    attention_first,
    attention_second,
    expand_weight,
    expand_momentum,
    expand_first,
    expand_second,
    contract_weight,
    contract_momentum,
    contract_first,
    contract_second,
    vectors,
    vectors_momentum,
    vectors_first,
    vectors_second,
):
    attn_full, vector_full = (
        lax.all_gather(attention_weight.astype(jnp.bfloat16), "fsdp", axis=1, tiled=True),
        lax.all_gather(vectors.astype(jnp.bfloat16), "fsdp", axis=1, tiled=True),
    )
    vector_rows = vector_full.astype(jnp.float32)
    gain_one, gain_two, shift_one, shift_two = (
        vector_rows[0],
        vector_rows[1],
        vector_rows[2],
        vector_rows[3],
    )
    bias_query, bias_value, bias_mixed, bias_down = (
        vector_rows[4],
        vector_rows[5],
        vector_rows[6],
        vector_rows[7],
    )
    bias_up = vector_rows[8:].reshape(FF)
    projected = jnp.einsum("td,nde->nte", tokens, attn_full[:3], preferred_element_type=jnp.float32)
    query_all = ((projected[0] + bias_query) * 0.125).astype(jnp.bfloat16)
    key_all = projected[1].astype(jnp.bfloat16)
    value_all = (projected[2] + bias_value).astype(jnp.bfloat16)
    query_heads = query_all.reshape(SEQ_DEV, LEN, H, HD)
    key_heads = key_all.reshape(SEQ_DEV, LEN, H, HD)
    value_heads = value_all.reshape(SEQ_DEV, LEN, H, HD)
    block_rows = min(512, LEN)
    head_group = min(8, H)
    context_rows = []
    log_sums = []
    seq_index = 0
    for row_start in range(0, LEN, block_rows):
        block_pieces = []
        for head_start in range(0, H, head_group):
            head_part = slice(head_start, head_start + head_group)
            scores = block_scores(
                query_heads[seq_index, row_start : row_start + block_rows, head_part],
                key_heads[seq_index, :, head_part],
                segment_ids[seq_index, row_start : row_start + block_rows],
                segment_ids[seq_index],
            )
            row_max = jnp.max(scores, axis=-1, keepdims=True)
            exp_score = jnp.exp(scores - row_max)
            row_total = jnp.sum(exp_score, axis=-1, keepdims=True)
            probability = (exp_score / row_total).astype(jnp.bfloat16)
            block_pieces.append(
                jnp.einsum(
                    "hqk,khd->qhd",
                    probability,
                    value_heads[seq_index, :, head_part],
                    preferred_element_type=jnp.float32,
                )
            )
            log_sums.append(row_max + jnp.log(row_total))
        context_rows.append(jnp.concatenate(block_pieces, axis=1))
    mixed = jnp.concatenate(context_rows, axis=0).reshape(TOK_DEV, D).astype(jnp.bfloat16)
    attn_out = jnp.dot(mixed, attn_full[3], preferred_element_type=jnp.float32) + bias_mixed
    hidden, normed_one, scale_one = norm_forward(
        tokens.astype(jnp.float32) + attn_out, gain_one, shift_one
    )
    hidden_low = hidden.astype(jnp.bfloat16)
    ffn_expand, ffn_contract = (
        lax.all_gather(expand_weight.astype(jnp.bfloat16), "fsdp", axis=0, tiled=True),
        lax.all_gather(contract_weight.astype(jnp.bfloat16), "fsdp", axis=0, tiled=True),
    )
    pre_act = jnp.dot(hidden_low, ffn_expand, preferred_element_type=jnp.float32) + bias_up
    activated = jax.nn.gelu(pre_act, approximate=False).astype(jnp.bfloat16)
    branch = jnp.dot(activated, ffn_contract, preferred_element_type=jnp.float32) + bias_down
    layer_output, normed_two, scale_two = norm_forward(hidden + branch, gain_two, shift_two)
    grad_sum, grad_gain_two, grad_shift_two = norm_backward(
        cotangent.astype(jnp.float32), normed_two, scale_two, gain_two
    )
    grad_branch = grad_sum.astype(jnp.bfloat16)
    grad_act = product_back(grad_branch, ffn_contract)
    unused_value, gelu_pull = jax.vjp(partial(jax.nn.gelu, approximate=False), pre_act)
    grad_pre_low = gelu_pull(grad_act)[0].astype(jnp.bfloat16)
    grad_hidden = grad_sum + product_back(grad_pre_low, ffn_expand)
    contract_full = product_over(activated, grad_branch)
    expand_full = product_over(hidden_low, grad_pre_low)
    grad_expand, grad_contract = (
        lax.psum_scatter(expand_full, "fsdp", scatter_dimension=0, tiled=True),
        lax.psum_scatter(contract_full, "fsdp", scatter_dimension=0, tiled=True),
    )
    grad_resid, grad_gain_one, grad_shift_one = norm_backward(
        grad_hidden, normed_one, scale_one, gain_one
    )
    grad_attn_out = grad_resid.astype(jnp.bfloat16)
    grad_bias_mixed = jnp.sum(grad_attn_out.astype(jnp.float32), axis=0)
    grad_output_proj = product_over(mixed, grad_attn_out)
    grad_mixed = product_back(grad_attn_out, attn_full[3]).astype(jnp.bfloat16)
    grad_context = grad_mixed.reshape(SEQ_DEV, LEN, H, HD)
    query_grads = []
    lse_index = 0
    seq_index = 0
    key_totals = [
        jnp.zeros((LEN, head_group, HD), jnp.float32) for head_start in range(0, H, head_group)
    ]
    value_totals = [
        jnp.zeros((LEN, head_group, HD), jnp.float32) for head_start in range(0, H, head_group)
    ]
    for row_start in range(0, LEN, block_rows):
        block_pieces = []
        for group_index, head_start in enumerate(range(0, H, head_group)):
            head_part = slice(head_start, head_start + head_group)
            query_block = query_heads[seq_index, row_start : row_start + block_rows, head_part]
            key_block = key_heads[seq_index, :, head_part]
            value_block = value_heads[seq_index, :, head_part]
            ctx_grad = grad_context[seq_index, row_start : row_start + block_rows, head_part]
            scores = block_scores(
                query_block,
                key_block,
                segment_ids[seq_index, row_start : row_start + block_rows],
                segment_ids[seq_index],
            )
            probability = jnp.exp(scores - log_sums[lse_index])
            lse_index = lse_index + 1
            value_totals[group_index] = value_totals[group_index] + jnp.einsum(
                "hqk,qhd->khd",
                probability.astype(jnp.bfloat16),
                ctx_grad,
                preferred_element_type=jnp.float32,
            )
            prob_grad = jnp.einsum(
                "qhd,khd->hqk", ctx_grad, value_block, preferred_element_type=jnp.float32
            )
            row_dot = jnp.sum(probability * prob_grad, axis=-1, keepdims=True)
            score_grad = (probability * (prob_grad - row_dot)).astype(jnp.bfloat16)
            block_pieces.append(
                jnp.einsum(
                    "hqk,khd->qhd", score_grad, key_block, preferred_element_type=jnp.float32
                ).astype(jnp.bfloat16)
            )
            key_totals[group_index] = key_totals[group_index] + jnp.einsum(
                "hqk,qhd->khd", score_grad, query_block, preferred_element_type=jnp.float32
            )
        query_grads.append(jnp.concatenate(block_pieces, axis=1))
    key_grads = jnp.concatenate(
        [key_total.astype(jnp.bfloat16) for key_total in key_totals], axis=1
    )
    value_grads = jnp.concatenate(
        [value_total.astype(jnp.bfloat16) for value_total in value_totals], axis=1
    )
    grad_query = jnp.concatenate(query_grads, axis=0).reshape(TOK_DEV, D) * 0.125
    grad_keys = key_grads.reshape(TOK_DEV, D)
    grad_values = value_grads.reshape(TOK_DEV, D)
    stacked_grads = jnp.stack([grad_query, grad_keys, grad_values])
    grad_qkv = jnp.einsum("td,nte->nde", tokens, stacked_grads, preferred_element_type=jnp.float32)
    input_grad = (
        grad_resid
        + jnp.einsum(
            "nte,nde->td", stacked_grads, attn_full[:3], preferred_element_type=jnp.float32
        )
    ).astype(jnp.bfloat16)
    grad_attention_full = jnp.concatenate([grad_qkv, grad_output_proj[None]], axis=0)
    vector_head = jnp.stack(
        [
            grad_gain_one,
            grad_gain_two,
            grad_shift_one,
            grad_shift_two,
            jnp.sum(grad_query.astype(jnp.float32), axis=0),
            jnp.sum(grad_values.astype(jnp.float32), axis=0),
            grad_bias_mixed,
            jnp.sum(grad_branch.astype(jnp.float32), axis=0),
        ]
    )
    grad_bias_up = jnp.sum(grad_pre_low.astype(jnp.float32), axis=0).reshape(FF // D, D)
    grad_vectors_full = jnp.concatenate([vector_head, grad_bias_up], axis=0)
    grad_attention, grad_vectors = (
        lax.psum_scatter(grad_attention_full, "fsdp", scatter_dimension=1, tiled=True),
        lax.psum_scatter(grad_vectors_full, "fsdp", scatter_dimension=1, tiled=True),
    )
    attention_new = inner_step(
        attention_weight, grad_attention, attention_first[0], attention_second[0], 0.03, 0.1
    )
    expand_new = inner_step(
        expand_weight, grad_expand, expand_first[0], expand_second[0], 0.03, 0.1
    )
    contract_new = inner_step(
        contract_weight, grad_contract, contract_first[0], contract_second[0], 0.015, 0.1
    )
    vectors_new = inner_step(vectors, grad_vectors, vectors_first[0], vectors_second[0], 0.2, 0.0)
    summed = (
        lax.psum((attention_weight - attention_new[0]).astype(jnp.bfloat16), "rep").astype(
            jnp.float32
        ),
        lax.psum((expand_weight - expand_new[0]).astype(jnp.bfloat16), "rep").astype(jnp.float32),
        lax.psum((contract_weight - contract_new[0]).astype(jnp.bfloat16), "rep").astype(
            jnp.float32
        ),
        lax.psum((vectors - vectors_new[0]).astype(jnp.bfloat16), "rep").astype(jnp.float32),
    )
    groups_count = lax.axis_size("rep")
    results = []
    for weight_now, momentum_now, inner_new, diff_total in zip(
        (attention_weight, expand_weight, contract_weight, vectors),
        (attention_momentum, expand_momentum, contract_momentum, vectors_momentum),
        (attention_new, expand_new, contract_new, vectors_new),
        summed,
    ):
        mean_diff = diff_total / groups_count
        momentum_new = 0.5 * momentum_now + mean_diff
        outer_new = weight_now - 0.7 * (mean_diff + 0.5 * momentum_new)
        results.append(
            (
                inner_new[1][None],
                inner_new[2][None],
                jnp.stack([mean_diff, momentum_new, outer_new]),
                outer_new.astype(jnp.bfloat16),
            )
        )
    return (
        layer_output.astype(jnp.bfloat16),
        input_grad,
        results[0][0],
        results[0][1],
        results[0][2],
        results[0][3],
        results[1][0],
        results[1][1],
        results[1][2],
        results[1][3],
        results[2][0],
        results[2][1],
        results[2][2],
        results[2][3],
        results[3][0],
        results[3][1],
        results[3][2],
        results[3][3],
    )


NEG=-1e30
QB=256
def attn_windows(seg_row):
    length = seg_row.shape[0]
    nb = length // QB
    firsts = seg_row[::QB]
    lasts = seg_row[QB-1::QB]
    begin = jnp.sum((seg_row[None, :] < firsts[:, None]).astype(jnp.int32), axis=1)
    end = jnp.sum((seg_row[None, :] <= lasts[:, None]).astype(jnp.int32), axis=1)
    start = begin // 128
    count = (end - start * 128 + QB - 1) // QB
    start = jnp.minimum(start, (length - count * QB) // 128)
    return start.astype(jnp.int32), count.astype(jnp.int32)
def lane_half(shape, h):
    lane = lax.broadcasted_iota(jnp.int32, shape, len(shape)-1)
    return (lane < 64) if h == 0 else (lane >= 64)
def dot(a, b, ca, cb):
    return lax.dot_general(a, b, (((ca,), (cb,)), ((), ())), preferred_element_type=jnp.float32)
def fold(value, join):
    part = value.shape[0] // 8
    parts = [value[i * part:(i + 1) * part] for i in range(8)]
    while len(parts) > 1:
        parts = [join(a, b) for a, b in zip(parts[::2], parts[1::2])]
    return parts[0]
def fwd_kernel(start_ref, count_ref, qkv_ref, segr_ref, segc_ref, o_ref, lse_ref, vt_ref):
    length = qkv_ref.shape[0]
    vt_ref[...] = qkv_ref[:, 256:384].T
    nb = length // QB
    for i in range(nb):
        rows = slice(i*QB, (i+1)*QB)
        for nn in range(1, nb+1):
            @pl.when(count_ref[i] == nn)
            def _():
                nk = nn*QB
                lo = pl.multiple_of(start_ref[i]*128, 128)
                kw = qkv_ref[pl.ds(lo, nk), 128:256]
                qb = qkv_ref[rows, 0:128]
                same = segc_ref[pl.ds(lo, nk), :] == segr_ref[:, rows]
                outs = []
                for h in range(2):
                    qh = jnp.where(lane_half(qb.shape, h), qb, jnp.zeros_like(qb))
                    st = jnp.where(same, dot(kw, qh, 1, 1), NEG)
                    m = jnp.max(fold(st, jnp.maximum), axis=0, keepdims=True)
                    p = jnp.exp(st - m)
                    l = jnp.sum(fold(p, jnp.add), axis=0, keepdims=True)
                    weighted = dot(vt_ref[h*64:(h+1)*64, pl.ds(lo, nk)], p.astype(jnp.bfloat16), 1, 0)
                    outs.append(weighted * (1.0 / l))
                    lse_ref[0, h:h+1, rows] = m + jnp.log(l)
                o_ref[rows, :] = jnp.concatenate(outs, axis=0).T.astype(jnp.bfloat16)
def bwd_kernel(start_ref, count_ref, qkv_ref, do_ref, lse_ref, segr_ref, segc_ref, d_ref, sums_ref, dk_acc, dv_acc, kt_ref):
    length = qkv_ref.shape[0]
    kt_ref[...] = qkv_ref[:, 128:256].T
    nb = length // QB
    dk_acc[...] = jnp.zeros_like(dk_acc)
    dv_acc[...] = jnp.zeros_like(dv_acc)
    for i in range(nb):
        rows = slice(i*QB, (i+1)*QB)
        for nn in range(1, nb+1):
            @pl.when(count_ref[i] == nn)
            def _():
                nk = nn*QB
                lo = pl.multiple_of(start_ref[i]*128, 128)
                win = pl.ds(lo, nk)
                kw = qkv_ref[win, 128:256]
                vw = qkv_ref[win, 256:384]
                qb = qkv_ref[rows, 0:128]
                db = do_ref[rows, :]
                same = segc_ref[win, :] == segr_ref[:, rows]
                dqs = []; dks = 0.0; dvs = 0.0
                for h in range(2):
                    hm = lane_half(qb.shape, h)
                    qh = jnp.where(hm, qb, jnp.zeros_like(qb))
                    dh = jnp.where(hm, db, jnp.zeros_like(db))
                    st = jnp.where(same, dot(kw, qh, 1, 1), NEG)
                    p = jnp.exp(st - lse_ref[0, h:h+1, rows])
                    dpt = dot(vw, dh, 1, 1)
                    rd = jnp.sum(fold(p * dpt, jnp.add), axis=0, keepdims=True)
                    ds = (p * (dpt - rd)).astype(jnp.bfloat16)
                    dvs = dvs + dot(p.astype(jnp.bfloat16), dh, 1, 0)
                    dks = dks + dot(ds, qh, 1, 0)
                    dqs.append(dot(kt_ref[h*64:(h+1)*64, win], ds, 1, 0))
                d_ref[rows, 0:128] = jnp.concatenate(dqs, axis=0).T.astype(jnp.bfloat16) * 0.125
                dk_acc[win, :] += dks
                dv_acc[win, :] += dvs
    d_ref[:, 128:256] = dk_acc[...].astype(jnp.bfloat16)
    d_ref[:, 256:384] = dv_acc[...].astype(jnp.bfloat16)
    sums_ref[0] = jnp.sum(d_ref[...].astype(jnp.float32), axis=0, keepdims=True)
def attn_fwd(qkv, seg):
    T, width = qkv.shape
    start, count = attn_windows(seg[0])
    segc = seg.reshape(T, 1)
    heads = width // 384
    return pl.pallas_call(
        fwd_kernel,
        out_shape=(jax.ShapeDtypeStruct((T, width // 3), jnp.bfloat16), jax.ShapeDtypeStruct((heads, 2, T), jnp.float32)),
        grid_spec=pltpu.PrefetchScalarGridSpec(
            num_scalar_prefetch=2, grid=(heads,),
            in_specs=[
                pl.BlockSpec((T, 384), lambda h, *_: (0, h)),
                pl.BlockSpec((1, T), lambda h, *_: (0, 0)),
                pl.BlockSpec((T, 1), lambda h, *_: (0, 0)),
            ],
            out_specs=(pl.BlockSpec((T, 128), lambda h, *_: (0, h)), pl.BlockSpec((1, 2, T), lambda h, *_: (h, 0, 0))),
            scratch_shapes=[pltpu.VMEM((128, T), jnp.bfloat16)],
        ),
        cost_estimate=cost(20 * T * T * width, 3 * T * width, T * T * width // 128),
        name="attn_fwd",
    )(start, count, qkv, seg, segc)


def attn_bwd(qkv, do, lse, seg, part):
    T, width = qkv.shape
    start, count = attn_windows(seg[0])
    segc = seg.reshape(T, 1)
    heads = width // 768
    first = part * heads
    return pl.pallas_call(
        bwd_kernel,
        out_shape=(jax.ShapeDtypeStruct((T, width // 2), jnp.bfloat16), jax.ShapeDtypeStruct((heads, 1, 384), jnp.float32)),
        grid_spec=pltpu.PrefetchScalarGridSpec(
            num_scalar_prefetch=2, grid=(heads,),
            in_specs=[
                pl.BlockSpec((T, 384), lambda h, *_: (0, first + h)),
                pl.BlockSpec((T, 128), lambda h, *_: (0, first + h)),
                pl.BlockSpec((1, 2, T), lambda h, *_: (first + h, 0, 0)),
                pl.BlockSpec((1, T), lambda h, *_: (0, 0)),
                pl.BlockSpec((T, 1), lambda h, *_: (0, 0)),
            ],
            out_specs=(pl.BlockSpec((T, 384), lambda h, *_: (0, h)), pl.BlockSpec((1, 1, 384), lambda h, *_: (h, 0, 0))),
            scratch_shapes=[pltpu.VMEM((T, 128), jnp.float32)] * 2 + [pltpu.VMEM((128, T), jnp.bfloat16)],
        ),
        cost_estimate=cost(20 * T * T * width, 6 * T * width, T * T * width // 64),
        name="attn_bwd",
    )(start, count, qkv, do, lse, seg, segc)


MESH_ID = pl.DeviceIdType.MESH


def bits_of():
    rep = lax.axis_index("rep")
    fsdp = lax.axis_index("fsdp")
    return dict(
        rep=rep, fsdp=fsdp, x=rep // 2, c=rep % 2, z1=fsdp // 4, z0=(fsdp // 2) % 2, y=fsdp % 2
    )


def partner_of(at, which):
    rep, fsdp = at["rep"], at["fsdp"]
    if which == "c":
        rep = rep + 1 - 2 * at["c"]
    elif which == "x":
        rep = rep + 2 - 4 * at["x"]
    elif which == "y":
        fsdp = fsdp + 1 - 2 * at["y"]
    elif which == "z0":
        fsdp = fsdp + 2 - 4 * at["z0"]
    elif which == "z1":
        fsdp = fsdp + 4 - 8 * at["z1"]
    else:
        rep = rep + 1 - 2 * at["c"]
        fsdp = fsdp + 2 - 4 * at["z0"]
    return (rep, fsdp)


REL = [(a, b, d) for d in (0, 1) for b in (0, 1) for a in (0, 1)]


def gather_kernel(
    qkv_in, wo_in, vec_in, tok_in, seg_in,
    qkv_out, wo_out, vec_out, tok_out, seg_out,
    tok_buf, seg_buf, send_sem, recv_sem, local_sem,
):
    at = bits_of()
    other = {k: partner_of(at, k) for k in ("c", "x", "y", "z0", "z1", "swap")}
    barrier = pltpu.get_barrier_semaphore()
    for k in ("c", "x", "y", "z0", "z1"):
        pl.semaphore_signal(barrier, inc=1, device_id=other[k], device_id_type=MESH_ID)
    moves = at["c"] != at["z0"]

    @pl.when(moves)
    def _():
        pl.semaphore_signal(barrier, inc=1, device_id=other["swap"], device_id_type=MESH_ID)
        pl.semaphore_wait(barrier, 6)

    @pl.when(jnp.logical_not(moves))
    def _():
        pl.semaphore_wait(barrier, 5)

    def flip(bit, rel):
        return bit + rel - 2 * bit * rel

    def shard(rel):
        return 4 * flip(at["z1"], rel[1]) + 2 * flip(at["z0"], rel[0]) + flip(at["y"], rel[2])

    counter = [0]
    started = []

    def send(src, dst, which):
        k = counter[0]
        counter[0] += 1
        copy = pltpu.make_async_remote_copy(
            src_ref=src, dst_ref=dst, send_sem=send_sem.at[k], recv_sem=recv_sem.at[k],
            device_id=other[which], device_id_type=MESH_ID,
        )
        copy.start()
        started.append(copy)
        return copy

    class Piece:
        def __init__(self, own, slot, split_x):
            self.own, self.slot, self.split_x = own, slot, split_x
            self.part = (2 * at["x"] + at["c"]) if split_x else at["c"]
            self.part_x = (2 * (1 - at["x"]) + at["c"]) if split_x else None
            self.copies = {}

        def first(self):
            zero = (0, 0, 0)
            for which in ("z1", "z0", "y"):
                self.copies[which, zero] = send(
                    self.own(self.part), self.slot(shard(zero), self.part), which
                )
            self.copies["c", zero] = send(self.own(None), self.slot(shard(zero), None), "c")

        def onward(self, rel):
            here = self.slot(shard(rel), self.part)
            if rel == (0, 1, 0):
                self.copies["z0", rel] = send(here, here, "z0")
            if rel[2] == 0:
                self.copies["y", rel] = send(here, here, "y")
            if self.split_x:
                self.copies["x", rel] = send(here, here, "x")
            self.copies["c", rel] = send(here, here, "c")

        def arrive(self, which, came):
            self.copies[which, came].wait_recv()
            step = {"z0": (1, 0, 0), "z1": (0, 1, 0), "y": (0, 0, 1)}[which]
            self.onward(tuple(p + q for p, q in zip(came, step)))

        def near(self):
            self.arrive("z1", (0, 0, 0))
            self.arrive("z0", (0, 0, 0))

        def rest(self):
            self.arrive("y", (0, 0, 0))
            self.arrive("z0", (0, 1, 0))
            self.arrive("y", (0, 1, 0))
            self.arrive("y", (1, 0, 0))
            self.arrive("y", (1, 1, 0))

        def last(self):
            if self.split_x:
                for rel in REL[1:]:
                    self.copies["x", rel].wait_recv()
                    there = self.slot(shard(rel), self.part_x)
                    self.copies["cx", rel] = send(there, there, "c")

        def finish(self):
            for (which, rel), copy in self.copies.items():
                if which in ("c", "cx"):
                    copy.wait_recv()

    def rows(ref, count):
        full = ref.shape[-2] // 8
        def slot(f, part):
            if part is None:
                at_row, n = f * full, full
            else:
                at_row, n = f * full + part * (full // count), full // count
            at_row = pl.multiple_of(at_row, 8)
            return ref.at[pl.ds(at_row, n), :]
        return slot

    def own_rows(ref, count):
        full = ref.shape[-2]
        def own(part):
            if part is None:
                return ref
            row = pl.multiple_of(part * (full // count), 8)
            n = full // count
            return ref.at[pl.ds(row, n), :]
        return own

    qkv, wo = pieces = [
        Piece(own_rows(qkv_in, 4), rows(qkv_out, 4), True),
        Piece(own_rows(wo_in, 4), rows(wo_out, 4), True),
    ]
    zero = (0, 0, 0)
    vec_copies = [
        send(vec_in, vec_out.at[shard(zero)], which) for which in ("c", "z1", "z0", "y")
    ]
    pieces[0].first()
    tok_k, seg_k = counter[0], counter[0] + 1
    counter[0] += 2

    def swap_copy(src, dst, k):
        return pltpu.make_async_remote_copy(
            src_ref=src, dst_ref=dst, send_sem=send_sem.at[k], recv_sem=recv_sem.at[k],
            device_id=other["swap"], device_id_type=MESH_ID,
        )

    @pl.when(moves)
    def _():
        swap_copy(tok_in, tok_out, tok_k).start()
        swap_copy(seg_in, seg_out, seg_k).start()

    @pl.when(jnp.logical_not(moves))
    def _():
        one = pltpu.make_async_copy(tok_in, tok_buf, local_sem.at[0])
        two = pltpu.make_async_copy(seg_in, seg_buf, local_sem.at[1])
        one.start()
        two.start()
        one.wait()
        two.wait()
        three = pltpu.make_async_copy(tok_buf, tok_out, local_sem.at[0])
        four = pltpu.make_async_copy(seg_buf, seg_out, local_sem.at[1])
        three.start()
        four.start()
        three.wait()
        four.wait()

    wo.first()
    qkv.near()
    vec_copies[1].wait_recv()
    here = vec_out.at[shard((0, 1, 0))]
    vec_far = send(here, here, "z0")
    vec_more = [send(here, here, "y")]
    vec_copies[2].wait_recv()
    here = vec_out.at[shard((1, 0, 0))]
    vec_more.append(send(here, here, "y"))
    qkv.rest()
    wo.near()
    wo.rest()
    vec_far.wait_recv()
    here = vec_out.at[shard((1, 1, 0))]
    vec_more.append(send(here, here, "y"))
    qkv.last()
    wo.last()
    for piece in pieces:
        piece.finish()
    for copy in [vec_copies[0], vec_copies[3]] + vec_more:
        copy.wait_recv()
    for copy in started:
        copy.wait_send()

    @pl.when(moves)
    def _():
        swap_copy(tok_in, tok_out, tok_k).wait()
        swap_copy(seg_in, seg_out, seg_k).wait()


GATHER_COPIES = 29 * 2 + 8 + 2


def gather_all(qkv, wo, vec, tok, seg):
    bf = jnp.bfloat16
    shape = jax.ShapeDtypeStruct
    whole = pl.BlockSpec(memory_space=pl.ANY)
    return pl.pallas_call(
        gather_kernel,
        out_shape=(
            shape((8 * qkv.shape[0], qkv.shape[1]), bf),
            shape((8 * wo.shape[0], wo.shape[1]), bf),
            shape((8,) + vec.shape, bf),
            shape(tok.shape, bf),
            shape(seg.shape, seg.dtype),
        ),
        in_specs=[whole] * 5,
        out_specs=(whole,) * 5,
        scratch_shapes=[
            pltpu.VMEM(tok.shape, bf),
            pltpu.VMEM(seg.shape, seg.dtype),
            pltpu.SemaphoreType.DMA((GATHER_COPIES,)),
            pltpu.SemaphoreType.DMA((GATHER_COPIES,)),
            pltpu.SemaphoreType.DMA((2,)),
        ],
        compiler_params=pltpu.CompilerParams(collective_id=0, has_side_effects=True),
        name="gather_weights",
    )(qkv, wo, vec, tok, seg)


SHRINK = 1000
BF, F32 = jnp.bfloat16, jnp.float32
SHAPE = jax.ShapeDtypeStruct


def full_spec(shape):
    return pl.BlockSpec(shape, lambda *_: (0,) * len(shape), pipeline_mode=pl.Buffered(1))


def cost(flops, moved, exps=0):
    return pl.CostEstimate(flops=int(flops) // SHRINK, bytes_accessed=int(moved) // SHRINK, transcendentals=int(exps) // SHRINK)


def qkv_kernel(x_ref, w_ref, bias_ref, scale_ref, o_ref):
    for i in range(4):
        rows = slice(i * 256, (i + 1) * 256)
        z = dot(x_ref[rows, :], w_ref[...], 1, 0)
        o_ref[rows, :] = ((z + bias_ref[...]) * scale_ref[...]).astype(BF)


def qkv_call(x, w, bias, scale):
    tokens, width = x.shape[0], w.shape[1]
    tile = 768
    return pl.pallas_call(
        qkv_kernel,
        out_shape=SHAPE((tokens, width), BF),
        grid=(width // tile,),
        in_specs=[
            full_spec(x.shape),
            pl.BlockSpec((x.shape[1], tile), lambda j: (0, j)),
            pl.BlockSpec((1, tile), lambda j: (0, j)),
            pl.BlockSpec((1, tile), lambda j: (0, j)),
        ],
        out_specs=pl.BlockSpec((tokens, tile), lambda j: (0, j)),
        cost_estimate=cost(2 * tokens * D * width, 2 * (tokens * D + D * width + tokens * width)),
        name="qkv",
    )(x, w, bias, scale)


def mean_row(value):
    return jnp.mean(value, axis=-1, keepdims=True)


def mix_kernel(c_ref, w_ref, x_ref, rows_ref, n_ref, q_ref, low_ref):
    value = x_ref[...].astype(F32) + dot(c_ref[...], w_ref[...], 1, 0) + rows_ref[6:7, :]
    center = value - mean_row(value)
    inv = lax.rsqrt(mean_row(center * center) + 1e-05)
    normed = center * inv
    n_ref[...] = normed
    q_ref[...] = inv
    low_ref[...] = (normed * rows_ref[0:1, :] + rows_ref[2:3, :]).astype(BF)


def mix_call(mixed, w_out, tok, rows):
    t = tok.shape[0]
    tile = pl.BlockSpec((256, D), lambda i: (i, 0))
    return pl.pallas_call(
        mix_kernel,
        out_shape=(SHAPE((t, D), F32), SHAPE((t, 1), F32), SHAPE((t, D), BF)),
        grid=(t // 256,),
        in_specs=[tile, full_spec((D, D)), tile, full_spec(rows.shape)],
        out_specs=(tile, pl.BlockSpec((256, 1), lambda i: (i, 0)), tile),
        cost_estimate=cost(2 * t * D * D, 12 * t * D + 2 * D * D),
        name="mix_norm",
    )(mixed, w_out, tok, rows)


def up_kernel(place_ref, h_ref, *refs):
    parts, (bias_ref, g_ref, s_ref) = refs[:4], refs[4:]
    each = pl.num_programs(0) // 4

    def tile(w_ref):
        for i in range(8):
            rows = slice(i * 128, (i + 1) * 128)
            z = dot(h_ref[rows, :], w_ref[...], 1, 0) + bias_ref[...]
            phi, bell = erf_parts(z)
            g_ref[rows, :] = (z * phi).astype(BF)
            s_ref[rows, :] = (phi + z * bell * 0.3989422804014327).astype(BF)

    for k in range(4):
        pl.when(pl.program_id(0) // each == k)(partial(tile, parts[k]))


def up_call(low, parts, place, bias):
    t = low.shape[0]
    tile = 512
    each = FF // tile // 4
    where = lambda j, p: (0, p[j // each] * each + lax.rem(j, each))
    out = pl.BlockSpec((t, tile), where)

    def part(k):
        return pl.BlockSpec((D, tile), lambda j, p: (0, jnp.clip(j - k * each, 0, each - 1)))

    return pl.pallas_call(
        up_kernel,
        out_shape=(SHAPE((t, FF), BF), SHAPE((t, FF), BF)),
        grid_spec=pltpu.PrefetchScalarGridSpec(
            num_scalar_prefetch=1, grid=(FF // tile,),
            in_specs=[full_spec(low.shape)] + [part(k) for k in range(4)] + [pl.BlockSpec((1, tile), where)],
            out_specs=(out, out),
        ),
        cost_estimate=cost(2 * t * D * FF, 2 * (t * D + D * FF + 2 * t * FF), 2 * t * FF),
        name="up_gelu",
    )(place, low, *parts, bias)


def row_sum(value):
    return jnp.sum(value, axis=0, keepdims=True)


def norm_back(grad, normed, inv, gain):
    scaled = grad * gain
    return inv * (scaled - mean_row(scaled) - normed * mean_row(scaled * normed))


def down_kernel(
    core_ref, g_ref, own_ref, came_ref, n_ref, cot_ref, rows_ref, out_ref, dr_ref, dm_ref, sums_ref, m_ref
):
    half = D // 2
    m_ref[:, pl.ds(pl.multiple_of(core_ref[0] * half, half), half)] = dot(g_ref[...], own_ref[...], 1, 0)
    m_ref[:, pl.ds(pl.multiple_of((1 - core_ref[0]) * half, half), half)] = dot(g_ref[...], came_ref[...], 1, 0)
    hidden = n_ref[...] * rows_ref[0:1, :] + rows_ref[2:3, :]
    value = hidden + m_ref[...] + rows_ref[7:8, :]
    center = value - mean_row(value)
    inv = lax.rsqrt(mean_row(center * center) + 1e-05)
    normed = center * inv
    gain = rows_ref[1:2, :]
    out_ref[...] = (normed * gain + rows_ref[3:4, :]).astype(BF)
    grad = cot_ref[...].astype(F32)
    back = norm_back(grad, normed, inv, gain)
    low = back.astype(BF)
    dr_ref[...] = back
    dm_ref[...] = low

    @pl.when(pl.program_id(0) == 0)
    def _():
        sums_ref[...] = jnp.zeros_like(sums_ref)

    sums_ref[0:1, :] += row_sum(grad * normed)
    sums_ref[1:2, :] += row_sum(grad)
    sums_ref[2:3, :] += row_sum(low.astype(F32))


def down_call(act, own, came, normed, cot, rows, core):
    t = act.shape[0]
    tile = pl.BlockSpec((256, D), lambda i, c: (i, 0))
    return pl.pallas_call(
        down_kernel,
        out_shape=(SHAPE((t, D), BF), SHAPE((t, D), F32), SHAPE((t, D), BF), SHAPE((8, D), F32)),
        grid_spec=pltpu.PrefetchScalarGridSpec(
            num_scalar_prefetch=1, grid=(t // 256,),
            in_specs=[
                pl.BlockSpec((256, FF), lambda i, c: (i, 0)), full_spec((FF, D // 2)), full_spec((FF, D // 2)),
                tile, tile, full_spec(rows.shape),
            ],
            out_specs=(tile, tile, tile, pl.BlockSpec((8, D), lambda i, c: (0, 0))),
            scratch_shapes=[pltpu.VMEM((256, D), F32)],
        ),
        cost_estimate=cost(2 * t * D * FF, 2 * (t * FF + D * FF) + 14 * t * D),
        name="down_norm",
    )(core.reshape(1), act, own, came, normed, cot, rows)


def slope_kernel(core_ref, left_ref, right_ref, own_ref, came_ref, s_ref, o_ref, sums_ref):
    total = 0.0
    for i in range(4):
        rows = slice(i * 256, (i + 1) * 256)
        back = dot(left_ref[rows, :], own_ref[...], 1, 1) + dot(right_ref[rows, :], came_ref[...], 1, 1)
        z = (back * s_ref[rows, :].astype(F32)).astype(BF)
        o_ref[rows, :] = z
        total = total + row_sum(z.astype(F32))
    sums_ref[...] = total


def slope_call(dm, own, came, slope, core):
    t = dm.shape[0]
    tile = 512
    wide = pl.BlockSpec((t, tile), lambda j, c: (0, j))
    part = pl.BlockSpec((tile, D // 2), lambda j, c: (j, 0))
    return pl.pallas_call(
        slope_kernel,
        out_shape=(SHAPE((t, FF), BF), SHAPE((1, FF), F32)),
        grid_spec=pltpu.PrefetchScalarGridSpec(
            num_scalar_prefetch=1, grid=(FF // tile,),
            in_specs=[
                pl.BlockSpec((t, D // 2), lambda j, c: (0, c[0])),
                pl.BlockSpec((t, D // 2), lambda j, c: (0, 1 - c[0])),
                part, part, wide,
            ],
            out_specs=(wide, pl.BlockSpec((1, tile), lambda j, c: (0, j))),
        ),
        cost_estimate=cost(2 * t * D * FF, 2 * (t * D + D * FF + 2 * t * FF)),
        name="down_back",
    )(core.reshape(1), dm, dm, own, came, slope)


def hidden_kernel(place_ref, *refs):
    grads, parts = refs[:4], refs[4:8]
    dr_ref, n_ref, q_ref, wo_ref, rows_ref, r_ref, a_ref, c_ref, sums_ref = refs[8:]
    grad = dr_ref[...]
    for grad_ref, w_ref in zip(grads, parts):
        grad = grad + dot(grad_ref[...], w_ref[...], 1, 1)
    normed = n_ref[...]
    back = norm_back(grad, normed, q_ref[...], rows_ref[0:1, :])
    low = back.astype(BF)
    r_ref[...] = back
    a_ref[...] = low
    c_ref[...] = dot(low, wo_ref[...], 1, 1).astype(BF)

    @pl.when(pl.program_id(0) == 0)
    def _():
        sums_ref[...] = jnp.zeros_like(sums_ref)

    sums_ref[0:1, :] += row_sum(grad * normed)
    sums_ref[1:2, :] += row_sum(grad)
    sums_ref[2:3, :] += row_sum(low.astype(F32))


def hidden_call(dz, parts, place, dr, normed, inv, w_out, rows):
    t = dz.shape[0]
    tile = pl.BlockSpec((256, D), lambda i, p: (i, 0))

    def quarter(k):
        return pl.BlockSpec((256, FF // 4), lambda i, p: (i, p[k]))

    return pl.pallas_call(
        hidden_kernel,
        out_shape=(SHAPE((t, D), F32), SHAPE((t, D), BF), SHAPE((t, D), BF), SHAPE((8, D), F32)),
        grid_spec=pltpu.PrefetchScalarGridSpec(
            num_scalar_prefetch=1, grid=(t // 256,),
            in_specs=[quarter(k) for k in range(4)] + [full_spec((D, FF // 4))] * 4 + [
                tile, tile,
                pl.BlockSpec((256, 1), lambda i, p: (i, 0)), full_spec((D, D)), full_spec(rows.shape),
            ],
            out_specs=(tile, tile, tile, pl.BlockSpec((8, D), lambda i, p: (0, 0))),
        ),
        cost_estimate=cost(2 * t * D * (FF + D), 2 * (t * FF + D * FF) + 16 * t * D),
        name="up_back_norm",
    )(place, *([dz] * 4), *parts, dr, normed, inv, w_out, rows)


def input_kernel(a_ref, b_ref, w_ref, r_ref, o_ref):
    half = a_ref.shape[1]
    value = dot(a_ref[...], w_ref[:, :half], 1, 1) + dot(b_ref[...], w_ref[:, half:], 1, 1)
    o_ref[...] = (r_ref[...] + value).astype(BF)


def input_call(part_a, part_b, w_qkv, resid):
    t, width = part_a.shape
    tile = pl.BlockSpec((256, D), lambda i: (i, 0))
    wide = pl.BlockSpec((256, width), lambda i: (i, 0))
    return pl.pallas_call(
        input_kernel,
        out_shape=SHAPE((t, D), BF),
        grid=(t // 256,),
        in_specs=[wide, wide, full_spec(w_qkv.shape), tile],
        out_specs=tile,
        cost_estimate=cost(4 * t * D * width, 4 * (t * width + D * width) + 6 * t * D),
        name="input_back",
    )(part_a, part_b, w_qkv, resid)


def weight_kernel(half_ref, first_ref, second_ref, right_ref, *refs):
    o_ref, turned = refs[-2], refs[-1]

    @pl.when(pl.program_id(1) == 0)
    def _():
        part = first_ref.shape[1]
        turned[:part, :] = first_ref[...].T
        turned[part:, :] = second_ref[...].T

    value = dot(turned[...], right_ref[...], 1, 0)
    if len(refs) == 3:
        value = value + refs[0][...].astype(F32)
    o_ref[...] = value.astype(BF)


def weight_call(left, right, half, came=None):
    t, rows = left.shape
    width = right.shape[1]
    bm = 512
    bn = 1024 if width == 1024 else 512
    steps = rows // 2 // bm
    if steps == 1:
        first = lambda i, j, h: (0, h[0])
        second = lambda i, j, h: (0, 2 + h[0])
    else:
        block = lambda i, h: lax.div(i, steps // 2) * steps + h[0] * (steps // 2) + lax.rem(i, steps // 2)
        first = lambda i, j, h: (0, 2 * block(i, h))
        second = lambda i, j, h: (0, 2 * block(i, h) + 1)
    specs = [
        pl.BlockSpec((t, bm // 2), first),
        pl.BlockSpec((t, bm // 2), second),
        pl.BlockSpec((t, bn), lambda i, j, h: (0, j)),
    ]
    values = [left, left, right]
    out = pl.BlockSpec((bm, bn), lambda i, j, h: (i, j))
    if came is not None:
        specs.append(out)
        values.append(came)
    return pl.pallas_call(
        weight_kernel,
        out_shape=SHAPE((rows // 2, width), BF),
        grid_spec=pltpu.PrefetchScalarGridSpec(
            num_scalar_prefetch=1, grid=(steps, width // bn), in_specs=specs, out_specs=out,
            scratch_shapes=[pltpu.VMEM((bm, t), BF)],
        ),
        cost_estimate=cost(t * rows * width, t * rows + 2 * t * width + 2 * rows * width),
        name="weight_grad",
    )(half.reshape(1), *values)


def inner_kernel(rate, decay, w_ref, g_ref, m_ref, v_ref, m_out, v_out, d_out):
    weight = w_ref[...]
    new, m_out[...], v_out[...] = inner_step(
        weight, g_ref[...].astype(F32), m_ref[...], v_ref[...], rate, decay
    )
    d_out[...] = (weight - new).astype(BF)


def inner_call(weight, grad, first, second, rate, decay):
    rows, width = weight.shape
    block = 32 * 4096 // width
    tile = pl.BlockSpec((block, width), lambda i: (i, 0))
    like = SHAPE((rows, width), F32)
    return pl.pallas_call(
        partial(inner_kernel, rate, decay),
        out_shape=(like, like, SHAPE((rows, width), BF)),
        grid=(rows // block,),
        in_specs=[tile] * 4,
        out_specs=(tile,) * 3,
        cost_estimate=cost(20 * rows * width, 24 * rows * width),
        name="inner_step",
    )(weight, grad, first, second)


def outer_kernel(core_ref, w_ref, u_ref, own_ref, came_ref, o_ref, c_ref):
    mine = (core_ref[0] == pl.program_id(0)).astype(F32)
    total = own_ref[...].astype(F32) * mine + came_ref[...].astype(F32) * (1.0 - mine)
    mean = total * 0.25
    weight = w_ref[...]
    momentum = 0.5 * u_ref[...] + mean
    new = weight - 0.7 * (mean + 0.5 * momentum)
    o_ref[0] = mean
    o_ref[1] = momentum
    o_ref[2] = new
    c_ref[...] = new.astype(BF)


def outer_call(weight, momentum, own, came, core):
    rows, width = weight.shape
    block = 32 * 4096 // width
    steps = rows // 2 // block
    tile = pl.BlockSpec((block, width), lambda h, i, c: (h * steps + i, 0))
    part = pl.BlockSpec((block, width), lambda h, i, c: (i, 0))
    return pl.pallas_call(
        outer_kernel,
        out_shape=(SHAPE((3, rows, width), F32), SHAPE((rows, width), BF)),
        grid_spec=pltpu.PrefetchScalarGridSpec(
            num_scalar_prefetch=1, grid=(2, steps), in_specs=[tile, tile, part, part],
            out_specs=(pl.BlockSpec((3, block, width), lambda h, i, c: (0, h * steps + i, 0)), tile),
        ),
        cost_estimate=cost(10 * rows * width, 26 * rows * width),
        name="outer_step",
    )(core.reshape(1), weight, momentum, own, came)


def erf_parts(value):
    size = jnp.abs(value) * 0.7071067811865476
    share = 1.0 / (1.0 + 0.5 * size)
    inner = 0.17087277
    for coefficient in (
        -0.82215223, 1.48851587, -1.13520398, 0.27886807, -0.18628806, 0.09678418, 0.37409196, 1.00002368
    ):
        inner = coefficient + share * inner
    square = size * size
    half = 0.5 * share * jnp.exp(share * inner - 1.26551223 - square)
    return jnp.where(value >= 0, 1.0 - half, half), jnp.exp(-square)


def xor_pairs(bits):
    place = {"y": 0, "z0": 1, "z1": 2, "c": 3, "x": 4}
    flip = sum(1 << place[bit] for bit in bits)
    pairs = []
    for device in range(32):
        if bits == ("c", "z0") and ((device >> 3) & 1) == ((device >> 1) & 1):
            continue
        pairs.append((device, device ^ flip))
    return pairs


def exchange(value, *bits):
    return lax.ppermute(value, ("rep", "fsdp"), xor_pairs(bits))


def add_low(left, right):
    return (left.astype(jnp.float32) + right.astype(jnp.float32)).astype(jnp.bfloat16)


def pick(value, index, axis):
    return lax.dynamic_index_in_dim(value, index, axis, keepdims=False)


def half_axis(total, which):
    return 1 if which == "y" and total.ndim == 4 else 0


def halve(at, total, which):
    away = pick(total, 1 - at[which], half_axis(total, which))
    return away, exchange(away, which)


def join(at, total, came, which, *gates):
    return add_low(pick(total, at[which], half_axis(total, which)), after(came, *gates))


def slabs(total):
    return total.reshape(2, 2, -1, total.shape[-1])


def after(value, *earlier):
    return lax.optimization_barrier((value,) + earlier)[0]


def weave(value):
    rows = value.shape[1]
    return jnp.transpose(value.reshape(3, rows, D // 128, 128), (1, 2, 0, 3)).reshape(rows, 3 * D)


def unweave(value):
    rows = value.shape[0]
    return jnp.transpose(value.reshape(rows, D // 128, 3, 128), (2, 0, 1, 3)).reshape(3, rows, D)


def per_device_fast(
    tokens,
    cotangent,
    segment_ids,
    attention_weight,
    attention_momentum,
    attention_first,
    attention_second,
    expand_weight,
    expand_momentum,
    expand_first,
    expand_second,
    contract_weight,
    contract_momentum,
    contract_first,
    contract_second,
    vectors,
    vectors_momentum,
    vectors_first,
    vectors_second,
):
    bf, f32 = jnp.bfloat16, jnp.float32
    at = bits_of()
    core = at["c"].astype(jnp.int32)
    def swapped(value, came):
        return jnp.where(at["c"] != at["z0"], came, value)

    def cross(value):
        return exchange(value, "c", "z0")

    quarter = 2 * core + at["x"].astype(jnp.int32)
    place = jnp.stack([quarter, 2 * (1 - core) + quarter - 2 * core, quarter + 1 - 2 * at["x"], 3 - quarter])
    part = expand_weight.shape[1] // 4
    in_own = lax.all_gather(
        lax.dynamic_slice_in_dim(expand_weight, quarter * part, part, axis=1).astype(bf), "fsdp", axis=0, tiled=True
    )
    attn_low = attention_weight.astype(bf)
    w_qkv, w_out, vector_full, tok, seg = gather_all(
        weave(attn_low[:3]), attn_low[3], vectors.astype(bf), tokens, segment_ids,
    )
    cot_came = cross(after(cotangent, w_qkv))
    rows = jnp.swapaxes(vector_full, 0, 1).reshape(-1, D).astype(f32)
    bias_up = rows[8:].reshape(1, FF)
    bias_qkv = weave(jnp.stack([rows[4], jnp.zeros_like(rows[4]), rows[5]])[:, None])
    scale_qkv = weave(jnp.stack([jnp.full((1, D), 0.125, f32)] + [jnp.ones((1, D), f32)] * 2))
    part = contract_weight.shape[1] // 2
    down_half = lax.dynamic_slice_in_dim(contract_weight, core * part, part, axis=1).astype(bf)
    down_own = lax.all_gather(after(down_half, w_qkv), "fsdp", axis=0, tiled=True)
    in_near = after(in_own, w_qkv)
    in_far = exchange(in_near, "x")
    in_side = exchange(in_near, "c")
    qkv = qkv_call(tok, w_qkv, bias_qkv, scale_qkv)
    mixed, log_sum = attn_fwd(qkv, seg)
    in_parts = [in_own, after(in_side, mixed), in_far, exchange(after(in_far, mixed), "c")]
    normed, inv, hidden_low = mix_call(mixed, w_out, tok, rows)
    cot = swapped(cotangent, after(cot_came, hidden_low))
    activated, slope = up_call(after(hidden_low, cot), in_parts, place, bias_up)
    down_other = exchange(after(down_own, activated), "c")
    layer_output, grad_sum, grad_branch, sums_two = down_call(
        activated, down_own, down_other, normed, cot, rows, core
    )
    output_came = cross(layer_output)
    down_send = weight_call(activated, grad_branch, 1 - core)
    grad_pre, sums_up = slope_call(after(grad_branch, down_send), down_own, down_other, slope, core)
    down_came = exchange(down_send, "c")
    up_send = weight_call(hidden_low, grad_pre, 1 - core)
    down_total = slabs(weight_call(activated, after(grad_branch, up_send), core, down_came))
    up_came = exchange(up_send, "c")
    away_d, came_d = halve(at, down_total, "y")
    up_total = slabs(weight_call(hidden_low, after(grad_pre, away_d), core, up_came))
    away_u, came_u = halve(at, up_total, "y")
    grad_resid, grad_attn, grad_mixed, sums_one = hidden_call(
        after(grad_pre, away_u), in_parts, place, grad_sum, normed, inv, w_out, rows
    )
    proj_send = weight_call(mixed, grad_attn, 1 - core)
    proj_came = exchange(proj_send, "c")
    output = swapped(layer_output, after(output_came, proj_send))
    grad_a, sums_a = attn_bwd(qkv, after(grad_mixed, proj_send, output), log_sum, seg, 0)
    send_a = weight_call(tok, grad_a, 1 - core)
    came_a = exchange(send_a, "c")
    down_one = join(at, down_total, came_d, "y", send_a)
    away_d, came_d = halve(at, down_one, "z1")
    proj_total = slabs(weight_call(mixed, after(grad_attn, away_d), core, proj_came))
    away_p, came_p = halve(at, proj_total, "y")
    total_a = slabs(weight_call(tok, after(grad_a, away_p), core, came_a))
    away_a, came_one = halve(at, total_a, "y")
    up_one = join(at, up_total, came_u, "y", away_a)
    away_u, came_u = halve(at, up_one, "z1")
    grad_b, sums_b = attn_bwd(qkv, after(grad_mixed, away_u), log_sum, seg, 1)
    send_b = weight_call(tok, grad_b, 1 - core)
    came_b = exchange(send_b, "c")
    down_two = join(at, down_one, came_d, "z1", send_b)
    cross_d = cross(down_two)
    up_two = join(at, up_one, came_u, "z1", down_two)
    cross_u = cross(up_two)
    proj_one = join(at, proj_total, came_p, "y", up_two)
    away_p, came_p = halve(at, proj_one, "z1")
    a_one = join(at, total_a, came_one, "y", away_p)
    away_a, came_a = halve(at, a_one, "z1")
    total_b = slabs(weight_call(tok, after(grad_b, away_a), core, came_b))
    away_b, came_b = halve(at, total_b, "y")
    sums_qkv = jnp.concatenate([sums_a, sums_b], axis=0).reshape(D // 128, 3, 128)
    vector_grad = jnp.concatenate(
        [
            sums_one[0:1],
            sums_two[0:1],
            sums_one[1:2],
            sums_two[1:2],
            sums_qkv[:, 0].reshape(1, D),
            sums_qkv[:, 2].reshape(1, D),
            sums_one[2:3],
            sums_two[2:3],
            sums_up.reshape(FF // D, D),
        ],
        axis=0,
    )

    def vector_send(parts, which):
        half = parts.shape[1] // 2
        away = lax.dynamic_slice_in_dim(parts, (1 - at[which]) * half, half, axis=1)
        return exchange(away, which)

    def vector_join(parts, came, which, *gates):
        half = parts.shape[1] // 2
        return lax.dynamic_slice_in_dim(parts, at[which] * half, half, axis=1) + after(came, *gates)

    vec_came = vector_send(vector_grad, "z1")

    def inner(weight, grad, first, second, rate, decay):
        flat = (-1, weight.shape[-1])
        return inner_call(
            weight.reshape(flat), grad.reshape(flat), first.reshape(flat), second.reshape(flat), rate, decay
        )

    def rep_send(diff):
        halves = diff.reshape(2, diff.shape[0] // 2, diff.shape[1])
        away = pick(halves, 1 - at["c"], 0)
        return away, exchange(away, "c")

    def rep_join(diff, came, *gates):
        halves = diff.reshape(2, diff.shape[0] // 2, diff.shape[1])
        return add_low(pick(halves, at["c"], 0), after(came, *gates))

    def outer(weight, momentum, own, came):
        flat = (-1, weight.shape[-1])
        return outer_call(weight.reshape(flat), momentum.reshape(flat), own, came, core)

    grad_contract = swapped(down_two, after(cross_d, away_b))
    contract_new = inner(contract_weight, grad_contract, contract_first, contract_second, 0.015, 0.1)
    sent_c, came_c = rep_send(contract_new[2])
    vec_one = vector_join(vector_grad, vec_came, "z1", sent_c)
    vec_came = vector_send(vec_one, "c")
    grad_expand = swapped(up_two, after(cross_u, sent_c))
    expand_new = inner(expand_weight, grad_expand, expand_first, expand_second, 0.03, 0.1)
    sent_e, came_e = rep_send(expand_new[2])
    b_one = join(at, total_b, came_b, "y", sent_e)
    away_b, came_b = halve(at, b_one, "z1")
    half_c = rep_join(contract_new[2], came_c, away_b)
    rest_c = exchange(half_c, "x")
    half_e = rep_join(expand_new[2], came_e, half_c)
    rest_e = exchange(half_e, "x")
    vec_two = vector_join(vec_one, vec_came, "c", half_e)
    vec_came = vector_send(vec_two, "y")
    input_grad = input_call(after(grad_a, away_b, half_e), grad_b, w_qkv, grad_resid)
    proj_two = join(at, proj_one, came_p, "z1", input_grad)
    a_two = join(at, a_one, came_a, "z1", input_grad)
    cross_pa = cross(jnp.concatenate([proj_two, a_two], axis=1))
    vec_three = vector_join(vec_two, vec_came, "y", proj_two, a_two)
    vec_cross = cross(vec_three)
    full_c = add_low(half_c, after(rest_c, vec_three))
    back_c = exchange(full_c, "c")
    b_two = join(at, b_one, came_b, "z1", full_c)
    cross_b = cross(b_two)
    full_e = add_low(half_e, after(rest_e, b_two))
    back_e = exchange(full_e, "c")
    outer_c = outer(contract_weight, contract_momentum, full_c, after(back_c, full_e))
    grad_vectors = swapped(vec_three, after(vec_cross, outer_c[1]))
    inner_new, first_new, second_new = inner_step(
        vectors, grad_vectors, vectors_first[0], vectors_second[0], 0.2, 0.0
    )
    vec_diff = (vectors - inner_new).astype(bf)
    vec_near = exchange(vec_diff, "c")
    input_came = cross(after(input_grad, b_two, vec_diff))
    pa = swapped(jnp.concatenate([proj_two, a_two], axis=1), after(cross_pa, outer_c[1]))
    b_own = swapped(b_two, after(cross_b, vec_diff, pa))
    grad_qkv = jnp.concatenate([pa[:, D:], b_own], axis=1)
    grad_attention = jnp.concatenate([unweave(grad_qkv), pa[None, :, :D]], axis=0)
    attention_new = inner(attention_weight, grad_attention, attention_first, attention_second, 0.03, 0.1)
    sent_a, came_a = rep_send(attention_new[2])
    vec_half = add_low(vec_diff, after(vec_near, sent_a))
    vec_far = exchange(vec_half, "x")
    half_a = rep_join(attention_new[2], came_a, vec_half)
    rest_a = exchange(half_a, "x")
    outer_e = outer(expand_weight, expand_momentum, full_e, after(back_e, half_a))
    full_a = add_low(half_a, after(rest_a, outer_e[1]))
    back_a = exchange(full_a, "c")
    mean_diff = add_low(vec_half, after(vec_far, full_a)).astype(f32) / 4
    momentum_new = 0.5 * vectors_momentum + mean_diff
    outer_new = vectors - 0.7 * (mean_diff + 0.5 * momentum_new)
    input_grad = swapped(input_grad, after(input_came, full_a))
    outer_a = outer(attention_weight, attention_momentum, full_a, back_a)
    results = []
    for weight, first, new, (total, copy) in (
        (attention_weight, attention_first, attention_new, outer_a),
        (expand_weight, expand_first, expand_new, outer_e),
        (contract_weight, contract_first, contract_new, outer_c),
    ):
        results += [
            new[0].reshape(first.shape),
            new[1].reshape(first.shape),
            total.reshape((3,) + weight.shape),
            copy.reshape(weight.shape),
        ]
    results += [
        first_new[None],
        second_new[None],
        jnp.stack([mean_diff, momentum_new, outer_new]),
        outer_new.astype(bf),
    ]
    return (output, input_grad) + tuple(results)


def solution(mesh):
    placed = (
        P(("rep", "fsdp"), None),
        P(("rep", "fsdp"), None),
        P(("rep", "fsdp"), None),
        P(None, "fsdp", None),
        P(None, "fsdp", None),
        P("rep", None, "fsdp", None),
        P("rep", None, "fsdp", None),
        P("fsdp", None),
        P("fsdp", None),
        P("rep", "fsdp", None),
        P("rep", "fsdp", None),
        P("fsdp", None),
        P("fsdp", None),
        P("rep", "fsdp", None),
        P("rep", "fsdp", None),
        P(None, "fsdp"),
        P(None, "fsdp"),
        P("rep", None, "fsdp"),
        P("rep", None, "fsdp"),
    )
    small = mesh.shape["rep"] == 4 and mesh.shape["fsdp"] == 8
    body = per_device_fast if small else per_device
    return jax.shard_map(
        body,
        mesh=mesh,
        in_specs=placed,
        out_specs=(
            P(("rep", "fsdp"), None),
            P(("rep", "fsdp"), None),
            P("rep", None, "fsdp", None),
            P("rep", None, "fsdp", None),
            P(None, None, "fsdp", None),
            P(None, "fsdp", None),
            P("rep", "fsdp", None),
            P("rep", "fsdp", None),
            P(None, "fsdp", None),
            P("fsdp", None),
            P("rep", "fsdp", None),
            P("rep", "fsdp", None),
            P(None, "fsdp", None),
            P("fsdp", None),
            P("rep", None, "fsdp"),
            P("rep", None, "fsdp"),
            P(None, None, "fsdp"),
            P(None, "fsdp"),
        ),
        check_vma=False,
    )
```

```python
from functools import partial

import jax
import jax.numpy as jnp
from jax import lax
from jax.experimental import pallas as pl
from jax.experimental.pallas import tpu as pltpu
from jax.sharding import PartitionSpec as P

D = 1024
H = 16
HD = 64
FF = 4096
LEN = 1024
SEQ_DEV = 1
ADAM_STEP = 4
TOK_DEV = 1024


def norm_forward(values_in, gain_row, shift_row):
    center = values_in - jnp.mean(values_in, axis=-1, keepdims=True)
    inv_scale = lax.rsqrt(jnp.mean(center * center, axis=-1, keepdims=True) + 1e-05)
    normed = center * inv_scale
    return (normed * gain_row + shift_row, normed, inv_scale)


def norm_backward(grad_out, normed, inv_scale, gain_row):
    grad_gain = jnp.sum(grad_out * normed, axis=0)
    grad_shift = jnp.sum(grad_out, axis=0)
    scaled_grad = grad_out * gain_row
    grad_value = inv_scale * (
        scaled_grad
        - jnp.mean(scaled_grad, axis=-1, keepdims=True)
        - normed * jnp.mean(scaled_grad * normed, axis=-1, keepdims=True)
    )
    return (grad_value, grad_gain, grad_shift)


def product_over(left, right):
    return lax.dot_general(
        left, right, (((0,), (0,)), ((), ())), preferred_element_type=jnp.float32
    )


def product_back(left, right):
    return lax.dot_general(
        left, right, (((1,), (1,)), ((), ())), preferred_element_type=jnp.float32
    )


def block_scores(query_block, key_block, row_segments, all_segments):
    scores = jnp.einsum("qhd,khd->hqk", query_block, key_block, preferred_element_type=jnp.float32)
    same_doc = row_segments[:, None] == all_segments[None, :]
    return jnp.where(same_doc[None], scores, -1e30)


def inner_step(weight, gradient, first_moment, second_moment, learn_rate, weight_decay):
    first_new = 0.5 * first_moment + 0.5 * gradient
    second_new = 0.75 * second_moment + 0.25 * gradient * gradient
    update_dir = (
        first_new
        / (1.0 - 0.5**ADAM_STEP)
        / (jnp.sqrt(second_new / (1.0 - 0.75**ADAM_STEP)) + 1e-08)
    )
    return (weight - learn_rate * (update_dir + weight_decay * weight), first_new, second_new)


def per_device(
    tokens,
    cotangent,
    segment_ids,
    attention_weight,
    attention_momentum,
    attention_first,
    attention_second,
    expand_weight,
    expand_momentum,
    expand_first,
    expand_second,
    contract_weight,
    contract_momentum,
    contract_first,
    contract_second,
    vectors,
    vectors_momentum,
    vectors_first,
    vectors_second,
):
    attn_full, vector_full = (
        lax.all_gather(attention_weight.astype(jnp.bfloat16), "fsdp", axis=1, tiled=True),
        lax.all_gather(vectors.astype(jnp.bfloat16), "fsdp", axis=1, tiled=True),
    )
    vector_rows = vector_full.astype(jnp.float32)
    gain_one, gain_two, shift_one, shift_two = (
        vector_rows[0],
        vector_rows[1],
        vector_rows[2],
        vector_rows[3],
    )
    bias_query, bias_value, bias_mixed, bias_down = (
        vector_rows[4],
        vector_rows[5],
        vector_rows[6],
        vector_rows[7],
    )
    bias_up = vector_rows[8:].reshape(FF)
    projected = jnp.einsum("td,nde->nte", tokens, attn_full[:3], preferred_element_type=jnp.float32)
    query_all = ((projected[0] + bias_query) * 0.125).astype(jnp.bfloat16)
    key_all = projected[1].astype(jnp.bfloat16)
    value_all = (projected[2] + bias_value).astype(jnp.bfloat16)
    query_heads = query_all.reshape(SEQ_DEV, LEN, H, HD)
    key_heads = key_all.reshape(SEQ_DEV, LEN, H, HD)
    value_heads = value_all.reshape(SEQ_DEV, LEN, H, HD)
    block_rows = min(512, LEN)
    head_group = min(8, H)
    context_rows = []
    log_sums = []
    seq_index = 0
    for row_start in range(0, LEN, block_rows):
        block_pieces = []
        for head_start in range(0, H, head_group):
            head_part = slice(head_start, head_start + head_group)
            scores = block_scores(
                query_heads[seq_index, row_start : row_start + block_rows, head_part],
                key_heads[seq_index, :, head_part],
                segment_ids[seq_index, row_start : row_start + block_rows],
                segment_ids[seq_index],
            )
            row_max = jnp.max(scores, axis=-1, keepdims=True)
            exp_score = jnp.exp(scores - row_max)
            row_total = jnp.sum(exp_score, axis=-1, keepdims=True)
            probability = (exp_score / row_total).astype(jnp.bfloat16)
            block_pieces.append(
                jnp.einsum(
                    "hqk,khd->qhd",
                    probability,
                    value_heads[seq_index, :, head_part],
                    preferred_element_type=jnp.float32,
                )
            )
            log_sums.append(row_max + jnp.log(row_total))
        context_rows.append(jnp.concatenate(block_pieces, axis=1))
    mixed = jnp.concatenate(context_rows, axis=0).reshape(TOK_DEV, D).astype(jnp.bfloat16)
    attn_out = jnp.dot(mixed, attn_full[3], preferred_element_type=jnp.float32) + bias_mixed
    hidden, normed_one, scale_one = norm_forward(
        tokens.astype(jnp.float32) + attn_out, gain_one, shift_one
    )
    hidden_low = hidden.astype(jnp.bfloat16)
    ffn_expand, ffn_contract = (
        lax.all_gather(expand_weight.astype(jnp.bfloat16), "fsdp", axis=0, tiled=True),
        lax.all_gather(contract_weight.astype(jnp.bfloat16), "fsdp", axis=0, tiled=True),
    )
    pre_act = jnp.dot(hidden_low, ffn_expand, preferred_element_type=jnp.float32) + bias_up
    activated = jax.nn.gelu(pre_act, approximate=False).astype(jnp.bfloat16)
    branch = jnp.dot(activated, ffn_contract, preferred_element_type=jnp.float32) + bias_down
    layer_output, normed_two, scale_two = norm_forward(hidden + branch, gain_two, shift_two)
    grad_sum, grad_gain_two, grad_shift_two = norm_backward(
        cotangent.astype(jnp.float32), normed_two, scale_two, gain_two
    )
    grad_branch = grad_sum.astype(jnp.bfloat16)
    grad_act = product_back(grad_branch, ffn_contract)
    unused_value, gelu_pull = jax.vjp(partial(jax.nn.gelu, approximate=False), pre_act)
    grad_pre_low = gelu_pull(grad_act)[0].astype(jnp.bfloat16)
    grad_hidden = grad_sum + product_back(grad_pre_low, ffn_expand)
    contract_full = product_over(activated, grad_branch)
    expand_full = product_over(hidden_low, grad_pre_low)
    grad_expand, grad_contract = (
        lax.psum_scatter(expand_full, "fsdp", scatter_dimension=0, tiled=True),
        lax.psum_scatter(contract_full, "fsdp", scatter_dimension=0, tiled=True),
    )
    grad_resid, grad_gain_one, grad_shift_one = norm_backward(
        grad_hidden, normed_one, scale_one, gain_one
    )
    grad_attn_out = grad_resid.astype(jnp.bfloat16)
    grad_bias_mixed = jnp.sum(grad_attn_out.astype(jnp.float32), axis=0)
    grad_output_proj = product_over(mixed, grad_attn_out)
    grad_mixed = product_back(grad_attn_out, attn_full[3]).astype(jnp.bfloat16)
    grad_context = grad_mixed.reshape(SEQ_DEV, LEN, H, HD)
    query_grads = []
    lse_index = 0
    seq_index = 0
    key_totals = [
        jnp.zeros((LEN, head_group, HD), jnp.float32) for head_start in range(0, H, head_group)
    ]
    value_totals = [
        jnp.zeros((LEN, head_group, HD), jnp.float32) for head_start in range(0, H, head_group)
    ]
    for row_start in range(0, LEN, block_rows):
        block_pieces = []
        for group_index, head_start in enumerate(range(0, H, head_group)):
            head_part = slice(head_start, head_start + head_group)
            query_block = query_heads[seq_index, row_start : row_start + block_rows, head_part]
            key_block = key_heads[seq_index, :, head_part]
            value_block = value_heads[seq_index, :, head_part]
            ctx_grad = grad_context[seq_index, row_start : row_start + block_rows, head_part]
            scores = block_scores(
                query_block,
                key_block,
                segment_ids[seq_index, row_start : row_start + block_rows],
                segment_ids[seq_index],
            )
            probability = jnp.exp(scores - log_sums[lse_index])
            lse_index = lse_index + 1
            value_totals[group_index] = value_totals[group_index] + jnp.einsum(
                "hqk,qhd->khd",
                probability.astype(jnp.bfloat16),
                ctx_grad,
                preferred_element_type=jnp.float32,
            )
            prob_grad = jnp.einsum(
                "qhd,khd->hqk", ctx_grad, value_block, preferred_element_type=jnp.float32
            )
            row_dot = jnp.sum(probability * prob_grad, axis=-1, keepdims=True)
            score_grad = (probability * (prob_grad - row_dot)).astype(jnp.bfloat16)
            block_pieces.append(
                jnp.einsum(
                    "hqk,khd->qhd", score_grad, key_block, preferred_element_type=jnp.float32
                ).astype(jnp.bfloat16)
            )
            key_totals[group_index] = key_totals[group_index] + jnp.einsum(
                "hqk,qhd->khd", score_grad, query_block, preferred_element_type=jnp.float32
            )
        query_grads.append(jnp.concatenate(block_pieces, axis=1))
    key_grads = jnp.concatenate(
        [key_total.astype(jnp.bfloat16) for key_total in key_totals], axis=1
    )
    value_grads = jnp.concatenate(
        [value_total.astype(jnp.bfloat16) for value_total in value_totals], axis=1
    )
    grad_query = jnp.concatenate(query_grads, axis=0).reshape(TOK_DEV, D) * 0.125
    grad_keys = key_grads.reshape(TOK_DEV, D)
    grad_values = value_grads.reshape(TOK_DEV, D)
    stacked_grads = jnp.stack([grad_query, grad_keys, grad_values])
    grad_qkv = jnp.einsum("td,nte->nde", tokens, stacked_grads, preferred_element_type=jnp.float32)
    input_grad = (
        grad_resid
        + jnp.einsum(
            "nte,nde->td", stacked_grads, attn_full[:3], preferred_element_type=jnp.float32
        )
    ).astype(jnp.bfloat16)
    grad_attention_full = jnp.concatenate([grad_qkv, grad_output_proj[None]], axis=0)
    vector_head = jnp.stack(
        [
            grad_gain_one,
            grad_gain_two,
            grad_shift_one,
            grad_shift_two,
            jnp.sum(grad_query.astype(jnp.float32), axis=0),
            jnp.sum(grad_values.astype(jnp.float32), axis=0),
            grad_bias_mixed,
            jnp.sum(grad_branch.astype(jnp.float32), axis=0),
        ]
    )
    grad_bias_up = jnp.sum(grad_pre_low.astype(jnp.float32), axis=0).reshape(FF // D, D)
    grad_vectors_full = jnp.concatenate([vector_head, grad_bias_up], axis=0)
    grad_attention, grad_vectors = (
        lax.psum_scatter(grad_attention_full, "fsdp", scatter_dimension=1, tiled=True),
        lax.psum_scatter(grad_vectors_full, "fsdp", scatter_dimension=1, tiled=True),
    )
    attention_new = inner_step(
        attention_weight, grad_attention, attention_first[0], attention_second[0], 0.03, 0.1
    )
    expand_new = inner_step(
        expand_weight, grad_expand, expand_first[0], expand_second[0], 0.03, 0.1
    )
    contract_new = inner_step(
        contract_weight, grad_contract, contract_first[0], contract_second[0], 0.015, 0.1
    )
    vectors_new = inner_step(vectors, grad_vectors, vectors_first[0], vectors_second[0], 0.2, 0.0)
    summed = (
        lax.psum((attention_weight - attention_new[0]).astype(jnp.bfloat16), "rep").astype(
            jnp.float32
        ),
        lax.psum((expand_weight - expand_new[0]).astype(jnp.bfloat16), "rep").astype(jnp.float32),
        lax.psum((contract_weight - contract_new[0]).astype(jnp.bfloat16), "rep").astype(
            jnp.float32
        ),
        lax.psum((vectors - vectors_new[0]).astype(jnp.bfloat16), "rep").astype(jnp.float32),
    )
    groups_count = lax.axis_size("rep")
    results = []
    for weight_now, momentum_now, inner_new, diff_total in zip(
        (attention_weight, expand_weight, contract_weight, vectors),
        (attention_momentum, expand_momentum, contract_momentum, vectors_momentum),
        (attention_new, expand_new, contract_new, vectors_new),
        summed,
    ):
        mean_diff = diff_total / groups_count
        momentum_new = 0.5 * momentum_now + mean_diff
        outer_new = weight_now - 0.7 * (mean_diff + 0.5 * momentum_new)
        results.append(
            (
                inner_new[1][None],
                inner_new[2][None],
                jnp.stack([mean_diff, momentum_new, outer_new]),
                outer_new.astype(jnp.bfloat16),
            )
        )
    return (
        layer_output.astype(jnp.bfloat16),
        input_grad,
        results[0][0],
        results[0][1],
        results[0][2],
        results[0][3],
        results[1][0],
        results[1][1],
        results[1][2],
        results[1][3],
        results[2][0],
        results[2][1],
        results[2][2],
        results[2][3],
        results[3][0],
        results[3][1],
        results[3][2],
        results[3][3],
    )


NEG=-1e30
QB=256
def attn_windows(seg_row):
    length = seg_row.shape[0]
    nb = length // QB
    firsts = seg_row[::QB]
    lasts = seg_row[QB-1::QB]
    begin = jnp.sum((seg_row[None, :] < firsts[:, None]).astype(jnp.int32), axis=1)
    end = jnp.sum((seg_row[None, :] <= lasts[:, None]).astype(jnp.int32), axis=1)
    start = begin // 128
    count = (end - start * 128 + QB - 1) // QB
    start = jnp.minimum(start, (length - count * QB) // 128)
    return start.astype(jnp.int32), count.astype(jnp.int32)
def lane_half(shape, h):
    lane = lax.broadcasted_iota(jnp.int32, shape, len(shape)-1)
    return (lane < 64) if h == 0 else (lane >= 64)
def dot(a, b, ca, cb):
    return lax.dot_general(a, b, (((ca,), (cb,)), ((), ())), preferred_element_type=jnp.float32)
def fold(value, join):
    part = value.shape[0] // 8
    parts = [value[i * part:(i + 1) * part] for i in range(8)]
    while len(parts) > 1:
        parts = [join(a, b) for a, b in zip(parts[::2], parts[1::2])]
    return parts[0]
def fwd_kernel(start_ref, count_ref, qkv_ref, segr_ref, segc_ref, o_ref, lse_ref, vt_ref):
    length = qkv_ref.shape[0]
    vt_ref[...] = qkv_ref[:, 256:384].T
    nb = length // QB
    for i in range(nb):
        rows = slice(i*QB, (i+1)*QB)
        for nn in range(1, nb+1):
            @pl.when(count_ref[i] == nn)
            def _():
                nk = nn*QB
                lo = pl.multiple_of(start_ref[i]*128, 128)
                kw = qkv_ref[pl.ds(lo, nk), 128:256]
                qb = qkv_ref[rows, 0:128]
                same = segc_ref[pl.ds(lo, nk), :] == segr_ref[:, rows]
                outs = []
                for h in range(2):
                    qh = jnp.where(lane_half(qb.shape, h), qb, jnp.zeros_like(qb))
                    st = jnp.where(same, dot(kw, qh, 1, 1), NEG)
                    m = jnp.max(fold(st, jnp.maximum), axis=0, keepdims=True)
                    p = jnp.exp(st - m)
                    l = jnp.sum(fold(p, jnp.add), axis=0, keepdims=True)
                    weighted = dot(vt_ref[h*64:(h+1)*64, pl.ds(lo, nk)], p.astype(jnp.bfloat16), 1, 0)
                    outs.append(weighted * (1.0 / l))
                    lse_ref[0, h:h+1, rows] = m + jnp.log(l)
                o_ref[rows, :] = jnp.concatenate(outs, axis=0).T.astype(jnp.bfloat16)
def bwd_kernel(start_ref, count_ref, qkv_ref, do_ref, lse_ref, segr_ref, segc_ref, d_ref, sums_ref, dk_acc, dv_acc, kt_ref):
    length = qkv_ref.shape[0]
    kt_ref[...] = qkv_ref[:, 128:256].T
    nb = length // QB
    dk_acc[...] = jnp.zeros_like(dk_acc)
    dv_acc[...] = jnp.zeros_like(dv_acc)
    for i in range(nb):
        rows = slice(i*QB, (i+1)*QB)
        for nn in range(1, nb+1):
            @pl.when(count_ref[i] == nn)
            def _():
                nk = nn*QB
                lo = pl.multiple_of(start_ref[i]*128, 128)
                win = pl.ds(lo, nk)
                kw = qkv_ref[win, 128:256]
                vw = qkv_ref[win, 256:384]
                qb = qkv_ref[rows, 0:128]
                db = do_ref[rows, :]
                same = segc_ref[win, :] == segr_ref[:, rows]
                dqs = []; dks = 0.0; dvs = 0.0
                for h in range(2):
                    hm = lane_half(qb.shape, h)
                    qh = jnp.where(hm, qb, jnp.zeros_like(qb))
                    dh = jnp.where(hm, db, jnp.zeros_like(db))
                    st = jnp.where(same, dot(kw, qh, 1, 1), NEG)
                    p = jnp.exp(st - lse_ref[0, h:h+1, rows])
                    dpt = dot(vw, dh, 1, 1)
                    rd = jnp.sum(fold(p * dpt, jnp.add), axis=0, keepdims=True)
                    ds = (p * (dpt - rd)).astype(jnp.bfloat16)
                    dvs = dvs + dot(p.astype(jnp.bfloat16), dh, 1, 0)
                    dks = dks + dot(ds, qh, 1, 0)
                    dqs.append(dot(kt_ref[h*64:(h+1)*64, win], ds, 1, 0))
                d_ref[rows, 0:128] = jnp.concatenate(dqs, axis=0).T.astype(jnp.bfloat16) * 0.125
                dk_acc[win, :] += dks
                dv_acc[win, :] += dvs
    d_ref[:, 128:256] = dk_acc[...].astype(jnp.bfloat16)
    d_ref[:, 256:384] = dv_acc[...].astype(jnp.bfloat16)
    sums_ref[0] = jnp.sum(d_ref[...].astype(jnp.float32), axis=0, keepdims=True)
def attn_fwd(qkv, seg):
    T, width = qkv.shape
    start, count = attn_windows(seg[0])
    segc = seg.reshape(T, 1)
    heads = width // 384
    return pl.pallas_call(
        fwd_kernel,
        out_shape=(jax.ShapeDtypeStruct((T, width // 3), jnp.bfloat16), jax.ShapeDtypeStruct((heads, 2, T), jnp.float32)),
        grid_spec=pltpu.PrefetchScalarGridSpec(
            num_scalar_prefetch=2, grid=(heads,),
            in_specs=[
                pl.BlockSpec((T, 384), lambda h, *_: (0, h)),
                pl.BlockSpec((1, T), lambda h, *_: (0, 0)),
                pl.BlockSpec((T, 1), lambda h, *_: (0, 0)),
            ],
            out_specs=(pl.BlockSpec((T, 128), lambda h, *_: (0, h)), pl.BlockSpec((1, 2, T), lambda h, *_: (h, 0, 0))),
            scratch_shapes=[pltpu.VMEM((128, T), jnp.bfloat16)],
        ),
        cost_estimate=cost(20 * T * T * width, 3 * T * width, T * T * width // 128),
        name="attn_fwd",
    )(start, count, qkv, seg, segc)


def attn_bwd(qkv, do, lse, seg, part):
    T, width = qkv.shape
    start, count = attn_windows(seg[0])
    segc = seg.reshape(T, 1)
    heads = width // 768
    first = part * heads
    return pl.pallas_call(
        bwd_kernel,
        out_shape=(jax.ShapeDtypeStruct((T, width // 2), jnp.bfloat16), jax.ShapeDtypeStruct((heads, 1, 384), jnp.float32)),
        grid_spec=pltpu.PrefetchScalarGridSpec(
            num_scalar_prefetch=2, grid=(heads,),
            in_specs=[
                pl.BlockSpec((T, 384), lambda h, *_: (0, first + h)),
                pl.BlockSpec((T, 128), lambda h, *_: (0, first + h)),
                pl.BlockSpec((1, 2, T), lambda h, *_: (first + h, 0, 0)),
                pl.BlockSpec((1, T), lambda h, *_: (0, 0)),
                pl.BlockSpec((T, 1), lambda h, *_: (0, 0)),
            ],
            out_specs=(pl.BlockSpec((T, 384), lambda h, *_: (0, h)), pl.BlockSpec((1, 1, 384), lambda h, *_: (h, 0, 0))),
            scratch_shapes=[pltpu.VMEM((T, 128), jnp.float32)] * 2 + [pltpu.VMEM((128, T), jnp.bfloat16)],
        ),
        cost_estimate=cost(20 * T * T * width, 6 * T * width, T * T * width // 64),
        name="attn_bwd",
    )(start, count, qkv, do, lse, seg, segc)


MESH_ID = pl.DeviceIdType.MESH


def bits_of():
    rep = lax.axis_index("rep")
    fsdp = lax.axis_index("fsdp")
    return dict(
        rep=rep, fsdp=fsdp, x=rep // 2, c=rep % 2, z1=fsdp // 4, z0=(fsdp // 2) % 2, y=fsdp % 2
    )


def partner_of(at, which):
    rep, fsdp = at["rep"], at["fsdp"]
    if which == "c":
        rep = rep + 1 - 2 * at["c"]
    elif which == "x":
        rep = rep + 2 - 4 * at["x"]
    elif which == "y":
        fsdp = fsdp + 1 - 2 * at["y"]
    elif which == "z0":
        fsdp = fsdp + 2 - 4 * at["z0"]
    elif which == "z1":
        fsdp = fsdp + 4 - 8 * at["z1"]
    else:
        rep = rep + 1 - 2 * at["c"]
        fsdp = fsdp + 2 - 4 * at["z0"]
    return (rep, fsdp)


REL = [(a, b, d) for d in (0, 1) for b in (0, 1) for a in (0, 1)]


def gather_kernel(
    qkv_in, wo_in, vec_in, tok_in, seg_in,
    qkv_out, wo_out, vec_out, tok_out, seg_out,
    tok_buf, seg_buf, send_sem, recv_sem, local_sem,
):
    at = bits_of()
    other = {k: partner_of(at, k) for k in ("c", "x", "y", "z0", "z1", "swap")}
    barrier = pltpu.get_barrier_semaphore()
    for k in ("c", "x", "y", "z0", "z1"):
        pl.semaphore_signal(barrier, inc=1, device_id=other[k], device_id_type=MESH_ID)
    moves = at["c"] != at["z0"]

    @pl.when(moves)
    def _():
        pl.semaphore_signal(barrier, inc=1, device_id=other["swap"], device_id_type=MESH_ID)
        pl.semaphore_wait(barrier, 6)

    @pl.when(jnp.logical_not(moves))
    def _():
        pl.semaphore_wait(barrier, 5)

    def flip(bit, rel):
        return bit + rel - 2 * bit * rel

    def shard(rel):
        return 4 * flip(at["z1"], rel[1]) + 2 * flip(at["z0"], rel[0]) + flip(at["y"], rel[2])

    counter = [0]
    started = []

    def send(src, dst, which):
        k = counter[0]
        counter[0] += 1
        copy = pltpu.make_async_remote_copy(
            src_ref=src, dst_ref=dst, send_sem=send_sem.at[k], recv_sem=recv_sem.at[k],
            device_id=other[which], device_id_type=MESH_ID,
        )
        copy.start()
        started.append(copy)
        return copy

    class Piece:
        def __init__(self, own, slot, split_x):
            self.own, self.slot, self.split_x = own, slot, split_x
            self.part = (2 * at["x"] + at["c"]) if split_x else at["c"]
            self.part_x = (2 * (1 - at["x"]) + at["c"]) if split_x else None
            self.copies = {}

        def first(self):
            zero = (0, 0, 0)
            for which in ("z1", "z0", "y"):
                self.copies[which, zero] = send(
                    self.own(self.part), self.slot(shard(zero), self.part), which
                )
            self.copies["c", zero] = send(self.own(None), self.slot(shard(zero), None), "c")

        def onward(self, rel):
            here = self.slot(shard(rel), self.part)
            if rel == (0, 1, 0):
                self.copies["z0", rel] = send(here, here, "z0")
            if rel[2] == 0:
                self.copies["y", rel] = send(here, here, "y")
            if self.split_x:
                self.copies["x", rel] = send(here, here, "x")
            self.copies["c", rel] = send(here, here, "c")

        def arrive(self, which, came):
            self.copies[which, came].wait_recv()
            step = {"z0": (1, 0, 0), "z1": (0, 1, 0), "y": (0, 0, 1)}[which]
            self.onward(tuple(p + q for p, q in zip(came, step)))

        def near(self):
            self.arrive("z1", (0, 0, 0))
            self.arrive("z0", (0, 0, 0))

        def rest(self):
            self.arrive("y", (0, 0, 0))
            self.arrive("z0", (0, 1, 0))
            self.arrive("y", (0, 1, 0))
            self.arrive("y", (1, 0, 0))
            self.arrive("y", (1, 1, 0))

        def last(self):
            if self.split_x:
                for rel in REL[1:]:
                    self.copies["x", rel].wait_recv()
                    there = self.slot(shard(rel), self.part_x)
                    self.copies["cx", rel] = send(there, there, "c")

        def finish(self):
            for (which, rel), copy in self.copies.items():
                if which in ("c", "cx"):
                    copy.wait_recv()

    def rows(ref, count):
        full = ref.shape[-2] // 8
        def slot(f, part):
            if part is None:
                at_row, n = f * full, full
            else:
                at_row, n = f * full + part * (full // count), full // count
            at_row = pl.multiple_of(at_row, 8)
            return ref.at[pl.ds(at_row, n), :]
        return slot

    def own_rows(ref, count):
        full = ref.shape[-2]
        def own(part):
            if part is None:
                return ref
            row = pl.multiple_of(part * (full // count), 8)
            n = full // count
            return ref.at[pl.ds(row, n), :]
        return own

    qkv, wo = pieces = [
        Piece(own_rows(qkv_in, 4), rows(qkv_out, 4), True),
        Piece(own_rows(wo_in, 4), rows(wo_out, 4), True),
    ]
    zero = (0, 0, 0)
    vec_copies = [
        send(vec_in, vec_out.at[shard(zero)], which) for which in ("c", "z1", "z0", "y")
    ]
    pieces[0].first()
    tok_k, seg_k = counter[0], counter[0] + 1
    counter[0] += 2

    def swap_copy(src, dst, k):
        return pltpu.make_async_remote_copy(
            src_ref=src, dst_ref=dst, send_sem=send_sem.at[k], recv_sem=recv_sem.at[k],
            device_id=other["swap"], device_id_type=MESH_ID,
        )

    @pl.when(moves)
    def _():
        swap_copy(tok_in, tok_out, tok_k).start()
        swap_copy(seg_in, seg_out, seg_k).start()

    @pl.when(jnp.logical_not(moves))
    def _():
        one = pltpu.make_async_copy(tok_in, tok_buf, local_sem.at[0])
        two = pltpu.make_async_copy(seg_in, seg_buf, local_sem.at[1])
        one.start()
        two.start()
        one.wait()
        two.wait()
        three = pltpu.make_async_copy(tok_buf, tok_out, local_sem.at[0])
        four = pltpu.make_async_copy(seg_buf, seg_out, local_sem.at[1])
        three.start()
        four.start()
        three.wait()
        four.wait()

    wo.first()
    qkv.near()
    vec_copies[1].wait_recv()
    here = vec_out.at[shard((0, 1, 0))]
    vec_far = send(here, here, "z0")
    vec_more = [send(here, here, "y")]
    vec_copies[2].wait_recv()
    here = vec_out.at[shard((1, 0, 0))]
    vec_more.append(send(here, here, "y"))
    qkv.rest()
    wo.near()
    wo.rest()
    vec_far.wait_recv()
    here = vec_out.at[shard((1, 1, 0))]
    vec_more.append(send(here, here, "y"))
    qkv.last()
    wo.last()
    for piece in pieces:
        piece.finish()
    for copy in [vec_copies[0], vec_copies[3]] + vec_more:
        copy.wait_recv()
    for copy in started:
        copy.wait_send()

    @pl.when(moves)
    def _():
        swap_copy(tok_in, tok_out, tok_k).wait()
        swap_copy(seg_in, seg_out, seg_k).wait()


GATHER_COPIES = 29 * 2 + 8 + 2


def gather_all(qkv, wo, vec, tok, seg):
    bf = jnp.bfloat16
    shape = jax.ShapeDtypeStruct
    whole = pl.BlockSpec(memory_space=pl.ANY)
    return pl.pallas_call(
        gather_kernel,
        out_shape=(
            shape((8 * qkv.shape[0], qkv.shape[1]), bf),
            shape((8 * wo.shape[0], wo.shape[1]), bf),
            shape((8,) + vec.shape, bf),
            shape(tok.shape, bf),
            shape(seg.shape, seg.dtype),
        ),
        in_specs=[whole] * 5,
        out_specs=(whole,) * 5,
        scratch_shapes=[
            pltpu.VMEM(tok.shape, bf),
            pltpu.VMEM(seg.shape, seg.dtype),
            pltpu.SemaphoreType.DMA((GATHER_COPIES,)),
            pltpu.SemaphoreType.DMA((GATHER_COPIES,)),
            pltpu.SemaphoreType.DMA((2,)),
        ],
        compiler_params=pltpu.CompilerParams(collective_id=0, has_side_effects=True),
        name="gather_weights",
    )(qkv, wo, vec, tok, seg)


SHRINK = 1000
BF, F32 = jnp.bfloat16, jnp.float32
SHAPE = jax.ShapeDtypeStruct


def full_spec(shape):
    return pl.BlockSpec(shape, lambda *_: (0,) * len(shape), pipeline_mode=pl.Buffered(1))


def cost(flops, moved, exps=0):
    return pl.CostEstimate(flops=int(flops) // SHRINK, bytes_accessed=int(moved) // SHRINK, transcendentals=int(exps) // SHRINK)


def qkv_kernel(x_ref, w_ref, bias_ref, scale_ref, o_ref):
    for i in range(4):
        rows = slice(i * 256, (i + 1) * 256)
        z = dot(x_ref[rows, :], w_ref[...], 1, 0)
        o_ref[rows, :] = ((z + bias_ref[...]) * scale_ref[...]).astype(BF)


def qkv_call(x, w, bias, scale):
    tokens, width = x.shape[0], w.shape[1]
    tile = 768
    return pl.pallas_call(
        qkv_kernel,
        out_shape=SHAPE((tokens, width), BF),
        grid=(width // tile,),
        in_specs=[
            full_spec(x.shape),
            pl.BlockSpec((x.shape[1], tile), lambda j: (0, j)),
            pl.BlockSpec((1, tile), lambda j: (0, j)),
            pl.BlockSpec((1, tile), lambda j: (0, j)),
        ],
        out_specs=pl.BlockSpec((tokens, tile), lambda j: (0, j)),
        cost_estimate=cost(2 * tokens * D * width, 2 * (tokens * D + D * width + tokens * width)),
        name="qkv",
    )(x, w, bias, scale)


def mean_row(value):
    return jnp.mean(value, axis=-1, keepdims=True)


def mix_kernel(c_ref, w_ref, x_ref, rows_ref, n_ref, q_ref, low_ref):
    value = x_ref[...].astype(F32) + dot(c_ref[...], w_ref[...], 1, 0) + rows_ref[6:7, :]
    center = value - mean_row(value)
    inv = lax.rsqrt(mean_row(center * center) + 1e-05)
    normed = center * inv
    n_ref[...] = normed
    q_ref[...] = inv
    low_ref[...] = (normed * rows_ref[0:1, :] + rows_ref[2:3, :]).astype(BF)


def mix_call(mixed, w_out, tok, rows):
    t = tok.shape[0]
    tile = pl.BlockSpec((256, D), lambda i: (i, 0))
    return pl.pallas_call(
        mix_kernel,
        out_shape=(SHAPE((t, D), F32), SHAPE((t, 1), F32), SHAPE((t, D), BF)),
        grid=(t // 256,),
        in_specs=[tile, full_spec((D, D)), tile, full_spec(rows.shape)],
        out_specs=(tile, pl.BlockSpec((256, 1), lambda i: (i, 0)), tile),
        cost_estimate=cost(2 * t * D * D, 12 * t * D + 2 * D * D),
        name="mix_norm",
    )(mixed, w_out, tok, rows)


def up_kernel(place_ref, h_ref, *refs):
    parts, (bias_ref, g_ref, s_ref) = refs[:4], refs[4:]
    each = pl.num_programs(0) // 4

    def tile(w_ref):
        for i in range(8):
            rows = slice(i * 128, (i + 1) * 128)
            z = dot(h_ref[rows, :], w_ref[...], 1, 0) + bias_ref[...]
            phi, bell = erf_parts(z)
            g_ref[rows, :] = (z * phi).astype(BF)
            s_ref[rows, :] = (phi + z * bell * 0.3989422804014327).astype(BF)

    for k in range(4):
        pl.when(pl.program_id(0) // each == k)(partial(tile, parts[k]))


def up_call(low, parts, place, bias):
    t = low.shape[0]
    tile = 512
    each = FF // tile // 4
    where = lambda j, p: (0, p[j // each] * each + lax.rem(j, each))
    out = pl.BlockSpec((t, tile), where)

    def part(k):
        return pl.BlockSpec((D, tile), lambda j, p: (0, jnp.clip(j - k * each, 0, each - 1)))

    return pl.pallas_call(
        up_kernel,
        out_shape=(SHAPE((t, FF), BF), SHAPE((t, FF), BF)),
        grid_spec=pltpu.PrefetchScalarGridSpec(
            num_scalar_prefetch=1, grid=(FF // tile,),
            in_specs=[full_spec(low.shape)] + [part(k) for k in range(4)] + [pl.BlockSpec((1, tile), where)],
            out_specs=(out, out),
        ),
        cost_estimate=cost(2 * t * D * FF, 2 * (t * D + D * FF + 2 * t * FF), 2 * t * FF),
        name="up_gelu",
    )(place, low, *parts, bias)


def row_sum(value):
    return jnp.sum(value, axis=0, keepdims=True)


def norm_back(grad, normed, inv, gain):
    scaled = grad * gain
    return inv * (scaled - mean_row(scaled) - normed * mean_row(scaled * normed))


def down_kernel(
    core_ref, g_ref, own_ref, came_ref, n_ref, cot_ref, rows_ref, out_ref, dr_ref, dm_ref, sums_ref, m_ref
):
    half = D // 2
    m_ref[:, pl.ds(pl.multiple_of(core_ref[0] * half, half), half)] = dot(g_ref[...], own_ref[...], 1, 0)
    m_ref[:, pl.ds(pl.multiple_of((1 - core_ref[0]) * half, half), half)] = dot(g_ref[...], came_ref[...], 1, 0)
    hidden = n_ref[...] * rows_ref[0:1, :] + rows_ref[2:3, :]
    value = hidden + m_ref[...] + rows_ref[7:8, :]
    center = value - mean_row(value)
    inv = lax.rsqrt(mean_row(center * center) + 1e-05)
    normed = center * inv
    gain = rows_ref[1:2, :]
    out_ref[...] = (normed * gain + rows_ref[3:4, :]).astype(BF)
    grad = cot_ref[...].astype(F32)
    back = norm_back(grad, normed, inv, gain)
    low = back.astype(BF)
    dr_ref[...] = back
    dm_ref[...] = low

    @pl.when(pl.program_id(0) == 0)
    def _():
        sums_ref[...] = jnp.zeros_like(sums_ref)

    sums_ref[0:1, :] += row_sum(grad * normed)
    sums_ref[1:2, :] += row_sum(grad)
    sums_ref[2:3, :] += row_sum(low.astype(F32))


def down_call(act, own, came, normed, cot, rows, core):
    t = act.shape[0]
    tile = pl.BlockSpec((256, D), lambda i, c: (i, 0))
    return pl.pallas_call(
        down_kernel,
        out_shape=(SHAPE((t, D), BF), SHAPE((t, D), F32), SHAPE((t, D), BF), SHAPE((8, D), F32)),
        grid_spec=pltpu.PrefetchScalarGridSpec(
            num_scalar_prefetch=1, grid=(t // 256,),
            in_specs=[
                pl.BlockSpec((256, FF), lambda i, c: (i, 0)), full_spec((FF, D // 2)), full_spec((FF, D // 2)),
                tile, tile, full_spec(rows.shape),
            ],
            out_specs=(tile, tile, tile, pl.BlockSpec((8, D), lambda i, c: (0, 0))),
            scratch_shapes=[pltpu.VMEM((256, D), F32)],
        ),
        cost_estimate=cost(2 * t * D * FF, 2 * (t * FF + D * FF) + 14 * t * D),
        name="down_norm",
    )(core.reshape(1), act, own, came, normed, cot, rows)


def slope_kernel(core_ref, left_ref, right_ref, own_ref, came_ref, s_ref, o_ref, sums_ref):
    total = 0.0
    for i in range(4):
        rows = slice(i * 256, (i + 1) * 256)
        back = dot(left_ref[rows, :], own_ref[...], 1, 1) + dot(right_ref[rows, :], came_ref[...], 1, 1)
        z = (back * s_ref[rows, :].astype(F32)).astype(BF)
        o_ref[rows, :] = z
        total = total + row_sum(z.astype(F32))
    sums_ref[...] = total


def slope_call(dm, own, came, slope, core):
    t = dm.shape[0]
    tile = 512
    wide = pl.BlockSpec((t, tile), lambda j, c: (0, j))
    part = pl.BlockSpec((tile, D // 2), lambda j, c: (j, 0))
    return pl.pallas_call(
        slope_kernel,
        out_shape=(SHAPE((t, FF), BF), SHAPE((1, FF), F32)),
        grid_spec=pltpu.PrefetchScalarGridSpec(
            num_scalar_prefetch=1, grid=(FF // tile,),
            in_specs=[
                pl.BlockSpec((t, D // 2), lambda j, c: (0, c[0])),
                pl.BlockSpec((t, D // 2), lambda j, c: (0, 1 - c[0])),
                part, part, wide,
            ],
            out_specs=(wide, pl.BlockSpec((1, tile), lambda j, c: (0, j))),
        ),
        cost_estimate=cost(2 * t * D * FF, 2 * (t * D + D * FF + 2 * t * FF)),
        name="down_back",
    )(core.reshape(1), dm, dm, own, came, slope)


def hidden_kernel(place_ref, *refs):
    grads, parts = refs[:4], refs[4:8]
    dr_ref, n_ref, q_ref, wo_ref, rows_ref, r_ref, a_ref, c_ref, sums_ref = refs[8:]
    grad = dr_ref[...]
    for grad_ref, w_ref in zip(grads, parts):
        grad = grad + dot(grad_ref[...], w_ref[...], 1, 1)
    normed = n_ref[...]
    back = norm_back(grad, normed, q_ref[...], rows_ref[0:1, :])
    low = back.astype(BF)
    r_ref[...] = back
    a_ref[...] = low
    c_ref[...] = dot(low, wo_ref[...], 1, 1).astype(BF)

    @pl.when(pl.program_id(0) == 0)
    def _():
        sums_ref[...] = jnp.zeros_like(sums_ref)

    sums_ref[0:1, :] += row_sum(grad * normed)
    sums_ref[1:2, :] += row_sum(grad)
    sums_ref[2:3, :] += row_sum(low.astype(F32))


def hidden_call(dz, parts, place, dr, normed, inv, w_out, rows):
    t = dz.shape[0]
    tile = pl.BlockSpec((256, D), lambda i, p: (i, 0))

    def quarter(k):
        return pl.BlockSpec((256, FF // 4), lambda i, p: (i, p[k]))

    return pl.pallas_call(
        hidden_kernel,
        out_shape=(SHAPE((t, D), F32), SHAPE((t, D), BF), SHAPE((t, D), BF), SHAPE((8, D), F32)),
        grid_spec=pltpu.PrefetchScalarGridSpec(
            num_scalar_prefetch=1, grid=(t // 256,),
            in_specs=[quarter(k) for k in range(4)] + [full_spec((D, FF // 4))] * 4 + [
                tile, tile,
                pl.BlockSpec((256, 1), lambda i, p: (i, 0)), full_spec((D, D)), full_spec(rows.shape),
            ],
            out_specs=(tile, tile, tile, pl.BlockSpec((8, D), lambda i, p: (0, 0))),
        ),
        cost_estimate=cost(2 * t * D * (FF + D), 2 * (t * FF + D * FF) + 16 * t * D),
        name="up_back_norm",
    )(place, *([dz] * 4), *parts, dr, normed, inv, w_out, rows)


def input_kernel(a_ref, b_ref, w_ref, r_ref, o_ref):
    half = a_ref.shape[1]
    value = dot(a_ref[...], w_ref[:, :half], 1, 1) + dot(b_ref[...], w_ref[:, half:], 1, 1)
    o_ref[...] = (r_ref[...] + value).astype(BF)


def input_call(part_a, part_b, w_qkv, resid):
    t, width = part_a.shape
    tile = pl.BlockSpec((256, D), lambda i: (i, 0))
    wide = pl.BlockSpec((256, width), lambda i: (i, 0))
    return pl.pallas_call(
        input_kernel,
        out_shape=SHAPE((t, D), BF),
        grid=(t // 256,),
        in_specs=[wide, wide, full_spec(w_qkv.shape), tile],
        out_specs=tile,
        cost_estimate=cost(4 * t * D * width, 4 * (t * width + D * width) + 6 * t * D),
        name="input_back",
    )(part_a, part_b, w_qkv, resid)


def weight_kernel(half_ref, first_ref, second_ref, right_ref, *refs):
    o_ref, turned = refs[-2], refs[-1]

    @pl.when(pl.program_id(1) == 0)
    def _():
        part = first_ref.shape[1]
        turned[:part, :] = first_ref[...].T
        turned[part:, :] = second_ref[...].T

    value = dot(turned[...], right_ref[...], 1, 0)
    if len(refs) == 3:
        value = value + refs[0][...].astype(F32)
    o_ref[...] = value.astype(BF)


def weight_call(left, right, half, came=None):
    t, rows = left.shape
    width = right.shape[1]
    bm = 512
    bn = 1024 if width == 1024 else 512
    steps = rows // 2 // bm
    if steps == 1:
        first = lambda i, j, h: (0, h[0])
        second = lambda i, j, h: (0, 2 + h[0])
    else:
        block = lambda i, h: lax.div(i, steps // 2) * steps + h[0] * (steps // 2) + lax.rem(i, steps // 2)
        first = lambda i, j, h: (0, 2 * block(i, h))
        second = lambda i, j, h: (0, 2 * block(i, h) + 1)
    specs = [
        pl.BlockSpec((t, bm // 2), first),
        pl.BlockSpec((t, bm // 2), second),
        pl.BlockSpec((t, bn), lambda i, j, h: (0, j)),
    ]
    values = [left, left, right]
    out = pl.BlockSpec((bm, bn), lambda i, j, h: (i, j))
    if came is not None:
        specs.append(out)
        values.append(came)
    return pl.pallas_call(
        weight_kernel,
        out_shape=SHAPE((rows // 2, width), BF),
        grid_spec=pltpu.PrefetchScalarGridSpec(
            num_scalar_prefetch=1, grid=(steps, width // bn), in_specs=specs, out_specs=out,
            scratch_shapes=[pltpu.VMEM((bm, t), BF)],
        ),
        cost_estimate=cost(t * rows * width, t * rows + 2 * t * width + 2 * rows * width),
        name="weight_grad",
    )(half.reshape(1), *values)


def inner_kernel(rate, decay, w_ref, g_ref, m_ref, v_ref, m_out, v_out, d_out):
    weight = w_ref[...]
    new, m_out[...], v_out[...] = inner_step(
        weight, g_ref[...].astype(F32), m_ref[...], v_ref[...], rate, decay
    )
    d_out[...] = (weight - new).astype(BF)


def inner_call(weight, grad, first, second, rate, decay):
    rows, width = weight.shape
    block = 32 * 4096 // width
    tile = pl.BlockSpec((block, width), lambda i: (i, 0))
    like = SHAPE((rows, width), F32)
    return pl.pallas_call(
        partial(inner_kernel, rate, decay),
        out_shape=(like, like, SHAPE((rows, width), BF)),
        grid=(rows // block,),
        in_specs=[tile] * 4,
        out_specs=(tile,) * 3,
        cost_estimate=cost(20 * rows * width, 24 * rows * width),
        name="inner_step",
    )(weight, grad, first, second)


def outer_kernel(core_ref, w_ref, u_ref, own_ref, came_ref, o_ref, c_ref):
    mine = (core_ref[0] == pl.program_id(0)).astype(F32)
    total = own_ref[...].astype(F32) * mine + came_ref[...].astype(F32) * (1.0 - mine)
    mean = total * 0.25
    weight = w_ref[...]
    momentum = 0.5 * u_ref[...] + mean
    new = weight - 0.7 * (mean + 0.5 * momentum)
    o_ref[0] = mean
    o_ref[1] = momentum
    o_ref[2] = new
    c_ref[...] = new.astype(BF)


def outer_call(weight, momentum, own, came, core):
    rows, width = weight.shape
    block = 32 * 4096 // width
    steps = rows // 2 // block
    tile = pl.BlockSpec((block, width), lambda h, i, c: (h * steps + i, 0))
    part = pl.BlockSpec((block, width), lambda h, i, c: (i, 0))
    return pl.pallas_call(
        outer_kernel,
        out_shape=(SHAPE((3, rows, width), F32), SHAPE((rows, width), BF)),
        grid_spec=pltpu.PrefetchScalarGridSpec(
            num_scalar_prefetch=1, grid=(2, steps), in_specs=[tile, tile, part, part],
            out_specs=(pl.BlockSpec((3, block, width), lambda h, i, c: (0, h * steps + i, 0)), tile),
        ),
        cost_estimate=cost(10 * rows * width, 26 * rows * width),
        name="outer_step",
    )(core.reshape(1), weight, momentum, own, came)


def erf_parts(value):
    size = jnp.abs(value) * 0.7071067811865476
    share = 1.0 / (1.0 + 0.5 * size)
    inner = 0.17087277
    for coefficient in (
        -0.82215223, 1.48851587, -1.13520398, 0.27886807, -0.18628806, 0.09678418, 0.37409196, 1.00002368
    ):
        inner = coefficient + share * inner
    square = size * size
    half = 0.5 * share * jnp.exp(share * inner - 1.26551223 - square)
    return jnp.where(value >= 0, 1.0 - half, half), jnp.exp(-square)


def xor_pairs(bits):
    place = {"y": 0, "z0": 1, "z1": 2, "c": 3, "x": 4}
    flip = sum(1 << place[bit] for bit in bits)
    pairs = []
    for device in range(32):
        if bits == ("c", "z0") and ((device >> 3) & 1) == ((device >> 1) & 1):
            continue
        pairs.append((device, device ^ flip))
    return pairs


def exchange(value, *bits):
    return lax.ppermute(value, ("rep", "fsdp"), xor_pairs(bits))


def add_low(left, right):
    return (left.astype(jnp.float32) + right.astype(jnp.float32)).astype(jnp.bfloat16)


def pick(value, index, axis):
    return lax.dynamic_index_in_dim(value, index, axis, keepdims=False)


def half_axis(total, which):
    return 1 if which == "y" and total.ndim == 4 else 0


def halve(at, total, which):
    away = pick(total, 1 - at[which], half_axis(total, which))
    return away, exchange(away, which)


def join(at, total, came, which, *gates):
    return add_low(pick(total, at[which], half_axis(total, which)), after(came, *gates))


def slabs(total):
    return total.reshape(2, 2, -1, total.shape[-1])


def after(value, *earlier):
    return lax.optimization_barrier((value,) + earlier)[0]


def weave(value):
    rows = value.shape[1]
    return jnp.transpose(value.reshape(3, rows, D // 128, 128), (1, 2, 0, 3)).reshape(rows, 3 * D)


def unweave(value):
    rows = value.shape[0]
    return jnp.transpose(value.reshape(rows, D // 128, 3, 128), (2, 0, 1, 3)).reshape(3, rows, D)


def per_device_fast(
    tokens,
    cotangent,
    segment_ids,
    attention_weight,
    attention_momentum,
    attention_first,
    attention_second,
    expand_weight,
    expand_momentum,
    expand_first,
    expand_second,
    contract_weight,
    contract_momentum,
    contract_first,
    contract_second,
    vectors,
    vectors_momentum,
    vectors_first,
    vectors_second,
):
    bf, f32 = jnp.bfloat16, jnp.float32
    at = bits_of()
    core = at["c"].astype(jnp.int32)
    def swapped(value, came):
        return jnp.where(at["c"] != at["z0"], came, value)

    def cross(value):
        return exchange(value, "c", "z0")

    quarter = 2 * core + at["x"].astype(jnp.int32)
    place = jnp.stack([quarter, 2 * (1 - core) + quarter - 2 * core, quarter + 1 - 2 * at["x"], 3 - quarter])
    part = expand_weight.shape[1] // 4
    in_own = lax.all_gather(
        lax.dynamic_slice_in_dim(expand_weight, quarter * part, part, axis=1).astype(bf), "fsdp", axis=0, tiled=True
    )
    attn_low = attention_weight.astype(bf)
    w_qkv, w_out, vector_full, tok, seg = gather_all(
        weave(attn_low[:3]), attn_low[3], vectors.astype(bf), tokens, segment_ids,
    )
    cot_came = cross(after(cotangent, w_qkv))
    rows = jnp.swapaxes(vector_full, 0, 1).reshape(-1, D).astype(f32)
    bias_up = rows[8:].reshape(1, FF)
    bias_qkv = weave(jnp.stack([rows[4], jnp.zeros_like(rows[4]), rows[5]])[:, None])
    scale_qkv = weave(jnp.stack([jnp.full((1, D), 0.125, f32)] + [jnp.ones((1, D), f32)] * 2))
    part = contract_weight.shape[1] // 2
    down_half = lax.dynamic_slice_in_dim(contract_weight, core * part, part, axis=1).astype(bf)
    down_own = lax.all_gather(after(down_half, w_qkv), "fsdp", axis=0, tiled=True)
    in_near = after(in_own, w_qkv)
    in_far = exchange(in_near, "x")
    in_side = exchange(in_near, "c")
    qkv = qkv_call(tok, w_qkv, bias_qkv, scale_qkv)
    mixed, log_sum = attn_fwd(qkv, seg)
    in_parts = [in_own, after(in_side, mixed), in_far, exchange(after(in_far, mixed), "c")]
    normed, inv, hidden_low = mix_call(mixed, w_out, tok, rows)
    cot = swapped(cotangent, after(cot_came, hidden_low))
    activated, slope = up_call(after(hidden_low, cot), in_parts, place, bias_up)
    down_other = exchange(after(down_own, activated), "c")
    layer_output, grad_sum, grad_branch, sums_two = down_call(
        activated, down_own, down_other, normed, cot, rows, core
    )
    output_came = cross(layer_output)
    down_send = weight_call(activated, grad_branch, 1 - core)
    grad_pre, sums_up = slope_call(after(grad_branch, down_send), down_own, down_other, slope, core)
    down_came = exchange(down_send, "c")
    up_send = weight_call(hidden_low, grad_pre, 1 - core)
    down_total = slabs(weight_call(activated, after(grad_branch, up_send), core, down_came))
    up_came = exchange(up_send, "c")
    away_d, came_d = halve(at, down_total, "y")
    up_total = slabs(weight_call(hidden_low, after(grad_pre, away_d), core, up_came))
    away_u, came_u = halve(at, up_total, "y")
    grad_resid, grad_attn, grad_mixed, sums_one = hidden_call(
        after(grad_pre, away_u), in_parts, place, grad_sum, normed, inv, w_out, rows
    )
    proj_send = weight_call(mixed, grad_attn, 1 - core)
    proj_came = exchange(proj_send, "c")
    output = swapped(layer_output, after(output_came, proj_send))
    grad_a, sums_a = attn_bwd(qkv, after(grad_mixed, proj_send, output), log_sum, seg, 0)
    send_a = weight_call(tok, grad_a, 1 - core)
    came_a = exchange(send_a, "c")
    down_one = join(at, down_total, came_d, "y", send_a)
    away_d, came_d = halve(at, down_one, "z1")
    proj_total = slabs(weight_call(mixed, after(grad_attn, away_d), core, proj_came))
    away_p, came_p = halve(at, proj_total, "y")
    total_a = slabs(weight_call(tok, after(grad_a, away_p), core, came_a))
    away_a, came_one = halve(at, total_a, "y")
    up_one = join(at, up_total, came_u, "y", away_a)
    away_u, came_u = halve(at, up_one, "z1")
    grad_b, sums_b = attn_bwd(qkv, after(grad_mixed, away_u), log_sum, seg, 1)
    send_b = weight_call(tok, grad_b, 1 - core)
    came_b = exchange(send_b, "c")
    down_two = join(at, down_one, came_d, "z1", send_b)
    cross_d = cross(down_two)
    proj_one = join(at, proj_total, came_p, "y", down_two)
    away_p, came_p = halve(at, proj_one, "z1")
    a_one = join(at, total_a, came_one, "y", away_p)
    away_a, came_a = halve(at, a_one, "z1")
    total_b = slabs(weight_call(tok, after(grad_b, away_a), core, came_b))
    away_b, came_b = halve(at, total_b, "y")
    sums_qkv = jnp.concatenate([sums_a, sums_b], axis=0).reshape(D // 128, 3, 128)
    vector_grad = jnp.concatenate(
        [
            sums_one[0:1],
            sums_two[0:1],
            sums_one[1:2],
            sums_two[1:2],
            sums_qkv[:, 0].reshape(1, D),
            sums_qkv[:, 2].reshape(1, D),
            sums_one[2:3],
            sums_two[2:3],
            sums_up.reshape(FF // D, D),
        ],
        axis=0,
    )

    def vector_send(parts, which):
        half = parts.shape[1] // 2
        away = lax.dynamic_slice_in_dim(parts, (1 - at[which]) * half, half, axis=1)
        return exchange(away, which)

    def vector_join(parts, came, which, *gates):
        half = parts.shape[1] // 2
        return lax.dynamic_slice_in_dim(parts, at[which] * half, half, axis=1) + after(came, *gates)

    vec_came = vector_send(vector_grad, "z1")

    def inner(weight, grad, first, second, rate, decay):
        flat = (-1, weight.shape[-1])
        return inner_call(
            weight.reshape(flat), grad.reshape(flat), first.reshape(flat), second.reshape(flat), rate, decay
        )

    def rep_send(diff):
        halves = diff.reshape(2, diff.shape[0] // 2, diff.shape[1])
        away = pick(halves, 1 - at["c"], 0)
        return away, exchange(away, "c")

    def rep_join(diff, came, *gates):
        halves = diff.reshape(2, diff.shape[0] // 2, diff.shape[1])
        return add_low(pick(halves, at["c"], 0), after(came, *gates))

    def outer(weight, momentum, own, came):
        flat = (-1, weight.shape[-1])
        return outer_call(weight.reshape(flat), momentum.reshape(flat), own, came, core)

    grad_contract = swapped(down_two, after(cross_d, away_b))
    contract_new = inner(contract_weight, grad_contract, contract_first, contract_second, 0.015, 0.1)
    sent_c, came_c = rep_send(contract_new[2])
    up_two = join(at, up_one, came_u, "z1", sent_c)
    cross_u = cross(up_two)
    vec_one = vector_join(vector_grad, vec_came, "z1", up_two)
    vec_came = vector_send(vec_one, "c")
    b_one = join(at, total_b, came_b, "y", up_two)
    away_b, came_b = halve(at, b_one, "z1")
    half_c = rep_join(contract_new[2], came_c, away_b)
    rest_c = exchange(half_c, "x")
    vec_two = vector_join(vec_one, vec_came, "c", half_c)
    vec_came = vector_send(vec_two, "y")
    input_grad = input_call(after(grad_a, away_b, half_c), grad_b, w_qkv, grad_resid)
    grad_expand = swapped(up_two, after(cross_u, input_grad))
    expand_new = inner(expand_weight, grad_expand, expand_first, expand_second, 0.03, 0.1)
    sent_e, came_e = rep_send(expand_new[2])
    proj_two = join(at, proj_one, came_p, "z1", sent_e)
    a_two = join(at, a_one, came_a, "z1", sent_e)
    cross_pa = cross(jnp.concatenate([proj_two, a_two], axis=1))
    vec_three = vector_join(vec_two, vec_came, "y", proj_two, a_two)
    vec_cross = cross(vec_three)
    full_c = add_low(half_c, after(rest_c, vec_three))
    back_c = exchange(full_c, "c")
    half_e = rep_join(expand_new[2], came_e, full_c)
    rest_e = exchange(half_e, "x")
    b_two = join(at, b_one, came_b, "z1", half_e)
    cross_b = cross(b_two)
    outer_c = outer(contract_weight, contract_momentum, full_c, after(back_c, b_two))
    grad_vectors = swapped(vec_three, after(vec_cross, outer_c[1]))
    inner_new, first_new, second_new = inner_step(
        vectors, grad_vectors, vectors_first[0], vectors_second[0], 0.2, 0.0
    )
    vec_diff = (vectors - inner_new).astype(bf)
    vec_near = exchange(vec_diff, "c")
    input_came = cross(after(input_grad, b_two, vec_diff))
    pa = swapped(jnp.concatenate([proj_two, a_two], axis=1), after(cross_pa, outer_c[1]))
    b_own = swapped(b_two, after(cross_b, vec_diff, pa))
    grad_qkv = jnp.concatenate([pa[:, D:], b_own], axis=1)
    grad_attention = jnp.concatenate([unweave(grad_qkv), pa[None, :, :D]], axis=0)
    attention_new = inner(attention_weight, grad_attention, attention_first, attention_second, 0.03, 0.1)
    sent_a, came_a = rep_send(attention_new[2])
    vec_half = add_low(vec_diff, after(vec_near, sent_a))
    vec_far = exchange(vec_half, "x")
    full_e = add_low(half_e, after(rest_e, vec_half))
    back_e = exchange(full_e, "c")
    half_a = rep_join(attention_new[2], came_a, full_e)
    rest_a = exchange(half_a, "x")
    outer_e = outer(expand_weight, expand_momentum, full_e, after(back_e, half_a))
    full_a = add_low(half_a, after(rest_a, outer_e[1]))
    back_a = exchange(full_a, "c")
    mean_diff = add_low(vec_half, after(vec_far, full_a)).astype(f32) / 4
    momentum_new = 0.5 * vectors_momentum + mean_diff
    outer_new = vectors - 0.7 * (mean_diff + 0.5 * momentum_new)
    input_grad = swapped(input_grad, after(input_came, full_a))
    outer_a = outer(attention_weight, attention_momentum, full_a, back_a)
    results = []
    for weight, first, new, (total, copy) in (
        (attention_weight, attention_first, attention_new, outer_a),
        (expand_weight, expand_first, expand_new, outer_e),
        (contract_weight, contract_first, contract_new, outer_c),
    ):
        results += [
            new[0].reshape(first.shape),
            new[1].reshape(first.shape),
            total.reshape((3,) + weight.shape),
            copy.reshape(weight.shape),
        ]
    results += [
        first_new[None],
        second_new[None],
        jnp.stack([mean_diff, momentum_new, outer_new]),
        outer_new.astype(bf),
    ]
    return (output, input_grad) + tuple(results)


def solution(mesh):
    placed = (
        P(("rep", "fsdp"), None),
        P(("rep", "fsdp"), None),
        P(("rep", "fsdp"), None),
        P(None, "fsdp", None),
        P(None, "fsdp", None),
        P("rep", None, "fsdp", None),
        P("rep", None, "fsdp", None),
        P("fsdp", None),
        P("fsdp", None),
        P("rep", "fsdp", None),
        P("rep", "fsdp", None),
        P("fsdp", None),
        P("fsdp", None),
        P("rep", "fsdp", None),
        P("rep", "fsdp", None),
        P(None, "fsdp"),
        P(None, "fsdp"),
        P("rep", None, "fsdp"),
        P("rep", None, "fsdp"),
    )
    small = mesh.shape["rep"] == 4 and mesh.shape["fsdp"] == 8
    body = per_device_fast if small else per_device
    return jax.shard_map(
        body,
        mesh=mesh,
        in_specs=placed,
        out_specs=(
            P(("rep", "fsdp"), None),
            P(("rep", "fsdp"), None),
            P("rep", None, "fsdp", None),
            P("rep", None, "fsdp", None),
            P(None, None, "fsdp", None),
            P(None, "fsdp", None),
            P("rep", "fsdp", None),
            P("rep", "fsdp", None),
            P(None, "fsdp", None),
            P("fsdp", None),
            P("rep", "fsdp", None),
            P("rep", "fsdp", None),
            P(None, "fsdp", None),
            P("fsdp", None),
            P("rep", None, "fsdp"),
            P("rep", None, "fsdp"),
            P(None, None, "fsdp"),
            P(None, "fsdp"),
        ),
        check_vma=False,
    )
```

```python
from functools import partial

import jax
import jax.numpy as jnp
from jax import lax
from jax.experimental import pallas as pl
from jax.experimental.pallas import tpu as pltpu
from jax.sharding import PartitionSpec as P

D = 1024
H = 16
HD = 64
FF = 4096
LEN = 1024
SEQ_DEV = 1
ADAM_STEP = 4
TOK_DEV = 1024


def norm_forward(values_in, gain_row, shift_row):
    center = values_in - jnp.mean(values_in, axis=-1, keepdims=True)
    inv_scale = lax.rsqrt(jnp.mean(center * center, axis=-1, keepdims=True) + 1e-05)
    normed = center * inv_scale
    return (normed * gain_row + shift_row, normed, inv_scale)


def norm_backward(grad_out, normed, inv_scale, gain_row):
    grad_gain = jnp.sum(grad_out * normed, axis=0)
    grad_shift = jnp.sum(grad_out, axis=0)
    scaled_grad = grad_out * gain_row
    grad_value = inv_scale * (
        scaled_grad
        - jnp.mean(scaled_grad, axis=-1, keepdims=True)
        - normed * jnp.mean(scaled_grad * normed, axis=-1, keepdims=True)
    )
    return (grad_value, grad_gain, grad_shift)


def product_over(left, right):
    return lax.dot_general(
        left, right, (((0,), (0,)), ((), ())), preferred_element_type=jnp.float32
    )


def product_back(left, right):
    return lax.dot_general(
        left, right, (((1,), (1,)), ((), ())), preferred_element_type=jnp.float32
    )


def block_scores(query_block, key_block, row_segments, all_segments):
    scores = jnp.einsum("qhd,khd->hqk", query_block, key_block, preferred_element_type=jnp.float32)
    same_doc = row_segments[:, None] == all_segments[None, :]
    return jnp.where(same_doc[None], scores, -1e30)


def inner_step(weight, gradient, first_moment, second_moment, learn_rate, weight_decay):
    first_new = 0.5 * first_moment + 0.5 * gradient
    second_new = 0.75 * second_moment + 0.25 * gradient * gradient
    update_dir = (
        first_new
        / (1.0 - 0.5**ADAM_STEP)
        / (jnp.sqrt(second_new / (1.0 - 0.75**ADAM_STEP)) + 1e-08)
    )
    return (weight - learn_rate * (update_dir + weight_decay * weight), first_new, second_new)


def per_device(
    tokens,
    cotangent,
    segment_ids,
    attention_weight,
    attention_momentum,
    attention_first,
    attention_second,
    expand_weight,
    expand_momentum,
    expand_first,
    expand_second,
    contract_weight,
    contract_momentum,
    contract_first,
    contract_second,
    vectors,
    vectors_momentum,
    vectors_first,
    vectors_second,
):
    attn_full, vector_full = (
        lax.all_gather(attention_weight.astype(jnp.bfloat16), "fsdp", axis=1, tiled=True),
        lax.all_gather(vectors.astype(jnp.bfloat16), "fsdp", axis=1, tiled=True),
    )
    vector_rows = vector_full.astype(jnp.float32)
    gain_one, gain_two, shift_one, shift_two = (
        vector_rows[0],
        vector_rows[1],
        vector_rows[2],
        vector_rows[3],
    )
    bias_query, bias_value, bias_mixed, bias_down = (
        vector_rows[4],
        vector_rows[5],
        vector_rows[6],
        vector_rows[7],
    )
    bias_up = vector_rows[8:].reshape(FF)
    projected = jnp.einsum("td,nde->nte", tokens, attn_full[:3], preferred_element_type=jnp.float32)
    query_all = ((projected[0] + bias_query) * 0.125).astype(jnp.bfloat16)
    key_all = projected[1].astype(jnp.bfloat16)
    value_all = (projected[2] + bias_value).astype(jnp.bfloat16)
    query_heads = query_all.reshape(SEQ_DEV, LEN, H, HD)
    key_heads = key_all.reshape(SEQ_DEV, LEN, H, HD)
    value_heads = value_all.reshape(SEQ_DEV, LEN, H, HD)
    block_rows = min(512, LEN)
    head_group = min(8, H)
    context_rows = []
    log_sums = []
    seq_index = 0
    for row_start in range(0, LEN, block_rows):
        block_pieces = []
        for head_start in range(0, H, head_group):
            head_part = slice(head_start, head_start + head_group)
            scores = block_scores(
                query_heads[seq_index, row_start : row_start + block_rows, head_part],
                key_heads[seq_index, :, head_part],
                segment_ids[seq_index, row_start : row_start + block_rows],
                segment_ids[seq_index],
            )
            row_max = jnp.max(scores, axis=-1, keepdims=True)
            exp_score = jnp.exp(scores - row_max)
            row_total = jnp.sum(exp_score, axis=-1, keepdims=True)
            probability = (exp_score / row_total).astype(jnp.bfloat16)
            block_pieces.append(
                jnp.einsum(
                    "hqk,khd->qhd",
                    probability,
                    value_heads[seq_index, :, head_part],
                    preferred_element_type=jnp.float32,
                )
            )
            log_sums.append(row_max + jnp.log(row_total))
        context_rows.append(jnp.concatenate(block_pieces, axis=1))
    mixed = jnp.concatenate(context_rows, axis=0).reshape(TOK_DEV, D).astype(jnp.bfloat16)
    attn_out = jnp.dot(mixed, attn_full[3], preferred_element_type=jnp.float32) + bias_mixed
    hidden, normed_one, scale_one = norm_forward(
        tokens.astype(jnp.float32) + attn_out, gain_one, shift_one
    )
    hidden_low = hidden.astype(jnp.bfloat16)
    ffn_expand, ffn_contract = (
        lax.all_gather(expand_weight.astype(jnp.bfloat16), "fsdp", axis=0, tiled=True),
        lax.all_gather(contract_weight.astype(jnp.bfloat16), "fsdp", axis=0, tiled=True),
    )
    pre_act = jnp.dot(hidden_low, ffn_expand, preferred_element_type=jnp.float32) + bias_up
    activated = jax.nn.gelu(pre_act, approximate=False).astype(jnp.bfloat16)
    branch = jnp.dot(activated, ffn_contract, preferred_element_type=jnp.float32) + bias_down
    layer_output, normed_two, scale_two = norm_forward(hidden + branch, gain_two, shift_two)
    grad_sum, grad_gain_two, grad_shift_two = norm_backward(
        cotangent.astype(jnp.float32), normed_two, scale_two, gain_two
    )
    grad_branch = grad_sum.astype(jnp.bfloat16)
    grad_act = product_back(grad_branch, ffn_contract)
    unused_value, gelu_pull = jax.vjp(partial(jax.nn.gelu, approximate=False), pre_act)
    grad_pre_low = gelu_pull(grad_act)[0].astype(jnp.bfloat16)
    grad_hidden = grad_sum + product_back(grad_pre_low, ffn_expand)
    contract_full = product_over(activated, grad_branch)
    expand_full = product_over(hidden_low, grad_pre_low)
    grad_expand, grad_contract = (
        lax.psum_scatter(expand_full, "fsdp", scatter_dimension=0, tiled=True),
        lax.psum_scatter(contract_full, "fsdp", scatter_dimension=0, tiled=True),
    )
    grad_resid, grad_gain_one, grad_shift_one = norm_backward(
        grad_hidden, normed_one, scale_one, gain_one
    )
    grad_attn_out = grad_resid.astype(jnp.bfloat16)
    grad_bias_mixed = jnp.sum(grad_attn_out.astype(jnp.float32), axis=0)
    grad_output_proj = product_over(mixed, grad_attn_out)
    grad_mixed = product_back(grad_attn_out, attn_full[3]).astype(jnp.bfloat16)
    grad_context = grad_mixed.reshape(SEQ_DEV, LEN, H, HD)
    query_grads = []
    lse_index = 0
    seq_index = 0
    key_totals = [
        jnp.zeros((LEN, head_group, HD), jnp.float32) for head_start in range(0, H, head_group)
    ]
    value_totals = [
        jnp.zeros((LEN, head_group, HD), jnp.float32) for head_start in range(0, H, head_group)
    ]
    for row_start in range(0, LEN, block_rows):
        block_pieces = []
        for group_index, head_start in enumerate(range(0, H, head_group)):
            head_part = slice(head_start, head_start + head_group)
            query_block = query_heads[seq_index, row_start : row_start + block_rows, head_part]
            key_block = key_heads[seq_index, :, head_part]
            value_block = value_heads[seq_index, :, head_part]
            ctx_grad = grad_context[seq_index, row_start : row_start + block_rows, head_part]
            scores = block_scores(
                query_block,
                key_block,
                segment_ids[seq_index, row_start : row_start + block_rows],
                segment_ids[seq_index],
            )
            probability = jnp.exp(scores - log_sums[lse_index])
            lse_index = lse_index + 1
            value_totals[group_index] = value_totals[group_index] + jnp.einsum(
                "hqk,qhd->khd",
                probability.astype(jnp.bfloat16),
                ctx_grad,
                preferred_element_type=jnp.float32,
            )
            prob_grad = jnp.einsum(
                "qhd,khd->hqk", ctx_grad, value_block, preferred_element_type=jnp.float32
            )
            row_dot = jnp.sum(probability * prob_grad, axis=-1, keepdims=True)
            score_grad = (probability * (prob_grad - row_dot)).astype(jnp.bfloat16)
            block_pieces.append(
                jnp.einsum(
                    "hqk,khd->qhd", score_grad, key_block, preferred_element_type=jnp.float32
                ).astype(jnp.bfloat16)
            )
            key_totals[group_index] = key_totals[group_index] + jnp.einsum(
                "hqk,qhd->khd", score_grad, query_block, preferred_element_type=jnp.float32
            )
        query_grads.append(jnp.concatenate(block_pieces, axis=1))
    key_grads = jnp.concatenate(
        [key_total.astype(jnp.bfloat16) for key_total in key_totals], axis=1
    )
    value_grads = jnp.concatenate(
        [value_total.astype(jnp.bfloat16) for value_total in value_totals], axis=1
    )
    grad_query = jnp.concatenate(query_grads, axis=0).reshape(TOK_DEV, D) * 0.125
    grad_keys = key_grads.reshape(TOK_DEV, D)
    grad_values = value_grads.reshape(TOK_DEV, D)
    stacked_grads = jnp.stack([grad_query, grad_keys, grad_values])
    grad_qkv = jnp.einsum("td,nte->nde", tokens, stacked_grads, preferred_element_type=jnp.float32)
    input_grad = (
        grad_resid
        + jnp.einsum(
            "nte,nde->td", stacked_grads, attn_full[:3], preferred_element_type=jnp.float32
        )
    ).astype(jnp.bfloat16)
    grad_attention_full = jnp.concatenate([grad_qkv, grad_output_proj[None]], axis=0)
    vector_head = jnp.stack(
        [
            grad_gain_one,
            grad_gain_two,
            grad_shift_one,
            grad_shift_two,
            jnp.sum(grad_query.astype(jnp.float32), axis=0),
            jnp.sum(grad_values.astype(jnp.float32), axis=0),
            grad_bias_mixed,
            jnp.sum(grad_branch.astype(jnp.float32), axis=0),
        ]
    )
    grad_bias_up = jnp.sum(grad_pre_low.astype(jnp.float32), axis=0).reshape(FF // D, D)
    grad_vectors_full = jnp.concatenate([vector_head, grad_bias_up], axis=0)
    grad_attention, grad_vectors = (
        lax.psum_scatter(grad_attention_full, "fsdp", scatter_dimension=1, tiled=True),
        lax.psum_scatter(grad_vectors_full, "fsdp", scatter_dimension=1, tiled=True),
    )
    attention_new = inner_step(
        attention_weight, grad_attention, attention_first[0], attention_second[0], 0.03, 0.1
    )
    expand_new = inner_step(
        expand_weight, grad_expand, expand_first[0], expand_second[0], 0.03, 0.1
    )
    contract_new = inner_step(
        contract_weight, grad_contract, contract_first[0], contract_second[0], 0.015, 0.1
    )
    vectors_new = inner_step(vectors, grad_vectors, vectors_first[0], vectors_second[0], 0.2, 0.0)
    summed = (
        lax.psum((attention_weight - attention_new[0]).astype(jnp.bfloat16), "rep").astype(
            jnp.float32
        ),
        lax.psum((expand_weight - expand_new[0]).astype(jnp.bfloat16), "rep").astype(jnp.float32),
        lax.psum((contract_weight - contract_new[0]).astype(jnp.bfloat16), "rep").astype(
            jnp.float32
        ),
        lax.psum((vectors - vectors_new[0]).astype(jnp.bfloat16), "rep").astype(jnp.float32),
    )
    groups_count = lax.axis_size("rep")
    results = []
    for weight_now, momentum_now, inner_new, diff_total in zip(
        (attention_weight, expand_weight, contract_weight, vectors),
        (attention_momentum, expand_momentum, contract_momentum, vectors_momentum),
        (attention_new, expand_new, contract_new, vectors_new),
        summed,
    ):
        mean_diff = diff_total / groups_count
        momentum_new = 0.5 * momentum_now + mean_diff
        outer_new = weight_now - 0.7 * (mean_diff + 0.5 * momentum_new)
        results.append(
            (
                inner_new[1][None],
                inner_new[2][None],
                jnp.stack([mean_diff, momentum_new, outer_new]),
                outer_new.astype(jnp.bfloat16),
            )
        )
    return (
        layer_output.astype(jnp.bfloat16),
        input_grad,
        results[0][0],
        results[0][1],
        results[0][2],
        results[0][3],
        results[1][0],
        results[1][1],
        results[1][2],
        results[1][3],
        results[2][0],
        results[2][1],
        results[2][2],
        results[2][3],
        results[3][0],
        results[3][1],
        results[3][2],
        results[3][3],
    )


NEG=-1e30
QB=256
def attn_windows(seg_row):
    length = seg_row.shape[0]
    nb = length // QB
    firsts = seg_row[::QB]
    lasts = seg_row[QB-1::QB]
    begin = jnp.sum((seg_row[None, :] < firsts[:, None]).astype(jnp.int32), axis=1)
    end = jnp.sum((seg_row[None, :] <= lasts[:, None]).astype(jnp.int32), axis=1)
    start = begin // 128
    count = (end - start * 128 + QB - 1) // QB
    start = jnp.minimum(start, (length - count * QB) // 128)
    return start.astype(jnp.int32), count.astype(jnp.int32)
def lane_half(shape, h):
    lane = lax.broadcasted_iota(jnp.int32, shape, len(shape)-1)
    return (lane < 64) if h == 0 else (lane >= 64)
def dot(a, b, ca, cb):
    return lax.dot_general(a, b, (((ca,), (cb,)), ((), ())), preferred_element_type=jnp.float32)
def fold(value, join):
    part = value.shape[0] // 8
    parts = [value[i * part:(i + 1) * part] for i in range(8)]
    while len(parts) > 1:
        parts = [join(a, b) for a, b in zip(parts[::2], parts[1::2])]
    return parts[0]
def fwd_kernel(start_ref, count_ref, qkv_ref, segr_ref, segc_ref, o_ref, lse_ref, vt_ref):
    length = qkv_ref.shape[0]
    vt_ref[...] = qkv_ref[:, 256:384].T
    nb = length // QB
    for i in range(nb):
        rows = slice(i*QB, (i+1)*QB)
        for nn in range(1, nb+1):
            @pl.when(count_ref[i] == nn)
            def _():
                nk = nn*QB
                lo = pl.multiple_of(start_ref[i]*128, 128)
                kw = qkv_ref[pl.ds(lo, nk), 128:256]
                qb = qkv_ref[rows, 0:128]
                same = segc_ref[pl.ds(lo, nk), :] == segr_ref[:, rows]
                outs = []
                for h in range(2):
                    qh = jnp.where(lane_half(qb.shape, h), qb, jnp.zeros_like(qb))
                    st = jnp.where(same, dot(kw, qh, 1, 1), NEG)
                    m = jnp.max(fold(st, jnp.maximum), axis=0, keepdims=True)
                    p = jnp.exp(st - m)
                    l = jnp.sum(fold(p, jnp.add), axis=0, keepdims=True)
                    weighted = dot(vt_ref[h*64:(h+1)*64, pl.ds(lo, nk)], p.astype(jnp.bfloat16), 1, 0)
                    outs.append(weighted * (1.0 / l))
                    lse_ref[0, h:h+1, rows] = m + jnp.log(l)
                o_ref[rows, :] = jnp.concatenate(outs, axis=0).T.astype(jnp.bfloat16)
def bwd_kernel(start_ref, count_ref, qkv_ref, do_ref, lse_ref, segr_ref, segc_ref, d_ref, sums_ref, dk_acc, dv_acc, kt_ref):
    length = qkv_ref.shape[0]
    kt_ref[...] = qkv_ref[:, 128:256].T
    nb = length // QB
    dk_acc[...] = jnp.zeros_like(dk_acc)
    dv_acc[...] = jnp.zeros_like(dv_acc)
    for i in range(nb):
        rows = slice(i*QB, (i+1)*QB)
        for nn in range(1, nb+1):
            @pl.when(count_ref[i] == nn)
            def _():
                nk = nn*QB
                lo = pl.multiple_of(start_ref[i]*128, 128)
                win = pl.ds(lo, nk)
                kw = qkv_ref[win, 128:256]
                vw = qkv_ref[win, 256:384]
                qb = qkv_ref[rows, 0:128]
                db = do_ref[rows, :]
                same = segc_ref[win, :] == segr_ref[:, rows]
                dqs = []; dks = 0.0; dvs = 0.0
                for h in range(2):
                    hm = lane_half(qb.shape, h)
                    qh = jnp.where(hm, qb, jnp.zeros_like(qb))
                    dh = jnp.where(hm, db, jnp.zeros_like(db))
                    st = jnp.where(same, dot(kw, qh, 1, 1), NEG)
                    p = jnp.exp(st - lse_ref[0, h:h+1, rows])
                    dpt = dot(vw, dh, 1, 1)
                    rd = jnp.sum(fold(p * dpt, jnp.add), axis=0, keepdims=True)
                    ds = (p * (dpt - rd)).astype(jnp.bfloat16)
                    dvs = dvs + dot(p.astype(jnp.bfloat16), dh, 1, 0)
                    dks = dks + dot(ds, qh, 1, 0)
                    dqs.append(dot(kt_ref[h*64:(h+1)*64, win], ds, 1, 0))
                d_ref[rows, 0:128] = jnp.concatenate(dqs, axis=0).T.astype(jnp.bfloat16) * 0.125
                dk_acc[win, :] += dks
                dv_acc[win, :] += dvs
    d_ref[:, 128:256] = dk_acc[...].astype(jnp.bfloat16)
    d_ref[:, 256:384] = dv_acc[...].astype(jnp.bfloat16)
    sums_ref[0] = jnp.sum(d_ref[...].astype(jnp.float32), axis=0, keepdims=True)
def attn_fwd(qkv, seg):
    T, width = qkv.shape
    start, count = attn_windows(seg[0])
    segc = seg.reshape(T, 1)
    heads = width // 384
    return pl.pallas_call(
        fwd_kernel,
        out_shape=(jax.ShapeDtypeStruct((T, width // 3), jnp.bfloat16), jax.ShapeDtypeStruct((heads, 2, T), jnp.float32)),
        grid_spec=pltpu.PrefetchScalarGridSpec(
            num_scalar_prefetch=2, grid=(heads,),
            in_specs=[
                pl.BlockSpec((T, 384), lambda h, *_: (0, h)),
                pl.BlockSpec((1, T), lambda h, *_: (0, 0)),
                pl.BlockSpec((T, 1), lambda h, *_: (0, 0)),
            ],
            out_specs=(pl.BlockSpec((T, 128), lambda h, *_: (0, h)), pl.BlockSpec((1, 2, T), lambda h, *_: (h, 0, 0))),
            scratch_shapes=[pltpu.VMEM((128, T), jnp.bfloat16)],
        ),
        cost_estimate=cost(20 * T * T * width, 3 * T * width, T * T * width // 128),
        name="attn_fwd",
    )(start, count, qkv, seg, segc)


def attn_bwd(qkv, do, lse, seg, part):
    T, width = qkv.shape
    start, count = attn_windows(seg[0])
    segc = seg.reshape(T, 1)
    heads = width // 768
    first = part * heads
    return pl.pallas_call(
        bwd_kernel,
        out_shape=(jax.ShapeDtypeStruct((T, width // 2), jnp.bfloat16), jax.ShapeDtypeStruct((heads, 1, 384), jnp.float32)),
        grid_spec=pltpu.PrefetchScalarGridSpec(
            num_scalar_prefetch=2, grid=(heads,),
            in_specs=[
                pl.BlockSpec((T, 384), lambda h, *_: (0, first + h)),
                pl.BlockSpec((T, 128), lambda h, *_: (0, first + h)),
                pl.BlockSpec((1, 2, T), lambda h, *_: (first + h, 0, 0)),
                pl.BlockSpec((1, T), lambda h, *_: (0, 0)),
                pl.BlockSpec((T, 1), lambda h, *_: (0, 0)),
            ],
            out_specs=(pl.BlockSpec((T, 384), lambda h, *_: (0, h)), pl.BlockSpec((1, 1, 384), lambda h, *_: (h, 0, 0))),
            scratch_shapes=[pltpu.VMEM((T, 128), jnp.float32)] * 2 + [pltpu.VMEM((128, T), jnp.bfloat16)],
        ),
        cost_estimate=cost(20 * T * T * width, 6 * T * width, T * T * width // 64),
        name="attn_bwd",
    )(start, count, qkv, do, lse, seg, segc)


MESH_ID = pl.DeviceIdType.MESH


def bits_of():
    rep = lax.axis_index("rep")
    fsdp = lax.axis_index("fsdp")
    return dict(
        rep=rep, fsdp=fsdp, x=rep // 2, c=rep % 2, z1=fsdp // 4, z0=(fsdp // 2) % 2, y=fsdp % 2
    )


def partner_of(at, which):
    rep, fsdp = at["rep"], at["fsdp"]
    if which == "c":
        rep = rep + 1 - 2 * at["c"]
    elif which == "x":
        rep = rep + 2 - 4 * at["x"]
    elif which == "y":
        fsdp = fsdp + 1 - 2 * at["y"]
    elif which == "z0":
        fsdp = fsdp + 2 - 4 * at["z0"]
    elif which == "z1":
        fsdp = fsdp + 4 - 8 * at["z1"]
    else:
        rep = rep + 1 - 2 * at["c"]
        fsdp = fsdp + 2 - 4 * at["z0"]
    return (rep, fsdp)


REL = [(a, b, d) for d in (0, 1) for b in (0, 1) for a in (0, 1)]


def gather_kernel(
    qkv_in, wo_in, vec_in, tok_in, seg_in,
    qkv_out, wo_out, vec_out, tok_out, seg_out,
    tok_buf, seg_buf, send_sem, recv_sem, local_sem,
):
    at = bits_of()
    other = {k: partner_of(at, k) for k in ("c", "x", "y", "z0", "z1", "swap")}
    barrier = pltpu.get_barrier_semaphore()
    for k in ("c", "x", "y", "z0", "z1"):
        pl.semaphore_signal(barrier, inc=1, device_id=other[k], device_id_type=MESH_ID)
    moves = at["c"] != at["z0"]

    @pl.when(moves)
    def _():
        pl.semaphore_signal(barrier, inc=1, device_id=other["swap"], device_id_type=MESH_ID)
        pl.semaphore_wait(barrier, 6)

    @pl.when(jnp.logical_not(moves))
    def _():
        pl.semaphore_wait(barrier, 5)

    def flip(bit, rel):
        return bit + rel - 2 * bit * rel

    def shard(rel):
        return 4 * flip(at["z1"], rel[1]) + 2 * flip(at["z0"], rel[0]) + flip(at["y"], rel[2])

    counter = [0]
    started = []

    def send(src, dst, which):
        k = counter[0]
        counter[0] += 1
        copy = pltpu.make_async_remote_copy(
            src_ref=src, dst_ref=dst, send_sem=send_sem.at[k], recv_sem=recv_sem.at[k],
            device_id=other[which], device_id_type=MESH_ID,
        )
        copy.start()
        started.append(copy)
        return copy

    class Piece:
        def __init__(self, own, slot, split_x):
            self.own, self.slot, self.split_x = own, slot, split_x
            self.part = (2 * at["x"] + at["c"]) if split_x else at["c"]
            self.part_x = (2 * (1 - at["x"]) + at["c"]) if split_x else None
            self.copies = {}

        def first(self):
            zero = (0, 0, 0)
            for which in ("z1", "z0", "y"):
                self.copies[which, zero] = send(
                    self.own(self.part), self.slot(shard(zero), self.part), which
                )
            self.copies["c", zero] = send(self.own(None), self.slot(shard(zero), None), "c")

        def onward(self, rel):
            here = self.slot(shard(rel), self.part)
            if rel == (0, 1, 0):
                self.copies["z0", rel] = send(here, here, "z0")
            if rel[2] == 0:
                self.copies["y", rel] = send(here, here, "y")
            if self.split_x:
                self.copies["x", rel] = send(here, here, "x")
            self.copies["c", rel] = send(here, here, "c")

        def arrive(self, which, came):
            self.copies[which, came].wait_recv()
            step = {"z0": (1, 0, 0), "z1": (0, 1, 0), "y": (0, 0, 1)}[which]
            self.onward(tuple(p + q for p, q in zip(came, step)))

        def near(self):
            self.arrive("z1", (0, 0, 0))
            self.arrive("z0", (0, 0, 0))

        def rest(self):
            self.arrive("y", (0, 0, 0))
            self.arrive("z0", (0, 1, 0))
            self.arrive("y", (0, 1, 0))
            self.arrive("y", (1, 0, 0))
            self.arrive("y", (1, 1, 0))

        def last(self):
            if self.split_x:
                for rel in REL[1:]:
                    self.copies["x", rel].wait_recv()
                    there = self.slot(shard(rel), self.part_x)
                    self.copies["cx", rel] = send(there, there, "c")

        def finish(self):
            for (which, rel), copy in self.copies.items():
                if which in ("c", "cx"):
                    copy.wait_recv()

    def rows(ref, count):
        full = ref.shape[-2] // 8
        def slot(f, part):
            if part is None:
                at_row, n = f * full, full
            else:
                at_row, n = f * full + part * (full // count), full // count
            at_row = pl.multiple_of(at_row, 8)
            return ref.at[pl.ds(at_row, n), :]
        return slot

    def own_rows(ref, count):
        full = ref.shape[-2]
        def own(part):
            if part is None:
                return ref
            row = pl.multiple_of(part * (full // count), 8)
            n = full // count
            return ref.at[pl.ds(row, n), :]
        return own

    qkv, wo = pieces = [
        Piece(own_rows(qkv_in, 4), rows(qkv_out, 4), True),
        Piece(own_rows(wo_in, 4), rows(wo_out, 4), True),
    ]
    zero = (0, 0, 0)
    vec_copies = [
        send(vec_in, vec_out.at[shard(zero)], which) for which in ("c", "z1", "z0", "y")
    ]
    pieces[0].first()
    tok_k, seg_k = counter[0], counter[0] + 1
    counter[0] += 2

    def swap_copy(src, dst, k):
        return pltpu.make_async_remote_copy(
            src_ref=src, dst_ref=dst, send_sem=send_sem.at[k], recv_sem=recv_sem.at[k],
            device_id=other["swap"], device_id_type=MESH_ID,
        )

    @pl.when(moves)
    def _():
        swap_copy(tok_in, tok_out, tok_k).start()
        swap_copy(seg_in, seg_out, seg_k).start()

    @pl.when(jnp.logical_not(moves))
    def _():
        one = pltpu.make_async_copy(tok_in, tok_buf, local_sem.at[0])
        two = pltpu.make_async_copy(seg_in, seg_buf, local_sem.at[1])
        one.start()
        two.start()
        one.wait()
        two.wait()
        three = pltpu.make_async_copy(tok_buf, tok_out, local_sem.at[0])
        four = pltpu.make_async_copy(seg_buf, seg_out, local_sem.at[1])
        three.start()
        four.start()
        three.wait()
        four.wait()

    wo.first()
    qkv.near()
    vec_copies[1].wait_recv()
    here = vec_out.at[shard((0, 1, 0))]
    vec_far = send(here, here, "z0")
    vec_more = [send(here, here, "y")]
    vec_copies[2].wait_recv()
    here = vec_out.at[shard((1, 0, 0))]
    vec_more.append(send(here, here, "y"))
    qkv.rest()
    wo.near()
    wo.rest()
    vec_far.wait_recv()
    here = vec_out.at[shard((1, 1, 0))]
    vec_more.append(send(here, here, "y"))
    qkv.last()
    wo.last()
    for piece in pieces:
        piece.finish()
    for copy in [vec_copies[0], vec_copies[3]] + vec_more:
        copy.wait_recv()
    for copy in started:
        copy.wait_send()

    @pl.when(moves)
    def _():
        swap_copy(tok_in, tok_out, tok_k).wait()
        swap_copy(seg_in, seg_out, seg_k).wait()


GATHER_COPIES = 29 * 2 + 8 + 2


def gather_all(qkv, wo, vec, tok, seg):
    bf = jnp.bfloat16
    shape = jax.ShapeDtypeStruct
    whole = pl.BlockSpec(memory_space=pl.ANY)
    return pl.pallas_call(
        gather_kernel,
        out_shape=(
            shape((8 * qkv.shape[0], qkv.shape[1]), bf),
            shape((8 * wo.shape[0], wo.shape[1]), bf),
            shape((8,) + vec.shape, bf),
            shape(tok.shape, bf),
            shape(seg.shape, seg.dtype),
        ),
        in_specs=[whole] * 5,
        out_specs=(whole,) * 5,
        scratch_shapes=[
            pltpu.VMEM(tok.shape, bf),
            pltpu.VMEM(seg.shape, seg.dtype),
            pltpu.SemaphoreType.DMA((GATHER_COPIES,)),
            pltpu.SemaphoreType.DMA((GATHER_COPIES,)),
            pltpu.SemaphoreType.DMA((2,)),
        ],
        compiler_params=pltpu.CompilerParams(collective_id=0, has_side_effects=True),
        name="gather_weights",
    )(qkv, wo, vec, tok, seg)


SHRINK = 1000
BF, F32 = jnp.bfloat16, jnp.float32
SHAPE = jax.ShapeDtypeStruct


def full_spec(shape):
    return pl.BlockSpec(shape, lambda *_: (0,) * len(shape), pipeline_mode=pl.Buffered(1))


def cost(flops, moved, exps=0):
    return pl.CostEstimate(flops=int(flops) // SHRINK, bytes_accessed=int(moved) // SHRINK, transcendentals=int(exps) // SHRINK)


def qkv_kernel(x_ref, w_ref, bias_ref, scale_ref, o_ref):
    for i in range(4):
        rows = slice(i * 256, (i + 1) * 256)
        z = dot(x_ref[rows, :], w_ref[...], 1, 0)
        o_ref[rows, :] = ((z + bias_ref[...]) * scale_ref[...]).astype(BF)


def qkv_call(x, w, bias, scale):
    tokens, width = x.shape[0], w.shape[1]
    tile = 768
    return pl.pallas_call(
        qkv_kernel,
        out_shape=SHAPE((tokens, width), BF),
        grid=(width // tile,),
        in_specs=[
            full_spec(x.shape),
            pl.BlockSpec((x.shape[1], tile), lambda j: (0, j)),
            pl.BlockSpec((1, tile), lambda j: (0, j)),
            pl.BlockSpec((1, tile), lambda j: (0, j)),
        ],
        out_specs=pl.BlockSpec((tokens, tile), lambda j: (0, j)),
        cost_estimate=cost(2 * tokens * D * width, 2 * (tokens * D + D * width + tokens * width)),
        name="qkv",
    )(x, w, bias, scale)


def mean_row(value):
    return jnp.mean(value, axis=-1, keepdims=True)


def mix_kernel(c_ref, w_ref, x_ref, rows_ref, n_ref, q_ref, low_ref):
    value = x_ref[...].astype(F32) + dot(c_ref[...], w_ref[...], 1, 0) + rows_ref[6:7, :]
    center = value - mean_row(value)
    inv = lax.rsqrt(mean_row(center * center) + 1e-05)
    normed = center * inv
    n_ref[...] = normed
    q_ref[...] = inv
    low_ref[...] = (normed * rows_ref[0:1, :] + rows_ref[2:3, :]).astype(BF)


def mix_call(mixed, w_out, tok, rows):
    t = tok.shape[0]
    tile = pl.BlockSpec((256, D), lambda i: (i, 0))
    return pl.pallas_call(
        mix_kernel,
        out_shape=(SHAPE((t, D), F32), SHAPE((t, 1), F32), SHAPE((t, D), BF)),
        grid=(t // 256,),
        in_specs=[tile, full_spec((D, D)), tile, full_spec(rows.shape)],
        out_specs=(tile, pl.BlockSpec((256, 1), lambda i: (i, 0)), tile),
        cost_estimate=cost(2 * t * D * D, 12 * t * D + 2 * D * D),
        name="mix_norm",
    )(mixed, w_out, tok, rows)


def up_kernel(place_ref, h_ref, *refs):
    parts, (bias_ref, g_ref, s_ref) = refs[:4], refs[4:]
    each = pl.num_programs(0) // 4

    def tile(w_ref):
        for i in range(8):
            rows = slice(i * 128, (i + 1) * 128)
            z = dot(h_ref[rows, :], w_ref[...], 1, 0) + bias_ref[...]
            phi, bell = erf_parts(z)
            g_ref[rows, :] = (z * phi).astype(BF)
            s_ref[rows, :] = (phi + z * bell * 0.3989422804014327).astype(BF)

    for k in range(4):
        pl.when(pl.program_id(0) // each == k)(partial(tile, parts[k]))


def up_call(low, parts, place, bias):
    t = low.shape[0]
    tile = 512
    each = FF // tile // 4
    where = lambda j, p: (0, p[j // each] * each + lax.rem(j, each))
    out = pl.BlockSpec((t, tile), where)

    def part(k):
        return pl.BlockSpec((D, tile), lambda j, p: (0, jnp.clip(j - k * each, 0, each - 1)))

    return pl.pallas_call(
        up_kernel,
        out_shape=(SHAPE((t, FF), BF), SHAPE((t, FF), BF)),
        grid_spec=pltpu.PrefetchScalarGridSpec(
            num_scalar_prefetch=1, grid=(FF // tile,),
            in_specs=[full_spec(low.shape)] + [part(k) for k in range(4)] + [pl.BlockSpec((1, tile), where)],
            out_specs=(out, out),
        ),
        cost_estimate=cost(2 * t * D * FF, 2 * (t * D + D * FF + 2 * t * FF), 2 * t * FF),
        name="up_gelu",
    )(place, low, *parts, bias)


def row_sum(value):
    return jnp.sum(value, axis=0, keepdims=True)


def norm_back(grad, normed, inv, gain):
    scaled = grad * gain
    return inv * (scaled - mean_row(scaled) - normed * mean_row(scaled * normed))


def down_kernel(
    core_ref, g_ref, own_ref, came_ref, n_ref, cot_ref, rows_ref, out_ref, dr_ref, dm_ref, sums_ref, m_ref
):
    half = D // 2
    m_ref[:, pl.ds(pl.multiple_of(core_ref[0] * half, half), half)] = dot(g_ref[...], own_ref[...], 1, 0)
    m_ref[:, pl.ds(pl.multiple_of((1 - core_ref[0]) * half, half), half)] = dot(g_ref[...], came_ref[...], 1, 0)
    hidden = n_ref[...] * rows_ref[0:1, :] + rows_ref[2:3, :]
    value = hidden + m_ref[...] + rows_ref[7:8, :]
    center = value - mean_row(value)
    inv = lax.rsqrt(mean_row(center * center) + 1e-05)
    normed = center * inv
    gain = rows_ref[1:2, :]
    out_ref[...] = (normed * gain + rows_ref[3:4, :]).astype(BF)
    grad = cot_ref[...].astype(F32)
    back = norm_back(grad, normed, inv, gain)
    low = back.astype(BF)
    dr_ref[...] = back
    dm_ref[...] = low

    @pl.when(pl.program_id(0) == 0)
    def _():
        sums_ref[...] = jnp.zeros_like(sums_ref)

    sums_ref[0:1, :] += row_sum(grad * normed)
    sums_ref[1:2, :] += row_sum(grad)
    sums_ref[2:3, :] += row_sum(low.astype(F32))


def down_call(act, own, came, normed, cot, rows, core):
    t = act.shape[0]
    tile = pl.BlockSpec((256, D), lambda i, c: (i, 0))
    return pl.pallas_call(
        down_kernel,
        out_shape=(SHAPE((t, D), BF), SHAPE((t, D), F32), SHAPE((t, D), BF), SHAPE((8, D), F32)),
        grid_spec=pltpu.PrefetchScalarGridSpec(
            num_scalar_prefetch=1, grid=(t // 256,),
            in_specs=[
                pl.BlockSpec((256, FF), lambda i, c: (i, 0)), full_spec((FF, D // 2)), full_spec((FF, D // 2)),
                tile, tile, full_spec(rows.shape),
            ],
            out_specs=(tile, tile, tile, pl.BlockSpec((8, D), lambda i, c: (0, 0))),
            scratch_shapes=[pltpu.VMEM((256, D), F32)],
        ),
        cost_estimate=cost(2 * t * D * FF, 2 * (t * FF + D * FF) + 14 * t * D),
        name="down_norm",
    )(core.reshape(1), act, own, came, normed, cot, rows)


def slope_kernel(core_ref, left_ref, right_ref, own_ref, came_ref, s_ref, o_ref, sums_ref):
    total = 0.0
    for i in range(4):
        rows = slice(i * 256, (i + 1) * 256)
        back = dot(left_ref[rows, :], own_ref[...], 1, 1) + dot(right_ref[rows, :], came_ref[...], 1, 1)
        z = (back * s_ref[rows, :].astype(F32)).astype(BF)
        o_ref[rows, :] = z
        total = total + row_sum(z.astype(F32))
    sums_ref[...] = total


def slope_call(dm, own, came, slope, core):
    t = dm.shape[0]
    tile = 512
    wide = pl.BlockSpec((t, tile), lambda j, c: (0, j))
    part = pl.BlockSpec((tile, D // 2), lambda j, c: (j, 0))
    return pl.pallas_call(
        slope_kernel,
        out_shape=(SHAPE((t, FF), BF), SHAPE((1, FF), F32)),
        grid_spec=pltpu.PrefetchScalarGridSpec(
            num_scalar_prefetch=1, grid=(FF // tile,),
            in_specs=[
                pl.BlockSpec((t, D // 2), lambda j, c: (0, c[0])),
                pl.BlockSpec((t, D // 2), lambda j, c: (0, 1 - c[0])),
                part, part, wide,
            ],
            out_specs=(wide, pl.BlockSpec((1, tile), lambda j, c: (0, j))),
        ),
        cost_estimate=cost(2 * t * D * FF, 2 * (t * D + D * FF + 2 * t * FF)),
        name="down_back",
    )(core.reshape(1), dm, dm, own, came, slope)


def hidden_kernel(place_ref, *refs):
    grads, parts = refs[:4], refs[4:8]
    dr_ref, n_ref, q_ref, wo_ref, rows_ref, r_ref, a_ref, c_ref, sums_ref = refs[8:]
    grad = dr_ref[...]
    for grad_ref, w_ref in zip(grads, parts):
        grad = grad + dot(grad_ref[...], w_ref[...], 1, 1)
    normed = n_ref[...]
    back = norm_back(grad, normed, q_ref[...], rows_ref[0:1, :])
    low = back.astype(BF)
    r_ref[...] = back
    a_ref[...] = low
    c_ref[...] = dot(low, wo_ref[...], 1, 1).astype(BF)

    @pl.when(pl.program_id(0) == 0)
    def _():
        sums_ref[...] = jnp.zeros_like(sums_ref)

    sums_ref[0:1, :] += row_sum(grad * normed)
    sums_ref[1:2, :] += row_sum(grad)
    sums_ref[2:3, :] += row_sum(low.astype(F32))


def hidden_call(dz, parts, place, dr, normed, inv, w_out, rows):
    t = dz.shape[0]
    tile = pl.BlockSpec((256, D), lambda i, p: (i, 0))

    def quarter(k):
        return pl.BlockSpec((256, FF // 4), lambda i, p: (i, p[k]))

    return pl.pallas_call(
        hidden_kernel,
        out_shape=(SHAPE((t, D), F32), SHAPE((t, D), BF), SHAPE((t, D), BF), SHAPE((8, D), F32)),
        grid_spec=pltpu.PrefetchScalarGridSpec(
            num_scalar_prefetch=1, grid=(t // 256,),
            in_specs=[quarter(k) for k in range(4)] + [full_spec((D, FF // 4))] * 4 + [
                tile, tile,
                pl.BlockSpec((256, 1), lambda i, p: (i, 0)), full_spec((D, D)), full_spec(rows.shape),
            ],
            out_specs=(tile, tile, tile, pl.BlockSpec((8, D), lambda i, p: (0, 0))),
        ),
        cost_estimate=cost(2 * t * D * (FF + D), 2 * (t * FF + D * FF) + 16 * t * D),
        name="up_back_norm",
    )(place, *([dz] * 4), *parts, dr, normed, inv, w_out, rows)


def input_kernel(a_ref, b_ref, w_ref, r_ref, o_ref):
    half = a_ref.shape[1]
    value = dot(a_ref[...], w_ref[:, :half], 1, 1) + dot(b_ref[...], w_ref[:, half:], 1, 1)
    o_ref[...] = (r_ref[...] + value).astype(BF)


def input_call(part_a, part_b, w_qkv, resid):
    t, width = part_a.shape
    tile = pl.BlockSpec((256, D), lambda i: (i, 0))
    wide = pl.BlockSpec((256, width), lambda i: (i, 0))
    return pl.pallas_call(
        input_kernel,
        out_shape=SHAPE((t, D), BF),
        grid=(t // 256,),
        in_specs=[wide, wide, full_spec(w_qkv.shape), tile],
        out_specs=tile,
        cost_estimate=cost(4 * t * D * width, 4 * (t * width + D * width) + 6 * t * D),
        name="input_back",
    )(part_a, part_b, w_qkv, resid)


def weight_kernel(at_ref, *refs):
    left, right_ref, rest, turned = refs[:4], refs[4], refs[5:-1], refs[-1]

    @pl.when(pl.program_id(1) == 0)
    def _():
        part = left[0].shape[1]
        for k in range(4):
            turned[k * part:(k + 1) * part, :] = left[k][...].T

    value = dot(turned[...], right_ref[...], 1, 0)
    if len(rest) == 1:
        rest[0][...] = value.astype(BF)
        return
    came_ref, away_ref, keep_ref = rest
    value = (value + came_ref[...].astype(F32)).astype(BF)
    rows = away_ref.shape[0]
    if rows < value.shape[0]:
        away_ref[...] = value[:rows]
        keep_ref[...] = value[rows:]
    else:
        first = pl.program_id(0) < pl.num_programs(0) // 2

        @pl.when(first)
        def _():
            away_ref[...] = value

        @pl.when(jnp.logical_not(first))
        def _():
            keep_ref[...] = value


def weight_call(left, right, half, y, came=None):
    t, rows = left.shape
    width = right.shape[1]
    bm = 512
    bn = 1024 if width == 1024 else 512
    steps = rows // 2 // bm

    def column(k):
        def place(i, j, at):
            if steps == 1:
                side, z1 = (1 - at[1] if k < 2 else at[1]), k % 2
                return (0, z1 * 4 + at[0] * 2 + side)
            side = at[1] + (1 - 2 * at[1]) * (1 - i // 2)
            return (0, (lax.rem(i, 2) * 4 + at[0] * 2 + side) * 4 + k)

        return pl.BlockSpec((t, bm // 4), place)

    specs = [column(k) for k in range(4)] + [pl.BlockSpec((t, bn), lambda i, j, at: (0, j))]
    values = [left] * 4 + [right]
    out = pl.BlockSpec((bm, bn), lambda i, j, at: (i, j))
    if came is None:
        shapes = SHAPE((rows // 2, width), BF)
    else:
        specs.append(out)
        values.append(came)
        shapes = (SHAPE((rows // 4, width), BF),) * 2
        if steps == 1:
            out = (pl.BlockSpec((bm // 2, bn), lambda i, j, at: (0, j)),) * 2
        else:
            out = (
                pl.BlockSpec((bm, bn), lambda i, j, at: (jnp.minimum(i, steps // 2 - 1), j)),
                pl.BlockSpec((bm, bn), lambda i, j, at: (jnp.maximum(i - steps // 2, 0), j)),
            )
    return pl.pallas_call(
        weight_kernel,
        out_shape=shapes,
        grid_spec=pltpu.PrefetchScalarGridSpec(
            num_scalar_prefetch=1, grid=(steps, width // bn), in_specs=specs, out_specs=out,
            scratch_shapes=[pltpu.VMEM((bm, t), BF)],
        ),
        cost_estimate=cost(t * rows * width, t * rows + 2 * t * width + 2 * rows * width),
        name="weight_grad",
    )(jnp.stack([half, y]), *values)


def inner_kernel(rate, decay, w_ref, g_ref, m_ref, v_ref, m_out, v_out, d_out):
    weight = w_ref[...]
    new, m_out[...], v_out[...] = inner_step(
        weight, g_ref[...].astype(F32), m_ref[...], v_ref[...], rate, decay
    )
    d_out[...] = (weight - new).astype(BF)


def inner_call(weight, grad, first, second, rate, decay):
    rows, width = weight.shape
    block = 32 * 4096 // width
    tile = pl.BlockSpec((block, width), lambda i: (i, 0))
    like = SHAPE((rows, width), F32)
    return pl.pallas_call(
        partial(inner_kernel, rate, decay),
        out_shape=(like, like, SHAPE((rows, width), BF)),
        grid=(rows // block,),
        in_specs=[tile] * 4,
        out_specs=(tile,) * 3,
        cost_estimate=cost(20 * rows * width, 24 * rows * width),
        name="inner_step",
    )(weight, grad, first, second)


def outer_kernel(core_ref, w_ref, u_ref, own_ref, came_ref, o_ref, c_ref):
    mine = (core_ref[0] == pl.program_id(0)).astype(F32)
    total = own_ref[...].astype(F32) * mine + came_ref[...].astype(F32) * (1.0 - mine)
    mean = total * 0.25
    weight = w_ref[...]
    momentum = 0.5 * u_ref[...] + mean
    new = weight - 0.7 * (mean + 0.5 * momentum)
    o_ref[0] = mean
    o_ref[1] = momentum
    o_ref[2] = new
    c_ref[...] = new.astype(BF)


def outer_call(weight, momentum, own, came, core):
    rows, width = weight.shape
    block = 32 * 4096 // width
    steps = rows // 2 // block
    tile = pl.BlockSpec((block, width), lambda h, i, c: (h * steps + i, 0))
    part = pl.BlockSpec((block, width), lambda h, i, c: (i, 0))
    return pl.pallas_call(
        outer_kernel,
        out_shape=(SHAPE((3, rows, width), F32), SHAPE((rows, width), BF)),
        grid_spec=pltpu.PrefetchScalarGridSpec(
            num_scalar_prefetch=1, grid=(2, steps), in_specs=[tile, tile, part, part],
            out_specs=(pl.BlockSpec((3, block, width), lambda h, i, c: (0, h * steps + i, 0)), tile),
        ),
        cost_estimate=cost(10 * rows * width, 26 * rows * width),
        name="outer_step",
    )(core.reshape(1), weight, momentum, own, came)


def erf_parts(value):
    size = jnp.abs(value) * 0.7071067811865476
    share = 1.0 / (1.0 + 0.5 * size)
    inner = 0.17087277
    for coefficient in (
        -0.82215223, 1.48851587, -1.13520398, 0.27886807, -0.18628806, 0.09678418, 0.37409196, 1.00002368
    ):
        inner = coefficient + share * inner
    square = size * size
    half = 0.5 * share * jnp.exp(share * inner - 1.26551223 - square)
    return jnp.where(value >= 0, 1.0 - half, half), jnp.exp(-square)


def xor_pairs(bits):
    place = {"y": 0, "z0": 1, "z1": 2, "c": 3, "x": 4}
    flip = sum(1 << place[bit] for bit in bits)
    pairs = []
    for device in range(32):
        if bits == ("c", "z0") and ((device >> 3) & 1) == ((device >> 1) & 1):
            continue
        pairs.append((device, device ^ flip))
    return pairs


def exchange(value, *bits):
    return lax.ppermute(value, ("rep", "fsdp"), xor_pairs(bits))


def add_low(left, right):
    return (left.astype(jnp.float32) + right.astype(jnp.float32)).astype(jnp.bfloat16)


def pick(value, index, axis):
    return lax.dynamic_index_in_dim(value, index, axis, keepdims=False)


def halve(at, total, which):
    away = pick(total.reshape(2, -1, total.shape[-1]), 1 - at[which], 0)
    return away, exchange(away, which)


def join(at, total, came, which, *gates):
    return add_low(pick(total.reshape(2, -1, total.shape[-1]), at[which], 0), after(came, *gates))


def join_kept(kept, came, *gates):
    return add_low(kept, after(came, *gates))


def after(value, *earlier):
    return lax.optimization_barrier((value,) + earlier)[0]


def weave(value):
    rows = value.shape[1]
    return jnp.transpose(value.reshape(3, rows, D // 128, 128), (1, 2, 0, 3)).reshape(rows, 3 * D)


def unweave(value):
    rows = value.shape[0]
    return jnp.transpose(value.reshape(rows, D // 128, 3, 128), (2, 0, 1, 3)).reshape(3, rows, D)


def per_device_fast(
    tokens,
    cotangent,
    segment_ids,
    attention_weight,
    attention_momentum,
    attention_first,
    attention_second,
    expand_weight,
    expand_momentum,
    expand_first,
    expand_second,
    contract_weight,
    contract_momentum,
    contract_first,
    contract_second,
    vectors,
    vectors_momentum,
    vectors_first,
    vectors_second,
):
    bf, f32 = jnp.bfloat16, jnp.float32
    at = bits_of()
    core = at["c"].astype(jnp.int32)
    side = at["y"].astype(jnp.int32)
    def swapped(value, came):
        return jnp.where(at["c"] != at["z0"], came, value)

    def cross(value):
        return exchange(value, "c", "z0")

    quarter = 2 * core + at["x"].astype(jnp.int32)
    place = jnp.stack([quarter, 2 * (1 - core) + quarter - 2 * core, quarter + 1 - 2 * at["x"], 3 - quarter])
    part = expand_weight.shape[1] // 4
    in_own = lax.all_gather(
        lax.dynamic_slice_in_dim(expand_weight, quarter * part, part, axis=1).astype(bf), "fsdp", axis=0, tiled=True
    )
    attn_low = attention_weight.astype(bf)
    w_qkv, w_out, vector_full, tok, seg = gather_all(
        weave(attn_low[:3]), attn_low[3], vectors.astype(bf), tokens, segment_ids,
    )
    cot_came = cross(after(cotangent, w_qkv))
    rows = jnp.swapaxes(vector_full, 0, 1).reshape(-1, D).astype(f32)
    bias_up = rows[8:].reshape(1, FF)
    bias_qkv = weave(jnp.stack([rows[4], jnp.zeros_like(rows[4]), rows[5]])[:, None])
    scale_qkv = weave(jnp.stack([jnp.full((1, D), 0.125, f32)] + [jnp.ones((1, D), f32)] * 2))
    part = contract_weight.shape[1] // 2
    down_half = lax.dynamic_slice_in_dim(contract_weight, core * part, part, axis=1).astype(bf)
    down_own = lax.all_gather(after(down_half, w_qkv), "fsdp", axis=0, tiled=True)
    in_near = after(in_own, w_qkv)
    in_far = exchange(in_near, "x")
    in_side = exchange(in_near, "c")
    qkv = qkv_call(tok, w_qkv, bias_qkv, scale_qkv)
    mixed, log_sum = attn_fwd(qkv, seg)
    in_parts = [in_own, after(in_side, mixed), in_far, exchange(after(in_far, mixed), "c")]
    normed, inv, hidden_low = mix_call(mixed, w_out, tok, rows)
    cot = swapped(cotangent, after(cot_came, hidden_low))
    activated, slope = up_call(after(hidden_low, cot), in_parts, place, bias_up)
    down_other = exchange(after(down_own, activated), "c")
    layer_output, grad_sum, grad_branch, sums_two = down_call(
        activated, down_own, down_other, normed, cot, rows, core
    )
    output_came = cross(layer_output)
    down_send = weight_call(activated, grad_branch, 1 - core, side)
    grad_pre, sums_up = slope_call(after(grad_branch, down_send), down_own, down_other, slope, core)
    down_came = exchange(down_send, "c")
    up_send = weight_call(hidden_low, grad_pre, 1 - core, side)
    away_d, down_kept = weight_call(activated, after(grad_branch, up_send), core, side, down_came)
    up_came = exchange(up_send, "c")
    came_d = exchange(away_d, "y")
    away_u, up_kept = weight_call(hidden_low, after(grad_pre, away_d), core, side, up_came)
    came_u = exchange(away_u, "y")
    grad_resid, grad_attn, grad_mixed, sums_one = hidden_call(
        after(grad_pre, away_u), in_parts, place, grad_sum, normed, inv, w_out, rows
    )
    proj_send = weight_call(mixed, grad_attn, 1 - core, side)
    proj_came = exchange(proj_send, "c")
    output = swapped(layer_output, after(output_came, proj_send))
    grad_a, sums_a = attn_bwd(qkv, after(grad_mixed, proj_send, output), log_sum, seg, 0)
    send_a = weight_call(tok, grad_a, 1 - core, side)
    came_a = exchange(send_a, "c")
    down_one = join_kept(down_kept, came_d, send_a)
    away_d, came_d = halve(at, down_one, "z1")
    away_p, proj_kept = weight_call(mixed, after(grad_attn, away_d), core, side, proj_came)
    came_p = exchange(away_p, "y")
    away_a, a_kept = weight_call(tok, after(grad_a, away_p), core, side, came_a)
    came_one = exchange(away_a, "y")
    up_one = join_kept(up_kept, came_u, away_a)
    away_u, came_u = halve(at, up_one, "z1")
    grad_b, sums_b = attn_bwd(qkv, after(grad_mixed, away_u), log_sum, seg, 1)
    send_b = weight_call(tok, grad_b, 1 - core, side)
    came_b = exchange(send_b, "c")
    down_two = join(at, down_one, came_d, "z1", send_b)
    cross_d = cross(down_two)
    proj_one = join_kept(proj_kept, came_p, down_two)
    away_p, came_p = halve(at, proj_one, "z1")
    a_one = join_kept(a_kept, came_one, away_p)
    away_a, came_a = halve(at, a_one, "z1")
    away_b, b_kept = weight_call(tok, after(grad_b, away_a), core, side, came_b)
    came_b = exchange(away_b, "y")
    sums_qkv = jnp.concatenate([sums_a, sums_b], axis=0).reshape(D // 128, 3, 128)
    vector_grad = jnp.concatenate(
        [
            sums_one[0:1],
            sums_two[0:1],
            sums_one[1:2],
            sums_two[1:2],
            sums_qkv[:, 0].reshape(1, D),
            sums_qkv[:, 2].reshape(1, D),
            sums_one[2:3],
            sums_two[2:3],
            sums_up.reshape(FF // D, D),
        ],
        axis=0,
    )

    def vector_send(parts, which):
        half = parts.shape[1] // 2
        away = lax.dynamic_slice_in_dim(parts, (1 - at[which]) * half, half, axis=1)
        return exchange(away, which)

    def vector_join(parts, came, which, *gates):
        half = parts.shape[1] // 2
        return lax.dynamic_slice_in_dim(parts, at[which] * half, half, axis=1) + after(came, *gates)

    vec_came = vector_send(vector_grad, "z1")

    def inner(weight, grad, first, second, rate, decay):
        flat = (-1, weight.shape[-1])
        return inner_call(
            weight.reshape(flat), grad.reshape(flat), first.reshape(flat), second.reshape(flat), rate, decay
        )

    def rep_send(diff):
        halves = diff.reshape(2, diff.shape[0] // 2, diff.shape[1])
        away = pick(halves, 1 - at["c"], 0)
        return away, exchange(away, "c")

    def rep_join(diff, came, *gates):
        halves = diff.reshape(2, diff.shape[0] // 2, diff.shape[1])
        return add_low(pick(halves, at["c"], 0), after(came, *gates))

    def outer(weight, momentum, own, came):
        flat = (-1, weight.shape[-1])
        return outer_call(weight.reshape(flat), momentum.reshape(flat), own, came, core)

    grad_contract = swapped(down_two, after(cross_d, away_b))
    contract_new = inner(contract_weight, grad_contract, contract_first, contract_second, 0.015, 0.1)
    sent_c, came_c = rep_send(contract_new[2])
    up_two = join(at, up_one, came_u, "z1", sent_c)
    cross_u = cross(up_two)
    vec_one = vector_join(vector_grad, vec_came, "z1", up_two)
    vec_came = vector_send(vec_one, "c")
    b_one = join_kept(b_kept, came_b, up_two)
    away_b, came_b = halve(at, b_one, "z1")
    half_c = rep_join(contract_new[2], came_c, away_b)
    rest_c = exchange(half_c, "x")
    vec_two = vector_join(vec_one, vec_came, "c", half_c)
    vec_came = vector_send(vec_two, "y")
    input_grad = input_call(after(grad_a, away_b, half_c), grad_b, w_qkv, grad_resid)
    grad_expand = swapped(up_two, after(cross_u, input_grad))
    expand_new = inner(expand_weight, grad_expand, expand_first, expand_second, 0.03, 0.1)
    sent_e, came_e = rep_send(expand_new[2])
    proj_two = join(at, proj_one, came_p, "z1", sent_e)
    a_two = join(at, a_one, came_a, "z1", sent_e)
    cross_pa = cross(jnp.concatenate([proj_two, a_two], axis=1))
    vec_three = vector_join(vec_two, vec_came, "y", proj_two, a_two)
    vec_cross = cross(vec_three)
    full_c = add_low(half_c, after(rest_c, vec_three))
    back_c = exchange(full_c, "c")
    half_e = rep_join(expand_new[2], came_e, full_c)
    rest_e = exchange(half_e, "x")
    b_two = join(at, b_one, came_b, "z1", half_e)
    cross_b = cross(b_two)
    outer_c = outer(contract_weight, contract_momentum, full_c, after(back_c, b_two))
    grad_vectors = swapped(vec_three, after(vec_cross, outer_c[1]))
    inner_new, first_new, second_new = inner_step(
        vectors, grad_vectors, vectors_first[0], vectors_second[0], 0.2, 0.0
    )
    vec_diff = (vectors - inner_new).astype(bf)
    vec_near = exchange(vec_diff, "c")
    input_came = cross(after(input_grad, b_two, vec_diff))
    pa = swapped(jnp.concatenate([proj_two, a_two], axis=1), after(cross_pa, outer_c[1]))
    b_own = swapped(b_two, after(cross_b, vec_diff, pa))
    grad_qkv = jnp.concatenate([pa[:, D:], b_own], axis=1)
    grad_attention = jnp.concatenate([unweave(grad_qkv), pa[None, :, :D]], axis=0)
    attention_new = inner(attention_weight, grad_attention, attention_first, attention_second, 0.03, 0.1)
    sent_a, came_a = rep_send(attention_new[2])
    vec_half = add_low(vec_diff, after(vec_near, sent_a))
    vec_far = exchange(vec_half, "x")
    full_e = add_low(half_e, after(rest_e, vec_half))
    back_e = exchange(full_e, "c")
    half_a = rep_join(attention_new[2], came_a, full_e)
    rest_a = exchange(half_a, "x")
    outer_e = outer(expand_weight, expand_momentum, full_e, after(back_e, half_a))
    full_a = add_low(half_a, after(rest_a, outer_e[1]))
    back_a = exchange(full_a, "c")
    mean_diff = add_low(vec_half, after(vec_far, full_a)).astype(f32) / 4
    momentum_new = 0.5 * vectors_momentum + mean_diff
    outer_new = vectors - 0.7 * (mean_diff + 0.5 * momentum_new)
    input_grad = swapped(input_grad, after(input_came, full_a))
    outer_a = outer(attention_weight, attention_momentum, full_a, back_a)
    results = []
    for weight, first, new, (total, copy) in (
        (attention_weight, attention_first, attention_new, outer_a),
        (expand_weight, expand_first, expand_new, outer_e),
        (contract_weight, contract_first, contract_new, outer_c),
    ):
        results += [
            new[0].reshape(first.shape),
            new[1].reshape(first.shape),
            total.reshape((3,) + weight.shape),
            copy.reshape(weight.shape),
        ]
    results += [
        first_new[None],
        second_new[None],
        jnp.stack([mean_diff, momentum_new, outer_new]),
        outer_new.astype(bf),
    ]
    return (output, input_grad) + tuple(results)


def solution(mesh):
    placed = (
        P(("rep", "fsdp"), None),
        P(("rep", "fsdp"), None),
        P(("rep", "fsdp"), None),
        P(None, "fsdp", None),
        P(None, "fsdp", None),
        P("rep", None, "fsdp", None),
        P("rep", None, "fsdp", None),
        P("fsdp", None),
        P("fsdp", None),
        P("rep", "fsdp", None),
        P("rep", "fsdp", None),
        P("fsdp", None),
        P("fsdp", None),
        P("rep", "fsdp", None),
        P("rep", "fsdp", None),
        P(None, "fsdp"),
        P(None, "fsdp"),
        P("rep", None, "fsdp"),
        P("rep", None, "fsdp"),
    )
    small = mesh.shape["rep"] == 4 and mesh.shape["fsdp"] == 8
    body = per_device_fast if small else per_device
    return jax.shard_map(
        body,
        mesh=mesh,
        in_specs=placed,
        out_specs=(
            P(("rep", "fsdp"), None),
            P(("rep", "fsdp"), None),
            P("rep", None, "fsdp", None),
            P("rep", None, "fsdp", None),
            P(None, None, "fsdp", None),
            P(None, "fsdp", None),
            P("rep", "fsdp", None),
            P("rep", "fsdp", None),
            P(None, "fsdp", None),
            P("fsdp", None),
            P("rep", "fsdp", None),
            P("rep", "fsdp", None),
            P(None, "fsdp", None),
            P("fsdp", None),
            P("rep", None, "fsdp"),
            P("rep", None, "fsdp"),
            P(None, None, "fsdp"),
            P(None, "fsdp"),
        ),
        check_vma=False,
    )
```

```python
from functools import partial

import jax
import jax.numpy as jnp
from jax import lax
from jax.experimental import pallas as pl
from jax.experimental.pallas import tpu as pltpu
from jax.sharding import PartitionSpec as P

D = 1024
H = 16
HD = 64
FF = 4096
LEN = 1024
SEQ_DEV = 1
ADAM_STEP = 4
TOK_DEV = 1024


def norm_forward(values_in, gain_row, shift_row):
    center = values_in - jnp.mean(values_in, axis=-1, keepdims=True)
    inv_scale = lax.rsqrt(jnp.mean(center * center, axis=-1, keepdims=True) + 1e-05)
    normed = center * inv_scale
    return (normed * gain_row + shift_row, normed, inv_scale)


def norm_backward(grad_out, normed, inv_scale, gain_row):
    grad_gain = jnp.sum(grad_out * normed, axis=0)
    grad_shift = jnp.sum(grad_out, axis=0)
    scaled_grad = grad_out * gain_row
    grad_value = inv_scale * (
        scaled_grad
        - jnp.mean(scaled_grad, axis=-1, keepdims=True)
        - normed * jnp.mean(scaled_grad * normed, axis=-1, keepdims=True)
    )
    return (grad_value, grad_gain, grad_shift)


def product_over(left, right):
    return lax.dot_general(
        left, right, (((0,), (0,)), ((), ())), preferred_element_type=jnp.float32
    )


def product_back(left, right):
    return lax.dot_general(
        left, right, (((1,), (1,)), ((), ())), preferred_element_type=jnp.float32
    )


def block_scores(query_block, key_block, row_segments, all_segments):
    scores = jnp.einsum("qhd,khd->hqk", query_block, key_block, preferred_element_type=jnp.float32)
    same_doc = row_segments[:, None] == all_segments[None, :]
    return jnp.where(same_doc[None], scores, -1e30)


def inner_step(weight, gradient, first_moment, second_moment, learn_rate, weight_decay):
    first_new = 0.5 * first_moment + 0.5 * gradient
    second_new = 0.75 * second_moment + 0.25 * gradient * gradient
    update_dir = (
        first_new
        / (1.0 - 0.5**ADAM_STEP)
        / (jnp.sqrt(second_new / (1.0 - 0.75**ADAM_STEP)) + 1e-08)
    )
    return (weight - learn_rate * (update_dir + weight_decay * weight), first_new, second_new)


def per_device(
    tokens,
    cotangent,
    segment_ids,
    attention_weight,
    attention_momentum,
    attention_first,
    attention_second,
    expand_weight,
    expand_momentum,
    expand_first,
    expand_second,
    contract_weight,
    contract_momentum,
    contract_first,
    contract_second,
    vectors,
    vectors_momentum,
    vectors_first,
    vectors_second,
):
    attn_full, vector_full = (
        lax.all_gather(attention_weight.astype(jnp.bfloat16), "fsdp", axis=1, tiled=True),
        lax.all_gather(vectors.astype(jnp.bfloat16), "fsdp", axis=1, tiled=True),
    )
    vector_rows = vector_full.astype(jnp.float32)
    gain_one, gain_two, shift_one, shift_two = (
        vector_rows[0],
        vector_rows[1],
        vector_rows[2],
        vector_rows[3],
    )
    bias_query, bias_value, bias_mixed, bias_down = (
        vector_rows[4],
        vector_rows[5],
        vector_rows[6],
        vector_rows[7],
    )
    bias_up = vector_rows[8:].reshape(FF)
    projected = jnp.einsum("td,nde->nte", tokens, attn_full[:3], preferred_element_type=jnp.float32)
    query_all = ((projected[0] + bias_query) * 0.125).astype(jnp.bfloat16)
    key_all = projected[1].astype(jnp.bfloat16)
    value_all = (projected[2] + bias_value).astype(jnp.bfloat16)
    query_heads = query_all.reshape(SEQ_DEV, LEN, H, HD)
    key_heads = key_all.reshape(SEQ_DEV, LEN, H, HD)
    value_heads = value_all.reshape(SEQ_DEV, LEN, H, HD)
    block_rows = min(512, LEN)
    head_group = min(8, H)
    context_rows = []
    log_sums = []
    seq_index = 0
    for row_start in range(0, LEN, block_rows):
        block_pieces = []
        for head_start in range(0, H, head_group):
            head_part = slice(head_start, head_start + head_group)
            scores = block_scores(
                query_heads[seq_index, row_start : row_start + block_rows, head_part],
                key_heads[seq_index, :, head_part],
                segment_ids[seq_index, row_start : row_start + block_rows],
                segment_ids[seq_index],
            )
            row_max = jnp.max(scores, axis=-1, keepdims=True)
            exp_score = jnp.exp(scores - row_max)
            row_total = jnp.sum(exp_score, axis=-1, keepdims=True)
            probability = (exp_score / row_total).astype(jnp.bfloat16)
            block_pieces.append(
                jnp.einsum(
                    "hqk,khd->qhd",
                    probability,
                    value_heads[seq_index, :, head_part],
                    preferred_element_type=jnp.float32,
                )
            )
            log_sums.append(row_max + jnp.log(row_total))
        context_rows.append(jnp.concatenate(block_pieces, axis=1))
    mixed = jnp.concatenate(context_rows, axis=0).reshape(TOK_DEV, D).astype(jnp.bfloat16)
    attn_out = jnp.dot(mixed, attn_full[3], preferred_element_type=jnp.float32) + bias_mixed
    hidden, normed_one, scale_one = norm_forward(
        tokens.astype(jnp.float32) + attn_out, gain_one, shift_one
    )
    hidden_low = hidden.astype(jnp.bfloat16)
    ffn_expand, ffn_contract = (
        lax.all_gather(expand_weight.astype(jnp.bfloat16), "fsdp", axis=0, tiled=True),
        lax.all_gather(contract_weight.astype(jnp.bfloat16), "fsdp", axis=0, tiled=True),
    )
    pre_act = jnp.dot(hidden_low, ffn_expand, preferred_element_type=jnp.float32) + bias_up
    activated = jax.nn.gelu(pre_act, approximate=False).astype(jnp.bfloat16)
    branch = jnp.dot(activated, ffn_contract, preferred_element_type=jnp.float32) + bias_down
    layer_output, normed_two, scale_two = norm_forward(hidden + branch, gain_two, shift_two)
    grad_sum, grad_gain_two, grad_shift_two = norm_backward(
        cotangent.astype(jnp.float32), normed_two, scale_two, gain_two
    )
    grad_branch = grad_sum.astype(jnp.bfloat16)
    grad_act = product_back(grad_branch, ffn_contract)
    unused_value, gelu_pull = jax.vjp(partial(jax.nn.gelu, approximate=False), pre_act)
    grad_pre_low = gelu_pull(grad_act)[0].astype(jnp.bfloat16)
    grad_hidden = grad_sum + product_back(grad_pre_low, ffn_expand)
    contract_full = product_over(activated, grad_branch)
    expand_full = product_over(hidden_low, grad_pre_low)
    grad_expand, grad_contract = (
        lax.psum_scatter(expand_full, "fsdp", scatter_dimension=0, tiled=True),
        lax.psum_scatter(contract_full, "fsdp", scatter_dimension=0, tiled=True),
    )
    grad_resid, grad_gain_one, grad_shift_one = norm_backward(
        grad_hidden, normed_one, scale_one, gain_one
    )
    grad_attn_out = grad_resid.astype(jnp.bfloat16)
    grad_bias_mixed = jnp.sum(grad_attn_out.astype(jnp.float32), axis=0)
    grad_output_proj = product_over(mixed, grad_attn_out)
    grad_mixed = product_back(grad_attn_out, attn_full[3]).astype(jnp.bfloat16)
    grad_context = grad_mixed.reshape(SEQ_DEV, LEN, H, HD)
    query_grads = []
    lse_index = 0
    seq_index = 0
    key_totals = [
        jnp.zeros((LEN, head_group, HD), jnp.float32) for head_start in range(0, H, head_group)
    ]
    value_totals = [
        jnp.zeros((LEN, head_group, HD), jnp.float32) for head_start in range(0, H, head_group)
    ]
    for row_start in range(0, LEN, block_rows):
        block_pieces = []
        for group_index, head_start in enumerate(range(0, H, head_group)):
            head_part = slice(head_start, head_start + head_group)
            query_block = query_heads[seq_index, row_start : row_start + block_rows, head_part]
            key_block = key_heads[seq_index, :, head_part]
            value_block = value_heads[seq_index, :, head_part]
            ctx_grad = grad_context[seq_index, row_start : row_start + block_rows, head_part]
            scores = block_scores(
                query_block,
                key_block,
                segment_ids[seq_index, row_start : row_start + block_rows],
                segment_ids[seq_index],
            )
            probability = jnp.exp(scores - log_sums[lse_index])
            lse_index = lse_index + 1
            value_totals[group_index] = value_totals[group_index] + jnp.einsum(
                "hqk,qhd->khd",
                probability.astype(jnp.bfloat16),
                ctx_grad,
                preferred_element_type=jnp.float32,
            )
            prob_grad = jnp.einsum(
                "qhd,khd->hqk", ctx_grad, value_block, preferred_element_type=jnp.float32
            )
            row_dot = jnp.sum(probability * prob_grad, axis=-1, keepdims=True)
            score_grad = (probability * (prob_grad - row_dot)).astype(jnp.bfloat16)
            block_pieces.append(
                jnp.einsum(
                    "hqk,khd->qhd", score_grad, key_block, preferred_element_type=jnp.float32
                ).astype(jnp.bfloat16)
            )
            key_totals[group_index] = key_totals[group_index] + jnp.einsum(
                "hqk,qhd->khd", score_grad, query_block, preferred_element_type=jnp.float32
            )
        query_grads.append(jnp.concatenate(block_pieces, axis=1))
    key_grads = jnp.concatenate(
        [key_total.astype(jnp.bfloat16) for key_total in key_totals], axis=1
    )
    value_grads = jnp.concatenate(
        [value_total.astype(jnp.bfloat16) for value_total in value_totals], axis=1
    )
    grad_query = jnp.concatenate(query_grads, axis=0).reshape(TOK_DEV, D) * 0.125
    grad_keys = key_grads.reshape(TOK_DEV, D)
    grad_values = value_grads.reshape(TOK_DEV, D)
    stacked_grads = jnp.stack([grad_query, grad_keys, grad_values])
    grad_qkv = jnp.einsum("td,nte->nde", tokens, stacked_grads, preferred_element_type=jnp.float32)
    input_grad = (
        grad_resid
        + jnp.einsum(
            "nte,nde->td", stacked_grads, attn_full[:3], preferred_element_type=jnp.float32
        )
    ).astype(jnp.bfloat16)
    grad_attention_full = jnp.concatenate([grad_qkv, grad_output_proj[None]], axis=0)
    vector_head = jnp.stack(
        [
            grad_gain_one,
            grad_gain_two,
            grad_shift_one,
            grad_shift_two,
            jnp.sum(grad_query.astype(jnp.float32), axis=0),
            jnp.sum(grad_values.astype(jnp.float32), axis=0),
            grad_bias_mixed,
            jnp.sum(grad_branch.astype(jnp.float32), axis=0),
        ]
    )
    grad_bias_up = jnp.sum(grad_pre_low.astype(jnp.float32), axis=0).reshape(FF // D, D)
    grad_vectors_full = jnp.concatenate([vector_head, grad_bias_up], axis=0)
    grad_attention, grad_vectors = (
        lax.psum_scatter(grad_attention_full, "fsdp", scatter_dimension=1, tiled=True),
        lax.psum_scatter(grad_vectors_full, "fsdp", scatter_dimension=1, tiled=True),
    )
    attention_new = inner_step(
        attention_weight, grad_attention, attention_first[0], attention_second[0], 0.03, 0.1
    )
    expand_new = inner_step(
        expand_weight, grad_expand, expand_first[0], expand_second[0], 0.03, 0.1
    )
    contract_new = inner_step(
        contract_weight, grad_contract, contract_first[0], contract_second[0], 0.015, 0.1
    )
    vectors_new = inner_step(vectors, grad_vectors, vectors_first[0], vectors_second[0], 0.2, 0.0)
    summed = (
        lax.psum((attention_weight - attention_new[0]).astype(jnp.bfloat16), "rep").astype(
            jnp.float32
        ),
        lax.psum((expand_weight - expand_new[0]).astype(jnp.bfloat16), "rep").astype(jnp.float32),
        lax.psum((contract_weight - contract_new[0]).astype(jnp.bfloat16), "rep").astype(
            jnp.float32
        ),
        lax.psum((vectors - vectors_new[0]).astype(jnp.bfloat16), "rep").astype(jnp.float32),
    )
    groups_count = lax.axis_size("rep")
    results = []
    for weight_now, momentum_now, inner_new, diff_total in zip(
        (attention_weight, expand_weight, contract_weight, vectors),
        (attention_momentum, expand_momentum, contract_momentum, vectors_momentum),
        (attention_new, expand_new, contract_new, vectors_new),
        summed,
    ):
        mean_diff = diff_total / groups_count
        momentum_new = 0.5 * momentum_now + mean_diff
        outer_new = weight_now - 0.7 * (mean_diff + 0.5 * momentum_new)
        results.append(
            (
                inner_new[1][None],
                inner_new[2][None],
                jnp.stack([mean_diff, momentum_new, outer_new]),
                outer_new.astype(jnp.bfloat16),
            )
        )
    return (
        layer_output.astype(jnp.bfloat16),
        input_grad,
        results[0][0],
        results[0][1],
        results[0][2],
        results[0][3],
        results[1][0],
        results[1][1],
        results[1][2],
        results[1][3],
        results[2][0],
        results[2][1],
        results[2][2],
        results[2][3],
        results[3][0],
        results[3][1],
        results[3][2],
        results[3][3],
    )


NEG=-1e30
QB=256
def attn_windows(seg_row):
    length = seg_row.shape[0]
    nb = length // QB
    firsts = seg_row[::QB]
    lasts = seg_row[QB-1::QB]
    begin = jnp.sum((seg_row[None, :] < firsts[:, None]).astype(jnp.int32), axis=1)
    end = jnp.sum((seg_row[None, :] <= lasts[:, None]).astype(jnp.int32), axis=1)
    start = begin // 128
    count = (end - start * 128 + QB - 1) // QB
    start = jnp.minimum(start, (length - count * QB) // 128)
    return start.astype(jnp.int32), count.astype(jnp.int32)
def lane_half(shape, h):
    lane = lax.broadcasted_iota(jnp.int32, shape, len(shape)-1)
    return (lane < 64) if h == 0 else (lane >= 64)
def dot(a, b, ca, cb):
    return lax.dot_general(a, b, (((ca,), (cb,)), ((), ())), preferred_element_type=jnp.float32)
def fold(value, join):
    part = value.shape[0] // 8
    parts = [value[i * part:(i + 1) * part] for i in range(8)]
    while len(parts) > 1:
        parts = [join(a, b) for a, b in zip(parts[::2], parts[1::2])]
    return parts[0]
def fwd_kernel(start_ref, count_ref, qkv_ref, segr_ref, segc_ref, o_ref, lse_ref, vt_ref):
    length = qkv_ref.shape[0]
    vt_ref[...] = qkv_ref[:, 256:384].T
    nb = length // QB
    for i in range(nb):
        rows = slice(i*QB, (i+1)*QB)
        for nn in range(1, nb+1):
            @pl.when(count_ref[i] == nn)
            def _():
                nk = nn*QB
                lo = pl.multiple_of(start_ref[i]*128, 128)
                kw = qkv_ref[pl.ds(lo, nk), 128:256]
                qb = qkv_ref[rows, 0:128]
                same = segc_ref[pl.ds(lo, nk), :] == segr_ref[:, rows]
                outs = []
                for h in range(2):
                    qh = jnp.where(lane_half(qb.shape, h), qb, jnp.zeros_like(qb))
                    st = jnp.where(same, dot(kw, qh, 1, 1), NEG)
                    m = jnp.max(fold(st, jnp.maximum), axis=0, keepdims=True)
                    p = jnp.exp(st - m)
                    l = jnp.sum(fold(p, jnp.add), axis=0, keepdims=True)
                    weighted = dot(vt_ref[h*64:(h+1)*64, pl.ds(lo, nk)], p.astype(jnp.bfloat16), 1, 0)
                    outs.append(weighted * (1.0 / l))
                    lse_ref[0, h:h+1, rows] = m + jnp.log(l)
                o_ref[rows, :] = jnp.concatenate(outs, axis=0).T.astype(jnp.bfloat16)
def bwd_kernel(start_ref, count_ref, qkv_ref, do_ref, lse_ref, segr_ref, segc_ref, d_ref, sums_ref, dk_acc, dv_acc, kt_ref):
    length = qkv_ref.shape[0]
    kt_ref[...] = qkv_ref[:, 128:256].T
    nb = length // QB
    dk_acc[...] = jnp.zeros_like(dk_acc)
    dv_acc[...] = jnp.zeros_like(dv_acc)
    for i in range(nb):
        rows = slice(i*QB, (i+1)*QB)
        for nn in range(1, nb+1):
            @pl.when(count_ref[i] == nn)
            def _():
                nk = nn*QB
                lo = pl.multiple_of(start_ref[i]*128, 128)
                win = pl.ds(lo, nk)
                kw = qkv_ref[win, 128:256]
                vw = qkv_ref[win, 256:384]
                qb = qkv_ref[rows, 0:128]
                db = do_ref[rows, :]
                same = segc_ref[win, :] == segr_ref[:, rows]
                dqs = []; dks = 0.0; dvs = 0.0
                for h in range(2):
                    hm = lane_half(qb.shape, h)
                    qh = jnp.where(hm, qb, jnp.zeros_like(qb))
                    dh = jnp.where(hm, db, jnp.zeros_like(db))
                    st = jnp.where(same, dot(kw, qh, 1, 1), NEG)
                    p = jnp.exp(st - lse_ref[0, h:h+1, rows])
                    dpt = dot(vw, dh, 1, 1)
                    rd = jnp.sum(fold(p * dpt, jnp.add), axis=0, keepdims=True)
                    ds = (p * (dpt - rd)).astype(jnp.bfloat16)
                    dvs = dvs + dot(p.astype(jnp.bfloat16), dh, 1, 0)
                    dks = dks + dot(ds, qh, 1, 0)
                    dqs.append(dot(kt_ref[h*64:(h+1)*64, win], ds, 1, 0))
                d_ref[rows, 0:128] = jnp.concatenate(dqs, axis=0).T.astype(jnp.bfloat16) * 0.125
                dk_acc[win, :] += dks
                dv_acc[win, :] += dvs
    d_ref[:, 128:256] = dk_acc[...].astype(jnp.bfloat16)
    d_ref[:, 256:384] = dv_acc[...].astype(jnp.bfloat16)
    sums_ref[0] = jnp.sum(d_ref[...].astype(jnp.float32), axis=0, keepdims=True)
def attn_fwd(qkv, seg):
    T, width = qkv.shape
    start, count = attn_windows(seg[0])
    segc = seg.reshape(T, 1)
    heads = width // 384
    return pl.pallas_call(
        fwd_kernel,
        out_shape=(jax.ShapeDtypeStruct((T, width // 3), jnp.bfloat16), jax.ShapeDtypeStruct((heads, 2, T), jnp.float32)),
        grid_spec=pltpu.PrefetchScalarGridSpec(
            num_scalar_prefetch=2, grid=(heads,),
            in_specs=[
                pl.BlockSpec((T, 384), lambda h, *_: (0, h)),
                pl.BlockSpec((1, T), lambda h, *_: (0, 0)),
                pl.BlockSpec((T, 1), lambda h, *_: (0, 0)),
            ],
            out_specs=(pl.BlockSpec((T, 128), lambda h, *_: (0, h)), pl.BlockSpec((1, 2, T), lambda h, *_: (h, 0, 0))),
            scratch_shapes=[pltpu.VMEM((128, T), jnp.bfloat16)],
        ),
        cost_estimate=cost(20 * T * T * width, 3 * T * width, T * T * width // 128),
        name="attn_fwd",
    )(start, count, qkv, seg, segc)


def attn_bwd(qkv, do, lse, seg, part):
    T, width = qkv.shape
    start, count = attn_windows(seg[0])
    segc = seg.reshape(T, 1)
    heads = width // 768
    first = part * heads
    return pl.pallas_call(
        bwd_kernel,
        out_shape=(jax.ShapeDtypeStruct((T, width // 2), jnp.bfloat16), jax.ShapeDtypeStruct((heads, 1, 384), jnp.float32)),
        grid_spec=pltpu.PrefetchScalarGridSpec(
            num_scalar_prefetch=2, grid=(heads,),
            in_specs=[
                pl.BlockSpec((T, 384), lambda h, *_: (0, first + h)),
                pl.BlockSpec((T, 128), lambda h, *_: (0, first + h)),
                pl.BlockSpec((1, 2, T), lambda h, *_: (first + h, 0, 0)),
                pl.BlockSpec((1, T), lambda h, *_: (0, 0)),
                pl.BlockSpec((T, 1), lambda h, *_: (0, 0)),
            ],
            out_specs=(pl.BlockSpec((T, 384), lambda h, *_: (0, h)), pl.BlockSpec((1, 1, 384), lambda h, *_: (h, 0, 0))),
            scratch_shapes=[pltpu.VMEM((T, 128), jnp.float32)] * 2 + [pltpu.VMEM((128, T), jnp.bfloat16)],
        ),
        cost_estimate=cost(20 * T * T * width, 6 * T * width, T * T * width // 64),
        name="attn_bwd",
    )(start, count, qkv, do, lse, seg, segc)


MESH_ID = pl.DeviceIdType.MESH


def bits_of():
    rep = lax.axis_index("rep")
    fsdp = lax.axis_index("fsdp")
    return dict(
        rep=rep, fsdp=fsdp, x=rep // 2, c=rep % 2, z1=fsdp // 4, z0=(fsdp // 2) % 2, y=fsdp % 2
    )


def partner_of(at, which):
    rep, fsdp = at["rep"], at["fsdp"]
    if which == "c":
        rep = rep + 1 - 2 * at["c"]
    elif which == "x":
        rep = rep + 2 - 4 * at["x"]
    elif which == "y":
        fsdp = fsdp + 1 - 2 * at["y"]
    elif which == "z0":
        fsdp = fsdp + 2 - 4 * at["z0"]
    elif which == "z1":
        fsdp = fsdp + 4 - 8 * at["z1"]
    else:
        rep = rep + 1 - 2 * at["c"]
        fsdp = fsdp + 2 - 4 * at["z0"]
    return (rep, fsdp)


REL = [(a, b, d) for d in (0, 1) for b in (0, 1) for a in (0, 1)]


def gather_kernel(
    qkv_in, wo_in, vec_in, tok_in, seg_in,
    qkv_out, wo_out, vec_out, tok_out, seg_out,
    tok_buf, seg_buf, send_sem, recv_sem, local_sem,
):
    at = bits_of()
    other = {k: partner_of(at, k) for k in ("c", "x", "y", "z0", "z1", "swap")}
    barrier = pltpu.get_barrier_semaphore()
    for k in ("c", "x", "y", "z0", "z1"):
        pl.semaphore_signal(barrier, inc=1, device_id=other[k], device_id_type=MESH_ID)
    moves = at["c"] != at["z0"]

    @pl.when(moves)
    def _():
        pl.semaphore_signal(barrier, inc=1, device_id=other["swap"], device_id_type=MESH_ID)
        pl.semaphore_wait(barrier, 6)

    @pl.when(jnp.logical_not(moves))
    def _():
        pl.semaphore_wait(barrier, 5)

    def flip(bit, rel):
        return bit + rel - 2 * bit * rel

    def shard(rel):
        return 4 * flip(at["z1"], rel[1]) + 2 * flip(at["z0"], rel[0]) + flip(at["y"], rel[2])

    counter = [0]
    started = []

    def send(src, dst, which):
        k = counter[0]
        counter[0] += 1
        copy = pltpu.make_async_remote_copy(
            src_ref=src, dst_ref=dst, send_sem=send_sem.at[k], recv_sem=recv_sem.at[k],
            device_id=other[which], device_id_type=MESH_ID,
        )
        copy.start()
        started.append(copy)
        return copy

    class Piece:
        def __init__(self, own, slot, split_x):
            self.own, self.slot, self.split_x = own, slot, split_x
            self.part = (2 * at["x"] + at["c"]) if split_x else at["c"]
            self.part_x = (2 * (1 - at["x"]) + at["c"]) if split_x else None
            self.copies = {}

        def first(self):
            zero = (0, 0, 0)
            for which in ("z1", "z0", "y"):
                self.copies[which, zero] = send(
                    self.own(self.part), self.slot(shard(zero), self.part), which
                )
            self.copies["c", zero] = send(self.own(None), self.slot(shard(zero), None), "c")

        def onward(self, rel):
            here = self.slot(shard(rel), self.part)
            if rel == (0, 1, 0):
                self.copies["z0", rel] = send(here, here, "z0")
            if rel[2] == 0:
                self.copies["y", rel] = send(here, here, "y")
            if self.split_x:
                self.copies["x", rel] = send(here, here, "x")
            self.copies["c", rel] = send(here, here, "c")

        def arrive(self, which, came):
            self.copies[which, came].wait_recv()
            step = {"z0": (1, 0, 0), "z1": (0, 1, 0), "y": (0, 0, 1)}[which]
            self.onward(tuple(p + q for p, q in zip(came, step)))

        def near(self):
            self.arrive("z1", (0, 0, 0))
            self.arrive("z0", (0, 0, 0))

        def rest(self):
            self.arrive("y", (0, 0, 0))
            self.arrive("z0", (0, 1, 0))
            self.arrive("y", (0, 1, 0))
            self.arrive("y", (1, 0, 0))
            self.arrive("y", (1, 1, 0))

        def last(self):
            if self.split_x:
                for rel in REL[1:]:
                    self.copies["x", rel].wait_recv()
                    there = self.slot(shard(rel), self.part_x)
                    self.copies["cx", rel] = send(there, there, "c")

        def finish(self):
            for (which, rel), copy in self.copies.items():
                if which in ("c", "cx"):
                    copy.wait_recv()

    def rows(ref, count):
        full = ref.shape[-2] // 8
        def slot(f, part):
            if part is None:
                at_row, n = f * full, full
            else:
                at_row, n = f * full + part * (full // count), full // count
            at_row = pl.multiple_of(at_row, 8)
            return ref.at[pl.ds(at_row, n), :]
        return slot

    def own_rows(ref, count):
        full = ref.shape[-2]
        def own(part):
            if part is None:
                return ref
            row = pl.multiple_of(part * (full // count), 8)
            n = full // count
            return ref.at[pl.ds(row, n), :]
        return own

    qkv, wo = pieces = [
        Piece(own_rows(qkv_in, 4), rows(qkv_out, 4), True),
        Piece(own_rows(wo_in, 4), rows(wo_out, 4), True),
    ]
    zero = (0, 0, 0)
    vec_copies = [
        send(vec_in, vec_out.at[shard(zero)], which) for which in ("c", "z1", "z0", "y")
    ]
    pieces[0].first()
    tok_k, seg_k = counter[0], counter[0] + 1
    counter[0] += 2

    def swap_copy(src, dst, k):
        return pltpu.make_async_remote_copy(
            src_ref=src, dst_ref=dst, send_sem=send_sem.at[k], recv_sem=recv_sem.at[k],
            device_id=other["swap"], device_id_type=MESH_ID,
        )

    @pl.when(moves)
    def _():
        swap_copy(tok_in, tok_out, tok_k).start()
        swap_copy(seg_in, seg_out, seg_k).start()

    @pl.when(jnp.logical_not(moves))
    def _():
        one = pltpu.make_async_copy(tok_in, tok_buf, local_sem.at[0])
        two = pltpu.make_async_copy(seg_in, seg_buf, local_sem.at[1])
        one.start()
        two.start()
        one.wait()
        two.wait()
        three = pltpu.make_async_copy(tok_buf, tok_out, local_sem.at[0])
        four = pltpu.make_async_copy(seg_buf, seg_out, local_sem.at[1])
        three.start()
        four.start()
        three.wait()
        four.wait()

    wo.first()
    qkv.near()
    vec_copies[1].wait_recv()
    here = vec_out.at[shard((0, 1, 0))]
    vec_far = send(here, here, "z0")
    vec_more = [send(here, here, "y")]
    vec_copies[2].wait_recv()
    here = vec_out.at[shard((1, 0, 0))]
    vec_more.append(send(here, here, "y"))
    qkv.rest()
    wo.near()
    wo.rest()
    vec_far.wait_recv()
    here = vec_out.at[shard((1, 1, 0))]
    vec_more.append(send(here, here, "y"))
    qkv.last()
    wo.last()
    for piece in pieces:
        piece.finish()
    for copy in [vec_copies[0], vec_copies[3]] + vec_more:
        copy.wait_recv()
    for copy in started:
        copy.wait_send()

    @pl.when(moves)
    def _():
        swap_copy(tok_in, tok_out, tok_k).wait()
        swap_copy(seg_in, seg_out, seg_k).wait()


GATHER_COPIES = 29 * 2 + 8 + 2


def gather_all(qkv, wo, vec, tok, seg):
    bf = jnp.bfloat16
    shape = jax.ShapeDtypeStruct
    whole = pl.BlockSpec(memory_space=pl.ANY)
    return pl.pallas_call(
        gather_kernel,
        out_shape=(
            shape((8 * qkv.shape[0], qkv.shape[1]), bf),
            shape((8 * wo.shape[0], wo.shape[1]), bf),
            shape((8,) + vec.shape, bf),
            shape(tok.shape, bf),
            shape(seg.shape, seg.dtype),
        ),
        in_specs=[whole] * 5,
        out_specs=(whole,) * 5,
        scratch_shapes=[
            pltpu.VMEM(tok.shape, bf),
            pltpu.VMEM(seg.shape, seg.dtype),
            pltpu.SemaphoreType.DMA((GATHER_COPIES,)),
            pltpu.SemaphoreType.DMA((GATHER_COPIES,)),
            pltpu.SemaphoreType.DMA((2,)),
        ],
        compiler_params=pltpu.CompilerParams(collective_id=0, has_side_effects=True),
        name="gather_weights",
    )(qkv, wo, vec, tok, seg)


SHRINK = 1000
BF, F32 = jnp.bfloat16, jnp.float32
SHAPE = jax.ShapeDtypeStruct


def full_spec(shape):
    return pl.BlockSpec(shape, lambda *_: (0,) * len(shape), pipeline_mode=pl.Buffered(1))


def cost(flops, moved, exps=0):
    return pl.CostEstimate(flops=int(flops) // SHRINK, bytes_accessed=int(moved) // SHRINK, transcendentals=int(exps) // SHRINK)


def qkv_kernel(x_ref, w_ref, bias_ref, scale_ref, o_ref):
    for i in range(4):
        rows = slice(i * 256, (i + 1) * 256)
        z = dot(x_ref[rows, :], w_ref[...], 1, 0)
        o_ref[rows, :] = ((z + bias_ref[...]) * scale_ref[...]).astype(BF)


def qkv_call(x, w, bias, scale):
    tokens, width = x.shape[0], w.shape[1]
    tile = 768
    return pl.pallas_call(
        qkv_kernel,
        out_shape=SHAPE((tokens, width), BF),
        grid=(width // tile,),
        in_specs=[
            full_spec(x.shape),
            pl.BlockSpec((x.shape[1], tile), lambda j: (0, j)),
            pl.BlockSpec((1, tile), lambda j: (0, j)),
            pl.BlockSpec((1, tile), lambda j: (0, j)),
        ],
        out_specs=pl.BlockSpec((tokens, tile), lambda j: (0, j)),
        cost_estimate=cost(2 * tokens * D * width, 2 * (tokens * D + D * width + tokens * width)),
        name="qkv",
    )(x, w, bias, scale)


def mean_row(value):
    return jnp.mean(value, axis=-1, keepdims=True)


def mix_kernel(c_ref, w_ref, x_ref, rows_ref, n_ref, q_ref, low_ref):
    value = x_ref[...].astype(F32) + dot(c_ref[...], w_ref[...], 1, 0) + rows_ref[6:7, :]
    center = value - mean_row(value)
    inv = lax.rsqrt(mean_row(center * center) + 1e-05)
    normed = center * inv
    n_ref[...] = normed
    q_ref[...] = inv
    low_ref[...] = (normed * rows_ref[0:1, :] + rows_ref[2:3, :]).astype(BF)


def mix_call(mixed, w_out, tok, rows):
    t = tok.shape[0]
    tile = pl.BlockSpec((256, D), lambda i: (i, 0))
    return pl.pallas_call(
        mix_kernel,
        out_shape=(SHAPE((t, D), F32), SHAPE((t, 1), F32), SHAPE((t, D), BF)),
        grid=(t // 256,),
        in_specs=[tile, full_spec((D, D)), tile, full_spec(rows.shape)],
        out_specs=(tile, pl.BlockSpec((256, 1), lambda i: (i, 0)), tile),
        cost_estimate=cost(2 * t * D * D, 12 * t * D + 2 * D * D),
        name="mix_norm",
    )(mixed, w_out, tok, rows)


def up_kernel(place_ref, h_ref, *refs):
    parts, (bias_ref, g_ref, s_ref) = refs[:4], refs[4:]
    each = pl.num_programs(0) // 4

    def tile(w_ref):
        for i in range(8):
            rows = slice(i * 128, (i + 1) * 128)
            z = dot(h_ref[rows, :], w_ref[...], 1, 0) + bias_ref[...]
            phi, bell = erf_parts(z)
            g_ref[rows, :] = (z * phi).astype(BF)
            s_ref[rows, :] = (phi + z * bell * 0.3989422804014327).astype(BF)

    for k in range(4):
        pl.when(pl.program_id(0) // each == k)(partial(tile, parts[k]))


def up_call(low, parts, place, bias):
    t = low.shape[0]
    tile = 512
    each = FF // tile // 4
    where = lambda j, p: (0, p[j // each] * each + lax.rem(j, each))
    out = pl.BlockSpec((t, tile), where)

    def part(k):
        return pl.BlockSpec((D, tile), lambda j, p: (0, jnp.clip(j - k * each, 0, each - 1)))

    return pl.pallas_call(
        up_kernel,
        out_shape=(SHAPE((t, FF), BF), SHAPE((t, FF), BF)),
        grid_spec=pltpu.PrefetchScalarGridSpec(
            num_scalar_prefetch=1, grid=(FF // tile,),
            in_specs=[full_spec(low.shape)] + [part(k) for k in range(4)] + [pl.BlockSpec((1, tile), where)],
            out_specs=(out, out),
        ),
        cost_estimate=cost(2 * t * D * FF, 2 * (t * D + D * FF + 2 * t * FF), 2 * t * FF),
        name="up_gelu",
    )(place, low, *parts, bias)


def row_sum(value):
    return jnp.sum(value, axis=0, keepdims=True)


def norm_back(grad, normed, inv, gain):
    scaled = grad * gain
    return inv * (scaled - mean_row(scaled) - normed * mean_row(scaled * normed))


def down_kernel(
    core_ref, g_ref, own_ref, came_ref, n_ref, cot_ref, rows_ref, out_ref, dr_ref, dm_ref, sums_ref, m_ref
):
    half = D // 2
    m_ref[:, pl.ds(pl.multiple_of(core_ref[0] * half, half), half)] = dot(g_ref[...], own_ref[...], 1, 0)
    m_ref[:, pl.ds(pl.multiple_of((1 - core_ref[0]) * half, half), half)] = dot(g_ref[...], came_ref[...], 1, 0)
    hidden = n_ref[...] * rows_ref[0:1, :] + rows_ref[2:3, :]
    value = hidden + m_ref[...] + rows_ref[7:8, :]
    center = value - mean_row(value)
    inv = lax.rsqrt(mean_row(center * center) + 1e-05)
    normed = center * inv
    gain = rows_ref[1:2, :]
    out_ref[...] = (normed * gain + rows_ref[3:4, :]).astype(BF)
    grad = cot_ref[...].astype(F32)
    back = norm_back(grad, normed, inv, gain)
    low = back.astype(BF)
    dr_ref[...] = back
    dm_ref[...] = low

    @pl.when(pl.program_id(0) == 0)
    def _():
        sums_ref[...] = jnp.zeros_like(sums_ref)

    sums_ref[0:1, :] += row_sum(grad * normed)
    sums_ref[1:2, :] += row_sum(grad)
    sums_ref[2:3, :] += row_sum(low.astype(F32))


def down_call(act, own, came, normed, cot, rows, core):
    t = act.shape[0]
    tile = pl.BlockSpec((256, D), lambda i, c: (i, 0))
    return pl.pallas_call(
        down_kernel,
        out_shape=(SHAPE((t, D), BF), SHAPE((t, D), F32), SHAPE((t, D), BF), SHAPE((8, D), F32)),
        grid_spec=pltpu.PrefetchScalarGridSpec(
            num_scalar_prefetch=1, grid=(t // 256,),
            in_specs=[
                pl.BlockSpec((256, FF), lambda i, c: (i, 0)), full_spec((FF, D // 2)), full_spec((FF, D // 2)),
                tile, tile, full_spec(rows.shape),
            ],
            out_specs=(tile, tile, tile, pl.BlockSpec((8, D), lambda i, c: (0, 0))),
            scratch_shapes=[pltpu.VMEM((256, D), F32)],
        ),
        cost_estimate=cost(2 * t * D * FF, 2 * (t * FF + D * FF) + 14 * t * D),
        name="down_norm",
    )(core.reshape(1), act, own, came, normed, cot, rows)


def slope_kernel(core_ref, left_ref, right_ref, own_ref, came_ref, s_ref, o_ref, sums_ref):
    total = 0.0
    for i in range(4):
        rows = slice(i * 256, (i + 1) * 256)
        back = dot(left_ref[rows, :], own_ref[...], 1, 1) + dot(right_ref[rows, :], came_ref[...], 1, 1)
        z = (back * s_ref[rows, :].astype(F32)).astype(BF)
        o_ref[rows, :] = z
        total = total + row_sum(z.astype(F32))
    sums_ref[...] = total


def slope_call(dm, own, came, slope, core):
    t = dm.shape[0]
    tile = 512
    wide = pl.BlockSpec((t, tile), lambda j, c: (0, j))
    part = pl.BlockSpec((tile, D // 2), lambda j, c: (j, 0))
    return pl.pallas_call(
        slope_kernel,
        out_shape=(SHAPE((t, FF), BF), SHAPE((1, FF), F32)),
        grid_spec=pltpu.PrefetchScalarGridSpec(
            num_scalar_prefetch=1, grid=(FF // tile,),
            in_specs=[
                pl.BlockSpec((t, D // 2), lambda j, c: (0, c[0])),
                pl.BlockSpec((t, D // 2), lambda j, c: (0, 1 - c[0])),
                part, part, wide,
            ],
            out_specs=(wide, pl.BlockSpec((1, tile), lambda j, c: (0, j))),
        ),
        cost_estimate=cost(2 * t * D * FF, 2 * (t * D + D * FF + 2 * t * FF)),
        name="down_back",
    )(core.reshape(1), dm, dm, own, came, slope)


def hidden_kernel(place_ref, *refs):
    grads, parts = refs[:4], refs[4:8]
    dr_ref, n_ref, q_ref, wo_ref, rows_ref, r_ref, a_ref, c_ref, sums_ref = refs[8:]
    grad = dr_ref[...]
    for grad_ref, w_ref in zip(grads, parts):
        grad = grad + dot(grad_ref[...], w_ref[...], 1, 1)
    normed = n_ref[...]
    back = norm_back(grad, normed, q_ref[...], rows_ref[0:1, :])
    low = back.astype(BF)
    r_ref[...] = back
    a_ref[...] = low
    c_ref[...] = dot(low, wo_ref[...], 1, 1).astype(BF)

    @pl.when(pl.program_id(0) == 0)
    def _():
        sums_ref[...] = jnp.zeros_like(sums_ref)

    sums_ref[0:1, :] += row_sum(grad * normed)
    sums_ref[1:2, :] += row_sum(grad)
    sums_ref[2:3, :] += row_sum(low.astype(F32))


def hidden_call(dz, parts, place, dr, normed, inv, w_out, rows):
    t = dz.shape[0]
    tile = pl.BlockSpec((256, D), lambda i, p: (i, 0))

    def quarter(k):
        return pl.BlockSpec((256, FF // 4), lambda i, p: (i, p[k]))

    return pl.pallas_call(
        hidden_kernel,
        out_shape=(SHAPE((t, D), F32), SHAPE((t, D), BF), SHAPE((t, D), BF), SHAPE((8, D), F32)),
        grid_spec=pltpu.PrefetchScalarGridSpec(
            num_scalar_prefetch=1, grid=(t // 256,),
            in_specs=[quarter(k) for k in range(4)] + [full_spec((D, FF // 4))] * 4 + [
                tile, tile,
                pl.BlockSpec((256, 1), lambda i, p: (i, 0)), full_spec((D, D)), full_spec(rows.shape),
            ],
            out_specs=(tile, tile, tile, pl.BlockSpec((8, D), lambda i, p: (0, 0))),
        ),
        cost_estimate=cost(2 * t * D * (FF + D), 2 * (t * FF + D * FF) + 16 * t * D),
        name="up_back_norm",
    )(place, *([dz] * 4), *parts, dr, normed, inv, w_out, rows)


def input_kernel(a_ref, b_ref, w_ref, r_ref, o_ref):
    half = a_ref.shape[1]
    value = dot(a_ref[...], w_ref[:, :half], 1, 1) + dot(b_ref[...], w_ref[:, half:], 1, 1)
    o_ref[...] = (r_ref[...] + value).astype(BF)


def input_call(part_a, part_b, w_qkv, resid):
    t, width = part_a.shape
    tile = pl.BlockSpec((256, D), lambda i: (i, 0))
    wide = pl.BlockSpec((256, width), lambda i: (i, 0))
    return pl.pallas_call(
        input_kernel,
        out_shape=SHAPE((t, D), BF),
        grid=(t // 256,),
        in_specs=[wide, wide, full_spec(w_qkv.shape), tile],
        out_specs=tile,
        cost_estimate=cost(4 * t * D * width, 4 * (t * width + D * width) + 6 * t * D),
        name="input_back",
    )(part_a, part_b, w_qkv, resid)


def weight_kernel(at_ref, *refs):
    left, right_ref, rest, turned = refs[:4], refs[4], refs[5:-1], refs[-1]

    @pl.when(pl.program_id(1) == 0)
    def _():
        part = left[0].shape[1]
        for k in range(4):
            turned[k * part:(k + 1) * part, :] = left[k][...].T

    value = dot(turned[...], right_ref[...], 1, 0)
    if len(rest) == 1:
        rest[0][...] = value.astype(BF)
        return
    came_ref, away_ref, keep_ref = rest
    value = (value + came_ref[...].astype(F32)).astype(BF)
    rows = away_ref.shape[0]
    if rows < value.shape[0]:
        away_ref[...] = value[:rows]
        keep_ref[...] = value[rows:]
    else:
        first = pl.program_id(0) < pl.num_programs(0) // 2

        @pl.when(first)
        def _():
            away_ref[...] = value

        @pl.when(jnp.logical_not(first))
        def _():
            keep_ref[...] = value


def weight_call(left, right, half, y, came=None):
    t, rows = left.shape
    width = right.shape[1]
    bm = 512
    bn = 1024 if width == 1024 else 512
    steps = rows // 2 // bm

    def column(k):
        def place(i, j, at):
            if steps == 1:
                side, z1 = (1 - at[1] if k < 2 else at[1]), k % 2
                return (0, z1 * 4 + at[0] * 2 + side)
            side = at[1] + (1 - 2 * at[1]) * (1 - i // 2)
            return (0, (lax.rem(i, 2) * 4 + at[0] * 2 + side) * 4 + k)

        return pl.BlockSpec((t, bm // 4), place)

    specs = [column(k) for k in range(4)] + [pl.BlockSpec((t, bn), lambda i, j, at: (0, j))]
    values = [left] * 4 + [right]
    out = pl.BlockSpec((bm, bn), lambda i, j, at: (i, j))
    if came is None:
        shapes = SHAPE((rows // 2, width), BF)
    else:
        specs.append(out)
        values.append(came)
        shapes = (SHAPE((rows // 4, width), BF),) * 2
        if steps == 1:
            out = (pl.BlockSpec((bm // 2, bn), lambda i, j, at: (0, j)),) * 2
        else:
            out = (
                pl.BlockSpec((bm, bn), lambda i, j, at: (jnp.minimum(i, steps // 2 - 1), j)),
                pl.BlockSpec((bm, bn), lambda i, j, at: (jnp.maximum(i - steps // 2, 0), j)),
            )
    return pl.pallas_call(
        weight_kernel,
        out_shape=shapes,
        grid_spec=pltpu.PrefetchScalarGridSpec(
            num_scalar_prefetch=1, grid=(steps, width // bn), in_specs=specs, out_specs=out,
            scratch_shapes=[pltpu.VMEM((bm, t), BF)],
        ),
        cost_estimate=cost(t * rows * width, t * rows + 2 * t * width + 2 * rows * width),
        name="weight_grad",
    )(jnp.stack([half, y]), *values)


def inner_kernel(rate, decay, w_ref, g_ref, m_ref, v_ref, m_out, v_out, d_out):
    weight = w_ref[...]
    new, m_out[...], v_out[...] = inner_step(
        weight, g_ref[...].astype(F32), m_ref[...], v_ref[...], rate, decay
    )
    d_out[...] = (weight - new).astype(BF)


def inner_call(weight, grad, first, second, rate, decay):
    rows, width = weight.shape
    block = 32 * 4096 // width
    tile = pl.BlockSpec((block, width), lambda i: (i, 0))
    like = SHAPE((rows, width), F32)
    return pl.pallas_call(
        partial(inner_kernel, rate, decay),
        out_shape=(like, like, SHAPE((rows, width), BF)),
        grid=(rows // block,),
        in_specs=[tile] * 4,
        out_specs=(tile,) * 3,
        cost_estimate=cost(20 * rows * width, 24 * rows * width),
        name="inner_step",
    )(weight, grad, first, second)


def outer_kernel(core_ref, w_ref, u_ref, own_ref, came_ref, o_ref, c_ref):
    mine = (core_ref[0] == pl.program_id(0)).astype(F32)
    total = own_ref[...].astype(F32) * mine + came_ref[...].astype(F32) * (1.0 - mine)
    mean = total * 0.25
    weight = w_ref[...]
    momentum = 0.5 * u_ref[...] + mean
    new = weight - 0.7 * (mean + 0.5 * momentum)
    o_ref[0] = mean
    o_ref[1] = momentum
    o_ref[2] = new
    c_ref[...] = new.astype(BF)


def outer_call(weight, momentum, own, came, core):
    rows, width = weight.shape
    block = 32 * 4096 // width
    steps = rows // 2 // block
    tile = pl.BlockSpec((block, width), lambda h, i, c: (h * steps + i, 0))
    part = pl.BlockSpec((block, width), lambda h, i, c: (i, 0))
    return pl.pallas_call(
        outer_kernel,
        out_shape=(SHAPE((3, rows, width), F32), SHAPE((rows, width), BF)),
        grid_spec=pltpu.PrefetchScalarGridSpec(
            num_scalar_prefetch=1, grid=(2, steps), in_specs=[tile, tile, part, part],
            out_specs=(pl.BlockSpec((3, block, width), lambda h, i, c: (0, h * steps + i, 0)), tile),
        ),
        cost_estimate=cost(10 * rows * width, 26 * rows * width),
        name="outer_step",
    )(core.reshape(1), weight, momentum, own, came)


def erf_parts(value):
    size = jnp.abs(value) * 0.7071067811865476
    share = 1.0 / (1.0 + 0.5 * size)
    inner = 0.17087277
    for coefficient in (
        -0.82215223, 1.48851587, -1.13520398, 0.27886807, -0.18628806, 0.09678418, 0.37409196, 1.00002368
    ):
        inner = coefficient + share * inner
    square = size * size
    half = 0.5 * share * jnp.exp(share * inner - 1.26551223 - square)
    return jnp.where(value >= 0, 1.0 - half, half), jnp.exp(-square)


def xor_pairs(bits):
    place = {"y": 0, "z0": 1, "z1": 2, "c": 3, "x": 4}
    flip = sum(1 << place[bit] for bit in bits)
    pairs = []
    for device in range(32):
        if bits == ("c", "z0") and ((device >> 3) & 1) == ((device >> 1) & 1):
            continue
        pairs.append((device, device ^ flip))
    return pairs


def exchange(value, *bits):
    return lax.ppermute(value, ("rep", "fsdp"), xor_pairs(bits))


def add_low(left, right):
    return (left.astype(jnp.float32) + right.astype(jnp.float32)).astype(jnp.bfloat16)


def pick(value, index, axis):
    return lax.dynamic_index_in_dim(value, index, axis, keepdims=False)


def halve(at, total, which):
    away = pick(total.reshape(2, -1, total.shape[-1]), 1 - at[which], 0)
    return away, exchange(away, which)


def join(at, total, came, which, *gates):
    return add_low(pick(total.reshape(2, -1, total.shape[-1]), at[which], 0), after(came, *gates))


def join_kept(kept, came, *gates):
    return add_low(kept, after(came, *gates))


def after(value, *earlier):
    return lax.optimization_barrier((value,) + earlier)[0]


def weave(value):
    rows = value.shape[1]
    return jnp.transpose(value.reshape(3, rows, D // 128, 128), (1, 2, 0, 3)).reshape(rows, 3 * D)


def unweave(value):
    rows = value.shape[0]
    return jnp.transpose(value.reshape(rows, D // 128, 3, 128), (2, 0, 1, 3)).reshape(3, rows, D)


def per_device_fast(
    tokens,
    cotangent,
    segment_ids,
    attention_weight,
    attention_momentum,
    attention_first,
    attention_second,
    expand_weight,
    expand_momentum,
    expand_first,
    expand_second,
    contract_weight,
    contract_momentum,
    contract_first,
    contract_second,
    vectors,
    vectors_momentum,
    vectors_first,
    vectors_second,
):
    bf, f32 = jnp.bfloat16, jnp.float32
    at = bits_of()
    core = at["c"].astype(jnp.int32)
    side = at["y"].astype(jnp.int32)
    def swapped(value, came):
        return jnp.where(at["c"] != at["z0"], came, value)

    def cross(value):
        return exchange(value, "c", "z0")

    quarter = 2 * core + at["x"].astype(jnp.int32)
    place = jnp.stack([quarter, 2 * (1 - core) + quarter - 2 * core, quarter + 1 - 2 * at["x"], 3 - quarter])
    part = expand_weight.shape[1] // 4
    in_own = lax.all_gather(
        lax.dynamic_slice_in_dim(expand_weight, quarter * part, part, axis=1).astype(bf), "fsdp", axis=0, tiled=True
    )
    attn_low = attention_weight.astype(bf)
    w_qkv, w_out, vector_full, tok, seg = gather_all(
        weave(attn_low[:3]), attn_low[3], vectors.astype(bf), tokens, segment_ids,
    )
    cot_came = cross(after(cotangent, w_qkv))
    rows = jnp.swapaxes(vector_full, 0, 1).reshape(-1, D).astype(f32)
    bias_up = rows[8:].reshape(1, FF)
    bias_qkv = weave(jnp.stack([rows[4], jnp.zeros_like(rows[4]), rows[5]])[:, None])
    scale_qkv = weave(jnp.stack([jnp.full((1, D), 0.125, f32)] + [jnp.ones((1, D), f32)] * 2))
    part = contract_weight.shape[1] // 2
    down_half = lax.dynamic_slice_in_dim(contract_weight, core * part, part, axis=1).astype(bf)
    down_own = lax.all_gather(after(down_half, w_qkv), "fsdp", axis=0, tiled=True)
    in_near = after(in_own, w_qkv)
    in_far = exchange(in_near, "x")
    in_side = exchange(in_near, "c")
    qkv = qkv_call(tok, w_qkv, bias_qkv, scale_qkv)
    mixed, log_sum = attn_fwd(qkv, seg)
    in_parts = [in_own, after(in_side, mixed), in_far, exchange(after(in_far, mixed), "c")]
    normed, inv, hidden_low = mix_call(mixed, w_out, tok, rows)
    cot = swapped(cotangent, after(cot_came, hidden_low))
    activated, slope = up_call(after(hidden_low, cot), in_parts, place, bias_up)
    down_other = exchange(after(down_own, activated), "c")
    layer_output, grad_sum, grad_branch, sums_two = down_call(
        activated, down_own, down_other, normed, cot, rows, core
    )
    output_came = cross(layer_output)
    down_send = weight_call(activated, grad_branch, 1 - core, side)
    grad_pre, sums_up = slope_call(after(grad_branch, down_send), down_own, down_other, slope, core)
    down_came = exchange(down_send, "c")
    up_send = weight_call(hidden_low, grad_pre, 1 - core, side)
    away_d, down_kept = weight_call(activated, after(grad_branch, up_send), core, side, down_came)
    up_came = exchange(up_send, "c")
    came_d = exchange(away_d, "y")
    away_u, up_kept = weight_call(hidden_low, after(grad_pre, away_d), core, side, up_came)
    came_u = exchange(away_u, "y")
    grad_resid, grad_attn, grad_mixed, sums_one = hidden_call(
        after(grad_pre, away_u), in_parts, place, grad_sum, normed, inv, w_out, rows
    )
    proj_send = weight_call(mixed, grad_attn, 1 - core, side)
    proj_came = exchange(proj_send, "c")
    output = swapped(layer_output, after(output_came, proj_send))
    down_one = join_kept(down_kept, came_d, output)
    away_d, came_d = halve(at, down_one, "z1")
    grad_a, sums_a = attn_bwd(qkv, after(grad_mixed, proj_send, away_d), log_sum, seg, 0)
    send_a = weight_call(tok, grad_a, 1 - core, side)
    came_a = exchange(send_a, "c")
    away_p, proj_kept = weight_call(mixed, after(grad_attn, send_a), core, side, proj_came)
    came_p = exchange(away_p, "y")
    away_a, a_kept = weight_call(tok, after(grad_a, away_p), core, side, came_a)
    came_one = exchange(away_a, "y")
    up_one = join_kept(up_kept, came_u, away_a)
    away_u, came_u = halve(at, up_one, "z1")
    grad_b, sums_b = attn_bwd(qkv, after(grad_mixed, away_u), log_sum, seg, 1)
    send_b = weight_call(tok, grad_b, 1 - core, side)
    came_b = exchange(send_b, "c")
    down_two = join(at, down_one, came_d, "z1", send_b)
    cross_d = cross(down_two)
    proj_one = join_kept(proj_kept, came_p, down_two)
    away_p, came_p = halve(at, proj_one, "z1")
    a_one = join_kept(a_kept, came_one, away_p)
    away_a, came_a = halve(at, a_one, "z1")
    away_b, b_kept = weight_call(tok, after(grad_b, away_a), core, side, came_b)
    came_b = exchange(away_b, "y")
    sums_qkv = jnp.concatenate([sums_a, sums_b], axis=0).reshape(D // 128, 3, 128)
    vector_grad = jnp.concatenate(
        [
            sums_one[0:1],
            sums_two[0:1],
            sums_one[1:2],
            sums_two[1:2],
            sums_qkv[:, 0].reshape(1, D),
            sums_qkv[:, 2].reshape(1, D),
            sums_one[2:3],
            sums_two[2:3],
            sums_up.reshape(FF // D, D),
        ],
        axis=0,
    )

    def vector_send(parts, which):
        half = parts.shape[1] // 2
        away = lax.dynamic_slice_in_dim(parts, (1 - at[which]) * half, half, axis=1)
        return exchange(away, which)

    def vector_join(parts, came, which, *gates):
        half = parts.shape[1] // 2
        return lax.dynamic_slice_in_dim(parts, at[which] * half, half, axis=1) + after(came, *gates)

    vec_came = vector_send(vector_grad, "z1")

    def inner(weight, grad, first, second, rate, decay):
        flat = (-1, weight.shape[-1])
        return inner_call(
            weight.reshape(flat), grad.reshape(flat), first.reshape(flat), second.reshape(flat), rate, decay
        )

    def rep_send(diff):
        halves = diff.reshape(2, diff.shape[0] // 2, diff.shape[1])
        away = pick(halves, 1 - at["c"], 0)
        return away, exchange(away, "c")

    def rep_join(diff, came, *gates):
        halves = diff.reshape(2, diff.shape[0] // 2, diff.shape[1])
        return add_low(pick(halves, at["c"], 0), after(came, *gates))

    def outer(weight, momentum, own, came):
        flat = (-1, weight.shape[-1])
        return outer_call(weight.reshape(flat), momentum.reshape(flat), own, came, core)

    grad_contract = swapped(down_two, after(cross_d, away_b))
    contract_new = inner(contract_weight, grad_contract, contract_first, contract_second, 0.015, 0.1)
    sent_c, came_c = rep_send(contract_new[2])
    up_two = join(at, up_one, came_u, "z1", sent_c)
    cross_u = cross(up_two)
    vec_one = vector_join(vector_grad, vec_came, "z1", up_two)
    vec_came = vector_send(vec_one, "c")
    b_one = join_kept(b_kept, came_b, up_two)
    away_b, came_b = halve(at, b_one, "z1")
    half_c = rep_join(contract_new[2], came_c, away_b)
    rest_c = exchange(half_c, "x")
    vec_two = vector_join(vec_one, vec_came, "c", half_c)
    vec_came = vector_send(vec_two, "y")
    input_grad = input_call(after(grad_a, away_b, half_c), grad_b, w_qkv, grad_resid)
    grad_expand = swapped(up_two, after(cross_u, input_grad))
    expand_new = inner(expand_weight, grad_expand, expand_first, expand_second, 0.03, 0.1)
    sent_e, came_e = rep_send(expand_new[2])
    proj_two = join(at, proj_one, came_p, "z1", sent_e)
    a_two = join(at, a_one, came_a, "z1", sent_e)
    cross_pa = cross(jnp.concatenate([proj_two, a_two], axis=1))
    vec_three = vector_join(vec_two, vec_came, "y", proj_two, a_two)
    vec_cross = cross(vec_three)
    full_c = add_low(half_c, after(rest_c, vec_three))
    back_c = exchange(full_c, "c")
    half_e = rep_join(expand_new[2], came_e, full_c)
    rest_e = exchange(half_e, "x")
    b_two = join(at, b_one, came_b, "z1", half_e)
    cross_b = cross(b_two)
    outer_c = outer(contract_weight, contract_momentum, full_c, after(back_c, b_two))
    grad_vectors = swapped(vec_three, after(vec_cross, outer_c[1]))
    inner_new, first_new, second_new = inner_step(
        vectors, grad_vectors, vectors_first[0], vectors_second[0], 0.2, 0.0
    )
    vec_diff = (vectors - inner_new).astype(bf)
    vec_near = exchange(vec_diff, "c")
    input_came = cross(after(input_grad, b_two, vec_diff))
    pa = swapped(jnp.concatenate([proj_two, a_two], axis=1), after(cross_pa, outer_c[1]))
    b_own = swapped(b_two, after(cross_b, vec_diff, pa))
    grad_qkv = jnp.concatenate([pa[:, D:], b_own], axis=1)
    grad_attention = jnp.concatenate([unweave(grad_qkv), pa[None, :, :D]], axis=0)
    attention_new = inner(attention_weight, grad_attention, attention_first, attention_second, 0.03, 0.1)
    sent_a, came_a = rep_send(attention_new[2])
    vec_half = add_low(vec_diff, after(vec_near, sent_a))
    vec_far = exchange(vec_half, "x")
    full_e = add_low(half_e, after(rest_e, vec_half))
    back_e = exchange(full_e, "c")
    half_a = rep_join(attention_new[2], came_a, full_e)
    rest_a = exchange(half_a, "x")
    outer_e = outer(expand_weight, expand_momentum, full_e, after(back_e, half_a))
    full_a = add_low(half_a, after(rest_a, outer_e[1]))
    back_a = exchange(full_a, "c")
    mean_diff = add_low(vec_half, after(vec_far, full_a)).astype(f32) / 4
    momentum_new = 0.5 * vectors_momentum + mean_diff
    outer_new = vectors - 0.7 * (mean_diff + 0.5 * momentum_new)
    input_grad = swapped(input_grad, after(input_came, full_a))
    outer_a = outer(attention_weight, attention_momentum, full_a, back_a)
    results = []
    for weight, first, new, (total, copy) in (
        (attention_weight, attention_first, attention_new, outer_a),
        (expand_weight, expand_first, expand_new, outer_e),
        (contract_weight, contract_first, contract_new, outer_c),
    ):
        results += [
            new[0].reshape(first.shape),
            new[1].reshape(first.shape),
            total.reshape((3,) + weight.shape),
            copy.reshape(weight.shape),
        ]
    results += [
        first_new[None],
        second_new[None],
        jnp.stack([mean_diff, momentum_new, outer_new]),
        outer_new.astype(bf),
    ]
    return (output, input_grad) + tuple(results)


def solution(mesh):
    placed = (
        P(("rep", "fsdp"), None),
        P(("rep", "fsdp"), None),
        P(("rep", "fsdp"), None),
        P(None, "fsdp", None),
        P(None, "fsdp", None),
        P("rep", None, "fsdp", None),
        P("rep", None, "fsdp", None),
        P("fsdp", None),
        P("fsdp", None),
        P("rep", "fsdp", None),
        P("rep", "fsdp", None),
        P("fsdp", None),
        P("fsdp", None),
        P("rep", "fsdp", None),
        P("rep", "fsdp", None),
        P(None, "fsdp"),
        P(None, "fsdp"),
        P("rep", None, "fsdp"),
        P("rep", None, "fsdp"),
    )
    small = mesh.shape["rep"] == 4 and mesh.shape["fsdp"] == 8
    body = per_device_fast if small else per_device
    return jax.shard_map(
        body,
        mesh=mesh,
        in_specs=placed,
        out_specs=(
            P(("rep", "fsdp"), None),
            P(("rep", "fsdp"), None),
            P("rep", None, "fsdp", None),
            P("rep", None, "fsdp", None),
            P(None, None, "fsdp", None),
            P(None, "fsdp", None),
            P("rep", "fsdp", None),
            P("rep", "fsdp", None),
            P(None, "fsdp", None),
            P("fsdp", None),
            P("rep", "fsdp", None),
            P("rep", "fsdp", None),
            P(None, "fsdp", None),
            P("fsdp", None),
            P("rep", None, "fsdp"),
            P("rep", None, "fsdp"),
            P(None, None, "fsdp"),
            P(None, "fsdp"),
        ),
        check_vma=False,
    )
```
